8 devices in a mesh: dp: 1 (over z), sp: 8 (over y, x, core).
Axes of the slice: x: 2, y: 2, z: 1, core: 2. Of those that a mesh axis runs over, the one named last changes fastest.
Arguments:
- hidden: bfloat16 [4096, 4096], P(('dp', 'sp'))
- positions: int32 [4096], P(('dp', 'sp'))
- d_attn: bfloat16 [4096, 4096], P(('dp', 'sp'))
- ln_weight: bfloat16 [4096], replicated
- w_q: bfloat16 [4096, 4096], replicated
- w_k: bfloat16 [4096, 1024], replicated
- w_v: bfloat16 [4096, 1024], replicated
- w_o: bfloat16 [4096, 4096], replicated
Outputs:
- output 1: bfloat16 [4096, 4096], P(('dp', 'sp'))
- output 2: bfloat16 [4096, 4096], P(('dp', 'sp'))
- output 3: bfloat16 [4096], P('dp')
- output 4: bfloat16 [4096, 4096], P('dp')
- output 5: bfloat16 [4096, 1024], P('dp')
- output 6: bfloat16 [4096, 1024], P('dp')
- output 7: bfloat16 [4096, 4096], P('dp')
All inputs are finite; a program needn't handle non-finite values.
Results may differ from the reference program's by a relative error of at most 0.0121239.
Values are sent between devices in bfloat16 or wider.
A program may use at most 1 GiB of HBM per device.

```python
import math
import jax
import jax.numpy as jnp
from jax import lax

MODEL_DIM = 4096
NUM_HEADS = 32
NUM_KV_HEADS = 8
HEAD_DIM = 128
SEQ_LEN = 4096
LN_EPS = 1e-5
ROPE_BASE = 10000.0
GROUP_SIZE = NUM_HEADS // NUM_KV_HEADS
ROW_BLOCK = math.gcd(SEQ_LEN, 64)
NUM_BLOCKS = SEQ_LEN // ROW_BLOCK
SCORE_SCALE = HEAD_DIM ** -0.5


def setup_inputs(seed: int = 0, part: int = 0) -> dict:
    base_key = jax.random.key(seed)
    part_keys = jax.random.split(jax.random.fold_in(base_key, part), 3)
    weight_keys = jax.random.split(base_key, 5)
    hidden = jax.random.normal(part_keys[0], (SEQ_LEN, MODEL_DIM), jnp.float32).astype(jnp.bfloat16)
    pos_steps = jax.random.randint(part_keys[1], (SEQ_LEN,), 1, 4, dtype=jnp.int32)
    positions = (jnp.cumsum(pos_steps) - pos_steps[0]).astype(jnp.int32)
    d_attn = jax.random.normal(part_keys[2], (SEQ_LEN, MODEL_DIM), jnp.float32).astype(jnp.bfloat16)
    ln_weight = (1.0 + 0.25 * jax.random.normal(weight_keys[0], (MODEL_DIM,), jnp.float32)).astype(jnp.bfloat16)
    q_scale = math.sqrt(math.log(SEQ_LEN) / MODEL_DIM)
    kv_scale = MODEL_DIM ** -0.5
    o_scale = (NUM_HEADS * HEAD_DIM) ** -0.5
    w_q = (jax.random.normal(weight_keys[1], (MODEL_DIM, NUM_HEADS * HEAD_DIM), jnp.float32) * q_scale).astype(jnp.bfloat16)
    w_k = (jax.random.normal(weight_keys[2], (MODEL_DIM, NUM_KV_HEADS * HEAD_DIM), jnp.float32) * kv_scale).astype(jnp.bfloat16)
    w_v = (jax.random.normal(weight_keys[3], (MODEL_DIM, NUM_KV_HEADS * HEAD_DIM), jnp.float32) * kv_scale).astype(jnp.bfloat16)
    w_o = (jax.random.normal(weight_keys[4], (NUM_HEADS * HEAD_DIM, MODEL_DIM), jnp.float32) * o_scale).astype(jnp.bfloat16)
    return {'hidden': hidden, 'positions': positions, 'd_attn': d_attn, 'ln_weight': ln_weight,
            'w_q': w_q, 'w_k': w_k, 'w_v': w_v, 'w_o': w_o}


def norm_f32(hid_f32, weight_f32):
    mean_val = jnp.mean(hid_f32, axis=-1, keepdims=True)
    centered = hid_f32 - mean_val
    var_val = jnp.mean(centered * centered, axis=-1, keepdims=True)
    return centered * lax.rsqrt(var_val + LN_EPS) * weight_f32


def rope_tables(positions):
    inv_freq = ROPE_BASE ** (-jnp.arange(0, HEAD_DIM, 2, dtype=jnp.float32) / HEAD_DIM)
    angles = positions.astype(jnp.float32)[:, None] * inv_freq[None, :]
    return jnp.cos(angles)[:, None, :], jnp.sin(angles)[:, None, :]


def apply_rope(values, cos_t, sin_t):
    rot_pairs = values.reshape(values.shape[:-1] + (HEAD_DIM // 2, 2))
    even_part = rot_pairs[..., 0]
    odd_part = rot_pairs[..., 1]
    new_even = even_part * cos_t - odd_part * sin_t
    new_odd = odd_part * cos_t + even_part * sin_t
    return jnp.stack([new_even, new_odd], axis=-1).reshape(values.shape)


def block_probs(q_f32, row_start, k_f32):
    scores = jnp.einsum('qgrd,kgd->grqk', q_f32, k_f32) * SCORE_SCALE
    row_ids = row_start + jnp.arange(ROW_BLOCK)
    col_ids = jnp.arange(SEQ_LEN)
    scores = jnp.where(row_ids[:, None] >= col_ids[None, :], scores, -jnp.inf)
    return jax.nn.softmax(scores, axis=-1)


def reference(hidden, positions, d_attn, ln_weight, w_q, w_k, w_v, w_o):
    normed32, norm_vjp = jax.vjp(norm_f32, hidden.astype(jnp.float32), ln_weight.astype(jnp.float32))
    normed = normed32.astype(jnp.bfloat16)
    cos_t, sin_t = rope_tables(positions)
    q_rot = apply_rope(jnp.dot(normed, w_q, preferred_element_type=jnp.float32).reshape(SEQ_LEN, NUM_HEADS, HEAD_DIM), cos_t, sin_t).astype(jnp.bfloat16)
    k_rot = apply_rope(jnp.dot(normed, w_k, preferred_element_type=jnp.float32).reshape(SEQ_LEN, NUM_KV_HEADS, HEAD_DIM), cos_t, sin_t).astype(jnp.bfloat16)
    v_all = jnp.dot(normed, w_v, preferred_element_type=jnp.float32).astype(jnp.bfloat16).reshape(SEQ_LEN, NUM_KV_HEADS, HEAD_DIM)
    q_grp = q_rot.reshape(NUM_BLOCKS, ROW_BLOCK, NUM_KV_HEADS, GROUP_SIZE, HEAD_DIM)
    k_f32 = k_rot.astype(jnp.float32)
    v_f32 = v_all.astype(jnp.float32)
    block_ids = jnp.arange(NUM_BLOCKS)

    def fwd_block(block_in):
        q_block, block_idx = block_in
        attn_prob = block_probs(q_block.astype(jnp.float32), block_idx * ROW_BLOCK, k_f32)
        prob_bf = attn_prob.astype(jnp.bfloat16).astype(jnp.float32)
        return jnp.einsum('grqk,kgd->qgrd', prob_bf, v_f32).astype(jnp.bfloat16)

    o_grp = lax.map(fwd_block, (q_grp, block_ids))
    o_tok = o_grp.reshape(SEQ_LEN, NUM_HEADS * HEAD_DIM)
    attn_out = jnp.dot(o_tok, w_o, preferred_element_type=jnp.float32).astype(jnp.bfloat16)
    d_o = jnp.dot(d_attn, w_o.T, preferred_element_type=jnp.float32).astype(jnp.bfloat16)
    dw_o = jnp.dot(o_tok.T, d_attn, preferred_element_type=jnp.float32)
    do_grp = d_o.reshape(NUM_BLOCKS, ROW_BLOCK, NUM_KV_HEADS, GROUP_SIZE, HEAD_DIM)

    def bwd_block(carry, block_in):
        dk_acc, dv_acc = carry
        q_block, do_block, block_idx = block_in
        q_f32 = q_block.astype(jnp.float32)
        do_f32 = do_block.astype(jnp.float32)
        attn_prob = block_probs(q_f32, block_idx * ROW_BLOCK, k_f32)
        prob_bf = attn_prob.astype(jnp.bfloat16).astype(jnp.float32)
        d_prob = jnp.einsum('qgrd,kgd->grqk', do_f32, v_f32)
        row_dot = jnp.sum(attn_prob * d_prob, axis=-1, keepdims=True)
        d_score = (attn_prob * (d_prob - row_dot) * SCORE_SCALE).astype(jnp.bfloat16).astype(jnp.float32)
        dq_block = jnp.einsum('grqk,kgd->qgrd', d_score, k_f32).astype(jnp.bfloat16)
        dk_acc = dk_acc + jnp.einsum('grqk,qgrd->kgd', d_score, q_f32)
        dv_acc = dv_acc + jnp.einsum('grqk,qgrd->kgd', prob_bf, do_f32)
        return (dk_acc, dv_acc), dq_block

    zero_acc = jnp.zeros((SEQ_LEN, NUM_KV_HEADS, HEAD_DIM), jnp.float32)
    kv_sums, dq_grp = lax.scan(bwd_block, (zero_acc, zero_acc), (q_grp, do_grp, block_ids))
    dk_bf = kv_sums[0].astype(jnp.bfloat16)
    dv_bf = kv_sums[1].astype(jnp.bfloat16)
    g_q = apply_rope(dq_grp.reshape(SEQ_LEN, NUM_HEADS, HEAD_DIM).astype(jnp.float32), cos_t, -sin_t).astype(jnp.bfloat16).reshape(SEQ_LEN, NUM_HEADS * HEAD_DIM)
    g_k = apply_rope(dk_bf.astype(jnp.float32), cos_t, -sin_t).astype(jnp.bfloat16).reshape(SEQ_LEN, NUM_KV_HEADS * HEAD_DIM)
    g_v = dv_bf.reshape(SEQ_LEN, NUM_KV_HEADS * HEAD_DIM)
    d_normed = (jnp.dot(g_q, w_q.T, preferred_element_type=jnp.float32)
                + jnp.dot(g_k, w_k.T, preferred_element_type=jnp.float32)
                + jnp.dot(g_v, w_v.T, preferred_element_type=jnp.float32))
    dw_q = jnp.dot(normed.T, g_q, preferred_element_type=jnp.float32)
    dw_k = jnp.dot(normed.T, g_k, preferred_element_type=jnp.float32)
    dw_v = jnp.dot(normed.T, g_v, preferred_element_type=jnp.float32)
    d_hid, d_lnw = norm_vjp(d_normed)
    return (attn_out, d_hid.astype(jnp.bfloat16), d_lnw.astype(jnp.bfloat16), dw_q.astype(jnp.bfloat16),
            dw_k.astype(jnp.bfloat16), dw_v.astype(jnp.bfloat16), dw_o.astype(jnp.bfloat16))
```

```python
import functools
import jax
import jax.numpy as jnp
from jax import lax
from jax.experimental import pallas as pl
from jax.experimental.pallas import tpu as pltpu
from jax.sharding import PartitionSpec as P

HEAD_DIM = 128
LN_EPS = 1e-5
ROPE_BASE = 10000.0
SCALE = HEAD_DIM ** -0.5
LOG2E = 1.4426950408889634
VMEM_LIMIT = 67_000_000
BF16 = jnp.bfloat16
F32 = jnp.float32


def norm_f32(hid_f32, weight_f32):
    mean_val = jnp.mean(hid_f32, axis=-1, keepdims=True)
    centered = hid_f32 - mean_val
    var_val = jnp.mean(centered * centered, axis=-1, keepdims=True)
    return centered * lax.rsqrt(var_val + LN_EPS) * weight_f32


def rope_tables(positions):
    inv_freq = ROPE_BASE ** (-jnp.arange(0, HEAD_DIM, 2, dtype=F32) / HEAD_DIM)
    angles = positions.astype(F32)[:, None] * inv_freq[None, :]
    cos_t = jnp.repeat(jnp.cos(angles), 2, axis=1)
    sin_t = jnp.repeat(jnp.sin(angles), 2, axis=1)
    sign = jnp.where(jnp.arange(HEAD_DIM) % 2 == 0, -1.0, 1.0).astype(F32)
    return cos_t, sin_t * sign[None, :]


def rotate(x, cos_t, sin_t):
    lane = lax.broadcasted_iota(jnp.int32, x.shape, 1)
    swapped = jnp.where(lane % 2 == 0, pltpu.roll(x, HEAD_DIM - 1, 1), pltpu.roll(x, 1, 1))
    return x * cos_t + swapped * sin_t


def qkv_kernel(dev_ref, h_ref, wq_ref, wk_ref, wv_ref, cos_ref, sin_ref, q_ref, k_ref, kt_ref, v_ref, vt_ref):
    h = h_ref[...]
    cos_t, sin_t = cos_ref[...], sin_ref[...]
    for n in range(q_ref.shape[1] // HEAD_DIM):
        cols = slice(n * HEAD_DIM, (n + 1) * HEAD_DIM)
        q_ref[:, cols] = rotate(jnp.dot(h, wq_ref[:, cols], preferred_element_type=F32), cos_t, sin_t).astype(BF16)
    k = rotate(jnp.dot(h, wk_ref[...], preferred_element_type=F32), cos_t, sin_t)
    k_ref[...] = k.astype(BF16)
    kt_ref[...] = k.T.astype(BF16)
    v = jnp.dot(h, wv_ref[...], preferred_element_type=F32)
    v_ref[...] = v.astype(BF16)
    vt_ref[...] = v.T.astype(BF16)


def qkv_proj(dev, h_all, w_q, w_k, w_v, cos_t, sin_t, width, bm=512):
    seq, feat = h_all.shape
    rows = lambda i, d: (i, 0)
    cols = lambda i, d: (0, i)
    mine = lambda i, d: (0, d[0])
    return pl.pallas_call(
        qkv_kernel,
        grid_spec=pltpu.PrefetchScalarGridSpec(
            num_scalar_prefetch=1, grid=(seq // bm,),
            in_specs=[pl.BlockSpec((bm, feat), rows), pl.BlockSpec((feat, width), mine), pl.BlockSpec((feat, HEAD_DIM), mine),
                      pl.BlockSpec((feat, HEAD_DIM), mine), pl.BlockSpec((bm, HEAD_DIM), rows), pl.BlockSpec((bm, HEAD_DIM), rows)],
            out_specs=[pl.BlockSpec((bm, width), rows), pl.BlockSpec((bm, HEAD_DIM), rows), pl.BlockSpec((HEAD_DIM, bm), cols),
                       pl.BlockSpec((bm, HEAD_DIM), rows), pl.BlockSpec((HEAD_DIM, bm), cols)]),
        out_shape=[jax.ShapeDtypeStruct((seq, width), BF16), jax.ShapeDtypeStruct((seq, HEAD_DIM), BF16),
                   jax.ShapeDtypeStruct((HEAD_DIM, seq), BF16), jax.ShapeDtypeStruct((seq, HEAD_DIM), BF16),
                   jax.ShapeDtypeStruct((HEAD_DIM, seq), BF16)],
        compiler_params=pltpu.CompilerParams(vmem_limit_bytes=VMEM_LIMIT),
        cost_estimate=pl.CostEstimate(flops=2 * seq * feat * (width + 256), bytes_accessed=seq * feat * 2, transcendentals=0),
        name="qkv_proj")(dev, h_all, w_q, w_k, w_v, cos_t, sin_t)


def do_kernel(dev_ref, g_ref, wo_ref, do_ref):
    do_ref[...] = lax.dot_general(g_ref[...], wo_ref[...], (((1,), (1,)), ((), ())), preferred_element_type=F32).astype(BF16)


def do_proj(dev, g_all, w_o, width, bm=512):
    seq, feat = g_all.shape
    return pl.pallas_call(
        do_kernel,
        grid_spec=pltpu.PrefetchScalarGridSpec(
            num_scalar_prefetch=1, grid=(seq // bm,),
            in_specs=[pl.BlockSpec((bm, feat), lambda i, d: (i, 0)), pl.BlockSpec((width, feat), lambda i, d: (d[0], 0))],
            out_specs=pl.BlockSpec((bm, width), lambda i, d: (i, 0))),
        out_shape=jax.ShapeDtypeStruct((seq, width), BF16),
        compiler_params=pltpu.CompilerParams(vmem_limit_bytes=VMEM_LIMIT),
        cost_estimate=pl.CostEstimate(flops=2 * seq * feat * width, bytes_accessed=seq * feat * 2, transcendentals=0),
        name="do_proj")(dev, g_all, w_o)


def stack_heads(x):
    return jnp.concatenate([x[:, n * HEAD_DIM:(n + 1) * HEAD_DIM] for n in range(x.shape[1] // HEAD_DIM)], axis=0)


def unstack_heads(ref, x, rows):
    for n in range(x.shape[0] // rows):
        ref[:, n * HEAD_DIM:(n + 1) * HEAD_DIM] = x[n * rows:(n + 1) * rows].astype(ref.dtype)


def causal(shape, bq, offset):
    rows = lax.rem(lax.broadcasted_iota(jnp.int32, shape, 0), bq) + offset
    return rows >= lax.broadcasted_iota(jnp.int32, shape, 1)


def fwd_kernel(bq, bk, q_ref, kt_ref, v_ref, o_ref, lse_ref, s_scr):
    qi = pl.program_id(0)
    q = stack_heads(q_ref[...])
    rows = q.shape[0]
    nfull = (qi * bq) // bk

    def scores(j):
        return jnp.dot(q, kt_ref[:, pl.ds(pl.multiple_of(j * bk, bk), bk)], preferred_element_type=F32) * (SCALE * LOG2E)

    def lane_max(m, s):
        for c in range(bk // 128):
            m = jnp.maximum(m, s[:, c * 128:(c + 1) * 128])
        return m

    def score_step(j, m):
        s = scores(j)
        s_scr[j] = s
        return lane_max(m, s)

    m = lax.fori_loop(0, nfull, score_step, jnp.full((rows, 128), -jnp.inf, F32))
    s = jnp.where(causal((rows, bk), bq, qi * bq - nfull * bk), scores(nfull), -jnp.inf)
    s_scr[nfull] = s
    m = jnp.max(lane_max(m, s), axis=1, keepdims=True)

    def value_step(j, carry):
        l, o = carry
        p = jnp.exp2(s_scr[j] - m)
        for t in range(bk // 128):
            l = l + p[:, t * 128:(t + 1) * 128]
        o = o + jnp.dot(p.astype(BF16), v_ref[pl.ds(pl.multiple_of(j * bk, bk), bk), :], preferred_element_type=F32)
        return l, o

    l, o = lax.fori_loop(0, nfull + 1, value_step, (jnp.zeros((rows, 128), F32), jnp.zeros((rows, HEAD_DIM), F32)))
    l = jnp.sum(l, axis=1, keepdims=True)
    unstack_heads(o_ref, o / l, bq)
    lse_ref[...] = (m + jnp.log2(l)).reshape(lse_ref.shape)


def attn_forward(q, kt, v, bq=256, bk=1024):
    seq, width = q.shape
    heads = width // HEAD_DIM
    return pl.pallas_call(
        functools.partial(fwd_kernel, bq, bk), grid=(seq // bq,),
        in_specs=[pl.BlockSpec((bq, width), lambda i: (i, 0)), pl.BlockSpec((HEAD_DIM, seq), lambda i: (0, 0)),
                  pl.BlockSpec((seq, HEAD_DIM), lambda i: (0, 0))],
        out_specs=[pl.BlockSpec((bq, width), lambda i: (i, 0)), pl.BlockSpec((heads, bq, 1), lambda i: (0, i, 0))],
        out_shape=[jax.ShapeDtypeStruct((seq, width), BF16), jax.ShapeDtypeStruct((heads, seq, 1), F32)],
        scratch_shapes=[pltpu.VMEM((seq // bk, heads * bq, bk), F32)],
        compiler_params=pltpu.CompilerParams(vmem_limit_bytes=VMEM_LIMIT),
        cost_estimate=pl.CostEstimate(flops=8 * seq * seq * width, bytes_accessed=seq * width * 8, transcendentals=0),
        name="attn_fwd")(q, kt, v)


def bwd_kernel(bq, bk, q_ref, do_ref, lse_ref, k_ref, kt_ref, vt_ref, cos_ref, sin_ref, gq_ref, gk_ref, gv_ref, p_scr, dp_scr, dkt_scr, dvt_scr):
    qi = pl.program_id(0)
    q = stack_heads(q_ref[...])
    do = stack_heads(do_ref[...])
    rows = q.shape[0]
    lse = lse_ref[...].reshape(rows, 1)
    q_t = q.T
    do_t = do.T
    nfull = (qi * bq) // bk

    @pl.when(qi == 0)
    def _():
        dkt_scr[...] = jnp.zeros_like(dkt_scr)
        dvt_scr[...] = jnp.zeros_like(dvt_scr)

    def prob_step(j, r, masked):
        sl = pl.ds(pl.multiple_of(j * bk, bk), bk)
        s = jnp.dot(q, kt_ref[:, sl], preferred_element_type=F32) * (SCALE * LOG2E)
        p = jnp.exp2(s - lse)
        if masked:
            p = jnp.where(causal((rows, bk), bq, qi * bq - nfull * bk), p, 0.0)
        dp = jnp.dot(do, vt_ref[:, sl], preferred_element_type=F32)
        pd = p * dp
        for t in range(bk // 128):
            r = r + pd[:, t * 128:(t + 1) * 128]
        p_scr[j] = p
        dp_scr[j] = dp
        dvt_scr[:, sl] += jnp.dot(do_t, p.astype(BF16), preferred_element_type=F32)
        return r

    r = lax.fori_loop(0, nfull, lambda j, r: prob_step(j, r, False), jnp.zeros((rows, 128), F32))
    r = prob_step(nfull, r, True)
    r = jnp.sum(r, axis=1, keepdims=True)

    def grad_step(j, dq):
        sl = pl.ds(pl.multiple_of(j * bk, bk), bk)
        ds = (p_scr[j] * (dp_scr[j] - r) * SCALE).astype(BF16)
        dkt_scr[:, sl] += jnp.dot(q_t, ds, preferred_element_type=F32)
        return dq + jnp.dot(ds, k_ref[sl, :], preferred_element_type=F32)

    dq = lax.fori_loop(0, nfull + 1, grad_step, jnp.zeros((rows, HEAD_DIM), F32))
    dq = dq.astype(BF16).astype(F32)
    start = pl.ds(pl.multiple_of(qi * bq, bq), bq)
    cos_t, sin_t = cos_ref[start, :], sin_ref[start, :]
    for n in range(rows // bq):
        gq_ref[:, n * HEAD_DIM:(n + 1) * HEAD_DIM] = rotate(dq[n * bq:(n + 1) * bq], cos_t, -sin_t).astype(BF16)

    @pl.when(qi == pl.num_programs(0) - 1)
    def _():
        dk = dkt_scr[...].T.astype(BF16).astype(F32)
        gk_ref[...] = rotate(dk, cos_ref[...], -sin_ref[...]).astype(BF16)
        gv_ref[...] = dvt_scr[...].T.astype(BF16)


def attn_backward(q, do, lse, k, kt, vt, cos_t, sin_t, bq=256, bk=512):
    seq, width = q.shape
    heads = width // HEAD_DIM
    tile = pl.BlockSpec((bq, width), lambda i: (i, 0))
    tall = pl.BlockSpec((seq, HEAD_DIM), lambda i: (0, 0))
    wide = pl.BlockSpec((HEAD_DIM, seq), lambda i: (0, 0))
    return pl.pallas_call(
        functools.partial(bwd_kernel, bq, bk), grid=(seq // bq,),
        in_specs=[tile, tile, pl.BlockSpec((heads, bq, 1), lambda i: (0, i, 0)), tall, wide, wide, tall, tall],
        out_specs=[tile, tall, tall],
        out_shape=[jax.ShapeDtypeStruct((seq, width), BF16), jax.ShapeDtypeStruct((seq, HEAD_DIM), BF16),
                   jax.ShapeDtypeStruct((seq, HEAD_DIM), BF16)],
        scratch_shapes=[pltpu.VMEM((seq // bk, heads * bq, bk), F32), pltpu.VMEM((seq // bk, heads * bq, bk), F32),
                        pltpu.VMEM((HEAD_DIM, seq), F32), pltpu.VMEM((HEAD_DIM, seq), F32)],
        compiler_params=pltpu.CompilerParams(vmem_limit_bytes=VMEM_LIMIT),
        cost_estimate=pl.CostEstimate(flops=16 * seq * seq * width, bytes_accessed=seq * width * 8, transcendentals=0),
        name="attn_bwd")(q, do, lse, k, kt, vt, cos_t, sin_t)


def solution(mesh):
    sp_size = mesh.shape['sp']
    pairs = [[i, i + 1] for i in range(0, sp_size, 2)]
    row_spec = P(('dp', 'sp'), None)
    pos_spec = P(('dp', 'sp'))
    full_spec = P(None, None)
    grad_spec = P('dp', None)

    def local_step(hidden, positions, d_attn, ln_weight, w_q, w_k, w_v, w_o):
        dev = lax.axis_index('sp')
        core = lax.rem(dev, 2)
        dev1 = dev.reshape(1)
        local_rows, feat = hidden.shape
        seq = local_rows * sp_size
        width = w_q.shape[1] // sp_size
        kv_width = w_k.shape[1] // sp_size
        normed32, norm_vjp = jax.vjp(norm_f32, hidden.astype(F32), ln_weight.astype(F32))
        normed = normed32.astype(BF16)
        pos_all = lax.all_gather(positions, 'sp', axis=0, tiled=True)
        h_all = lax.all_gather(normed, 'sp', axis=0, tiled=True)
        g_all = lax.all_gather(d_attn, 'sp', axis=0, tiled=True)
        cos_t, sin_t = rope_tables(pos_all)
        q, k, kt, v, vt = qkv_proj(dev1, h_all, w_q, w_k, w_v, cos_t, sin_t, width)
        o, lse = attn_forward(q, kt, v)
        o_all = lax.all_gather(o, 'sp', axis=0)
        do = do_proj(dev1, g_all, w_o, width)
        gq, gk, gv = attn_backward(q, do, lse, k, kt, vt, cos_t, sin_t)
        gq_all = lax.all_gather(gq, 'sp', axis=0)
        gk_all = lax.all_gather(gk, 'sp', axis=0)
        gv_all = lax.all_gather(gv, 'sp', axis=0)

        def own_rows(x_all):
            x = lax.dynamic_slice_in_dim(x_all, dev * local_rows, local_rows, axis=1)
            return jnp.transpose(x, (1, 0, 2)).reshape(local_rows, -1)

        def half(x_all):
            n = sp_size // 2
            return lax.dynamic_slice_in_dim(x_all, core * n, n, axis=0)

        attn_out = jnp.dot(own_rows(o_all), w_o, preferred_element_type=F32).astype(BF16)
        dw_o = jnp.einsum('ste,td->sed', half(o_all), g_all, preferred_element_type=F32).astype(BF16)
        dw_o = lax.all_gather(dw_o.reshape(-1, feat), 'sp', axis=0, tiled=True, axis_index_groups=pairs)

        def grad_in(x_all):
            x = half(x_all)
            y = jnp.einsum('td,ste->dse', h_all, x, preferred_element_type=F32).astype(BF16)
            return lax.all_gather(y.reshape(feat, -1), 'sp', axis=1, tiled=True, axis_index_groups=pairs)

        dw_q, dw_k, dw_v = grad_in(gq_all), grad_in(gk_all), grad_in(gv_all)
        d_normed = (jnp.einsum('te,de->td', own_rows(gq_all), w_q, preferred_element_type=F32)
                    + jnp.einsum('te,de->td', own_rows(gk_all), w_k, preferred_element_type=F32)
                    + jnp.einsum('te,de->td', own_rows(gv_all), w_v, preferred_element_type=F32))
        d_hid, d_lnw = norm_vjp(d_normed)
        d_lnw = lax.psum(d_lnw, 'sp')
        return (attn_out, d_hid.astype(BF16), d_lnw.astype(BF16), dw_q, dw_k, dw_v, dw_o)

    return jax.shard_map(local_step, mesh=mesh,
                         in_specs=(row_spec, pos_spec, row_spec, P(None), full_spec, full_spec, full_spec, full_spec),
                         out_specs=(row_spec, row_spec, P('dp'), grad_spec, grad_spec, grad_spec, grad_spec),
                         check_vma=False)
```

```python
import functools
import jax
import jax.numpy as jnp
from jax import lax
from jax.experimental import pallas as pl
from jax.experimental.pallas import tpu as pltpu
from jax.sharding import PartitionSpec as P

HEAD_DIM = 128
LN_EPS = 1e-5
ROPE_BASE = 10000.0
SCALE = HEAD_DIM ** -0.5
LOG2E = 1.4426950408889634
VMEM_LIMIT = 67_000_000
BF16 = jnp.bfloat16
F32 = jnp.float32
MESH = pl.DeviceIdType.MESH


def norm_f32(hid_f32, weight_f32):
    mean_val = jnp.mean(hid_f32, axis=-1, keepdims=True)
    centered = hid_f32 - mean_val
    var_val = jnp.mean(centered * centered, axis=-1, keepdims=True)
    return centered * lax.rsqrt(var_val + LN_EPS) * weight_f32


def rotate(x, cos_t, sin_t):
    lane = lax.broadcasted_iota(jnp.int32, x.shape, 1)
    swapped = jnp.where(lane % 2 == 0, pltpu.roll(x, HEAD_DIM - 1, 1), pltpu.roll(x, 1, 1))
    return x * cos_t + swapped * sin_t


def flip(i, bit):
    return i + bit - 2 * bit * ((i // bit) % 2)

X, Y, Z = 2, 4, 1

def gather_qkv_kernel(h_ref, pos_ref, freq_ref, wq_ref, wk_ref, wv_ref, hall_ref, q_ref, k_ref, kt_ref, v_ref, vt_ref, cos_ref, sin_ref,
                      w_scr, buf, pos_all, pos_send, pos_recv, send, recv, w_sem, load_sem, store_sem):
    me = lax.axis_index("sp")
    rows = h_ref.shape[0]
    half = rows // 2
    width = q_ref.shape[1]
    peers = [flip(me, 1), flip(me, 2), flip(flip(me, 2), 1), flip(me, 4), flip(flip(me, 4), 1), flip(flip(me, 4), 2), flip(flip(flip(me, 4), 2), 1)]
    barrier = pltpu.get_barrier_semaphore()
    for p in peers:
        pl.semaphore_signal(barrier, inc=1, device_id={"sp": p}, device_id_type=MESH)
    pl.semaphore_wait(barrier, len(peers))

    def piece(owner, part):
        return pl.ds(pl.multiple_of(owner * rows + part * half, half), half)

    def remote(n, src, owner, part, to):
        return pltpu.make_async_remote_copy(src_ref=src, dst_ref=hall_ref.at[piece(owner, part)], send_sem=send.at[n], recv_sem=recv.at[n],
                                            device_id={"sp": to}, device_id_type=MESH)
    xn, yn, zn = flip(me, X), flip(me, Y), flip(me, Z)
    dn = flip(xn, Y)
    own = lambda part: h_ref.at[pl.ds(part * half, half)]
    got = lambda owner, part: hall_ref.at[piece(owner, part)]
    pos_copies = [pltpu.make_async_remote_copy(src_ref=pos_ref, dst_ref=pos_all.at[me], send_sem=pos_send.at[i], recv_sem=pos_recv.at[i],
                                               device_id={"sp": p}, device_id_type=MESH) for i, p in enumerate(peers)]
    for c in pos_copies:
        c.start()
    s = [remote(0, own(0), me, 0, xn), remote(1, own(1), me, 1, yn), remote(2, own(1), me, 1, xn), remote(3, own(0), me, 0, yn),
         remote(4, got(xn, 0), xn, 0, yn), remote(5, got(yn, 1), yn, 1, xn),
         remote(6, own(0), me, 0, zn), remote(7, own(1), me, 1, zn),
         remote(8, got(xn, 0), xn, 0, zn), remote(9, got(yn, 1), yn, 1, zn),
         remote(10, got(xn, 1), xn, 1, zn), remote(11, got(yn, 0), yn, 0, zn),
         remote(12, got(dn, 0), dn, 0, zn), remote(13, got(dn, 1), dn, 1, zn)]
    for n in (0, 1, 6, 7, 2, 3):
        s[n].start()
    col = lambda n: pl.ds(pl.multiple_of(me * n, n), n)
    w_copies = [pltpu.make_async_copy(wq_ref.at[:, col(width)], w_scr.at[:, pl.ds(0, width)], w_sem.at[0]),
                pltpu.make_async_copy(wk_ref.at[:, col(HEAD_DIM)], w_scr.at[:, pl.ds(width, HEAD_DIM)], w_sem.at[1]),
                pltpu.make_async_copy(wv_ref.at[:, col(HEAD_DIM)], w_scr.at[:, pl.ds(width + HEAD_DIM, HEAD_DIM)], w_sem.at[2])]
    for c in w_copies:
        c.start()
    loads = [pltpu.make_async_copy(own(i), buf.at[i], load_sem.at[i]) for i in range(2)]
    for c in loads:
        c.start()
    pos_all[me] = pos_ref[...]
    for c in pos_copies:
        c.wait_recv()

    def compute(slot, owner, part):
        r0 = pl.multiple_of(owner * rows + part * half, half)
        out = pl.ds(r0, half)
        for t in range(half // 128):
            p = pos_all[owner, pl.ds(part * (half // 128) + t, 1), :]
            angle = jnp.broadcast_to(p, (128, 128)).T * freq_ref[...]
            sign = jnp.where(lax.broadcasted_iota(jnp.int32, (128, 128), 1) % 2 == 0, -1.0, 1.0)
            tr = pl.ds(pl.multiple_of(r0 + t * 128, 128), 128)
            cos_ref[tr, :] = jnp.cos(angle)
            sin_ref[tr, :] = jnp.sin(angle) * sign
        cos_t, sin_t = cos_ref[out, :], sin_ref[out, :]
        h = buf[slot]
        for n in range(width // 256):
            y = jnp.dot(h, w_scr[:, n * 256:(n + 1) * 256], preferred_element_type=F32)
            for e in range(2):
                q_ref[out, n * 256 + e * 128: n * 256 + (e + 1) * 128] = rotate(y[:, e * 128:(e + 1) * 128], cos_t, sin_t).astype(BF16)
        y = jnp.dot(h, w_scr[:, width:width + 256], preferred_element_type=F32)
        k, v = rotate(y[:, :128], cos_t, sin_t), y[:, 128:]
        k_ref[out, :] = k.astype(BF16)
        kt_ref[:, out] = k.T.astype(BF16)
        v_ref[out, :] = v.astype(BF16)
        vt_ref[:, out] = v.T.astype(BF16)

    def run(pairs_, slot0):
        cps = [pltpu.make_async_copy(got(o, p), buf.at[slot0 + i], load_sem.at[slot0 + i]) for i, (o, p) in enumerate(pairs_)]
        for c in cps:
            c.start()
        for c in cps:
            c.wait()
        (o0, p0), (o1, p1) = pairs_
        def body(i, _):
            compute(slot0 + i, o0 + i * (o1 - o0), p0 + i * (p1 - p0))
            return 0
        lax.fori_loop(0, 2, body, 0)

    for c in loads:
        c.wait()
    stores = [pltpu.make_async_copy(buf.at[i], got(me, i), store_sem.at[i]) for i in range(2)]
    for c in stores:
        c.start()
    for c in w_copies:
        c.wait()
    def body(i, _):
        compute(i, me, i)
        return 0
    lax.fori_loop(0, 2, body, 0)
    s[6].wait_recv(); s[7].wait_recv()
    run([(zn, 0), (zn, 1)], 2)
    for c in stores:
        c.wait()
    zx, zy, zd = flip(zn, X), flip(zn, Y), flip(dn, Z)
    s[0].wait_recv(); s[4].start(); s[8].start()
    s[1].wait_recv(); s[5].start(); s[9].start()
    run([(xn, 0), (yn, 1)], 0)
    s[8].wait_recv(); s[9].wait_recv()
    run([(zx, 0), (zy, 1)], 2)
    s[2].wait_recv(); s[10].start()
    s[3].wait_recv(); s[11].start()
    run([(xn, 1), (yn, 0)], 0)
    s[10].wait_recv(); s[11].wait_recv()
    run([(zx, 1), (zy, 0)], 2)
    s[4].wait_recv(); s[12].start()
    s[5].wait_recv(); s[13].start()
    run([(dn, 0), (dn, 1)], 0)
    s[12].wait_recv(); s[13].wait_recv()
    run([(zd, 0), (zd, 1)], 2)
    for c in s:
        c.wait_send()
    for c in pos_copies:
        c.wait_send()

def gather_qkv(h, pos, w_q, w_k, w_v, sp_size, cid=1):
    rows, feat = h.shape
    seq = rows * sp_size
    width = w_q.shape[1] // sp_size
    inv_freq = ROPE_BASE ** (-jnp.arange(0, HEAD_DIM, 2, dtype=F32) / HEAD_DIM)
    freq = jnp.repeat(inv_freq, 2)[None, :]
    any_ = pl.BlockSpec(memory_space=pl.ANY)
    vm = pl.BlockSpec(memory_space=pltpu.VMEM)
    return pl.pallas_call(gather_qkv_kernel,
        in_specs=[any_, vm, vm, any_, any_, any_],
        out_specs=[any_] + [vm] * 7,
        out_shape=[jax.ShapeDtypeStruct((seq, feat), BF16), jax.ShapeDtypeStruct((seq, width), BF16), jax.ShapeDtypeStruct((seq, HEAD_DIM), BF16),
                   jax.ShapeDtypeStruct((HEAD_DIM, seq), BF16), jax.ShapeDtypeStruct((seq, HEAD_DIM), BF16), jax.ShapeDtypeStruct((HEAD_DIM, seq), BF16),
                   jax.ShapeDtypeStruct((seq, HEAD_DIM), F32), jax.ShapeDtypeStruct((seq, HEAD_DIM), F32)],
        scratch_shapes=[pltpu.VMEM((feat, width + 256), BF16), pltpu.VMEM((4, rows // 2, feat), BF16), pltpu.VMEM((sp_size, rows // 128, 128), F32),
                        pltpu.SemaphoreType.DMA((7,)), pltpu.SemaphoreType.DMA((7,)), pltpu.SemaphoreType.DMA((14,)), pltpu.SemaphoreType.DMA((14,)),
                        pltpu.SemaphoreType.DMA((3,)), pltpu.SemaphoreType.DMA((4,)), pltpu.SemaphoreType.DMA((2,))],
        compiler_params=pltpu.CompilerParams(collective_id=cid, has_side_effects=True, vmem_limit_bytes=VMEM_LIMIT),
        name="gather_qkv")(h, pos.astype(F32).reshape(rows // 128, 128), freq, w_q, w_k, w_v)


def do_kernel(dev_ref, g_ref, wo_ref, do_ref):
    do_ref[...] = lax.dot_general(g_ref[...], wo_ref[...], (((1,), (1,)), ((), ())), preferred_element_type=F32).astype(BF16)


def do_proj(dev, g_all, w_o, width, bm=512):
    seq, feat = g_all.shape
    return pl.pallas_call(
        do_kernel,
        grid_spec=pltpu.PrefetchScalarGridSpec(
            num_scalar_prefetch=1, grid=(seq // bm,),
            in_specs=[pl.BlockSpec((bm, feat), lambda i, d: (i, 0)), pl.BlockSpec((width, feat), lambda i, d: (d[0], 0))],
            out_specs=pl.BlockSpec((bm, width), lambda i, d: (i, 0))),
        out_shape=jax.ShapeDtypeStruct((seq, width), BF16),
        compiler_params=pltpu.CompilerParams(vmem_limit_bytes=VMEM_LIMIT),
        cost_estimate=pl.CostEstimate(flops=2 * seq * feat * width, bytes_accessed=seq * feat * 2, transcendentals=0),
        name="do_proj")(dev, g_all, w_o)


def stack_heads(x):
    return jnp.concatenate([x[:, n * HEAD_DIM:(n + 1) * HEAD_DIM] for n in range(x.shape[1] // HEAD_DIM)], axis=0)


def unstack_heads(ref, x, rows):
    for n in range(x.shape[0] // rows):
        ref[:, n * HEAD_DIM:(n + 1) * HEAD_DIM] = x[n * rows:(n + 1) * rows].astype(ref.dtype)


def causal(shape, bq, offset):
    rows = lax.rem(lax.broadcasted_iota(jnp.int32, shape, 0), bq) + offset
    return rows >= lax.broadcasted_iota(jnp.int32, shape, 1)


def fwd_kernel(bq, bk, q_ref, kt_ref, v_ref, o_ref, lse_ref, s_scr):
    qi = pl.program_id(0)
    q = stack_heads(q_ref[...])
    rows = q.shape[0]
    nfull = (qi * bq) // bk

    def scores(j):
        return jnp.dot(q, kt_ref[:, pl.ds(pl.multiple_of(j * bk, bk), bk)], preferred_element_type=F32) * (SCALE * LOG2E)

    def lane_max(m, s):
        for c in range(bk // 128):
            m = jnp.maximum(m, s[:, c * 128:(c + 1) * 128])
        return m

    def score_step(j, m):
        s = scores(j)
        s_scr[j] = s
        return lane_max(m, s)

    m = lax.fori_loop(0, nfull, score_step, jnp.full((rows, 128), -jnp.inf, F32))
    s = jnp.where(causal((rows, bk), bq, qi * bq - nfull * bk), scores(nfull), -jnp.inf)
    s_scr[nfull] = s
    m = jnp.max(lane_max(m, s), axis=1, keepdims=True)

    def value_step(j, carry):
        l, o = carry
        p = jnp.exp2(s_scr[j] - m)
        for t in range(bk // 128):
            l = l + p[:, t * 128:(t + 1) * 128]
        o = o + jnp.dot(p.astype(BF16), v_ref[pl.ds(pl.multiple_of(j * bk, bk), bk), :], preferred_element_type=F32)
        return l, o

    l, o = lax.fori_loop(0, nfull + 1, value_step, (jnp.zeros((rows, 128), F32), jnp.zeros((rows, HEAD_DIM), F32)))
    l = jnp.sum(l, axis=1, keepdims=True)
    unstack_heads(o_ref, o / l, bq)
    lse_ref[...] = (m + jnp.log2(l)).reshape(lse_ref.shape)


def attn_forward(q, kt, v, bq=256, bk=1024):
    seq, width = q.shape
    heads = width // HEAD_DIM
    return pl.pallas_call(
        functools.partial(fwd_kernel, bq, bk), grid=(seq // bq,),
        in_specs=[pl.BlockSpec((bq, width), lambda i: (i, 0)), pl.BlockSpec((HEAD_DIM, seq), lambda i: (0, 0)),
                  pl.BlockSpec((seq, HEAD_DIM), lambda i: (0, 0))],
        out_specs=[pl.BlockSpec((bq, width), lambda i: (i, 0)), pl.BlockSpec((heads, bq, 1), lambda i: (0, i, 0))],
        out_shape=[jax.ShapeDtypeStruct((seq, width), BF16), jax.ShapeDtypeStruct((heads, seq, 1), F32)],
        scratch_shapes=[pltpu.VMEM((seq // bk, heads * bq, bk), F32)],
        compiler_params=pltpu.CompilerParams(vmem_limit_bytes=VMEM_LIMIT),
        cost_estimate=pl.CostEstimate(flops=8 * seq * seq * width, bytes_accessed=seq * width * 8, transcendentals=0),
        name="attn_fwd")(q, kt, v)


def bwd_kernel(bq, bk, q_ref, do_ref, lse_ref, k_ref, kt_ref, vt_ref, cos_ref, sin_ref, gq_ref, gk_ref, gv_ref, p_scr, dp_scr, dkt_scr, dvt_scr):
    qi = pl.program_id(0)
    q = stack_heads(q_ref[...])
    do = stack_heads(do_ref[...])
    rows = q.shape[0]
    lse = lse_ref[...].reshape(rows, 1)
    q_t = q.T
    do_t = do.T
    nfull = (qi * bq) // bk

    @pl.when(qi == 0)
    def _():
        dkt_scr[...] = jnp.zeros_like(dkt_scr)
        dvt_scr[...] = jnp.zeros_like(dvt_scr)

    def prob_step(j, r, masked):
        sl = pl.ds(pl.multiple_of(j * bk, bk), bk)
        s = jnp.dot(q, kt_ref[:, sl], preferred_element_type=F32) * (SCALE * LOG2E)
        p = jnp.exp2(s - lse)
        if masked:
            p = jnp.where(causal((rows, bk), bq, qi * bq - nfull * bk), p, 0.0)
        dp = jnp.dot(do, vt_ref[:, sl], preferred_element_type=F32)
        pd = p * dp
        for t in range(bk // 128):
            r = r + pd[:, t * 128:(t + 1) * 128]
        p_scr[j] = p
        dp_scr[j] = dp
        dvt_scr[:, sl] += jnp.dot(do_t, p.astype(BF16), preferred_element_type=F32)
        return r

    r = lax.fori_loop(0, nfull, lambda j, r: prob_step(j, r, False), jnp.zeros((rows, 128), F32))
    r = prob_step(nfull, r, True)
    r = jnp.sum(r, axis=1, keepdims=True)

    def grad_step(j, dq):
        sl = pl.ds(pl.multiple_of(j * bk, bk), bk)
        ds = (p_scr[j] * (dp_scr[j] - r) * SCALE).astype(BF16)
        dkt_scr[:, sl] += jnp.dot(q_t, ds, preferred_element_type=F32)
        return dq + jnp.dot(ds, k_ref[sl, :], preferred_element_type=F32)

    dq = lax.fori_loop(0, nfull + 1, grad_step, jnp.zeros((rows, HEAD_DIM), F32))
    dq = dq.astype(BF16).astype(F32)
    start = pl.ds(pl.multiple_of(qi * bq, bq), bq)
    cos_t, sin_t = cos_ref[start, :], sin_ref[start, :]
    for n in range(rows // bq):
        gq_ref[:, n * HEAD_DIM:(n + 1) * HEAD_DIM] = rotate(dq[n * bq:(n + 1) * bq], cos_t, -sin_t).astype(BF16)

    @pl.when(qi == pl.num_programs(0) - 1)
    def _():
        dk = dkt_scr[...].T.astype(BF16).astype(F32)
        gk_ref[...] = rotate(dk, cos_ref[...], -sin_ref[...]).astype(BF16)
        gv_ref[...] = dvt_scr[...].T.astype(BF16)


def attn_backward(q, do, lse, k, kt, vt, cos_t, sin_t, bq=256, bk=512):
    seq, width = q.shape
    heads = width // HEAD_DIM
    tile = pl.BlockSpec((bq, width), lambda i: (i, 0))
    tall = pl.BlockSpec((seq, HEAD_DIM), lambda i: (0, 0))
    wide = pl.BlockSpec((HEAD_DIM, seq), lambda i: (0, 0))
    return pl.pallas_call(
        functools.partial(bwd_kernel, bq, bk), grid=(seq // bq,),
        in_specs=[tile, tile, pl.BlockSpec((heads, bq, 1), lambda i: (0, i, 0)), tall, wide, wide, tall, tall],
        out_specs=[tile, tall, tall],
        out_shape=[jax.ShapeDtypeStruct((seq, width), BF16), jax.ShapeDtypeStruct((seq, HEAD_DIM), BF16),
                   jax.ShapeDtypeStruct((seq, HEAD_DIM), BF16)],
        scratch_shapes=[pltpu.VMEM((seq // bk, heads * bq, bk), F32), pltpu.VMEM((seq // bk, heads * bq, bk), F32),
                        pltpu.VMEM((HEAD_DIM, seq), F32), pltpu.VMEM((HEAD_DIM, seq), F32)],
        compiler_params=pltpu.CompilerParams(vmem_limit_bytes=VMEM_LIMIT),
        cost_estimate=pl.CostEstimate(flops=16 * seq * seq * width, bytes_accessed=seq * width * 8, transcendentals=0),
        name="attn_bwd")(q, do, lse, k, kt, vt, cos_t, sin_t)


def solution(mesh):
    sp_size = mesh.shape['sp']
    pairs = [[i, i + 1] for i in range(0, sp_size, 2)]
    row_spec = P(('dp', 'sp'), None)
    pos_spec = P(('dp', 'sp'))
    full_spec = P(None, None)
    grad_spec = P('dp', None)

    def local_step(hidden, positions, d_attn, ln_weight, w_q, w_k, w_v, w_o):
        dev = lax.axis_index('sp')
        core = lax.rem(dev, 2)
        dev1 = dev.reshape(1)
        local_rows, feat = hidden.shape
        seq = local_rows * sp_size
        width = w_q.shape[1] // sp_size
        kv_width = w_k.shape[1] // sp_size
        normed32, norm_vjp = jax.vjp(norm_f32, hidden.astype(F32), ln_weight.astype(F32))
        normed = normed32.astype(BF16)
        h_all, q, k, kt, v, vt, cos_t, sin_t = gather_qkv(normed, positions, w_q, w_k, w_v, sp_size)
        d_attn, k = lax.optimization_barrier((d_attn, k))
        g_all = lax.all_gather(d_attn, 'sp', axis=0, tiled=True)
        o, lse = attn_forward(q, kt, v)
        o_all = lax.all_gather(o, 'sp', axis=0)
        do = do_proj(dev1, g_all, w_o, width)
        gq, gk, gv = attn_backward(q, do, lse, k, kt, vt, cos_t, sin_t)
        gq, gk, gv, o_all = lax.optimization_barrier((gq, gk, gv, o_all))
        gq_all = lax.all_gather(gq, 'sp', axis=0)
        gk_all = lax.all_gather(gk, 'sp', axis=0)
        gv_all = lax.all_gather(gv, 'sp', axis=0)

        def own_rows(x_all):
            x = lax.dynamic_slice_in_dim(x_all, dev * local_rows, local_rows, axis=1)
            return jnp.transpose(x, (1, 0, 2)).reshape(local_rows, -1)

        def half(x_all):
            n = sp_size // 2
            return lax.dynamic_slice_in_dim(x_all, core * n, n, axis=0)

        attn_out = jnp.dot(own_rows(o_all), w_o, preferred_element_type=F32).astype(BF16)
        dw_o = jnp.einsum('ste,td->sed', half(o_all), g_all, preferred_element_type=F32).astype(BF16)
        dw_o = lax.all_gather(dw_o.reshape(-1, feat), 'sp', axis=0, tiled=True, axis_index_groups=pairs)

        def grad_in(x_all):
            x = half(x_all)
            y = jnp.einsum('td,ste->dse', h_all, x, preferred_element_type=F32).astype(BF16)
            return lax.all_gather(y.reshape(feat, -1), 'sp', axis=1, tiled=True, axis_index_groups=pairs)

        dw_q, dw_k, dw_v = grad_in(gq_all), grad_in(gk_all), grad_in(gv_all)
        d_normed = (jnp.einsum('te,de->td', own_rows(gq_all), w_q, preferred_element_type=F32)
                    + jnp.einsum('te,de->td', own_rows(gk_all), w_k, preferred_element_type=F32)
                    + jnp.einsum('te,de->td', own_rows(gv_all), w_v, preferred_element_type=F32))
        d_hid, d_lnw = norm_vjp(d_normed)
        d_lnw = lax.psum(d_lnw, 'sp')
        return (attn_out, d_hid.astype(BF16), d_lnw.astype(BF16), dw_q, dw_k, dw_v, dw_o)

    return jax.shard_map(local_step, mesh=mesh,
                         in_specs=(row_spec, pos_spec, row_spec, P(None), full_spec, full_spec, full_spec, full_spec),
                         out_specs=(row_spec, row_spec, P('dp'), grad_spec, grad_spec, grad_spec, grad_spec),
                         check_vma=False)
```

```python
import functools
import jax
import jax.numpy as jnp
from jax import lax
from jax.experimental import pallas as pl
from jax.experimental.pallas import tpu as pltpu
from jax.sharding import PartitionSpec as P

HEAD_DIM = 128
LN_EPS = 1e-5
ROPE_BASE = 10000.0
SCALE = HEAD_DIM ** -0.5
LOG2E = 1.4426950408889634
VMEM_LIMIT = 67_000_000
BF16 = jnp.bfloat16
F32 = jnp.float32
MESH = pl.DeviceIdType.MESH


def norm_f32(hid_f32, weight_f32):
    mean_val = jnp.mean(hid_f32, axis=-1, keepdims=True)
    centered = hid_f32 - mean_val
    var_val = jnp.mean(centered * centered, axis=-1, keepdims=True)
    return centered * lax.rsqrt(var_val + LN_EPS) * weight_f32


def rotate(x, cos_t, sin_t):
    lane = lax.broadcasted_iota(jnp.int32, x.shape, 1)
    swapped = jnp.where(lane % 2 == 0, pltpu.roll(x, HEAD_DIM - 1, 1), pltpu.roll(x, 1, 1))
    return x * cos_t + swapped * sin_t


def flip(i, bit):
    return i + bit - 2 * bit * ((i // bit) % 2)

X, Y, Z = 2, 4, 1

def gather_qkv_kernel(h_ref, pos_ref, freq_ref, wq_ref, wk_ref, wv_ref, hall_ref, ht_ref, q_ref, k_ref, kt_ref, v_ref, vt_ref, cos_ref, sin_ref,
                      w_scr, buf, tbuf, pos_all, pos_send, pos_recv, send, recv, w_sem, load_sem, store_sem, t_sem):
    me = lax.axis_index("sp")
    rows = h_ref.shape[0]
    half = rows // 2
    width = q_ref.shape[1]
    peers = [flip(me, 1), flip(me, 2), flip(flip(me, 2), 1), flip(me, 4), flip(flip(me, 4), 1), flip(flip(me, 4), 2), flip(flip(flip(me, 4), 2), 1)]
    barrier = pltpu.get_barrier_semaphore()
    for p in peers:
        pl.semaphore_signal(barrier, inc=1, device_id={"sp": p}, device_id_type=MESH)
    pl.semaphore_wait(barrier, len(peers))

    def piece(owner, part):
        return pl.ds(pl.multiple_of(owner * rows + part * half, half), half)

    def remote(n, src, owner, part, to):
        return pltpu.make_async_remote_copy(src_ref=src, dst_ref=hall_ref.at[piece(owner, part)], send_sem=send.at[n], recv_sem=recv.at[n],
                                            device_id={"sp": to}, device_id_type=MESH)
    xn, yn, zn = flip(me, X), flip(me, Y), flip(me, Z)
    dn = flip(xn, Y)
    own = lambda part: h_ref.at[pl.ds(part * half, half)]
    got = lambda owner, part: hall_ref.at[piece(owner, part)]
    pos_copies = [pltpu.make_async_remote_copy(src_ref=pos_ref, dst_ref=pos_all.at[me], send_sem=pos_send.at[i], recv_sem=pos_recv.at[i],
                                               device_id={"sp": p}, device_id_type=MESH) for i, p in enumerate(peers)]
    for c in pos_copies:
        c.start()
    s = [remote(0, own(0), me, 0, xn), remote(1, own(1), me, 1, yn), remote(2, own(1), me, 1, xn), remote(3, own(0), me, 0, yn),
         remote(4, got(xn, 0), xn, 0, yn), remote(5, got(yn, 1), yn, 1, xn),
         remote(6, own(0), me, 0, zn), remote(7, own(1), me, 1, zn),
         remote(8, got(xn, 0), xn, 0, zn), remote(9, got(yn, 1), yn, 1, zn),
         remote(10, got(xn, 1), xn, 1, zn), remote(11, got(yn, 0), yn, 0, zn),
         remote(12, got(dn, 0), dn, 0, zn), remote(13, got(dn, 1), dn, 1, zn)]
    for n in (0, 1, 6, 7, 2, 3):
        s[n].start()
    col = lambda n: pl.ds(pl.multiple_of(me * n, n), n)
    w_copies = [pltpu.make_async_copy(wq_ref.at[:, col(width)], w_scr.at[:, pl.ds(0, width)], w_sem.at[0]),
                pltpu.make_async_copy(wk_ref.at[:, col(HEAD_DIM)], w_scr.at[:, pl.ds(width, HEAD_DIM)], w_sem.at[1]),
                pltpu.make_async_copy(wv_ref.at[:, col(HEAD_DIM)], w_scr.at[:, pl.ds(width + HEAD_DIM, HEAD_DIM)], w_sem.at[2])]
    for c in w_copies:
        c.start()
    loads = [pltpu.make_async_copy(own(i), buf.at[i], load_sem.at[i]) for i in range(2)]
    for c in loads:
        c.start()
    pos_all[me] = pos_ref[...]
    for c in pos_copies:
        c.wait_recv()

    def t_copy(tslot, r0):
        return pltpu.make_async_copy(tbuf.at[tslot], ht_ref.at[:, pl.ds(r0, half)], t_sem.at[tslot])

    def compute(slot, owner, part, first=False):
        r0 = pl.multiple_of(owner * rows + part * half, half)
        out = pl.ds(r0, half)
        for t in range(half // 128):
            p = pos_all[owner, pl.ds(part * (half // 128) + t, 1), :]
            angle = jnp.broadcast_to(p, (128, 128)).T * freq_ref[...]
            sign = jnp.where(lax.broadcasted_iota(jnp.int32, (128, 128), 1) % 2 == 0, -1.0, 1.0)
            tr = pl.ds(pl.multiple_of(r0 + t * 128, 128), 128)
            cos_ref[tr, :] = jnp.cos(angle)
            sin_ref[tr, :] = jnp.sin(angle) * sign
        cos_t, sin_t = cos_ref[out, :], sin_ref[out, :]
        h = buf[slot]
        tslot = slot % 2
        if first is None or not first:
            t_copy(tslot, 0).wait()
        tbuf[tslot] = h.T
        t_copy(tslot, r0).start()
        for n in range(width // 256):
            y = jnp.dot(h, w_scr[:, n * 256:(n + 1) * 256], preferred_element_type=F32)
            for e in range(2):
                q_ref[out, n * 256 + e * 128: n * 256 + (e + 1) * 128] = rotate(y[:, e * 128:(e + 1) * 128], cos_t, sin_t).astype(BF16)
        y = jnp.dot(h, w_scr[:, width:width + 256], preferred_element_type=F32)
        k, v = rotate(y[:, :128], cos_t, sin_t), y[:, 128:]
        k_ref[out, :] = k.astype(BF16)
        kt_ref[:, out] = k.T.astype(BF16)
        v_ref[out, :] = v.astype(BF16)
        vt_ref[:, out] = v.T.astype(BF16)

    def run(pairs_, slot0):
        cps = [pltpu.make_async_copy(got(o, p), buf.at[slot0 + i], load_sem.at[slot0 + i]) for i, (o, p) in enumerate(pairs_)]
        for c in cps:
            c.start()
        for c in cps:
            c.wait()
        (o0, p0), (o1, p1) = pairs_
        def body(i, _):
            compute(slot0 + i, o0 + i * (o1 - o0), p0 + i * (p1 - p0))
            return 0
        lax.fori_loop(0, 2, body, 0)

    for c in loads:
        c.wait()
    stores = [pltpu.make_async_copy(buf.at[i], got(me, i), store_sem.at[i]) for i in range(2)]
    for c in stores:
        c.start()
    for c in w_copies:
        c.wait()
    def body(i, _):
        compute(i, me, i, True)
        return 0
    lax.fori_loop(0, 2, body, 0)
    s[6].wait_recv(); s[7].wait_recv()
    run([(zn, 0), (zn, 1)], 2)
    for c in stores:
        c.wait()
    zx, zy, zd = flip(zn, X), flip(zn, Y), flip(dn, Z)
    s[0].wait_recv(); s[4].start(); s[8].start()
    s[1].wait_recv(); s[5].start(); s[9].start()
    run([(xn, 0), (yn, 1)], 0)
    s[8].wait_recv(); s[9].wait_recv()
    run([(zx, 0), (zy, 1)], 2)
    s[2].wait_recv(); s[10].start()
    s[3].wait_recv(); s[11].start()
    run([(xn, 1), (yn, 0)], 0)
    s[10].wait_recv(); s[11].wait_recv()
    run([(zx, 1), (zy, 0)], 2)
    s[4].wait_recv(); s[12].start()
    s[5].wait_recv(); s[13].start()
    run([(dn, 0), (dn, 1)], 0)
    s[12].wait_recv(); s[13].wait_recv()
    run([(zd, 0), (zd, 1)], 2)
    for i in range(2):
        t_copy(i, 0).wait()
    for c in s:
        c.wait_send()
    for c in pos_copies:
        c.wait_send()

def gather_qkv(h, pos, w_q, w_k, w_v, sp_size, cid=1):
    rows, feat = h.shape
    seq = rows * sp_size
    width = w_q.shape[1] // sp_size
    inv_freq = ROPE_BASE ** (-jnp.arange(0, HEAD_DIM, 2, dtype=F32) / HEAD_DIM)
    freq = jnp.repeat(inv_freq, 2)[None, :]
    any_ = pl.BlockSpec(memory_space=pl.ANY)
    vm = pl.BlockSpec(memory_space=pltpu.VMEM)
    return pl.pallas_call(gather_qkv_kernel,
        in_specs=[any_, vm, vm, any_, any_, any_],
        out_specs=[any_, any_] + [vm] * 7,
        out_shape=[jax.ShapeDtypeStruct((seq, feat), BF16), jax.ShapeDtypeStruct((feat, seq), BF16), jax.ShapeDtypeStruct((seq, width), BF16), jax.ShapeDtypeStruct((seq, HEAD_DIM), BF16),
                   jax.ShapeDtypeStruct((HEAD_DIM, seq), BF16), jax.ShapeDtypeStruct((seq, HEAD_DIM), BF16), jax.ShapeDtypeStruct((HEAD_DIM, seq), BF16),
                   jax.ShapeDtypeStruct((seq, HEAD_DIM), F32), jax.ShapeDtypeStruct((seq, HEAD_DIM), F32)],
        scratch_shapes=[pltpu.VMEM((feat, width + 256), BF16), pltpu.VMEM((4, rows // 2, feat), BF16), pltpu.VMEM((2, feat, rows // 2), BF16), pltpu.VMEM((sp_size, rows // 128, 128), F32),
                        pltpu.SemaphoreType.DMA((7,)), pltpu.SemaphoreType.DMA((7,)), pltpu.SemaphoreType.DMA((14,)), pltpu.SemaphoreType.DMA((14,)),
                        pltpu.SemaphoreType.DMA((3,)), pltpu.SemaphoreType.DMA((4,)), pltpu.SemaphoreType.DMA((2,)), pltpu.SemaphoreType.DMA((2,))],
        compiler_params=pltpu.CompilerParams(collective_id=cid, has_side_effects=True, vmem_limit_bytes=VMEM_LIMIT),
        name="gather_qkv")(h, pos.astype(F32).reshape(rows // 128, 128), freq, w_q, w_k, w_v)


def do_kernel(dev_ref, g_ref, wo_ref, do_ref):
    do_ref[...] = lax.dot_general(g_ref[...], wo_ref[...], (((1,), (1,)), ((), ())), preferred_element_type=F32).astype(BF16)


def do_proj(dev, g_all, w_o, width, bm=512):
    seq, feat = g_all.shape
    return pl.pallas_call(
        do_kernel,
        grid_spec=pltpu.PrefetchScalarGridSpec(
            num_scalar_prefetch=1, grid=(seq // bm,),
            in_specs=[pl.BlockSpec((bm, feat), lambda i, d: (i, 0)), pl.BlockSpec((width, feat), lambda i, d: (d[0], 0))],
            out_specs=pl.BlockSpec((bm, width), lambda i, d: (i, 0))),
        out_shape=jax.ShapeDtypeStruct((seq, width), BF16),
        compiler_params=pltpu.CompilerParams(vmem_limit_bytes=VMEM_LIMIT),
        cost_estimate=pl.CostEstimate(flops=2 * seq * feat * width, bytes_accessed=seq * feat * 2, transcendentals=0),
        name="do_proj")(dev, g_all, w_o)


def stack_heads(x):
    return jnp.concatenate([x[:, n * HEAD_DIM:(n + 1) * HEAD_DIM] for n in range(x.shape[1] // HEAD_DIM)], axis=0)


def causal(shape, bq, offset):
    rows = lax.rem(lax.broadcasted_iota(jnp.int32, shape, 0), bq) + offset
    return rows >= lax.broadcasted_iota(jnp.int32, shape, 1)


def fwd_kernel(bq, bk, q_ref, kt_ref, v_ref, ot_ref, lse_ref, s_scr):
    qi = pl.program_id(0)
    q = stack_heads(q_ref[...])
    rows = q.shape[0]
    nfull = (qi * bq) // bk

    def scores(j):
        return jnp.dot(q, kt_ref[:, pl.ds(pl.multiple_of(j * bk, bk), bk)], preferred_element_type=F32) * (SCALE * LOG2E)

    def lane_max(m, s):
        for c in range(bk // 128):
            m = jnp.maximum(m, s[:, c * 128:(c + 1) * 128])
        return m

    def score_step(j, m):
        s = scores(j)
        s_scr[j] = s
        return lane_max(m, s)

    m = lax.fori_loop(0, nfull, score_step, jnp.full((rows, 128), -jnp.inf, F32))
    s = jnp.where(causal((rows, bk), bq, qi * bq - nfull * bk), scores(nfull), -jnp.inf)
    s_scr[nfull] = s
    m = jnp.max(lane_max(m, s), axis=1, keepdims=True)

    def value_step(j, carry):
        l, o = carry
        p = jnp.exp2(s_scr[j] - m)
        for t in range(bk // 128):
            l = l + p[:, t * 128:(t + 1) * 128]
        o = o + jnp.dot(p.astype(BF16), v_ref[pl.ds(pl.multiple_of(j * bk, bk), bk), :], preferred_element_type=F32)
        return l, o

    l, o = lax.fori_loop(0, nfull + 1, value_step, (jnp.zeros((rows, 128), F32), jnp.zeros((rows, HEAD_DIM), F32)))
    l = jnp.sum(l, axis=1, keepdims=True)
    o = (o / l).astype(BF16)
    for n in range(rows // bq):
        ot_ref[n * HEAD_DIM:(n + 1) * HEAD_DIM, :] = o[n * bq:(n + 1) * bq].T
    lse_ref[...] = (m + jnp.log2(l)).reshape(lse_ref.shape)


def attn_forward(q, kt, v, bq=256, bk=1024):
    seq, width = q.shape
    heads = width // HEAD_DIM
    return pl.pallas_call(
        functools.partial(fwd_kernel, bq, bk), grid=(seq // bq,),
        in_specs=[pl.BlockSpec((bq, width), lambda i: (i, 0)), pl.BlockSpec((HEAD_DIM, seq), lambda i: (0, 0)),
                  pl.BlockSpec((seq, HEAD_DIM), lambda i: (0, 0))],
        out_specs=[pl.BlockSpec((width, bq), lambda i: (0, i)), pl.BlockSpec((heads, bq, 1), lambda i: (0, i, 0))],
        out_shape=[jax.ShapeDtypeStruct((width, seq), BF16), jax.ShapeDtypeStruct((heads, seq, 1), F32)],
        scratch_shapes=[pltpu.VMEM((seq // bk, heads * bq, bk), F32)],
        compiler_params=pltpu.CompilerParams(vmem_limit_bytes=VMEM_LIMIT),
        cost_estimate=pl.CostEstimate(flops=8 * seq * seq * width, bytes_accessed=seq * width * 8, transcendentals=0),
        name="attn_fwd")(q, kt, v)


def bwd_kernel(bq, bk, more, *refs):
    q_ref, do_ref, lse_ref, k_ref, kt_ref, vt_ref, cos_ref, sin_ref = refs[:8]
    gq_ref, dkt_ref, dvt_ref, p_scr, dp_scr = refs[-5:]
    qi = pl.program_id(0)
    q = stack_heads(q_ref[...])
    do = stack_heads(do_ref[...])
    rows = q.shape[0]
    lse = lse_ref[...].reshape(rows, 1)
    q_t = q.T
    do_t = do.T
    nfull = (qi * bq) // bk

    @pl.when(qi == 0)
    def _():
        dkt_ref[...] = refs[8][...] if more else jnp.zeros_like(dkt_ref)
        dvt_ref[...] = refs[9][...] if more else jnp.zeros_like(dvt_ref)

    def prob_step(j, r, masked):
        sl = pl.ds(pl.multiple_of(j * bk, bk), bk)
        s = jnp.dot(q, kt_ref[:, sl], preferred_element_type=F32) * (SCALE * LOG2E)
        p = jnp.exp2(s - lse)
        if masked:
            p = jnp.where(causal((rows, bk), bq, qi * bq - nfull * bk), p, 0.0)
        dp = jnp.dot(do, vt_ref[:, sl], preferred_element_type=F32)
        pd = p * dp
        for t in range(bk // 128):
            r = r + pd[:, t * 128:(t + 1) * 128]
        p_scr[j] = p
        dp_scr[j] = dp
        dvt_ref[:, sl] += jnp.dot(do_t, p.astype(BF16), preferred_element_type=F32)
        return r

    r = lax.fori_loop(0, nfull, lambda j, r: prob_step(j, r, False), jnp.zeros((rows, 128), F32))
    r = prob_step(nfull, r, True)
    r = jnp.sum(r, axis=1, keepdims=True)

    def grad_step(j, dq):
        sl = pl.ds(pl.multiple_of(j * bk, bk), bk)
        ds = (p_scr[j] * (dp_scr[j] - r) * SCALE).astype(BF16)
        dkt_ref[:, sl] += jnp.dot(q_t, ds, preferred_element_type=F32)
        return dq + jnp.dot(ds, k_ref[sl, :], preferred_element_type=F32)

    dq = lax.fori_loop(0, nfull + 1, grad_step, jnp.zeros((rows, HEAD_DIM), F32))
    dq = dq.astype(BF16).astype(F32)
    cos_t, sin_t = cos_ref[...], sin_ref[...]
    for n in range(rows // bq):
        gq_ref[:, n * HEAD_DIM:(n + 1) * HEAD_DIM] = rotate(dq[n * bq:(n + 1) * bq], cos_t, -sin_t).astype(BF16)


def kv_kernel(dkt_ref, dvt_ref, cos_ref, sin_ref, gkv_ref):
    dk = dkt_ref[...].T.astype(BF16).astype(F32)
    gkv_ref[:, :HEAD_DIM] = rotate(dk, cos_ref[...], -sin_ref[...]).astype(BF16)
    gkv_ref[:, HEAD_DIM:] = dvt_ref[...].T.astype(BF16)


def attn_backward(part, q, do, lse, k, kt, vt, cos_t, sin_t, sums=None, bq=256, bk=512):
    seq = q.shape[0]
    width, heads = 2 * HEAD_DIM, 2
    tile = pl.BlockSpec((bq, width), lambda i: (i, part))
    rope = pl.BlockSpec((bq, HEAD_DIM), lambda i: (i, 0))
    tall = pl.BlockSpec((seq, HEAD_DIM), lambda i: (0, 0))
    wide = pl.BlockSpec((HEAD_DIM, seq), lambda i: (0, 0))
    last = sums is not None
    params = dict(compiler_params=pltpu.CompilerParams(vmem_limit_bytes=VMEM_LIMIT),
                  cost_estimate=pl.CostEstimate(flops=8 * seq * seq * width, bytes_accessed=seq * width * 8, transcendentals=0))
    return pl.pallas_call(
        functools.partial(bwd_kernel, bq, bk, last), grid=(seq // bq,),
        in_specs=[tile, tile, pl.BlockSpec((heads, bq, 1), lambda i: (part, i, 0)), tall, wide, wide, rope, rope] + ([wide, wide] if last else []),
        out_specs=[pl.BlockSpec((bq, width), lambda i: (i, 0)), wide, wide],
        out_shape=[jax.ShapeDtypeStruct((seq, width), BF16), jax.ShapeDtypeStruct((HEAD_DIM, seq), F32), jax.ShapeDtypeStruct((HEAD_DIM, seq), F32)],
        scratch_shapes=[pltpu.VMEM((seq // bk, heads * bq, bk), F32), pltpu.VMEM((seq // bk, heads * bq, bk), F32)],
        name="attn_bwd", **params)(q, do, lse, k, kt, vt, cos_t, sin_t, *(sums or ()))


def kv_grad(dkt, dvt, cos_t, sin_t, bq=512):
    seq = dkt.shape[1]
    wide = pl.BlockSpec((HEAD_DIM, bq), lambda i: (0, i))
    rope = pl.BlockSpec((bq, HEAD_DIM), lambda i: (i, 0))
    return pl.pallas_call(kv_kernel, grid=(seq // bq,), in_specs=[wide, wide, rope, rope],
                          out_specs=pl.BlockSpec((bq, 2 * HEAD_DIM), lambda i: (i, 0)),
                          out_shape=jax.ShapeDtypeStruct((seq, 2 * HEAD_DIM), BF16), name="kv_grad")(dkt, dvt, cos_t, sin_t)


def dw_o_kernel(core_ref, ot_ref, g_ref, final_ref, send_ref):
    y = jnp.dot(ot_ref[...], g_ref[...], preferred_element_type=F32).astype(BF16)
    final_ref[...] = y
    send_ref[...] = y


def dw_o_half(core, ot_all, g_all, bn=1024):
    n_dev, width, seq = ot_all.shape
    feat = g_all.shape[1]
    half = n_dev // 2
    return pl.pallas_call(
        dw_o_kernel,
        grid_spec=pltpu.PrefetchScalarGridSpec(
            num_scalar_prefetch=1, grid=(feat // bn, half),
            in_specs=[pl.BlockSpec((None, width, seq), lambda j, s, c: (c[0] * half + s, 0, 0)), pl.BlockSpec((seq, bn), lambda j, s, c: (0, j))],
            out_specs=[pl.BlockSpec((width, bn), lambda j, s, c: (c[0] * half + s, j)), pl.BlockSpec((width, bn), lambda j, s, c: (s, j))]),
        out_shape=[jax.ShapeDtypeStruct((n_dev * width, feat), BF16), jax.ShapeDtypeStruct((half * width, feat), BF16)],
        compiler_params=pltpu.CompilerParams(vmem_limit_bytes=VMEM_LIMIT),
        cost_estimate=pl.CostEstimate(flops=n_dev * width * feat * seq, bytes_accessed=seq * feat * 6, transcendentals=0),
        name="dw_o_half")(core, ot_all, g_all)


def dw_kernel(n_final, n_copy, core_ref, ht_ref, x_ref, *refs):
    recv = refs[:n_copy]
    outs = refs[-(n_final + 1 + n_copy):]
    y = jnp.dot(ht_ref[...], x_ref[...], preferred_element_type=F32).astype(BF16)
    w = y.shape[1] // n_final
    for n in range(n_final):
        outs[n][...] = y[:, n * w:(n + 1) * w]
    outs[n_final][...] = y
    for n in range(n_copy):
        outs[n_final + 1 + n][...] = recv[n][...]


def dw_half(name, core, ht, x_all, finals, final_shapes, final_cols, copies, bm=1024):
    n_dev, seq, cols = x_all.shape
    feat = ht.shape[0]
    half = n_dev // 2
    n_final = len(final_shapes)
    w = cols // n_final
    hbm = pl.BlockSpec(memory_space=pl.ANY)
    ins = [ht, x_all] + [c[0] for c in copies]
    in_specs = [pl.BlockSpec((bm, seq), lambda i, s, c: (i, 0)), pl.BlockSpec((None, seq, cols), lambda i, s, c: (c[0] * half + s, 0, 0))]
    in_specs += [c[1] for c in copies]
    out_specs = [pl.BlockSpec((bm, w), functools.partial(lambda f, i, s, c: (i, f(c[0] * half + s)), f)) for f in final_cols]
    out_specs += [pl.BlockSpec((bm, cols), lambda i, s, c: (i, s))] + [c[3] for c in copies]
    out_shape = [jax.ShapeDtypeStruct(sh, BF16) for sh in final_shapes] + [jax.ShapeDtypeStruct((feat, half * cols), BF16)]
    out_shape += [jax.ShapeDtypeStruct(c[2].shape, BF16) for c in copies]
    aliases = {}
    for n, f in enumerate(finals):
        if f is not None:
            aliases[1 + len(ins)] = n
            ins.append(f)
            in_specs.append(hbm)
    for n, c in enumerate(copies):
        aliases[1 + len(ins)] = n_final + 1 + n
        ins.append(c[2])
        in_specs.append(hbm)
    return pl.pallas_call(
        functools.partial(dw_kernel, n_final, len(copies)),
        grid_spec=pltpu.PrefetchScalarGridSpec(num_scalar_prefetch=1, grid=(feat // bm, half), in_specs=in_specs, out_specs=out_specs),
        out_shape=out_shape, input_output_aliases=aliases,
        compiler_params=pltpu.CompilerParams(vmem_limit_bytes=VMEM_LIMIT),
        cost_estimate=pl.CostEstimate(flops=2 * seq * feat * half * cols, bytes_accessed=seq * feat * 6, transcendentals=0),
        name=name)(core, *ins)


def copy_kernel(core_ref, recv_ref, _, out_ref):
    out_ref[...] = recv_ref[...]


def copy_in(core, recv, final, grid, recv_spec, final_spec):
    return pl.pallas_call(
        copy_kernel,
        grid_spec=pltpu.PrefetchScalarGridSpec(num_scalar_prefetch=1, grid=grid, in_specs=[recv_spec, pl.BlockSpec(memory_space=pl.ANY)],
                                               out_specs=final_spec),
        out_shape=jax.ShapeDtypeStruct(final.shape, BF16), input_output_aliases={2: 0},
        compiler_params=pltpu.CompilerParams(vmem_limit_bytes=VMEM_LIMIT), name="copy_in")(core, recv, final)


def solution(mesh):
    sp_size = mesh.shape['sp']
    row_spec = P(('dp', 'sp'), None)
    pos_spec = P(('dp', 'sp'))
    full_spec = P(None, None)
    grad_spec = P('dp', None)

    def local_step(hidden, positions, d_attn, ln_weight, w_q, w_k, w_v, w_o):
        dev = lax.axis_index('sp')
        core = lax.rem(dev, 2)
        dev1 = dev.reshape(1)
        local_rows, feat = hidden.shape
        width = w_q.shape[1] // sp_size
        normed32, norm_vjp = jax.vjp(norm_f32, hidden.astype(F32), ln_weight.astype(F32))
        normed = normed32.astype(BF16)
        h_all, ht, q, k, kt, v, vt, cos_t, sin_t = gather_qkv(normed, positions, w_q, w_k, w_v, sp_size)
        d_attn, k = lax.optimization_barrier((d_attn, k))
        g_all = lax.all_gather(d_attn, 'sp', axis=0, tiled=True)
        ot, lse = attn_forward(q, kt, v)
        ot, g_all = lax.optimization_barrier((ot, g_all))
        ot_all = lax.all_gather(ot, 'sp', axis=0)
        do = do_proj(dev1, g_all, w_o, width)
        ga, dkt, dvt = attn_backward(0, q, do, lse, k, kt, vt, cos_t, sin_t)
        ga, ot_all = lax.optimization_barrier((ga, ot_all))
        ga_all = lax.all_gather(ga, 'sp', axis=0)
        gb, dkt, dvt = attn_backward(1, q, do, lse, k, kt, vt, cos_t, sin_t, (dkt, dvt))
        gc = kv_grad(dkt, dvt, cos_t, sin_t)
        gc, ga_all = lax.optimization_barrier((gc, ga_all))
        gc_all = lax.all_gather(gc, 'sp', axis=0)
        gb, gc_all = lax.optimization_barrier((gb, gc_all))
        gb_all = lax.all_gather(gb, 'sp', axis=0)
        core1 = core.reshape(1)
        swap = lambda x: lax.ppermute(x, 'sp', [(i, i ^ 1) for i in range(sp_size)])
        n_half = sp_size // 2
        piece = 2 * HEAD_DIM

        def own_rows(x_all):
            x = lax.dynamic_slice_in_dim(x_all, dev * local_rows, local_rows, axis=1)
            return jnp.transpose(x, (1, 0, 2)).reshape(local_rows, -1)

        dw_o, o_send = dw_o_half(core1, ot_all, g_all)
        o_recv = swap(o_send)
        ot_own = lax.dynamic_slice_in_dim(ot_all, dev * local_rows, local_rows, axis=2).reshape(feat, local_rows)
        attn_out = jnp.einsum('et,ed->td', ot_own, w_o, preferred_element_type=F32).astype(BF16)
        steps = (feat // 1024) * n_half
        o_rows = feat // 2 // steps
        ride_o = (o_recv, pl.BlockSpec((o_rows, feat), lambda i, s, c: (i * n_half + s, 0)), dw_o,
                  pl.BlockSpec((o_rows, feat), lambda i, s, c: ((1 - c[0]) * steps + i * n_half + s, 0)))
        dw_q, a_send, dw_o = dw_half('dw_qa', core1, ht, ga_all, [None], [w_q.shape], [lambda d: 2 * d], [ride_o])
        a_recv = swap(a_send)
        ride_a = (a_recv, pl.BlockSpec((1024, piece), lambda i, s, c: (i, s)), dw_q,
                  pl.BlockSpec((1024, piece), lambda i, s, c: (i, 2 * ((1 - c[0]) * n_half + s))))
        dw_k, dw_v, c_send, dw_q = dw_half('dw_kv', core1, ht, gc_all, [None, None], [w_k.shape, w_v.shape], [lambda d: d, lambda d: d], [ride_a])
        c_recv = swap(c_send)
        ride_k = (c_recv, pl.BlockSpec((1024, HEAD_DIM), lambda i, s, c: (i, 2 * s)), dw_k,
                  pl.BlockSpec((1024, HEAD_DIM), lambda i, s, c: (i, (1 - c[0]) * n_half + s)))
        ride_v = (c_recv, pl.BlockSpec((1024, HEAD_DIM), lambda i, s, c: (i, 2 * s + 1)), dw_v,
                  pl.BlockSpec((1024, HEAD_DIM), lambda i, s, c: (i, (1 - c[0]) * n_half + s)))
        dw_q, b_send, dw_k, dw_v = dw_half('dw_qb', core1, ht, gb_all, [dw_q], [w_q.shape], [lambda d: 2 * d + 1], [ride_k, ride_v])
        b_recv = swap(b_send)
        dw_q = copy_in(core1, b_recv, dw_q, (feat // 1024, n_half), pl.BlockSpec((1024, piece), lambda i, s, c: (i, s)),
                       pl.BlockSpec((1024, piece), lambda i, s, c: (i, 2 * ((1 - c[0]) * n_half + s) + 1)))

        gq_tok = jnp.concatenate([own_rows(ga_all).reshape(local_rows, sp_size, piece), own_rows(gb_all).reshape(local_rows, sp_size, piece)],
                                 axis=2).reshape(local_rows, -1)
        gkv_tok = own_rows(gc_all).reshape(local_rows, sp_size, 2, HEAD_DIM)
        d_normed = (jnp.einsum('te,de->td', gq_tok, w_q, preferred_element_type=F32)
                    + jnp.einsum('te,de->td', gkv_tok[:, :, 0].reshape(local_rows, -1), w_k, preferred_element_type=F32)
                    + jnp.einsum('te,de->td', gkv_tok[:, :, 1].reshape(local_rows, -1), w_v, preferred_element_type=F32))
        d_hid, d_lnw = norm_vjp(d_normed)
        d_lnw = lax.psum(d_lnw, 'sp')
        return (attn_out, d_hid.astype(BF16), d_lnw.astype(BF16), dw_q, dw_k, dw_v, dw_o)

    return jax.shard_map(local_step, mesh=mesh,
                         in_specs=(row_spec, pos_spec, row_spec, P(None), full_spec, full_spec, full_spec, full_spec),
                         out_specs=(row_spec, row_spec, P('dp'), grad_spec, grad_spec, grad_spec, grad_spec),
                         check_vma=False)
```

```python
import functools
import jax
import jax.numpy as jnp
from jax import lax
from jax.experimental import pallas as pl
from jax.experimental.pallas import tpu as pltpu
from jax.sharding import PartitionSpec as P

HEAD_DIM = LANE = 128
PAIR = 2 * HEAD_DIM
CORE, X_BIT, Y_BIT = 1, 2, 4
LOW, HIGH, SLOTS = 0, 1, 2
SEND_ORDER = (0, 1, 6, 7, 2, 3)
N_COPIES, N_PEERS = 14, 7
LN_EPS = 1e-5
ROPE_BASE = 10000.0
SCALE = HEAD_DIM ** -0.5
LOG2E = 1.4426950408889634
VMEM_LIMIT = 67_000_000
BF16 = jnp.bfloat16
F32 = jnp.float32
MESH = pl.DeviceIdType.MESH
HBM = pl.BlockSpec(memory_space=pl.ANY)
SEM = pltpu.SemaphoreType.DMA
row = lambda i, *_: (i, 0)
col = lambda i, *_: (0, i)
whole = lambda *_: (0, 0)
ONCE = dict(pipeline_mode=pl.Buffered(1))
PARAMS = pltpu.CompilerParams(vmem_limit_bytes=VMEM_LIMIT)


def grid_place():
    return pl.program_id(0), pl.num_programs(0) - 1


def dot(x, y):
    return jnp.dot(x, y, preferred_element_type=F32)


def array(*shape, dtype=BF16):
    return jax.ShapeDtypeStruct(shape, dtype)


def remote_params(number):
    return pltpu.CompilerParams(collective_id=number, has_side_effects=True, vmem_limit_bytes=VMEM_LIMIT)


def cost(flops):
    return pl.CostEstimate(flops=flops, bytes_accessed=flops // HEAD_DIM, transcendentals=0)


def norm_f32(hid_f32, weight_f32):
    mean_val = jnp.mean(hid_f32, axis=-1, keepdims=True)
    centered = hid_f32 - mean_val
    var_val = jnp.mean(centered * centered, axis=-1, keepdims=True)
    return centered * lax.rsqrt(var_val + LN_EPS) * weight_f32


def rotate(x, cos_t, sin_t):
    lane = lax.broadcasted_iota(jnp.int32, x.shape, 1)
    swapped = jnp.where(lane % 2 == 0, pltpu.roll(x, HEAD_DIM - 1, 1), pltpu.roll(x, 1, 1))
    return x * cos_t + swapped * sin_t


def flip(i, bit):
    return i + bit - 2 * bit * ((i // bit) % 2)


def exchange(send, recv, block, own, to_partner):
    me = lax.axis_index("sp")
    xn, yn, zn = flip(me, X_BIT), flip(me, Y_BIT), flip(me, CORE)
    dn = flip(xn, Y_BIT)

    def copy(n, src, owner, part, to):
        return pltpu.make_async_remote_copy(src_ref=src, dst_ref=block(owner, part), send_sem=send.at[n], recv_sem=recv.at[n],
                                            device_id={"sp": to}, device_id_type=MESH)

    plan = [(me, LOW, xn), (me, HIGH, yn), (me, HIGH, xn), (me, LOW, yn), (xn, LOW, yn), (yn, HIGH, xn)]
    if to_partner:
        plan += [(me, LOW, zn), (me, HIGH, zn), (xn, LOW, zn), (yn, HIGH, zn), (xn, HIGH, zn), (yn, LOW, zn), (dn, LOW, zn), (dn, HIGH, zn)]
    return [copy(n, own(p) if o is me else block(o, p), o, p, to) for n, (o, p, to) in enumerate(plan)]


def greet(peers):
    barrier = pltpu.get_barrier_semaphore()
    for p in peers:
        pl.semaphore_signal(barrier, inc=1, device_id={"sp": p}, device_id_type=MESH)
    pl.semaphore_wait(barrier, len(peers))


def neighbours():
    me = lax.axis_index("sp")
    return [flip(me, CORE), flip(me, X_BIT), flip(me, Y_BIT)]


def everyone():
    me = lax.axis_index("sp")
    xn, yn = flip(me, X_BIT), flip(me, Y_BIT)
    dn = flip(xn, Y_BIT)
    return [flip(me, CORE), xn, flip(xn, CORE), yn, flip(yn, CORE), dn, flip(dn, CORE)]


def arrivals(me):
    xn, yn, zn = flip(me, X_BIT), flip(me, Y_BIT), flip(me, CORE)
    dn = flip(xn, Y_BIT)
    zx, zy, zd = flip(xn, CORE), flip(yn, CORE), flip(dn, CORE)
    return [[(me, LOW), (me, HIGH), (zn, LOW), (zn, HIGH)], [(xn, LOW), (yn, HIGH), (zx, LOW), (zy, HIGH)], [(xn, HIGH), (yn, LOW), (zx, HIGH), (zy, LOW)],
            [(dn, LOW), (dn, HIGH), (zd, LOW), (zd, HIGH)]]


def pass_on(copies, group):
    first, second = (SLOTS * (group - 1), SLOTS * (group - 1) + 1)
    copies[first].wait_recv()
    if group == 1:
        copies[4].start()
    if len(copies) > 6:
        copies[6 + 2 * group].start()
    copies[second].wait_recv()
    if group == 1:
        copies[5].start()
    if len(copies) > 6:
        copies[7 + 2 * group].start()


def from_partner(copies, group):
    copies[6 + 2 * group].wait_recv()
    copies[7 + 2 * group].wait_recv()


def gather_qkv_kernel(h_ref, pos_ref, freq_ref, wq_ref, wk_ref, wv_ref, hall_ref, ht_ref, q_ref, k_ref, kt_ref, v_ref, vt_ref, cos_ref, sin_ref,
                      w_scr, buf, tbuf, pos_all, pos_send, pos_recv, send, recv, w_sem, load_sem, store_sem, t_sem):
    me = lax.axis_index("sp")
    rows = h_ref.shape[0]
    half = rows // 2
    width = q_ref.shape[1]
    peers = everyone()
    greet(peers)
    own = lambda part: h_ref.at[pl.ds(part * half, half)]
    got = lambda owner, part: hall_ref.at[pl.ds(pl.multiple_of(owner * rows + part * half, half), half)]
    pos_copies = [pltpu.make_async_remote_copy(src_ref=pos_ref, dst_ref=pos_all.at[me], send_sem=pos_send.at[i], recv_sem=pos_recv.at[i],
                                               device_id={"sp": p}, device_id_type=MESH) for i, p in enumerate(peers)]
    for c in pos_copies:
        c.start()
    s = exchange(send, recv, got, own, True)
    for n in SEND_ORDER:
        s[n].start()
    col = lambda n: pl.ds(pl.multiple_of(me * n, n), n)
    w_copies = [pltpu.make_async_copy(wq_ref.at[:, col(width)], w_scr.at[:, pl.ds(0, width)], w_sem.at[0]),
                pltpu.make_async_copy(wk_ref.at[:, col(HEAD_DIM)], w_scr.at[:, pl.ds(width, HEAD_DIM)], w_sem.at[1]),
                pltpu.make_async_copy(wv_ref.at[:, col(HEAD_DIM)], w_scr.at[:, pl.ds(width + HEAD_DIM, HEAD_DIM)], w_sem.at[2])]
    for c in w_copies:
        c.start()
    loads = [pltpu.make_async_copy(own(i), buf.at[i], load_sem.at[i]) for i in range(SLOTS)]
    for c in loads:
        c.start()
    pos_all[me] = pos_ref[...]
    for c in pos_copies:
        c.wait_recv()

    def t_copy(tslot, r0):
        return pltpu.make_async_copy(tbuf.at[tslot], ht_ref.at[:, pl.ds(r0, half)], t_sem.at[tslot])

    def compute(slot, owner, part, first=False):
        r0 = pl.multiple_of(owner * rows + part * half, half)
        out = pl.ds(r0, half)
        for t in range(half // LANE):
            p = pos_all[owner, pl.ds(part * (half // LANE) + t, 1), :]
            angle = jnp.broadcast_to(p, (LANE, LANE)).T * freq_ref[...]
            sign = jnp.where(lax.broadcasted_iota(jnp.int32, (LANE, LANE), 1) % 2 == 0, -1.0, 1.0)
            tr = pl.ds(pl.multiple_of(r0 + t * LANE, LANE), LANE)
            cos_ref[tr, :] = jnp.cos(angle)
            sin_ref[tr, :] = jnp.sin(angle) * sign
        cos_t, sin_t = cos_ref[out, :], sin_ref[out, :]
        h = buf[slot]
        tslot = slot % 2
        if not first:
            t_copy(tslot, 0).wait()
        tbuf[tslot] = h.T
        t_copy(tslot, r0).start()
        for n in range(width // PAIR):
            y = dot(h, w_scr[:, n * PAIR:(n + 1) * PAIR])
            for e in range(SLOTS):
                q_ref[out, n * PAIR + e * LANE: n * PAIR + (e + 1) * LANE] = rotate(y[:, e * LANE:(e + 1) * LANE], cos_t, sin_t).astype(BF16)
        y = dot(h, w_scr[:, width:width + PAIR])
        k, v = rotate(y[:, :LANE], cos_t, sin_t), y[:, LANE:]
        k_ref[out, :] = k.astype(BF16)
        kt_ref[:, out] = k.T.astype(BF16)
        v_ref[out, :] = v.astype(BF16)
        vt_ref[:, out] = v.T.astype(BF16)

    def run(two, slot0):
        cps = [pltpu.make_async_copy(got(o, p), buf.at[slot0 + i], load_sem.at[slot0 + i]) for i, (o, p) in enumerate(two)]
        for c in cps:
            c.start()
        for c in cps:
            c.wait()
        (o0, p0), (o1, p1) = two

        def body(i, _):
            compute(slot0 + i, o0 + i * (o1 - o0), p0 + i * (p1 - p0))
            return 0

        lax.fori_loop(0, SLOTS, body, 0)

    for c in loads:
        c.wait()
    stores = [pltpu.make_async_copy(buf.at[i], got(me, i), store_sem.at[i]) for i in range(SLOTS)]
    for c in stores:
        c.start()
    for c in w_copies:
        c.wait()

    def body(i, _):
        compute(i, me, i, True)
        return 0

    lax.fori_loop(0, SLOTS, body, 0)
    groups = arrivals(me)
    from_partner(s, 0)
    run(groups[0][2:], 2)
    for c in stores:
        c.wait()
    for g in (1, 2, 3):
        pass_on(s, g)
        run(groups[g][:2], 0)
        from_partner(s, g)
        run(groups[g][2:], 2)
    for i in range(SLOTS):
        t_copy(i, 0).wait()
    for c in s:
        c.wait_send()
    for c in pos_copies:
        c.wait_send()


def gather_qkv(h, pos, w_q, w_k, w_v, sp_size):
    rows, feat = h.shape
    seq = rows * sp_size
    width = w_q.shape[1] // sp_size
    inv_freq = ROPE_BASE ** (-jnp.arange(0, HEAD_DIM, 2, dtype=F32) / HEAD_DIM)
    freq = jnp.repeat(inv_freq, 2)[None, :]
    vmem = pl.BlockSpec(memory_space=pltpu.VMEM)
    tall, wide = array(seq, HEAD_DIM), array(HEAD_DIM, seq)
    table = array(seq, HEAD_DIM, dtype=F32)
    return pl.pallas_call(
        gather_qkv_kernel,
        in_specs=[HBM, vmem, vmem, HBM, HBM, HBM],
        out_specs=[HBM, HBM] + [vmem] * 7,
        out_shape=[array(seq, feat), array(feat, seq), array(seq, width),
                   tall, wide, tall, wide, table, table],
        scratch_shapes=[pltpu.VMEM((feat, width + PAIR), BF16), pltpu.VMEM((4, rows // 2, feat), BF16), pltpu.VMEM((SLOTS, feat, rows // 2), BF16),
                        pltpu.VMEM((sp_size, rows // LANE, LANE), F32), SEM((N_PEERS,)), SEM((N_PEERS,)), SEM((N_COPIES,)), SEM((N_COPIES,)), SEM((3,)), SEM((4,)), SEM((SLOTS,)),
                        SEM((SLOTS,))],
        compiler_params=remote_params(1),
        name="gather_qkv")(h, pos.astype(F32).reshape(rows // LANE, LANE), freq, w_q, w_k, w_v)


def stack_heads(x):
    return jnp.concatenate([x[:, n * HEAD_DIM:(n + 1) * HEAD_DIM] for n in range(x.shape[1] // HEAD_DIM)], axis=0)


def causal(shape, bq, offset):
    rows = lax.rem(lax.broadcasted_iota(jnp.int32, shape, 0), bq) + offset
    return rows >= lax.broadcasted_iota(jnp.int32, shape, 1)


def fwd_step(qi, bq, bk, q_ref, kt_ref, v_ref, ot_ref, lse_ref, s_scr):
    q = stack_heads(q_ref[...])
    rows = q.shape[0]
    nfull = (qi * bq) // bk

    def scores(j):
        return dot(q, kt_ref[:, pl.ds(pl.multiple_of(j * bk, bk), bk)]) * (SCALE * LOG2E)

    def lane_max(m, s):
        for c in range(bk // LANE):
            m = jnp.maximum(m, s[:, c * LANE:(c + 1) * LANE])
        return m

    def score_step(j, m):
        s = scores(j)
        s_scr[j] = s
        return lane_max(m, s)

    m = lax.fori_loop(0, nfull, score_step, jnp.full((rows, LANE), -jnp.inf, F32))
    s = jnp.where(causal((rows, bk), bq, qi * bq - nfull * bk), scores(nfull), -jnp.inf)
    s_scr[nfull] = s
    m = jnp.max(lane_max(m, s), axis=1, keepdims=True)

    def value_step(j, carry):
        l, o = carry
        p = jnp.exp2(s_scr[j] - m)
        for t in range(bk // LANE):
            l = l + p[:, t * LANE:(t + 1) * LANE]
        o = o + dot(p.astype(BF16), v_ref[pl.ds(pl.multiple_of(j * bk, bk), bk), :])
        return l, o

    l, o = lax.fori_loop(0, nfull + 1, value_step, (jnp.zeros((rows, LANE), F32), jnp.zeros((rows, HEAD_DIM), F32)))
    l = jnp.sum(l, axis=1, keepdims=True)
    o = (o / l).astype(BF16)
    for n in range(rows // bq):
        ot_ref[n * HEAD_DIM:(n + 1) * HEAD_DIM, :] = o[n * bq:(n + 1) * bq].T
    lse_ref[...] = (m + jnp.log2(l)).reshape(lse_ref.shape)


def gather_fwd_kernel(n_fwd, relay, bq, bk, q_ref, kt_ref, v_ref, g_ref, wo_ref, ot_ref, lse_ref, gall_ref, do_ref,
                      s_scr, wo_scr, buf, send, recv, w_sem, load_sem, store_sem):
    step = pl.program_id(0)
    me = lax.axis_index("sp")
    rows, width = g_ref.shape[0], do_ref.shape[1]
    half = rows // 2
    own = lambda part: g_ref.at[pl.ds(part * half, half)]
    got = lambda owner, part: gall_ref.at[pl.ds(pl.multiple_of(owner * rows + part * half, half), half)]
    s = exchange(send, recv, got, own, True)
    w_copy = pltpu.make_async_copy(wo_ref.at[pl.ds(pl.multiple_of(me * width, width), width)], wo_scr, w_sem.at[0])
    loads = [pltpu.make_async_copy(own(i), buf.at[i], load_sem.at[i]) for i in range(SLOTS)]
    stores = [pltpu.make_async_copy(buf.at[i], got(me, i), store_sem.at[i]) for i in range(SLOTS)]

    @pl.when(step == 0)
    def _():
        greet(neighbours())
        for n in SEND_ORDER:
            s[n].start()
        w_copy.start()
        for c in loads:
            c.start()

    @pl.when(step == relay)
    def _():
        pass_on(s, 1)

    @pl.when(step < n_fwd)
    def _():
        fwd_step(step, bq, bk, q_ref, kt_ref, v_ref, ot_ref, lse_ref, s_scr)

    def compute(slot, owner, part):
        do_ref[pl.ds(pl.multiple_of(owner * rows + part * half, half), half), :] = lax.dot_general(
            buf[slot], wo_scr[...], (((1,), (1,)), ((), ())), preferred_element_type=F32).astype(BF16)

    def run(two, slot0, load=True):
        if load:
            cps = [pltpu.make_async_copy(got(o, p), buf.at[slot0 + i], load_sem.at[slot0 + i]) for i, (o, p) in enumerate(two)]
            for c in cps:
                c.start()
            for c in cps:
                c.wait()
        (o0, p0), (o1, p1) = two

        def body(i, _):
            compute(slot0 + i, o0 + i * (o1 - o0), p0 + i * (p1 - p0))
            return 0

        lax.fori_loop(0, SLOTS, body, 0)

    groups = arrivals(me)
    for g in range(4):
        @pl.when(step == n_fwd + g)
        def _():
            if g == 0:
                for c in loads:
                    c.wait()
                for c in stores:
                    c.start()
                w_copy.wait()
            elif g > 1:
                pass_on(s, g)
            run(groups[g][:2], 0, g > 0)
            if g == 0:
                for c in stores:
                    c.wait()
            from_partner(s, g)
            run(groups[g][2:], 2)
            if g == 3:
                for c in s:
                    c.wait_send()


def gather_forward(q, kt, v, g, w_o, bq=PAIR, bk=1024):
    seq, width = q.shape
    rows, feat = g.shape
    heads = width // HEAD_DIM
    n = seq // bq
    at = lambda i: jnp.minimum(i, n - 1)
    return pl.pallas_call(
        functools.partial(gather_fwd_kernel, n, (3 * n) // 4, bq, bk), grid=(n + 4,),
        in_specs=[pl.BlockSpec((bq, width), lambda i: (at(i), 0)), pl.BlockSpec((HEAD_DIM, seq), whole, **ONCE),
                  pl.BlockSpec((seq, HEAD_DIM), whole, **ONCE), HBM, HBM],
        out_specs=[pl.BlockSpec((width, bq), lambda i: (0, at(i))), pl.BlockSpec((heads, bq, 1), lambda i: (0, at(i), 0)), HBM,
                   pl.BlockSpec((seq, width), whole)],
        out_shape=[array(width, seq), array(heads, seq, 1, dtype=F32), array(seq, feat),
                   array(seq, width)],
        scratch_shapes=[pltpu.VMEM((seq // bk, heads * bq, bk), F32), pltpu.VMEM((width, feat), BF16), pltpu.VMEM((4, rows // 2, feat), BF16),
                        SEM((N_COPIES,)), SEM((N_COPIES,)), SEM((1,)), SEM((4,)), SEM((SLOTS,))],
        compiler_params=remote_params(2),
        name="gather_fwd")(q, kt, v, g, w_o)


def bwd_step(qi, bq, bk, q_ref, do_ref, lse_ref, k_ref, kt_ref, vt_ref, cos_ref, sin_ref, g_out, dkt_ref, dvt_ref, p_scr, dp_scr):
    q = stack_heads(q_ref[...])
    do = stack_heads(do_ref[...])
    rows = q.shape[0]
    lse = lse_ref[...].reshape(rows, 1)
    q_t = q.T
    do_t = do.T
    nfull = (qi * bq) // bk

    @pl.when(qi == 0)
    def _():
        dkt_ref[...] = jnp.zeros_like(dkt_ref)
        dvt_ref[...] = jnp.zeros_like(dvt_ref)

    def prob_step(j, r, masked):
        sl = pl.ds(pl.multiple_of(j * bk, bk), bk)
        s = dot(q, kt_ref[:, sl]) * (SCALE * LOG2E)
        p = jnp.exp2(s - lse)
        if masked:
            p = jnp.where(causal((rows, bk), bq, qi * bq - nfull * bk), p, 0.0)
        dp = dot(do, vt_ref[:, sl])
        pd = p * dp
        for t in range(bk // LANE):
            r = r + pd[:, t * LANE:(t + 1) * LANE]
        p_scr[j] = p
        dp_scr[j] = dp
        dvt_ref[:, sl] += dot(do_t, p.astype(BF16))
        return r

    r = lax.fori_loop(0, nfull, lambda j, r: prob_step(j, r, False), jnp.zeros((rows, LANE), F32))
    r = prob_step(nfull, r, True)
    r = jnp.sum(r, axis=1, keepdims=True)

    def grad_step(j, dq):
        sl = pl.ds(pl.multiple_of(j * bk, bk), bk)
        ds = (p_scr[j] * (dp_scr[j] - r) * SCALE).astype(BF16)
        dkt_ref[:, sl] += dot(q_t, ds)
        return dq + dot(ds, k_ref[sl, :])

    dq = lax.fori_loop(0, nfull + 1, grad_step, jnp.zeros((rows, HEAD_DIM), F32))
    dq = dq.astype(BF16).astype(F32)
    here = pl.ds(pl.multiple_of(qi * bq, bq), bq)
    cos_t, sin_t = cos_ref[here, :], sin_ref[here, :]
    for n in range(rows // bq):
        g_out[:, n * HEAD_DIM:(n + 1) * HEAD_DIM] = rotate(dq[n * bq:(n + 1) * bq], cos_t, -sin_t).astype(BF16)


def gather_bwd_kernel(relay, bq, bk, q_ref, do_ref, lse_ref, k_ref, kt_ref, vt_ref, cos_ref, sin_ref, ot_ref,
                      ga_ref, gb_ref, otg_ref, otz_ref, p_scr, dp_scr, dkt_scr, dvt_scr, buf, g_buf, kv_buf, send, recv, z_send, z_recv, load_sem, store_sem, g_sem, kv_sem):
    step = pl.program_id(0)
    last = pl.num_programs(0) - 1
    me = lax.axis_index("sp")
    width, seq = ot_ref.shape
    half = width // 2
    tokens = otz_ref.shape[2]
    zn = flip(me, CORE)
    own = lambda part: ot_ref.at[pl.ds(part * half, half)]
    got = lambda owner, part: otg_ref.at[owner // 2, pl.ds(part * half, half)]
    s = exchange(send, recv, got, own, False)
    xn, yn = flip(me, X_BIT), flip(me, Y_BIT)
    dn = flip(xn, Y_BIT)
    mine = pl.ds(pl.multiple_of(zn * tokens, tokens), tokens)

    def to_other(n, owner):
        src = ot_ref.at[:, mine] if n == 0 else otg_ref.at[owner // 2, :, mine]
        return pltpu.make_async_remote_copy(src_ref=src, dst_ref=otz_ref.at[owner // 2], send_sem=z_send.at[n], recv_sem=z_recv.at[n],
                                            device_id={"sp": zn}, device_id_type=MESH)

    z = [to_other(n, o) for n, o in enumerate((me, xn, yn, dn))]
    n_buf, slab = buf.shape[0], buf.shape[1]
    n_slab = width // slab

    def slab_copies(n):
        rows = pl.ds(pl.multiple_of(n * slab, slab), slab)
        slot = n % n_buf
        return (pltpu.make_async_copy(ot_ref.at[rows], buf.at[slot], load_sem.at[slot]),
                pltpu.make_async_copy(buf.at[slot], otg_ref.at[me // 2, rows], store_sem.at[slot]))

    @pl.when(step == 0)
    def _():
        greet(neighbours())
        for n in range(4):
            s[n].start()
        z[0].start()

    @pl.when(step == relay)
    def _():
        pass_on(s, 1)

    @pl.when((step >= 2) & (step < n_slab + 2))
    def _():
        slab_copies(step - 2)[1].wait()

    @pl.when((step >= 1) & (step < n_slab + 1))
    def _():
        slab_copies(step - 1)[0].wait()
        slab_copies(step - 1)[1].start()

    @pl.when(step < n_slab)
    def _():
        slab_copies(step)[0].start()

    def out_copies(src, sems, i, n, at):
        slot = lax.rem(i, SLOTS)
        rows, w = pl.ds(pl.multiple_of(i * n, n), n), src.shape[SLOTS] // SLOTS
        return [pltpu.make_async_copy(src.at[slot, :, m * w:(m + 1) * w], ref.at[rows, at:at + w], sems.at[slot, m]) for m, ref in enumerate((ga_ref, gb_ref))]

    def out_wait(*args):
        for c in out_copies(*args):
            c.wait()

    @pl.when(step >= SLOTS)
    def _():
        out_wait(g_buf, g_sem, step - SLOTS, bq, 0)

    bwd_step(step, bq, bk, q_ref, do_ref, lse_ref, k_ref, kt_ref, vt_ref, cos_ref, sin_ref, g_buf.at[lax.rem(step, SLOTS)], dkt_scr, dvt_scr, p_scr, dp_scr)
    for c in out_copies(g_buf, g_sem, step, bq, 0):
        c.start()

    @pl.when(step == last)
    def _():
        for n, c in ((1, 2), (2, 3)):
            s[c].wait_recv()
            z[n].start()

        n_kv, n_blocks = kv_buf.shape[1], seq // kv_buf.shape[1]

        def kv_rows(i, _):
            @pl.when(i >= SLOTS)
            def _():
                out_wait(kv_buf, kv_sem, i - SLOTS, n_kv, PAIR)

            rows, slot = pl.ds(pl.multiple_of(i * n_kv, n_kv), n_kv), lax.rem(i, SLOTS)
            dk = dkt_scr[:, rows].T.astype(BF16).astype(F32)
            kv_buf[slot, :, :HEAD_DIM] = rotate(dk, cos_ref[rows, :], -sin_ref[rows, :]).astype(BF16)
            kv_buf[slot, :, HEAD_DIM:] = dvt_scr[:, rows].T.astype(BF16)
            for c in out_copies(kv_buf, kv_sem, i, n_kv, PAIR):
                c.start()
            return 0

        lax.fori_loop(0, n_blocks, kv_rows, 0)
        for n in reversed(range(SLOTS)):
            out_wait(kv_buf, kv_sem, n_blocks - 1 - n, n_kv, PAIR)
            out_wait(g_buf, g_sem, last - n, bq, 0)
        for c in (4, 5):
            s[c].wait_recv()
        z[3].start()
        for c in z:
            c.wait_recv()
        for c in s + z:
            c.wait_send()


def gather_backward(q, do, lse, k, kt, vt, cos_t, sin_t, ot, sp_size, bq=PAIR, bk=512):
    seq, width = q.shape
    heads = width // HEAD_DIM
    chips, tokens = sp_size // 2, seq // sp_size
    n = seq // bq
    tile = pl.BlockSpec((bq, width), row)
    tall = pl.BlockSpec((seq, HEAD_DIM), whole, **ONCE)
    wide = pl.BlockSpec((HEAD_DIM, seq), whole, **ONCE)
    piece = array(seq, 3 * HEAD_DIM)
    return pl.pallas_call(
        functools.partial(gather_bwd_kernel, (9 * n) // 16, bq, bk), grid=(n,),
        in_specs=[tile, tile, pl.BlockSpec((heads, bq, 1), lambda i: (0, i, 0)), tall, wide, wide, tall, tall, HBM],
        out_specs=[HBM] * 4,
        out_shape=[piece, piece, array(chips, width, seq), array(chips, width, tokens)],
        scratch_shapes=[pltpu.VMEM((seq // bk, heads * bq, bk), F32), pltpu.VMEM((seq // bk, heads * bq, bk), F32),
                        pltpu.VMEM((HEAD_DIM, seq), F32), pltpu.VMEM((HEAD_DIM, seq), F32), pltpu.VMEM((SLOTS, width // 8, seq), BF16), pltpu.VMEM((SLOTS, bq, width), BF16),
                        pltpu.VMEM((SLOTS, 512, PAIR), BF16),
                        SEM((6,)), SEM((6,)), SEM((4,)), SEM((4,)), SEM((SLOTS,)), SEM((SLOTS,)), SEM((SLOTS, SLOTS)), SEM((SLOTS, SLOTS))],
        compiler_params=remote_params(3),
        name="gather_bwd")(q, do, lse, k, kt, vt, cos_t, sin_t, ot)


def dw_o_kernel(core_ref, ot_ref, g_ref, final_ref, send_ref):
    y = dot(ot_ref[...], g_ref[...]).astype(BF16)
    final_ref[...] = y
    send_ref[...] = y


def dw_o_half(core, ot_all, g_all, bn=1024):
    half, width, seq = ot_all.shape
    feat = g_all.shape[1]
    return pl.pallas_call(
        dw_o_kernel,
        grid_spec=pltpu.PrefetchScalarGridSpec(
            num_scalar_prefetch=1, grid=(feat // bn, half),
            in_specs=[pl.BlockSpec((None, width, seq), lambda j, s, c: (s, 0, 0)), pl.BlockSpec((seq, bn), col)],
            out_specs=[pl.BlockSpec((width, bn), lambda j, s, c: (2 * s + c[0], j)), pl.BlockSpec((width, bn), lambda j, s, c: (s, j))]),
        out_shape=[array(2 * half * width, feat), array(half * width, feat)],
        compiler_params=PARAMS, cost_estimate=cost(2 * half * width * feat * seq), name="dw_o_half")(core, ot_all, g_all)


def out_kernel(ids_ref, mine_ref, other_ref, w_ref, out_ref, o_scr):
    @pl.when(pl.program_id(0) == 0)
    def _():
        core = lax.rem(ids_ref[0], 2)
        width = mine_ref.shape[1]
        for s in range(mine_ref.shape[0]):
            for ref, d in ((mine_ref, 2 * s + core), (other_ref, 2 * s + 1 - core)):
                o_scr[:, pl.ds(pl.multiple_of(d * width, width), width)] = ref[s].T

    out_ref[...] = dot(o_scr[...], w_ref[...]).astype(BF16)


def out_proj(ids, ot_all, ot_other, w_o, bn=512):
    chips, width, tokens = ot_other.shape
    feat = w_o.shape[1]
    return pl.pallas_call(
        out_kernel,
        grid_spec=pltpu.PrefetchScalarGridSpec(
            num_scalar_prefetch=1, grid=(feat // bn,),
            in_specs=[pl.BlockSpec((chips, width, tokens), lambda i, c: (0, 0, c[0]), **ONCE), pl.BlockSpec((chips, width, tokens), lambda i, c: (0, 0, 0), **ONCE),
                      pl.BlockSpec((w_o.shape[0], bn), col)],
            out_specs=pl.BlockSpec((tokens, bn), col),
            scratch_shapes=[pltpu.VMEM((tokens, w_o.shape[0]), BF16)]),
        out_shape=array(tokens, feat), compiler_params=PARAMS, cost_estimate=cost(2 * tokens * w_o.size), name="out_proj")(ids, ot_all, ot_other, w_o)


def dev_stores(buf, slot, rows, dev, finals, sem):
    copies = []
    start = 0
    for n, ref in enumerate(finals):
        w = (buf.shape[2] - PAIR) if n == 0 else HEAD_DIM
        copies.append(pltpu.make_async_copy(buf.at[slot, :, start:start + w], ref.at[rows, pl.ds(pl.multiple_of(dev * w, w), w)], sem.at[slot, n]))
        start += w
    return copies


class Ride:
    def __init__(self, kind, ids_ref, recv, buf, finals, load_sem, store_sem):
        self.kind, self.ids, self.recv, self.buf, self.finals, self.load_sem, self.store_sem = kind, ids_ref, recv, buf, finals, load_sem, store_sem

    def load(self, i):
        n = self.buf.shape[1]
        slot = lax.rem(i, SLOTS)
        return pltpu.make_async_copy(self.recv.at[pl.ds(pl.multiple_of(i * n, n), n)], self.buf.at[slot], self.load_sem.at[slot])

    def stores(self, i):
        n = self.buf.shape[1]
        slot = lax.rem(i, SLOTS)
        if self.kind == "dev":
            return dev_stores(self.buf, slot, pl.ds(pl.multiple_of(i * n, n), n), self.ids[1], self.finals, self.store_sem)
        per = (HEAD_DIM * 4) // n
        block = (2 * lax.div(i, per) + 1 - lax.rem(self.ids[2], 2)) * per + lax.rem(i, per)
        return [pltpu.make_async_copy(self.buf.at[slot], self.finals[0].at[pl.ds(pl.multiple_of(block * n, n), n)], self.store_sem.at[slot, 0])]

    def begin(self, i):
        @pl.when(i >= SLOTS)
        def _():
            for c in self.stores(i - SLOTS):
                c.wait()

        self.load(i).start()

    def end(self, i, last):
        self.load(i).wait()
        for c in self.stores(i):
            c.start()

        @pl.when(i == last)
        def _():
            for n in reversed(range(SLOTS)):
                for c in self.stores(i - n):
                    c.wait()


def dw_kernel(kinds, n_alias, ids_ref, ht_ref, a_ref, b_ref, *refs):
    n = len(kinds)
    recvs = refs[:n]
    refs = refs[n + n_alias:]
    finals, refs = refs[:3], refs[3:]
    o_final, refs = (refs[:1], refs[1:]) if "o" in kinds else ((), refs)
    send_ref, x_scr, y_scr, y_sem, x_sem = refs[:5]
    extra = refs[5:]
    rides = [Ride(k, ids_ref, recvs[m], extra[3 * m], finals if k == "dev" else o_final, extra[3 * m + 1], extra[3 * m + 2]) for m, k in enumerate(kinds)]
    i, last = grid_place()
    bm, feat = ht_ref.shape[0], finals[0].shape[0]
    two = PAIR
    n_tok = send_ref.shape[0] - feat
    tokens = pltpu.make_async_copy(x_scr.at[pl.ds(pl.multiple_of(flip(ids_ref[2], CORE) * n_tok, n_tok), n_tok)], send_ref.at[pl.ds(feat, n_tok)], x_sem.at[0])

    @pl.when(i == 0)
    def _():
        for ref, at, to in ((a_ref, 0, 2 * two), (b_ref, two, 2 * two + HEAD_DIM)):
            x_scr[:, at:at + two] = ref[:, :two]
            x_scr[:, to:to + HEAD_DIM] = ref[:, two:]
        tokens.start()

    def stores(step):
        slot, rows = lax.rem(step, SLOTS), pl.ds(pl.multiple_of(step * bm, bm), bm)
        whole_rows = pltpu.make_async_copy(y_scr.at[slot], send_ref.at[rows], y_sem.at[slot, len(finals)])
        return dev_stores(y_scr, slot, rows, ids_ref[0], finals, y_sem) + [whole_rows]

    for r in rides:
        r.begin(i)

    @pl.when(i >= SLOTS)
    def _():
        for c in stores(i - SLOTS):
            c.wait()

    y = dot(ht_ref[...], x_scr[...]).astype(BF16)
    y_scr[lax.rem(i, SLOTS)] = y
    for c in stores(i):
        c.start()
    for r in rides:
        r.end(i, last)

    @pl.when(i == last)
    def _():
        tokens.wait()
        for n in reversed(range(SLOTS)):
            for c in stores(i - n):
                c.wait()


def ride_scratch(kinds, steps, feat, w):
    out = []
    for k in kinds:
        block = (feat // steps, w) if k == "dev" else (feat // (2 * steps), feat)
        out += [pltpu.VMEM((2,) + block, BF16), SEM((SLOTS,)), SEM((SLOTS, 3 if k == "dev" else 1))]
    return out


def dw_device(ids, ht, a, b, finals, rides, tokens, o_final=None, bm=512):
    feat, seq = ht.shape
    w = a.shape[1] + b.shape[1]
    kinds = [k for k, _ in rides]
    finals = list(finals) + ([o_final] if "o" in kinds else [])
    old = [f for f in finals if isinstance(f, jax.Array)]
    ins = [ht, a, b] + [r for _, r in rides] + old
    n_final, n_alias = len(finals), len(old)
    first = len(ins) - n_alias
    return pl.pallas_call(
        functools.partial(dw_kernel, kinds, n_alias),
        grid_spec=pltpu.PrefetchScalarGridSpec(
            num_scalar_prefetch=1, grid=(feat // bm,),
            in_specs=[pl.BlockSpec((bm, seq), row)] + [pl.BlockSpec(x.shape, whole, **ONCE) for x in (a, b)] + [HBM] * (len(ins) - 3),
            out_specs=[HBM] * (n_final + 1),
            scratch_shapes=[pltpu.VMEM((seq, w), BF16), pltpu.VMEM((SLOTS, bm, w), BF16), SEM((SLOTS, 4)), SEM((1,))] + ride_scratch(kinds, feat // bm, feat, w)),
        out_shape=[array(*f.shape) for f in finals] + [array(feat + tokens, w)],
        input_output_aliases={1 + first + n: n for n in range(n_alias)},
        compiler_params=PARAMS, cost_estimate=cost(2 * seq * feat * w), name="dw_device")(ids, *ins)


def dh_kernel(n_dev, ids_ref, wq_ref, wk_ref, wv_ref, *refs):
    own, other, refs = refs[:n_dev], refs[n_dev:n_dev + n_dev // 2], refs[n_dev + n_dev // 2:]
    recvs, refs = refs[:2], refs[2 + 3:]
    out_ref, finals, x_scr, refs = refs[0], refs[1:4], refs[4], refs[5:]
    i, last = grid_place()
    rides = [Ride("dev", (None, ids_ref[1 + n]), recvs[n], *refs[:1], finals, *refs[1:3]) if n == 0 else
             Ride("dev", (None, ids_ref[1 + n]), recvs[n], *refs[3:4], finals, *refs[4:]) for n in range(SLOTS)]
    for r in rides:
        r.begin(i)
    two = PAIR
    nq, nk = wq_ref.shape[1], wk_ref.shape[1]

    @pl.when(i == 0)
    def _():
        def place(t, dev, part):
            n = t.shape[0] - HEAD_DIM
            x_scr[pl.ds(pl.multiple_of(dev * 2 * two + part * two, two), n), :] = t[:n]
            x_scr[pl.ds(pl.multiple_of(nq + part * nk + dev * HEAD_DIM, HEAD_DIM), HEAD_DIM), :] = t[n:]

        for n in range(n_dev):
            place(own[n][...].T, ids_ref[3 + n // 2], n % 2)
        for n in range(n_dev // 2):
            t = other[n][...].T
            dev = ids_ref[3 + n_dev // 2 + n]
            place(t[:-HEAD_DIM], dev, 0)
            x_scr[pl.ds(pl.multiple_of(nq + nk + dev * HEAD_DIM, HEAD_DIM), HEAD_DIM), :] = t[-HEAD_DIM:]

    y = dot(wq_ref[...], x_scr[:nq, :]) + dot(wk_ref[...], x_scr[nq:nq + nk, :]) + dot(wv_ref[...], x_scr[nq + nk:, :])
    out_ref[...] = y.T
    for r in rides:
        r.end(i, last)


def dh_proj(ids, w_q, w_k, w_v, own, other, rides, finals, tokens, bf=512):
    feat = w_q.shape[0]
    w = other[0].shape[1]
    n = len(own)
    ins = [w_q, w_k, w_v, *own, *other, *rides, *finals]
    specs = [pl.BlockSpec((bf, x.shape[1]), row) for x in (w_q, w_k, w_v)]
    specs += [pl.BlockSpec((tokens, x.shape[1]), lambda i, c: (c[0], 0), **ONCE) for x in own]
    specs += [pl.BlockSpec((tokens, w), lambda i, c: (feat // tokens, 0), **ONCE) for _ in other]
    first = len(ins) - len(finals)
    return pl.pallas_call(
        functools.partial(dh_kernel, n),
        grid_spec=pltpu.PrefetchScalarGridSpec(
            num_scalar_prefetch=1, grid=(feat // bf,), in_specs=specs + [HBM] * (len(ins) - len(specs)),
            out_specs=[pl.BlockSpec((tokens, bf), col)] + [HBM] * len(finals),
            scratch_shapes=[pltpu.VMEM((w_q.shape[1] + 2 * w_k.shape[1], tokens), BF16)] + ride_scratch(["dev"] * len(rides), feat // bf, feat, w)),
        out_shape=[array(tokens, feat, dtype=F32)] + [array(*f.shape) for f in finals],
        input_output_aliases={1 + first + m: 1 + m for m in range(len(finals))},
        compiler_params=PARAMS, cost_estimate=cost(2 * tokens * (w_q.size + 2 * w_k.size)), name="dh_proj")(ids, *ins)


def sum_kernel(x_ref, out_ref, all_scr, send, recv):
    me = lax.axis_index("sp")
    peers = everyone()
    greet(peers)
    copies = [pltpu.make_async_remote_copy(src_ref=x_ref, dst_ref=all_scr.at[me], send_sem=send.at[n], recv_sem=recv.at[n],
                                           device_id={"sp": p}, device_id_type=MESH) for n, p in enumerate(peers)]
    for c in copies:
        c.start()
    all_scr[me] = x_ref[...]
    for c in copies:
        c.wait_recv()
    total = all_scr[0]
    for n in range(1, all_scr.shape[0]):
        total = total + all_scr[n]
    out_ref[...] = total.astype(BF16)
    for c in copies:
        c.wait_send()


def sum_devices(x, sp_size):
    n = x.shape[0] // HEAD_DIM
    vmem = pl.BlockSpec(memory_space=pltpu.VMEM)
    return pl.pallas_call(
        sum_kernel, in_specs=[vmem], out_specs=vmem, out_shape=array(n, HEAD_DIM),
        scratch_shapes=[pltpu.VMEM((sp_size, n, HEAD_DIM), F32), SEM((sp_size - 1,)), SEM((sp_size - 1,))],
        compiler_params=remote_params(4), name="sum_devices")(x.reshape(n, HEAD_DIM)).reshape(-1)


def solution(mesh):
    sp_size = mesh.shape['sp']
    row_spec = P(('dp', 'sp'), None)
    pos_spec = P(('dp', 'sp'))
    full_spec = P(None, None)
    grad_spec = P('dp', None)

    def local_step(hidden, positions, d_attn, ln_weight, w_q, w_k, w_v, w_o):
        dev = lax.axis_index('sp')
        core = lax.rem(dev, SLOTS)
        local_rows, _ = hidden.shape
        normed32, norm_vjp = jax.vjp(norm_f32, hidden.astype(F32), ln_weight.astype(F32))
        normed = normed32.astype(BF16)
        _, ht, q, k, kt, v, vt, cos_t, sin_t = gather_qkv(normed, positions, w_q, w_k, w_v, sp_size)
        ot, lse, g_all, do = gather_forward(q, kt, v, d_attn, w_o)
        ga, gb, ot_all, ot_other = gather_backward(q, do, lse, k, kt, vt, cos_t, sin_t, ot, sp_size)
        core1 = core.reshape(1)
        other = lambda d: flip(d, CORE)
        dev_x, dev_y = flip(dev, X_BIT), flip(dev, Y_BIT)
        dev_d = flip(dev_x, Y_BIT)

        def to(x, bit):
            return lax.ppermute(x, 'sp', [(i, i ^ bit) for i in range(sp_size)])

        after = lambda x, *done: lax.optimization_barrier((x,) + done)[0]
        ids = lambda *d: jnp.stack(d)
        ga_x, gb_y, gb_x, ga_y = to(ga, X_BIT), to(gb, Y_BIT), to(gb, X_BIT), to(ga, Y_BIT)
        dw_o, o_send = dw_o_half(core1, ot_all, g_all)
        o_recv = to(o_send, CORE)
        attn_out = out_proj(dev.reshape(1), ot_all, ot_other, w_o)
        blank = [array(*w.shape) for w in (w_q, w_k, w_v)]
        *finals, send0 = dw_device(ids(dev, dev, dev), ht, after(ga, attn_out, o_send), gb, blank, [], local_rows)
        recv0 = to(send0, CORE)
        ga_d, gb_d = to(after(ga_x, send0), Y_BIT), to(after(gb_y, send0), X_BIT)
        *finals, dw_o, send1 = dw_device(ids(dev_x, dev, dev), ht, ga_x, gb_x, finals, [('o', o_recv)], local_rows, dw_o)
        recv1 = to(send1, CORE)
        *finals, send2 = dw_device(ids(dev_y, other(dev), dev), ht, ga_y, gb_y, finals, [('dev', recv0)], local_rows)
        recv2 = to(send2, CORE)
        *finals, send3 = dw_device(ids(dev_d, other(dev_x), dev), ht, ga_d, gb_d, finals, [('dev', recv1)], local_rows)
        recv3 = to(send3, CORE)
        owners = [dev, dev_x, dev_y, dev_d]
        d_normed, dw_q, dw_k, dw_v = dh_proj(ids(dev, other(dev_y), other(dev_d), *owners, *map(other, owners)), w_q, w_k, w_v,
                                             [ga, gb, ga_x, gb_x, ga_y, gb_y, ga_d, gb_d], [recv0, recv1, recv2, recv3], [recv2, recv3], finals, local_rows)
        d_hid, d_lnw = norm_vjp(d_normed)
        d_lnw = sum_devices(d_lnw, sp_size)
        return (attn_out, d_hid.astype(BF16), d_lnw, dw_q, dw_k, dw_v, dw_o)

    return jax.shard_map(local_step, mesh=mesh,
                      in_specs=(row_spec, pos_spec, row_spec, P(None), full_spec, full_spec, full_spec, full_spec),
                      out_specs=(row_spec, row_spec, P('dp'), grad_spec, grad_spec, grad_spec, grad_spec),
                      check_vma=False)
```

```python
import functools
import jax
import jax.numpy as jnp
from jax import lax
from jax.experimental import pallas as pl
from jax.experimental.pallas import tpu as pltpu
from jax.sharding import PartitionSpec as P

HEAD_DIM = LANE = 128
PAIR = 2 * HEAD_DIM
CORE, X_BIT, Y_BIT = 1, 2, 4
LOW, HIGH, SLOTS = 0, 1, 2
CHUNKS, N_PEERS = 2, 7
LN_EPS = 1e-5
ROPE_BASE = 10000.0
SCALE = HEAD_DIM ** -0.5
LOG2E = 1.4426950408889634
VMEM_LIMIT = 67_000_000
BF16 = jnp.bfloat16
F32 = jnp.float32
MESH = pl.DeviceIdType.MESH
HBM = pl.BlockSpec(memory_space=pl.ANY)
SEM = pltpu.SemaphoreType.DMA
row = lambda i, *_: (i, 0)
col = lambda i, *_: (0, i)
whole = lambda *_: (0, 0)
ONCE = dict(pipeline_mode=pl.Buffered(1))
PARAMS = pltpu.CompilerParams(vmem_limit_bytes=VMEM_LIMIT)


def grid_place():
    return pl.program_id(0), pl.num_programs(0) - 1


def dot(x, y):
    return jnp.dot(x, y, preferred_element_type=F32)


def array(*shape, dtype=BF16):
    return jax.ShapeDtypeStruct(shape, dtype)


def remote_params(number):
    return pltpu.CompilerParams(collective_id=number, has_side_effects=True, vmem_limit_bytes=VMEM_LIMIT)


def cost(flops):
    return pl.CostEstimate(flops=flops, bytes_accessed=flops // HEAD_DIM, transcendentals=0)


def norm_f32(hid_f32, weight_f32):
    mean_val = jnp.mean(hid_f32, axis=-1, keepdims=True)
    centered = hid_f32 - mean_val
    var_val = jnp.mean(centered * centered, axis=-1, keepdims=True)
    return centered * lax.rsqrt(var_val + LN_EPS) * weight_f32


def rotate(x, cos_t, sin_t):
    lane = lax.broadcasted_iota(jnp.int32, x.shape, 1)
    swapped = jnp.where(lane % 2 == 0, pltpu.roll(x, HEAD_DIM - 1, 1), pltpu.roll(x, 1, 1))
    return x * cos_t + swapped * sin_t


def flip(i, bit):
    return i + bit - 2 * bit * ((i // bit) % 2)


class Exchange:
    def __init__(self, send, recv, block, own, chunks, partner):
        me = lax.axis_index("sp")
        xn, yn, zn = flip(me, X_BIT), flip(me, Y_BIT), flip(me, CORE)
        dn = flip(xn, Y_BIT)
        self.every = []

        def copy(owner, part, to, chunk=None):
            n = len(self.every)
            src = own(part) if owner is me else block(owner, part, chunk)
            self.every.append(pltpu.make_async_remote_copy(src_ref=src, dst_ref=block(owner, part, chunk), send_sem=send.at[n], recv_sem=recv.at[n],
                                                           device_id={"sp": to}, device_id_type=MESH))
            return self.every[-1]

        self.first = [copy(me, LOW, xn), copy(me, HIGH, yn)]
        self.second = [copy(me, HIGH, xn), copy(me, LOW, yn)]
        self.relay = [[copy(xn, LOW, yn, c), copy(yn, HIGH, xn, c)] for c in range(chunks)]
        if partner:
            self.to_own = [copy(me, LOW, zn), copy(me, HIGH, zn)]
            self.to_near = [[copy(xn, LOW, zn), copy(yn, HIGH, zn)], [copy(xn, HIGH, zn), copy(yn, LOW, zn)]]
            self.to_far = [[copy(dn, LOW, zn, c), copy(dn, HIGH, zn, c)] for c in range(chunks)]

    def begin(self):
        start_all(self.first)
        if hasattr(self, "to_own"):
            start_all(self.to_own)
        start_all(self.second)

    def near(self, n):
        for m, c in enumerate(self.second if n else self.first):
            c.wait_recv()
            if n == 0:
                start_all([r[m] for r in self.relay])
            if hasattr(self, "to_near"):
                self.to_near[n][m].start()

    def far(self, n):
        for m, c in enumerate(self.relay[n]):
            c.wait_recv()
            if hasattr(self, "to_far"):
                self.to_far[n][m].start()

    def finish(self):
        for c in self.every:
            c.wait_send()


def start_all(copies):
    for c in copies:
        c.start()


def wait_all(copies):
    for c in copies:
        c.wait()


def receive(copies):
    for c in copies:
        c.wait_recv()


def n_copies(chunks, partner):
    return 4 + 2 * chunks + (6 + 2 * chunks if partner else 0)


def greet(peers):
    barrier = pltpu.get_barrier_semaphore()
    for p in peers:
        pl.semaphore_signal(barrier, inc=1, device_id={"sp": p}, device_id_type=MESH)
    pl.semaphore_wait(barrier, len(peers))


def neighbours():
    me = lax.axis_index("sp")
    return [flip(me, CORE), flip(me, X_BIT), flip(me, Y_BIT)]


def everyone():
    me = lax.axis_index("sp")
    xn, yn = flip(me, X_BIT), flip(me, Y_BIT)
    dn = flip(xn, Y_BIT)
    return [flip(me, CORE), xn, flip(xn, CORE), yn, flip(yn, CORE), dn, flip(dn, CORE)]


def arrivals(me):
    xn, yn, zn = flip(me, X_BIT), flip(me, Y_BIT), flip(me, CORE)
    dn = flip(xn, Y_BIT)
    zx, zy, zd = flip(xn, CORE), flip(yn, CORE), flip(dn, CORE)
    return [[(me, LOW), (me, HIGH), (zn, LOW), (zn, HIGH)], [(xn, LOW), (yn, HIGH), (zx, LOW), (zy, HIGH)], [(xn, HIGH), (yn, LOW), (zx, HIGH), (zy, LOW)],
            [(dn, LOW), (dn, HIGH), (zd, LOW), (zd, HIGH)]]


def gather_qkv_kernel(x_ref, lnw_ref, pos_ref, freq_ref, wq_ref, wk_ref, wv_ref,
                      hall_ref, ht_ref, q_out, k_out, kt_out, v_out, vt_out, cos_out, sin_out,
                      q_ref, k_ref, kt_ref, v_ref, vt_ref, cos_ref, sin_ref, w_scr, buf, tbuf, pos_all,
                      pos_send, pos_recv, send, recv, w_sem, load_sem, store_sem, t_sem, out_sem):
    me = lax.axis_index("sp")
    rows = x_ref.shape[0]
    half = rows // 2
    chunk = half // CHUNKS
    width = q_ref.shape[1]

    def block(owner, part, c):
        start = owner * rows + part * half
        return hall_ref.at[pl.ds(pl.multiple_of(start, half), half) if c is None else pl.ds(pl.multiple_of(start + c * chunk, chunk), chunk)]

    own = lambda part: block(me, part, None)
    loads = [pltpu.make_async_copy(x_ref.at[pl.ds(p * half, half)], buf.at[p], load_sem.at[p]) for p in range(SLOTS)]
    start_all(loads)
    column = lambda n: pl.ds(pl.multiple_of(me * n, n), n)
    w_copies = [pltpu.make_async_copy(wq_ref.at[:, column(width)], w_scr.at[:, pl.ds(0, width)], w_sem.at[0]),
                pltpu.make_async_copy(wk_ref.at[:, column(HEAD_DIM)], w_scr.at[:, pl.ds(width, HEAD_DIM)], w_sem.at[1]),
                pltpu.make_async_copy(wv_ref.at[:, column(HEAD_DIM)], w_scr.at[:, pl.ds(width + HEAD_DIM, HEAD_DIM)], w_sem.at[2])]
    start_all(w_copies)
    peers = everyone()
    greet(peers)
    pos_copies = [pltpu.make_async_remote_copy(src_ref=pos_ref, dst_ref=pos_all.at[me], send_sem=pos_send.at[i], recv_sem=pos_recv.at[i],
                                               device_id={"sp": p}, device_id_type=MESH) for i, p in enumerate(peers)]
    start_all(pos_copies)
    pos_all[me] = pos_ref[...]
    links = Exchange(send, recv, block, own, CHUNKS, True)
    stores = [pltpu.make_async_copy(buf.at[p], own(p), store_sem.at[p]) for p in range(SLOTS)]
    slab = half // 8
    for p in range(SLOTS):
        loads[p].wait()

        def norm(n, _):
            here = pl.ds(pl.multiple_of(n * slab, slab), slab)
            buf[p, here, :] = norm_f32(buf[p, here, :].astype(F32), lnw_ref[...]).astype(BF16)
            return 0

        lax.fori_loop(0, half // slab, norm, 0)
        stores[p].start()
    for p in range(SLOTS):
        stores[p].wait()
        links.first[p].start()
    start_all(links.second + links.to_own)
    receive(pos_copies)

    def t_copy(tslot, r0, n):
        return pltpu.make_async_copy(tbuf.at[tslot, :, pl.ds(0, n)], ht_ref.at[:, pl.ds(r0, n)], t_sem.at[tslot])

    def compute(slot, r0, n, first):
        r0 = pl.multiple_of(r0, n)
        out = pl.ds(r0, n)
        for t in range(n // LANE):
            at = r0 + t * LANE
            p = pos_all[at // rows, pl.ds((at % rows) // LANE, 1), :]
            angle = jnp.broadcast_to(p, (LANE, LANE)).T * freq_ref[...]
            sign = jnp.where(lax.broadcasted_iota(jnp.int32, (LANE, LANE), 1) % 2 == 0, -1.0, 1.0)
            tr = pl.ds(pl.multiple_of(at, LANE), LANE)
            cos_ref[tr, :] = jnp.cos(angle)
            sin_ref[tr, :] = jnp.sin(angle) * sign
        cos_t, sin_t = cos_ref[out, :], sin_ref[out, :]
        h = buf[slot, :n]
        tslot = slot % 2
        if not first:
            t_copy(tslot, 0, n).wait()
        tbuf[tslot, :, :n] = h.T
        t_copy(tslot, r0, n).start()
        for m in range(width // PAIR):
            y = dot(h, w_scr[:, m * PAIR:(m + 1) * PAIR])
            for e in range(SLOTS):
                q_ref[out, m * PAIR + e * LANE: m * PAIR + (e + 1) * LANE] = rotate(y[:, e * LANE:(e + 1) * LANE], cos_t, sin_t).astype(BF16)
        y = dot(h, w_scr[:, width:width + PAIR])
        k, v = rotate(y[:, :LANE], cos_t, sin_t), y[:, LANE:]
        k_ref[out, :] = k.astype(BF16)
        kt_ref[:, out] = k.T.astype(BF16)
        v_ref[out, :] = v.astype(BF16)
        vt_ref[:, out] = v.T.astype(BF16)
        for m, (src, dst) in enumerate(results):
            at = (slice(None), out) if src.shape[0] == HEAD_DIM else (out,)
            pltpu.make_async_copy(src.at[at], dst.at[at], out_sem.at[m]).start()

    results = list(zip((q_ref, k_ref, kt_ref, v_ref, vt_ref, cos_ref, sin_ref), (q_out, k_out, kt_out, v_out, vt_out, cos_out, sin_out)))

    def run(two, slot0, c=None, first=False, load=True):
        n = half if c is None else chunk
        if load:
            cps = [pltpu.make_async_copy(block(o, p, c), buf.at[slot0 + i, pl.ds(0, n)], load_sem.at[slot0 + i]) for i, (o, p) in enumerate(two)]
            start_all(cps)
            wait_all(cps)
        starts = [o * rows + p * half + (0 if c is None else c * chunk) for o, p in two]

        def body(i, _):
            compute(slot0 + i, starts[0] + i * (starts[1] - starts[0]), n, first)
            return 0

        lax.fori_loop(0, SLOTS, body, 0)

    groups = arrivals(me)
    wait_all(w_copies)
    run(groups[0][:2], 0, first=True, load=False)
    receive(links.to_own)
    run(groups[0][2:], 2)
    for g in range(SLOTS):
        links.near(g)
        run(groups[g + 1][:2], 0)
        receive(links.to_near[g])
        run(groups[g + 1][2:], 2)
    wait_all([t_copy(i, 0, half) for i in range(SLOTS)])
    for c in range(CHUNKS):
        links.far(c)
        run(groups[3][:2], 0, c, first=c == 0)
        receive(links.to_far[c])
        run(groups[3][2:], 2, c)
    wait_all([t_copy(i, 0, chunk) for i in range(SLOTS)])
    for m, (src, dst) in enumerate(results):
        pltpu.make_async_copy(src, dst, out_sem.at[m]).wait()
    links.finish()
    for c in pos_copies:
        c.wait_send()


def gather_qkv(x, ln_weight, pos, w_q, w_k, w_v, sp_size):
    rows, feat = x.shape
    seq = rows * sp_size
    width = w_q.shape[1] // sp_size
    inv_freq = ROPE_BASE ** (-jnp.arange(0, HEAD_DIM, 2, dtype=F32) / HEAD_DIM)
    freq = jnp.repeat(inv_freq, 2)[None, :]
    vmem = pl.BlockSpec(memory_space=pltpu.VMEM)
    made = [array(seq, width), array(seq, HEAD_DIM), array(HEAD_DIM, seq), array(seq, HEAD_DIM), array(HEAD_DIM, seq)]
    made += [array(seq, HEAD_DIM, dtype=F32)] * 2
    n = n_copies(CHUNKS, True)
    return pl.pallas_call(
        gather_qkv_kernel,
        in_specs=[HBM, vmem, vmem, vmem, HBM, HBM, HBM],
        out_specs=[HBM] * (2 + len(made)),
        out_shape=[array(seq, feat), array(feat, seq)] + made,
        scratch_shapes=[pltpu.VMEM(m.shape, m.dtype) for m in made] + [
            pltpu.VMEM((feat, width + PAIR), BF16), pltpu.VMEM((4, rows // 2, feat), BF16), pltpu.VMEM((SLOTS, feat, rows // 2), BF16),
            pltpu.VMEM((sp_size, rows // LANE, LANE), F32), SEM((N_PEERS,)), SEM((N_PEERS,)), SEM((n,)), SEM((n,)), SEM((3,)), SEM((4,)), SEM((SLOTS,)),
            SEM((SLOTS,)), SEM((len(made),))],
        compiler_params=remote_params(1),
        name="gather_qkv")(x, ln_weight.astype(F32)[None], pos.astype(F32).reshape(rows // LANE, LANE), freq, w_q, w_k, w_v)


def stack_heads(x):
    return jnp.concatenate([x[:, n * HEAD_DIM:(n + 1) * HEAD_DIM] for n in range(x.shape[1] // HEAD_DIM)], axis=0)


def causal(shape, bq, offset):
    rows = lax.rem(lax.broadcasted_iota(jnp.int32, shape, 0), bq) + offset
    return rows >= lax.broadcasted_iota(jnp.int32, shape, 1)


def fwd_step(qi, bq, bk, q_ref, kt_ref, v_ref, ot_ref, lse_ref, s_scr):
    q = stack_heads(q_ref[...])
    rows = q.shape[0]
    nfull = (qi * bq) // bk

    def scores(j):
        return dot(q, kt_ref[:, pl.ds(pl.multiple_of(j * bk, bk), bk)]) * (SCALE * LOG2E)

    def lane_max(m, s):
        for c in range(bk // LANE):
            m = jnp.maximum(m, s[:, c * LANE:(c + 1) * LANE])
        return m

    def score_step(j, m):
        s = scores(j)
        s_scr[j] = s
        return lane_max(m, s)

    m = lax.fori_loop(0, nfull, score_step, jnp.full((rows, LANE), -jnp.inf, F32))
    s = jnp.where(causal((rows, bk), bq, qi * bq - nfull * bk), scores(nfull), -jnp.inf)
    s_scr[nfull] = s
    m = jnp.max(lane_max(m, s), axis=1, keepdims=True)

    def value_step(j, carry):
        l, o = carry
        p = jnp.exp2(s_scr[j] - m)
        for t in range(bk // LANE):
            l = l + p[:, t * LANE:(t + 1) * LANE]
        o = o + dot(p.astype(BF16), v_ref[pl.ds(pl.multiple_of(j * bk, bk), bk), :])
        return l, o

    l, o = lax.fori_loop(0, nfull + 1, value_step, (jnp.zeros((rows, LANE), F32), jnp.zeros((rows, HEAD_DIM), F32)))
    l = jnp.sum(l, axis=1, keepdims=True)
    o = (o / l).astype(BF16)
    for n in range(rows // bq):
        ot_ref[n * HEAD_DIM:(n + 1) * HEAD_DIM, :] = o[n * bq:(n + 1) * bq].T
    lse_ref[...] = (m + jnp.log2(l)).reshape(lse_ref.shape)


def gather_fwd_kernel(n_fwd, relay, bq, bk, q_ref, kt_ref, v_ref, g_ref, wo_ref, ot_ref, lse_ref, gall_ref, do_ref,
                      s_scr, wo_scr, buf, send, recv, w_sem, load_sem, store_sem):
    step = pl.program_id(0)
    me = lax.axis_index("sp")
    rows, width = g_ref.shape[0], do_ref.shape[1]
    half = rows // 2
    chunk = half // CHUNKS

    def block(owner, part, c):
        start = owner * rows + part * half
        return gall_ref.at[pl.ds(pl.multiple_of(start, half), half) if c is None else pl.ds(pl.multiple_of(start + c * chunk, chunk), chunk)]

    own = lambda part: g_ref.at[pl.ds(part * half, half)]
    links = Exchange(send, recv, block, own, CHUNKS, True)
    w_copy = pltpu.make_async_copy(wo_ref.at[pl.ds(pl.multiple_of(me * width, width), width)], wo_scr, w_sem.at[0])
    loads = [pltpu.make_async_copy(own(i), buf.at[i], load_sem.at[i]) for i in range(SLOTS)]
    stores = [pltpu.make_async_copy(buf.at[i], block(me, i, None), store_sem.at[i]) for i in range(SLOTS)]

    @pl.when(step == 0)
    def _():
        greet(neighbours())
        links.begin()
        w_copy.start()
        start_all(loads)

    @pl.when(step == relay)
    def _():
        links.near(0)

    @pl.when(step < n_fwd)
    def _():
        fwd_step(step, bq, bk, q_ref, kt_ref, v_ref, ot_ref, lse_ref, s_scr)

    def run(two, slot0, c=None, load=True):
        n = half if c is None else chunk
        if load:
            cps = [pltpu.make_async_copy(block(o, p, c), buf.at[slot0 + i, pl.ds(0, n)], load_sem.at[slot0 + i]) for i, (o, p) in enumerate(two)]
            start_all(cps)
            wait_all(cps)
        starts = [o * rows + p * half + (0 if c is None else c * chunk) for o, p in two]

        def body(i, _):
            do_ref[pl.ds(pl.multiple_of(starts[0] + i * (starts[1] - starts[0]), n), n), :] = lax.dot_general(
                buf[slot0 + i, :n], wo_scr[...], (((1,), (1,)), ((), ())), preferred_element_type=F32).astype(BF16)
            return 0

        lax.fori_loop(0, SLOTS, body, 0)

    groups = arrivals(me)

    @pl.when(step == n_fwd)
    def _():
        wait_all(loads)
        start_all(stores)
        w_copy.wait()
        run(groups[0][:2], 0, load=False)
        wait_all(stores)
        receive(links.to_own)
        run(groups[0][2:], 2)
        for g in range(SLOTS):
            if g:
                links.near(g)
            run(groups[g + 1][:2], 0)
            receive(links.to_near[g])
            run(groups[g + 1][2:], 2)
        for c in range(CHUNKS):
            links.far(c)
            run(groups[3][:2], 0, c)
            receive(links.to_far[c])
            run(groups[3][2:], 2, c)
        links.finish()


def gather_forward(q, kt, v, g, w_o, bq=PAIR, bk=1024):
    seq, width = q.shape
    rows, feat = g.shape
    heads = width // HEAD_DIM
    n = seq // bq
    at = lambda i: jnp.minimum(i, n - 1)
    return pl.pallas_call(
        functools.partial(gather_fwd_kernel, n, (3 * n) // 4, bq, bk), grid=(n + 1,),
        in_specs=[pl.BlockSpec((bq, width), lambda i: (at(i), 0)), pl.BlockSpec((HEAD_DIM, seq), whole, **ONCE),
                  pl.BlockSpec((seq, HEAD_DIM), whole, **ONCE), HBM, HBM],
        out_specs=[pl.BlockSpec((width, bq), lambda i: (0, at(i))), pl.BlockSpec((heads, bq, 1), lambda i: (0, at(i), 0)), HBM,
                   pl.BlockSpec((seq, width), whole)],
        out_shape=[array(width, seq), array(heads, seq, 1, dtype=F32), array(seq, feat),
                   array(seq, width)],
        scratch_shapes=[pltpu.VMEM((seq // bk, heads * bq, bk), F32), pltpu.VMEM((width, feat), BF16), pltpu.VMEM((4, rows // 2, feat), BF16),
                        SEM((n_copies(CHUNKS, True),)), SEM((n_copies(CHUNKS, True),)), SEM((1,)), SEM((4,)), SEM((SLOTS,))],
        compiler_params=remote_params(2),
        name="gather_fwd")(q, kt, v, g, w_o)


def bwd_step(qi, bq, bk, q_ref, do_ref, lse_ref, k_ref, kt_ref, vt_ref, cos_ref, sin_ref, g_out, dkt_ref, dvt_ref, p_scr, dp_scr):
    q = stack_heads(q_ref[...])
    do = stack_heads(do_ref[...])
    rows = q.shape[0]
    lse = lse_ref[...].reshape(rows, 1)
    q_t = q.T
    do_t = do.T
    nfull = (qi * bq) // bk

    @pl.when(qi == 0)
    def _():
        dkt_ref[...] = jnp.zeros_like(dkt_ref)
        dvt_ref[...] = jnp.zeros_like(dvt_ref)

    def prob_step(j, r, masked):
        sl = pl.ds(pl.multiple_of(j * bk, bk), bk)
        s = dot(q, kt_ref[:, sl]) * (SCALE * LOG2E)
        p = jnp.exp2(s - lse)
        if masked:
            p = jnp.where(causal((rows, bk), bq, qi * bq - nfull * bk), p, 0.0)
        dp = dot(do, vt_ref[:, sl])
        pd = p * dp
        for t in range(bk // LANE):
            r = r + pd[:, t * LANE:(t + 1) * LANE]
        p_scr[j] = p
        dp_scr[j] = dp
        dvt_ref[:, sl] += dot(do_t, p.astype(BF16))
        return r

    r = lax.fori_loop(0, nfull, lambda j, r: prob_step(j, r, False), jnp.zeros((rows, LANE), F32))
    r = prob_step(nfull, r, True)
    r = jnp.sum(r, axis=1, keepdims=True)

    def grad_step(j, dq):
        sl = pl.ds(pl.multiple_of(j * bk, bk), bk)
        ds = (p_scr[j] * (dp_scr[j] - r) * SCALE).astype(BF16)
        dkt_ref[:, sl] += dot(q_t, ds)
        return dq + dot(ds, k_ref[sl, :])

    dq = lax.fori_loop(0, nfull + 1, grad_step, jnp.zeros((rows, HEAD_DIM), F32))
    dq = dq.astype(BF16).astype(F32)
    here = pl.ds(pl.multiple_of(qi * bq, bq), bq)
    cos_t, sin_t = cos_ref[here, :], sin_ref[here, :]
    for n in range(rows // bq):
        g_out[:, n * HEAD_DIM:(n + 1) * HEAD_DIM] = rotate(dq[n * bq:(n + 1) * bq], cos_t, -sin_t).astype(BF16)


def gather_bwd_kernel(relay, bq, bk, q_ref, do_ref, lse_ref, k_ref, kt_ref, vt_ref, cos_ref, sin_ref, ot_ref,
                      ga_ref, gb_ref, otg_ref, otz_ref, p_scr, dp_scr, dkt_scr, dvt_scr, buf, g_buf, kv_buf, send, recv, z_send, z_recv, load_sem, store_sem, g_sem, kv_sem):
    step = pl.program_id(0)
    last = pl.num_programs(0) - 1
    me = lax.axis_index("sp")
    width, seq = ot_ref.shape
    half = width // 2
    tokens = otz_ref.shape[2]
    zn = flip(me, CORE)
    own = lambda part: ot_ref.at[pl.ds(part * half, half)]
    block = lambda owner, part, _: otg_ref.at[owner // 2, pl.ds(part * half, half)]
    links = Exchange(send, recv, block, own, 1, False)
    xn, yn = flip(me, X_BIT), flip(me, Y_BIT)
    dn = flip(xn, Y_BIT)
    mine = pl.ds(pl.multiple_of(zn * tokens, tokens), tokens)

    def to_other(n, owner):
        src = ot_ref.at[:, mine] if n == 0 else otg_ref.at[owner // 2, :, mine]
        return pltpu.make_async_remote_copy(src_ref=src, dst_ref=otz_ref.at[owner // 2], send_sem=z_send.at[n], recv_sem=z_recv.at[n],
                                            device_id={"sp": zn}, device_id_type=MESH)

    z = [to_other(n, o) for n, o in enumerate((me, xn, yn, dn))]
    n_buf, slab = buf.shape[0], buf.shape[1]
    n_slab = width // slab

    def slab_copies(n):
        rows = pl.ds(pl.multiple_of(n * slab, slab), slab)
        slot = n % n_buf
        return (pltpu.make_async_copy(ot_ref.at[rows], buf.at[slot], load_sem.at[slot]),
                pltpu.make_async_copy(buf.at[slot], otg_ref.at[me // 2, rows], store_sem.at[slot]))

    @pl.when(step == 0)
    def _():
        greet(neighbours())
        links.begin()
        z[0].start()

    @pl.when(step == relay)
    def _():
        links.near(0)

    @pl.when((step >= 2) & (step < n_slab + 2))
    def _():
        slab_copies(step - 2)[1].wait()

    @pl.when((step >= 1) & (step < n_slab + 1))
    def _():
        slab_copies(step - 1)[0].wait()
        slab_copies(step - 1)[1].start()

    @pl.when(step < n_slab)
    def _():
        slab_copies(step)[0].start()

    def out_copies(src, sems, i, n, at):
        slot = lax.rem(i, SLOTS)
        rows, w = pl.ds(pl.multiple_of(i * n, n), n), src.shape[SLOTS] // SLOTS
        return [pltpu.make_async_copy(src.at[slot, :, m * w:(m + 1) * w], ref.at[rows, at:at + w], sems.at[slot, m]) for m, ref in enumerate((ga_ref, gb_ref))]

    def out_wait(*args):
        for c in out_copies(*args):
            c.wait()

    @pl.when(step >= SLOTS)
    def _():
        out_wait(g_buf, g_sem, step - SLOTS, bq, 0)

    bwd_step(step, bq, bk, q_ref, do_ref, lse_ref, k_ref, kt_ref, vt_ref, cos_ref, sin_ref, g_buf.at[lax.rem(step, SLOTS)], dkt_scr, dvt_scr, p_scr, dp_scr)
    for c in out_copies(g_buf, g_sem, step, bq, 0):
        c.start()

    @pl.when(step == last)
    def _():
        links.near(1)
        start_all(z[1:3])

        n_kv, n_blocks = kv_buf.shape[1], seq // kv_buf.shape[1]

        def kv_rows(i, _):
            @pl.when(i >= SLOTS)
            def _():
                out_wait(kv_buf, kv_sem, i - SLOTS, n_kv, PAIR)

            rows, slot = pl.ds(pl.multiple_of(i * n_kv, n_kv), n_kv), lax.rem(i, SLOTS)
            dk = dkt_scr[:, rows].T.astype(BF16).astype(F32)
            kv_buf[slot, :, :HEAD_DIM] = rotate(dk, cos_ref[rows, :], -sin_ref[rows, :]).astype(BF16)
            kv_buf[slot, :, HEAD_DIM:] = dvt_scr[:, rows].T.astype(BF16)
            for c in out_copies(kv_buf, kv_sem, i, n_kv, PAIR):
                c.start()
            return 0

        lax.fori_loop(0, n_blocks, kv_rows, 0)
        for n in reversed(range(SLOTS)):
            out_wait(kv_buf, kv_sem, n_blocks - 1 - n, n_kv, PAIR)
            out_wait(g_buf, g_sem, last - n, bq, 0)
        links.far(0)
        z[3].start()
        receive(z)
        links.finish()
        for c in z:
            c.wait_send()


def gather_backward(q, do, lse, k, kt, vt, cos_t, sin_t, ot, sp_size, bq=PAIR, bk=512):
    seq, width = q.shape
    heads = width // HEAD_DIM
    chips, tokens = sp_size // 2, seq // sp_size
    n = seq // bq
    tile = pl.BlockSpec((bq, width), row)
    tall = pl.BlockSpec((seq, HEAD_DIM), whole, **ONCE)
    wide = pl.BlockSpec((HEAD_DIM, seq), whole, **ONCE)
    piece = array(seq, 3 * HEAD_DIM)
    return pl.pallas_call(
        functools.partial(gather_bwd_kernel, (9 * n) // 16, bq, bk), grid=(n,),
        in_specs=[tile, tile, pl.BlockSpec((heads, bq, 1), lambda i: (0, i, 0)), tall, wide, wide, tall, tall, HBM],
        out_specs=[HBM] * 4,
        out_shape=[piece, piece, array(chips, width, seq), array(chips, width, tokens)],
        scratch_shapes=[pltpu.VMEM((seq // bk, heads * bq, bk), F32), pltpu.VMEM((seq // bk, heads * bq, bk), F32),
                        pltpu.VMEM((HEAD_DIM, seq), F32), pltpu.VMEM((HEAD_DIM, seq), F32), pltpu.VMEM((SLOTS, width // 8, seq), BF16), pltpu.VMEM((SLOTS, bq, width), BF16),
                        pltpu.VMEM((SLOTS, 512, PAIR), BF16),
                        SEM((n_copies(1, False),)), SEM((n_copies(1, False),)), SEM((4,)), SEM((4,)), SEM((SLOTS,)), SEM((SLOTS,)), SEM((SLOTS, SLOTS)), SEM((SLOTS, SLOTS))],
        compiler_params=remote_params(3),
        name="gather_bwd")(q, do, lse, k, kt, vt, cos_t, sin_t, ot)


def dw_o_kernel(core_ref, ot_ref, g_ref, final_ref, send_ref):
    y = dot(ot_ref[...], g_ref[...]).astype(BF16)
    final_ref[...] = y
    send_ref[...] = y


def dw_o_half(core, ot_all, g_all, bn=1024):
    half, width, seq = ot_all.shape
    feat = g_all.shape[1]
    return pl.pallas_call(
        dw_o_kernel,
        grid_spec=pltpu.PrefetchScalarGridSpec(
            num_scalar_prefetch=1, grid=(feat // bn, half),
            in_specs=[pl.BlockSpec((None, width, seq), lambda j, s, c: (s, 0, 0)), pl.BlockSpec((seq, bn), col)],
            out_specs=[pl.BlockSpec((width, bn), lambda j, s, c: (2 * s + c[0], j)), pl.BlockSpec((width, bn), lambda j, s, c: (s, j))]),
        out_shape=[array(2 * half * width, feat), array(half * width, feat)],
        compiler_params=PARAMS, cost_estimate=cost(2 * half * width * feat * seq), name="dw_o_half")(core, ot_all, g_all)


def out_kernel(ids_ref, mine_ref, other_ref, w_ref, out_ref, o_scr):
    @pl.when(pl.program_id(0) == 0)
    def _():
        core = lax.rem(ids_ref[0], 2)
        width = mine_ref.shape[1]
        for s in range(mine_ref.shape[0]):
            for ref, d in ((mine_ref, 2 * s + core), (other_ref, 2 * s + 1 - core)):
                o_scr[:, pl.ds(pl.multiple_of(d * width, width), width)] = ref[s].T

    out_ref[...] = dot(o_scr[...], w_ref[...]).astype(BF16)


def out_proj(ids, ot_all, ot_other, w_o, bn=512):
    chips, width, tokens = ot_other.shape
    feat = w_o.shape[1]
    return pl.pallas_call(
        out_kernel,
        grid_spec=pltpu.PrefetchScalarGridSpec(
            num_scalar_prefetch=1, grid=(feat // bn,),
            in_specs=[pl.BlockSpec((chips, width, tokens), lambda i, c: (0, 0, c[0]), **ONCE), pl.BlockSpec((chips, width, tokens), lambda i, c: (0, 0, 0), **ONCE),
                      pl.BlockSpec((w_o.shape[0], bn), col)],
            out_specs=pl.BlockSpec((tokens, bn), col),
            scratch_shapes=[pltpu.VMEM((tokens, w_o.shape[0]), BF16)]),
        out_shape=array(tokens, feat), compiler_params=PARAMS, cost_estimate=cost(2 * tokens * w_o.size), name="out_proj")(ids, ot_all, ot_other, w_o)


def dev_stores(buf, slot, rows, dev, finals, sem):
    copies = []
    start = 0
    for n, ref in enumerate(finals):
        w = (buf.shape[2] - PAIR) if n == 0 else HEAD_DIM
        copies.append(pltpu.make_async_copy(buf.at[slot, :, start:start + w], ref.at[rows, pl.ds(pl.multiple_of(dev * w, w), w)], sem.at[slot, n]))
        start += w
    return copies


class Ride:
    def __init__(self, kind, ids_ref, recv, buf, finals, load_sem, store_sem):
        self.kind, self.ids, self.recv, self.buf, self.finals, self.load_sem, self.store_sem = kind, ids_ref, recv, buf, finals, load_sem, store_sem

    def load(self, i):
        n = self.buf.shape[1]
        slot = lax.rem(i, SLOTS)
        return pltpu.make_async_copy(self.recv.at[pl.ds(pl.multiple_of(i * n, n), n)], self.buf.at[slot], self.load_sem.at[slot])

    def stores(self, i):
        n = self.buf.shape[1]
        slot = lax.rem(i, SLOTS)
        if self.kind == "dev":
            return dev_stores(self.buf, slot, pl.ds(pl.multiple_of(i * n, n), n), self.ids[1], self.finals, self.store_sem)
        per = (HEAD_DIM * 4) // n
        block = (2 * lax.div(i, per) + 1 - lax.rem(self.ids[2], 2)) * per + lax.rem(i, per)
        return [pltpu.make_async_copy(self.buf.at[slot], self.finals[0].at[pl.ds(pl.multiple_of(block * n, n), n)], self.store_sem.at[slot, 0])]

    def begin(self, i):
        @pl.when(i >= SLOTS)
        def _():
            for c in self.stores(i - SLOTS):
                c.wait()

        self.load(i).start()

    def end(self, i, last):
        self.load(i).wait()
        for c in self.stores(i):
            c.start()

        @pl.when(i == last)
        def _():
            for n in reversed(range(SLOTS)):
                for c in self.stores(i - n):
                    c.wait()


def joined(a_ref, b_ref, x_ref, sem):
    copies, at = [], 0
    for part in (slice(0, PAIR), slice(PAIR, PAIR + HEAD_DIM)):
        w = part.stop - part.start
        for ref in (a_ref, b_ref):
            copies.append(pltpu.make_async_copy(ref.at[:, part], x_ref.at[:, at:at + w], sem.at[len(copies)]))
            at += w
    return copies


def dw_kernel(kinds, n_alias, ids_ref, ht_ref, a_ref, b_ref, *refs):
    n = len(kinds)
    recvs = refs[:n]
    refs = refs[n + n_alias:]
    finals, refs = refs[:3], refs[3:]
    o_final, refs = (refs[:1], refs[1:]) if "o" in kinds else ((), refs)
    send_ref, x_scr, y_scr, y_sem, x_sem, load_sem, *extra = refs
    rides = [Ride(k, ids_ref, recvs[m], extra[3 * m], finals if k == "dev" else o_final, extra[3 * m + 1], extra[3 * m + 2]) for m, k in enumerate(kinds)]
    i, last = grid_place()
    bm, feat = ht_ref.shape[0], finals[0].shape[0]
    n_tok = send_ref.shape[0] - feat
    tokens = pltpu.make_async_copy(x_scr.at[pl.ds(pl.multiple_of(flip(ids_ref[2], CORE) * n_tok, n_tok), n_tok)], send_ref.at[pl.ds(feat, n_tok)], x_sem.at[0])

    @pl.when(i == 0)
    def _():
        loads = joined(a_ref, b_ref, x_scr, load_sem)
        for c in loads:
            c.start()
        for c in loads:
            c.wait()
        tokens.start()

    def stores(step):
        slot, rows = lax.rem(step, SLOTS), pl.ds(pl.multiple_of(step * bm, bm), bm)
        whole_rows = pltpu.make_async_copy(y_scr.at[slot], send_ref.at[rows], y_sem.at[slot, len(finals)])
        return dev_stores(y_scr, slot, rows, ids_ref[0], finals, y_sem) + [whole_rows]

    for r in rides:
        r.begin(i)

    @pl.when(i >= SLOTS)
    def _():
        for c in stores(i - SLOTS):
            c.wait()

    y = dot(ht_ref[...], x_scr[...]).astype(BF16)
    y_scr[lax.rem(i, SLOTS)] = y
    for c in stores(i):
        c.start()
    for r in rides:
        r.end(i, last)

    @pl.when(i == last)
    def _():
        tokens.wait()
        for n in reversed(range(SLOTS)):
            for c in stores(i - n):
                c.wait()


def ride_scratch(kinds, steps, feat, w):
    out = []
    for k in kinds:
        block = (feat // steps, w) if k == "dev" else (feat // (2 * steps), feat)
        out += [pltpu.VMEM((2,) + block, BF16), SEM((SLOTS,)), SEM((SLOTS, 3 if k == "dev" else 1))]
    return out


def dw_device(ids, ht, a, b, finals, rides, tokens, o_final=None, bm=512):
    feat, seq = ht.shape
    w = a.shape[1] + b.shape[1]
    kinds = [k for k, _ in rides]
    finals = list(finals) + ([o_final] if "o" in kinds else [])
    old = [f for f in finals if isinstance(f, jax.Array)]
    ins = [ht, a, b] + [r for _, r in rides] + old
    n_final, n_alias = len(finals), len(old)
    first = len(ins) - n_alias
    return pl.pallas_call(
        functools.partial(dw_kernel, kinds, n_alias),
        grid_spec=pltpu.PrefetchScalarGridSpec(
            num_scalar_prefetch=1, grid=(feat // bm,),
            in_specs=[pl.BlockSpec((bm, seq), row)] + [HBM] * (len(ins) - 1),
            out_specs=[HBM] * (n_final + 1),
            scratch_shapes=[pltpu.VMEM((seq, w), BF16), pltpu.VMEM((SLOTS, bm, w), BF16), SEM((SLOTS, 4)), SEM((1,)), SEM((4,))] + ride_scratch(kinds, feat // bm, feat, w)),
        out_shape=[array(*f.shape) for f in finals] + [array(feat + tokens, w)],
        input_output_aliases={1 + first + n: n for n in range(n_alias)},
        compiler_params=PARAMS, cost_estimate=cost(2 * seq * feat * w), name="dw_device")(ids, *ins)


def dh_kernel(n_dev, n_ride, ids_ref, wq_ref, wk_ref, wv_ref, x_ref, lnw_ref, *refs):
    own, refs = refs[:n_dev], refs[n_dev:]
    n_other = n_dev // SLOTS - 1
    other, t_ref, recvs, refs = refs[:n_other], refs[n_other], refs[n_other + 1:n_other + 1 + n_ride], refs[n_other + 1 + n_ride + 3:]
    dx_ref, dlnw_ref, *refs = refs
    finals, (g_scr, hat_scr, rstd_scr, sum_scr, dy_scr), refs = refs[:3], refs[3:8], refs[8:]
    i, last = grid_place()
    rides = [Ride("dev", (None, ids_ref[1 + n]), recvs[n], refs[3 * n], finals, *refs[3 * n + 1:3 * n + 3]) for n in range(n_ride)]
    for r in rides:
        r.begin(i)
    nq, nk = wq_ref.shape[1], wk_ref.shape[1]
    tokens, feat = x_ref.shape
    bf = wq_ref.shape[0]
    slab = tokens // 8

    @pl.when(i == 0)
    def _():
        def place(t, dev, part):
            n = t.shape[0] - HEAD_DIM
            g_scr[pl.ds(pl.multiple_of(dev * 2 * PAIR + part * PAIR, PAIR), n), :] = t[:n]
            g_scr[pl.ds(pl.multiple_of(nq + part * nk + dev * HEAD_DIM, HEAD_DIM), HEAD_DIM), :] = t[n:]

        for n in range(n_dev):
            place(own[n][...].T, ids_ref[1 + n_ride + n // SLOTS], n % SLOTS)
        owner = 1 + n_ride + n_dev // SLOTS
        for n in range(n_other):
            t = other[n][...].T
            dev = ids_ref[owner + n]
            place(t[:-HEAD_DIM], dev, 0)
            g_scr[pl.ds(pl.multiple_of(nq + nk + dev * HEAD_DIM, HEAD_DIM), HEAD_DIM), :] = t[-HEAD_DIM:]
        for n in range(SLOTS):
            place(t_ref[n].T, ids_ref[owner + n_other], n)

        def stats(n, _):
            here = pl.ds(pl.multiple_of(n * slab, slab), slab)
            x = x_ref[here, :].astype(F32)
            centered = x - jnp.mean(x, axis=-1, keepdims=True)
            rstd = lax.rsqrt(jnp.mean(centered * centered, axis=-1, keepdims=True) + LN_EPS)
            hat_scr[here, :] = (centered * rstd).astype(F32)
            rstd_scr[here, :] = jnp.broadcast_to(rstd, (slab, LANE))
            return 0

        lax.fori_loop(0, tokens // slab, stats, 0)
        sum_scr[...] = jnp.zeros_like(sum_scr)

    y = (dot(wq_ref[...], g_scr[:nq, :]) + dot(wk_ref[...], g_scr[nq:nq + nk, :]) + dot(wv_ref[...], g_scr[nq + nk:, :])).T
    at = pl.ds(pl.multiple_of(i * bf, bf), bf)
    hat = hat_scr[:, at]
    dlnw_ref[...] = jnp.sum(y * hat, axis=0, keepdims=True)
    y = y * lnw_ref[...]
    dy_scr[:, at] = y
    yh = y * hat
    for n in range(bf // LANE):
        part = slice(n * LANE, (n + 1) * LANE)
        sum_scr[0] += y[:, part]
        sum_scr[1] += yh[:, part]
    for r in rides:
        r.end(i, last)

    @pl.when(i == last)
    def _():
        def finish(n, _):
            here = pl.ds(pl.multiple_of(n * slab, slab), slab)
            mean_y, mean_yh = (jnp.sum(sum_scr[m, here, :], axis=1, keepdims=True) / feat for m in range(SLOTS))
            dx_ref[here, :] = (rstd_scr[here, :1] * (dy_scr[here, :] - mean_y - hat_scr[here, :] * mean_yh)).astype(BF16)
            return 0

        lax.fori_loop(0, tokens // slab, finish, 0)


def dh_proj(ids, w_q, w_k, w_v, x, ln_weight, own, other, t_rows, rides, finals, bf=512):
    tokens, feat = x.shape
    w = other[0].shape[1]
    n = len(own)
    ins = [w_q, w_k, w_v, x, ln_weight.astype(F32)[None], *own, *other, t_rows, *rides, *finals]
    specs = [pl.BlockSpec((bf, m.shape[1]), row) for m in (w_q, w_k, w_v)] + [pl.BlockSpec(x.shape, whole, **ONCE), pl.BlockSpec((1, bf), col)]
    specs += [pl.BlockSpec((tokens, m.shape[1]), lambda i, c: (c[0], 0), **ONCE) for m in own]
    specs += [pl.BlockSpec((tokens, w), lambda i, c: (feat // tokens, 0), **ONCE) for _ in other]
    specs += [pl.BlockSpec(t_rows.shape, lambda i, c: (0, 0, 0), **ONCE)]
    first = len(ins) - len(finals)
    return pl.pallas_call(
        functools.partial(dh_kernel, n, len(rides)),
        grid_spec=pltpu.PrefetchScalarGridSpec(
            num_scalar_prefetch=1, grid=(feat // bf,), in_specs=specs + [HBM] * (len(ins) - len(specs)),
            out_specs=[pl.BlockSpec(x.shape, whole, **ONCE), pl.BlockSpec((1, bf), col)] + [HBM] * len(finals),
            scratch_shapes=[pltpu.VMEM((w_q.shape[1] + 2 * w_k.shape[1], tokens), BF16), pltpu.VMEM(x.shape, F32), pltpu.VMEM((tokens, LANE), F32),
                            pltpu.VMEM((SLOTS, tokens, LANE), F32), pltpu.VMEM(x.shape, F32)] + ride_scratch(["dev"] * len(rides), feat // bf, feat, w)),
        out_shape=[array(tokens, feat), array(1, feat, dtype=F32)] + [array(*f.shape) for f in finals],
        input_output_aliases={1 + first + m: 2 + m for m in range(len(finals))},
        compiler_params=PARAMS, cost_estimate=cost(2 * tokens * (w_q.size + 2 * w_k.size)), name="dh_proj")(ids, *ins)


def copy_kernel(ids_ref, recv, *refs):
    finals, (buf, load_sem, store_sem) = refs[3:6], refs[6:]
    n_blocks, n = buf.shape[:2]
    rows = [pl.ds(i * n, n) for i in range(n_blocks)]
    loads = [pltpu.make_async_copy(recv.at[r], buf.at[i], load_sem.at[i]) for i, r in enumerate(rows)]
    stores = [dev_stores(buf, i, r, ids_ref[0], finals, store_sem) for i, r in enumerate(rows)]
    for c in loads:
        c.start()
    for c, group in zip(loads, stores):
        c.wait()
        for d in group:
            d.start()
    for c in sum(stores, []):
        c.wait()


def copy_in(dev, recv, finals, n_blocks=8):
    feat, w = finals[0].shape[0], recv.shape[1]
    return pl.pallas_call(
        copy_kernel,
        grid_spec=pltpu.PrefetchScalarGridSpec(num_scalar_prefetch=1, grid=(1,), in_specs=[HBM] * 4, out_specs=[HBM] * 3,
                                               scratch_shapes=[pltpu.VMEM((n_blocks, feat // n_blocks, w), BF16), SEM((n_blocks,)), SEM((n_blocks, 3))]),
        out_shape=[array(*f.shape) for f in finals], input_output_aliases={2 + m: m for m in range(len(finals))},
        compiler_params=PARAMS, name="copy_in")(dev, recv, *finals)


def sum_kernel(x_ref, out_ref, all_scr, send, recv):
    me = lax.axis_index("sp")
    peers = everyone()
    greet(peers)
    copies = [pltpu.make_async_remote_copy(src_ref=x_ref, dst_ref=all_scr.at[me], send_sem=send.at[n], recv_sem=recv.at[n],
                                           device_id={"sp": p}, device_id_type=MESH) for n, p in enumerate(peers)]
    for c in copies:
        c.start()
    all_scr[me] = x_ref[...]
    for c in copies:
        c.wait_recv()
    total = all_scr[0]
    for n in range(1, all_scr.shape[0]):
        total = total + all_scr[n]
    out_ref[...] = total.astype(BF16)
    for c in copies:
        c.wait_send()


def sum_devices(x, sp_size):
    n = x.shape[0] // HEAD_DIM
    vmem = pl.BlockSpec(memory_space=pltpu.VMEM)
    return pl.pallas_call(
        sum_kernel, in_specs=[vmem], out_specs=vmem, out_shape=array(n, HEAD_DIM),
        scratch_shapes=[pltpu.VMEM((sp_size, n, HEAD_DIM), F32), SEM((sp_size - 1,)), SEM((sp_size - 1,))],
        compiler_params=remote_params(4), name="sum_devices")(x.reshape(n, HEAD_DIM)).reshape(-1)


def solution(mesh):
    sp_size = mesh.shape['sp']
    row_spec = P(('dp', 'sp'), None)
    pos_spec = P(('dp', 'sp'))
    full_spec = P(None, None)
    grad_spec = P('dp', None)

    def local_step(hidden, positions, d_attn, ln_weight, w_q, w_k, w_v, w_o):
        dev = lax.axis_index('sp')
        core = lax.rem(dev, SLOTS)
        local_rows, _ = hidden.shape
        _, ht, q, k, kt, v, vt, cos_t, sin_t = gather_qkv(hidden, ln_weight, positions, w_q, w_k, w_v, sp_size)
        ot, lse, g_all, do = gather_forward(q, kt, v, d_attn, w_o)
        ga, gb, ot_all, ot_other = gather_backward(q, do, lse, k, kt, vt, cos_t, sin_t, ot, sp_size)
        core1 = core.reshape(1)
        other = lambda d: flip(d, CORE)
        dev_x, dev_y = flip(dev, X_BIT), flip(dev, Y_BIT)
        dev_d = flip(dev_x, Y_BIT)

        def to(x, bit):
            return lax.ppermute(x, 'sp', [(i, i ^ bit) for i in range(sp_size)])

        after = lambda x, *done: lax.optimization_barrier((x,) + done)[0]
        ids = lambda *d: jnp.stack(d)
        ga_x, gb_y, gb_x, ga_y = to(ga, X_BIT), to(gb, Y_BIT), to(gb, X_BIT), to(ga, Y_BIT)
        dw_o, o_send = dw_o_half(core1, ot_all, g_all)
        o_recv = to(o_send, CORE)
        attn_out = out_proj(dev.reshape(1), ot_all, ot_other, w_o)
        blank = [array(*w.shape) for w in (w_q, w_k, w_v)]
        *finals, send0 = dw_device(ids(dev, dev, dev), ht, after(ga, attn_out, o_send), gb, blank, [], local_rows)
        recv0 = to(send0, CORE)
        ga_d, gb_d = to(after(ga_x, send0), Y_BIT), to(after(gb_y, send0), X_BIT)
        *finals, dw_o, send1 = dw_device(ids(dev_x, dev, dev), ht, ga_x, gb_x, finals, [('o', o_recv)], local_rows, dw_o)
        recv1 = to(send1, CORE)
        *finals, send2 = dw_device(ids(dev_y, other(dev), dev), ht, ga_y, gb_y, finals, [('dev', recv0)], local_rows)
        recv2 = to(send2, CORE)
        t_rows = jnp.stack([lax.dynamic_slice_in_dim(m, other(dev) * local_rows, local_rows, axis=0) for m in (ga_d, gb_d)])
        t_rows = to(t_rows, CORE)
        *finals, send3 = dw_device(ids(dev_d, other(dev_x), dev), ht, ga_d, gb_d, finals, [('dev', recv1)], local_rows)
        recv3 = to(send3, CORE)
        owners = [dev, dev_x, dev_y, dev_d]
        dx, d_lnw, dw_q, dw_k, dw_v = dh_proj(ids(dev, other(dev_y), *owners, *map(other, owners)), w_q, w_k, w_v, hidden, ln_weight,
                                              [ga, gb, ga_x, gb_x, ga_y, gb_y, ga_d, gb_d], [recv0, recv1, recv2], t_rows, [recv2], finals)
        d_lnw = sum_devices(d_lnw.reshape(-1), sp_size)
        dw_q, dw_k, dw_v = copy_in(other(dev_d).reshape(1), recv3, [dw_q, dw_k, dw_v])
        return (attn_out, dx, d_lnw, dw_q, dw_k, dw_v, dw_o)

    return jax.shard_map(local_step, mesh=mesh,
                      in_specs=(row_spec, pos_spec, row_spec, P(None), full_spec, full_spec, full_spec, full_spec),
                      out_specs=(row_spec, row_spec, P('dp'), grad_spec, grad_spec, grad_spec, grad_spec),
                      check_vma=False)
```

```python
import functools
import jax
import jax.numpy as jnp
from jax import lax
from jax.experimental import pallas as pl
from jax.experimental.pallas import tpu as pltpu
from jax.sharding import PartitionSpec as P

HEAD_DIM = LANE = 128
PAIR = 2 * HEAD_DIM
CORE, X_BIT, Y_BIT = 1, 2, 4
LOW, HIGH, SLOTS = 0, 1, 2
CHUNKS, N_PEERS = 2, 7
LN_EPS = 1e-5
ROPE_BASE = 10000.0
SCALE = HEAD_DIM ** -0.5
LOG2E = 1.4426950408889634
VMEM_LIMIT = 67_000_000
BF16 = jnp.bfloat16
F32 = jnp.float32
MESH = pl.DeviceIdType.MESH
HBM = pl.BlockSpec(memory_space=pl.ANY)
SEM = pltpu.SemaphoreType.DMA
row = lambda i, *_: (i, 0)
col = lambda i, *_: (0, i)
whole = lambda *_: (0, 0)
ONCE = dict(pipeline_mode=pl.Buffered(1))
PARAMS = pltpu.CompilerParams(vmem_limit_bytes=VMEM_LIMIT)


def grid_place():
    return pl.program_id(0), pl.num_programs(0) - 1


def dot(x, y):
    return jnp.dot(x, y, preferred_element_type=F32)


def array(*shape, dtype=BF16):
    return jax.ShapeDtypeStruct(shape, dtype)


def remote_params(number):
    return pltpu.CompilerParams(collective_id=number, has_side_effects=True, vmem_limit_bytes=VMEM_LIMIT)


def cost(flops):
    return pl.CostEstimate(flops=flops, bytes_accessed=flops // HEAD_DIM, transcendentals=0)


def norm_f32(hid_f32, weight_f32):
    mean_val = jnp.mean(hid_f32, axis=-1, keepdims=True)
    centered = hid_f32 - mean_val
    var_val = jnp.mean(centered * centered, axis=-1, keepdims=True)
    return centered * lax.rsqrt(var_val + LN_EPS) * weight_f32


def rotate(x, cos_t, sin_t):
    lane = lax.broadcasted_iota(jnp.int32, x.shape, 1)
    swapped = jnp.where(lane % 2 == 0, pltpu.roll(x, HEAD_DIM - 1, 1), pltpu.roll(x, 1, 1))
    return x * cos_t + swapped * sin_t


def flip(i, bit):
    return i + bit - 2 * bit * ((i // bit) % 2)


class Exchange:
    def __init__(self, send, recv, block, own, chunks, partner):
        me = lax.axis_index("sp")
        xn, yn, zn = flip(me, X_BIT), flip(me, Y_BIT), flip(me, CORE)
        dn = flip(xn, Y_BIT)
        self.every = []

        def copy(owner, part, to, chunk=None):
            n = len(self.every)
            src = own(part) if owner is me else block(owner, part, chunk)
            self.every.append(pltpu.make_async_remote_copy(src_ref=src, dst_ref=block(owner, part, chunk), send_sem=send.at[n], recv_sem=recv.at[n],
                                                           device_id={"sp": to}, device_id_type=MESH))
            return self.every[-1]

        self.first = [copy(me, LOW, xn), copy(me, HIGH, yn)]
        self.second = [copy(me, HIGH, xn), copy(me, LOW, yn)]
        self.relay = [[copy(xn, LOW, yn, c), copy(yn, HIGH, xn, c)] for c in range(chunks)]
        if partner:
            self.to_own = [copy(me, LOW, zn), copy(me, HIGH, zn)]
            self.to_near = [[copy(xn, LOW, zn), copy(yn, HIGH, zn)], [copy(xn, HIGH, zn), copy(yn, LOW, zn)]]
            self.to_far = [[copy(dn, LOW, zn, c), copy(dn, HIGH, zn, c)] for c in range(chunks)]

    def begin(self):
        start_all(self.first)
        if hasattr(self, "to_own"):
            start_all(self.to_own)
        start_all(self.second)

    def near(self, n):
        for m, c in enumerate(self.second if n else self.first):
            c.wait_recv()
            if n == 0:
                start_all([r[m] for r in self.relay])
            if hasattr(self, "to_near"):
                self.to_near[n][m].start()

    def far(self, n):
        for m, c in enumerate(self.relay[n]):
            c.wait_recv()
            if hasattr(self, "to_far"):
                self.to_far[n][m].start()

    def finish(self):
        for c in self.every:
            c.wait_send()


def start_all(copies):
    for c in copies:
        c.start()


def wait_all(copies):
    for c in copies:
        c.wait()


def receive(copies):
    for c in copies:
        c.wait_recv()


def n_copies(chunks, partner):
    return 4 + 2 * chunks + (6 + 2 * chunks if partner else 0)


def greet(peers):
    barrier = pltpu.get_barrier_semaphore()
    for p in peers:
        pl.semaphore_signal(barrier, inc=1, device_id={"sp": p}, device_id_type=MESH)
    pl.semaphore_wait(barrier, len(peers))


def neighbours():
    me = lax.axis_index("sp")
    return [flip(me, CORE), flip(me, X_BIT), flip(me, Y_BIT)]


def everyone():
    me = lax.axis_index("sp")
    xn, yn = flip(me, X_BIT), flip(me, Y_BIT)
    dn = flip(xn, Y_BIT)
    return [flip(me, CORE), xn, flip(xn, CORE), yn, flip(yn, CORE), dn, flip(dn, CORE)]


def arrivals(me):
    xn, yn, zn = flip(me, X_BIT), flip(me, Y_BIT), flip(me, CORE)
    dn = flip(xn, Y_BIT)
    zx, zy, zd = flip(xn, CORE), flip(yn, CORE), flip(dn, CORE)
    return [[(me, LOW), (me, HIGH), (zn, LOW), (zn, HIGH)], [(xn, LOW), (yn, HIGH), (zx, LOW), (zy, HIGH)], [(xn, HIGH), (yn, LOW), (zx, HIGH), (zy, LOW)],
            [(dn, LOW), (dn, HIGH), (zd, LOW), (zd, HIGH)]]


def gather_qkv_kernel(x_ref, lnw_ref, pos_ref, freq_ref, wq_ref, wk_ref, wv_ref,
                      hall_ref, ht_ref, q_out, k_out, kt_out, v_out, vt_out, cos_out, sin_out,
                      q_ref, k_ref, kt_ref, v_ref, vt_ref, cos_ref, sin_ref, w_scr, buf, tbuf, pos_all,
                      pos_send, pos_recv, send, recv, w_sem, load_sem, store_sem, t_sem, out_sem):
    me = lax.axis_index("sp")
    rows = x_ref.shape[0]
    half = rows // 2
    chunk = half // CHUNKS
    width = q_ref.shape[1]

    def block(owner, part, c):
        start = owner * rows + part * half
        return hall_ref.at[pl.ds(pl.multiple_of(start, half), half) if c is None else pl.ds(pl.multiple_of(start + c * chunk, chunk), chunk)]

    own = lambda part: block(me, part, None)
    loads = [pltpu.make_async_copy(x_ref.at[pl.ds(p * half, half)], buf.at[p], load_sem.at[p]) for p in range(SLOTS)]
    start_all(loads)
    column = lambda n: pl.ds(pl.multiple_of(me * n, n), n)
    w_copies = [pltpu.make_async_copy(wq_ref.at[:, column(width)], w_scr.at[:, pl.ds(0, width)], w_sem.at[0]),
                pltpu.make_async_copy(wk_ref.at[:, column(HEAD_DIM)], w_scr.at[:, pl.ds(width, HEAD_DIM)], w_sem.at[1]),
                pltpu.make_async_copy(wv_ref.at[:, column(HEAD_DIM)], w_scr.at[:, pl.ds(width + HEAD_DIM, HEAD_DIM)], w_sem.at[2])]
    start_all(w_copies)
    peers = everyone()
    greet(peers)
    pos_copies = [pltpu.make_async_remote_copy(src_ref=pos_ref, dst_ref=pos_all.at[me], send_sem=pos_send.at[i], recv_sem=pos_recv.at[i],
                                               device_id={"sp": p}, device_id_type=MESH) for i, p in enumerate(peers)]
    start_all(pos_copies)
    pos_all[me] = pos_ref[...]
    links = Exchange(send, recv, block, own, CHUNKS, True)
    stores = [pltpu.make_async_copy(buf.at[p], own(p), store_sem.at[p]) for p in range(SLOTS)]
    slab = half // 8
    for p in range(SLOTS):
        loads[p].wait()

        def norm(n, _):
            here = pl.ds(pl.multiple_of(n * slab, slab), slab)
            buf[p, here, :] = norm_f32(buf[p, here, :].astype(F32), lnw_ref[...]).astype(BF16)
            return 0

        lax.fori_loop(0, half // slab, norm, 0)
        stores[p].start()
    for p in range(SLOTS):
        stores[p].wait()
        links.first[p].start()
    start_all(links.second + links.to_own)
    receive(pos_copies)

    def t_copy(tslot, r0, n):
        return pltpu.make_async_copy(tbuf.at[tslot, :, pl.ds(0, n)], ht_ref.at[:, pl.ds(r0, n)], t_sem.at[tslot])

    def compute(slot, r0, n, first):
        r0 = pl.multiple_of(r0, n)
        out = pl.ds(r0, n)
        for t in range(n // LANE):
            at = r0 + t * LANE
            p = pos_all[at // rows, pl.ds((at % rows) // LANE, 1), :]
            angle = jnp.broadcast_to(p, (LANE, LANE)).T * freq_ref[...]
            sign = jnp.where(lax.broadcasted_iota(jnp.int32, (LANE, LANE), 1) % 2 == 0, -1.0, 1.0)
            tr = pl.ds(pl.multiple_of(at, LANE), LANE)
            cos_ref[tr, :] = jnp.cos(angle)
            sin_ref[tr, :] = jnp.sin(angle) * sign
        cos_t, sin_t = cos_ref[out, :], sin_ref[out, :]
        h = buf[slot, :n]
        tslot = slot % 2
        if not first:
            t_copy(tslot, 0, n).wait()
        tbuf[tslot, :, :n] = h.T
        t_copy(tslot, r0, n).start()
        for m in range(width // PAIR):
            y = dot(h, w_scr[:, m * PAIR:(m + 1) * PAIR])
            for e in range(SLOTS):
                q_ref[out, m * PAIR + e * LANE: m * PAIR + (e + 1) * LANE] = rotate(y[:, e * LANE:(e + 1) * LANE], cos_t, sin_t).astype(BF16)
        y = dot(h, w_scr[:, width:width + PAIR])
        k, v = rotate(y[:, :LANE], cos_t, sin_t), y[:, LANE:]
        k_ref[out, :] = k.astype(BF16)
        kt_ref[:, out] = k.T.astype(BF16)
        v_ref[out, :] = v.astype(BF16)
        vt_ref[:, out] = v.T.astype(BF16)
        for m, (src, dst) in enumerate(results):
            at = (slice(None), out) if src.shape[0] == HEAD_DIM else (out,)
            pltpu.make_async_copy(src.at[at], dst.at[at], out_sem.at[m]).start()

    results = list(zip((q_ref, k_ref, kt_ref, v_ref, vt_ref, cos_ref, sin_ref), (q_out, k_out, kt_out, v_out, vt_out, cos_out, sin_out)))

    def run(two, slot0, c=None, first=False, load=True):
        n = half if c is None else chunk
        if load:
            cps = [pltpu.make_async_copy(block(o, p, c), buf.at[slot0 + i, pl.ds(0, n)], load_sem.at[slot0 + i]) for i, (o, p) in enumerate(two)]
            start_all(cps)
            wait_all(cps)
        starts = [o * rows + p * half + (0 if c is None else c * chunk) for o, p in two]

        def body(i, _):
            compute(slot0 + i, starts[0] + i * (starts[1] - starts[0]), n, first)
            return 0

        lax.fori_loop(0, SLOTS, body, 0)

    groups = arrivals(me)
    wait_all(w_copies)
    run(groups[0][:2], 0, first=True, load=False)
    receive(links.to_own)
    run(groups[0][2:], 2)
    for g in range(SLOTS):
        links.near(g)
        run(groups[g + 1][:2], 0)
        receive(links.to_near[g])
        run(groups[g + 1][2:], 2)
    wait_all([t_copy(i, 0, half) for i in range(SLOTS)])
    for c in range(CHUNKS):
        links.far(c)
        run(groups[3][:2], 0, c, first=c == 0)
        receive(links.to_far[c])
        run(groups[3][2:], 2, c)
    wait_all([t_copy(i, 0, chunk) for i in range(SLOTS)])
    for m, (src, dst) in enumerate(results):
        pltpu.make_async_copy(src, dst, out_sem.at[m]).wait()
    links.finish()
    for c in pos_copies:
        c.wait_send()


def gather_qkv(x, ln_weight, pos, w_q, w_k, w_v, sp_size):
    rows, feat = x.shape
    seq = rows * sp_size
    width = w_q.shape[1] // sp_size
    inv_freq = ROPE_BASE ** (-jnp.arange(0, HEAD_DIM, 2, dtype=F32) / HEAD_DIM)
    freq = jnp.repeat(inv_freq, 2)[None, :]
    vmem = pl.BlockSpec(memory_space=pltpu.VMEM)
    made = [array(seq, width), array(seq, HEAD_DIM), array(HEAD_DIM, seq), array(seq, HEAD_DIM), array(HEAD_DIM, seq)]
    made += [array(seq, HEAD_DIM, dtype=F32)] * 2
    n = n_copies(CHUNKS, True)
    return pl.pallas_call(
        gather_qkv_kernel,
        in_specs=[HBM, vmem, vmem, vmem, HBM, HBM, HBM],
        out_specs=[HBM] * (2 + len(made)),
        out_shape=[array(seq, feat), array(feat, seq)] + made,
        scratch_shapes=[pltpu.VMEM(m.shape, m.dtype) for m in made] + [
            pltpu.VMEM((feat, width + PAIR), BF16), pltpu.VMEM((4, rows // 2, feat), BF16), pltpu.VMEM((SLOTS, feat, rows // 2), BF16),
            pltpu.VMEM((sp_size, rows // LANE, LANE), F32), SEM((N_PEERS,)), SEM((N_PEERS,)), SEM((n,)), SEM((n,)), SEM((3,)), SEM((4,)), SEM((SLOTS,)),
            SEM((SLOTS,)), SEM((len(made),))],
        compiler_params=remote_params(1),
        name="gather_qkv")(x, ln_weight.astype(F32)[None], pos.astype(F32).reshape(rows // LANE, LANE), freq, w_q, w_k, w_v)


def stack_heads(x):
    return jnp.concatenate([x[:, n * HEAD_DIM:(n + 1) * HEAD_DIM] for n in range(x.shape[1] // HEAD_DIM)], axis=0)


def causal(shape, bq, offset):
    rows = lax.rem(lax.broadcasted_iota(jnp.int32, shape, 0), bq) + offset
    return rows >= lax.broadcasted_iota(jnp.int32, shape, 1)


def fwd_step(qi, bq, bk, q_ref, kt_ref, v_ref, ot_ref, lse_ref, s_scr):
    q = stack_heads(q_ref[...])
    rows = q.shape[0]
    nfull = (qi * bq) // bk

    def scores(j):
        return dot(q, kt_ref[:, pl.ds(pl.multiple_of(j * bk, bk), bk)]) * (SCALE * LOG2E)

    def lane_max(m, s):
        for c in range(bk // LANE):
            m = jnp.maximum(m, s[:, c * LANE:(c + 1) * LANE])
        return m

    def score_step(j, m):
        s = scores(j)
        s_scr[j] = s
        return lane_max(m, s)

    m = lax.fori_loop(0, nfull, score_step, jnp.full((rows, LANE), -jnp.inf, F32))
    s = jnp.where(causal((rows, bk), bq, qi * bq - nfull * bk), scores(nfull), -jnp.inf)
    s_scr[nfull] = s
    m = jnp.max(lane_max(m, s), axis=1, keepdims=True)

    def value_step(j, carry):
        l, o = carry
        p = jnp.exp2(s_scr[j] - m)
        for t in range(bk // LANE):
            l = l + p[:, t * LANE:(t + 1) * LANE]
        o = o + dot(p.astype(BF16), v_ref[pl.ds(pl.multiple_of(j * bk, bk), bk), :])
        return l, o

    l, o = lax.fori_loop(0, nfull + 1, value_step, (jnp.zeros((rows, LANE), F32), jnp.zeros((rows, HEAD_DIM), F32)))
    l = jnp.sum(l, axis=1, keepdims=True)
    o = (o / l).astype(BF16)
    for n in range(rows // bq):
        ot_ref[n * HEAD_DIM:(n + 1) * HEAD_DIM, :] = o[n * bq:(n + 1) * bq].T
    lse_ref[...] = (m + jnp.log2(l)).reshape(lse_ref.shape)


def gather_fwd_kernel(n_fwd, relay, bq, bk, q_ref, kt_ref, v_ref, g_ref, wo_ref, ot_ref, lse_ref, gall_ref, do_ref,
                      s_scr, wo_scr, buf, send, recv, w_sem, load_sem, store_sem):
    step = pl.program_id(0)
    me = lax.axis_index("sp")
    rows, width = g_ref.shape[0], do_ref.shape[1]
    half = rows // 2
    chunk = half // CHUNKS

    def block(owner, part, c):
        start = owner * rows + part * half
        return gall_ref.at[pl.ds(pl.multiple_of(start, half), half) if c is None else pl.ds(pl.multiple_of(start + c * chunk, chunk), chunk)]

    own = lambda part: g_ref.at[pl.ds(part * half, half)]
    links = Exchange(send, recv, block, own, CHUNKS, True)
    w_copy = pltpu.make_async_copy(wo_ref.at[pl.ds(pl.multiple_of(me * width, width), width)], wo_scr, w_sem.at[0])
    loads = [pltpu.make_async_copy(own(i), buf.at[i], load_sem.at[i]) for i in range(SLOTS)]
    stores = [pltpu.make_async_copy(buf.at[i], block(me, i, None), store_sem.at[i]) for i in range(SLOTS)]

    @pl.when(step == 0)
    def _():
        greet(neighbours())
        links.begin()
        w_copy.start()
        start_all(loads)

    @pl.when(step == relay)
    def _():
        links.near(0)

    @pl.when(step < n_fwd)
    def _():
        fwd_step(step, bq, bk, q_ref, kt_ref, v_ref, ot_ref, lse_ref, s_scr)

    def run(two, slot0, c=None, load=True):
        n = half if c is None else chunk
        if load:
            cps = [pltpu.make_async_copy(block(o, p, c), buf.at[slot0 + i, pl.ds(0, n)], load_sem.at[slot0 + i]) for i, (o, p) in enumerate(two)]
            start_all(cps)
            wait_all(cps)
        starts = [o * rows + p * half + (0 if c is None else c * chunk) for o, p in two]

        def body(i, _):
            do_ref[pl.ds(pl.multiple_of(starts[0] + i * (starts[1] - starts[0]), n), n), :] = lax.dot_general(
                buf[slot0 + i, :n], wo_scr[...], (((1,), (1,)), ((), ())), preferred_element_type=F32).astype(BF16)
            return 0

        lax.fori_loop(0, SLOTS, body, 0)

    groups = arrivals(me)

    @pl.when(step == n_fwd)
    def _():
        wait_all(loads)
        start_all(stores)
        w_copy.wait()
        run(groups[0][:2], 0, load=False)
        wait_all(stores)
        receive(links.to_own)
        run(groups[0][2:], 2)
        for g in range(SLOTS):
            if g:
                links.near(g)
            run(groups[g + 1][:2], 0)
            receive(links.to_near[g])
            run(groups[g + 1][2:], 2)
        for c in range(CHUNKS):
            links.far(c)
            run(groups[3][:2], 0, c)
            receive(links.to_far[c])
            run(groups[3][2:], 2, c)
        links.finish()


def gather_forward(q, kt, v, g, w_o, bq=PAIR, bk=1024):
    seq, width = q.shape
    rows, feat = g.shape
    heads = width // HEAD_DIM
    n = seq // bq
    at = lambda i: jnp.minimum(i, n - 1)
    return pl.pallas_call(
        functools.partial(gather_fwd_kernel, n, (3 * n) // 4, bq, bk), grid=(n + 1,),
        in_specs=[pl.BlockSpec((bq, width), lambda i: (at(i), 0)), pl.BlockSpec((HEAD_DIM, seq), whole, **ONCE),
                  pl.BlockSpec((seq, HEAD_DIM), whole, **ONCE), HBM, HBM],
        out_specs=[pl.BlockSpec((width, bq), lambda i: (0, at(i))), pl.BlockSpec((heads, bq, 1), lambda i: (0, at(i), 0)), HBM,
                   pl.BlockSpec((seq, width), whole)],
        out_shape=[array(width, seq), array(heads, seq, 1, dtype=F32), array(seq, feat),
                   array(seq, width)],
        scratch_shapes=[pltpu.VMEM((seq // bk, heads * bq, bk), F32), pltpu.VMEM((width, feat), BF16), pltpu.VMEM((4, rows // 2, feat), BF16),
                        SEM((n_copies(CHUNKS, True),)), SEM((n_copies(CHUNKS, True),)), SEM((1,)), SEM((4,)), SEM((SLOTS,))],
        compiler_params=remote_params(2),
        name="gather_fwd")(q, kt, v, g, w_o)


def bwd_step(qi, bq, bk, q_ref, do_ref, lse_ref, k_ref, kt_ref, vt_ref, cos_ref, sin_ref, g_out, dkt_ref, dvt_ref, p_scr, dp_scr):
    q = stack_heads(q_ref[...])
    do = stack_heads(do_ref[...])
    rows = q.shape[0]
    lse = lse_ref[...].reshape(rows, 1)
    q_t = q.T
    do_t = do.T
    nfull = (qi * bq) // bk

    @pl.when(qi == 0)
    def _():
        dkt_ref[...] = jnp.zeros_like(dkt_ref)
        dvt_ref[...] = jnp.zeros_like(dvt_ref)

    def prob_step(j, r, masked):
        sl = pl.ds(pl.multiple_of(j * bk, bk), bk)
        s = dot(q, kt_ref[:, sl]) * (SCALE * LOG2E)
        p = jnp.exp2(s - lse)
        if masked:
            p = jnp.where(causal((rows, bk), bq, qi * bq - nfull * bk), p, 0.0)
        dp = dot(do, vt_ref[:, sl])
        pd = p * dp
        for t in range(bk // LANE):
            r = r + pd[:, t * LANE:(t + 1) * LANE]
        p_scr[j] = p
        dp_scr[j] = dp
        dvt_ref[:, sl] += dot(do_t, p.astype(BF16))
        return r

    r = lax.fori_loop(0, nfull, lambda j, r: prob_step(j, r, False), jnp.zeros((rows, LANE), F32))
    r = prob_step(nfull, r, True)
    r = jnp.sum(r, axis=1, keepdims=True)

    def grad_step(j, dq):
        sl = pl.ds(pl.multiple_of(j * bk, bk), bk)
        ds = (p_scr[j] * (dp_scr[j] - r) * SCALE).astype(BF16)
        dkt_ref[:, sl] += dot(q_t, ds)
        return dq + dot(ds, k_ref[sl, :])

    dq = lax.fori_loop(0, nfull + 1, grad_step, jnp.zeros((rows, HEAD_DIM), F32))
    dq = dq.astype(BF16).astype(F32)
    here = pl.ds(pl.multiple_of(qi * bq, bq), bq)
    cos_t, sin_t = cos_ref[here, :], sin_ref[here, :]
    for n in range(rows // bq):
        g_out[:, n * HEAD_DIM:(n + 1) * HEAD_DIM] = rotate(dq[n * bq:(n + 1) * bq], cos_t, -sin_t).astype(BF16)


def gather_bwd_kernel(relay, bq, bk, q_ref, do_ref, lse_ref, k_ref, kt_ref, vt_ref, cos_ref, sin_ref, ot_ref,
                      gq_ref, gk_ref, gv_ref, otg_ref, otz_ref, p_scr, dp_scr, dkt_scr, dvt_scr, buf, send, recv, z_send, z_recv, load_sem, store_sem):
    step = pl.program_id(0)
    last = pl.num_programs(0) - 1
    me = lax.axis_index("sp")
    width, seq = ot_ref.shape
    half = width // 2
    tokens = otz_ref.shape[2]
    zn = flip(me, CORE)
    own = lambda part: ot_ref.at[pl.ds(part * half, half)]
    block = lambda owner, part, _: otg_ref.at[owner // 2, pl.ds(part * half, half)]
    links = Exchange(send, recv, block, own, 1, False)
    xn, yn = flip(me, X_BIT), flip(me, Y_BIT)
    dn = flip(xn, Y_BIT)
    mine = pl.ds(pl.multiple_of(zn * tokens, tokens), tokens)

    def to_other(n, owner):
        src = ot_ref.at[:, mine] if n == 0 else otg_ref.at[owner // 2, :, mine]
        return pltpu.make_async_remote_copy(src_ref=src, dst_ref=otz_ref.at[owner // 2], send_sem=z_send.at[n], recv_sem=z_recv.at[n],
                                            device_id={"sp": zn}, device_id_type=MESH)

    z = [to_other(n, o) for n, o in enumerate((me, xn, yn, dn))]
    n_buf, slab = buf.shape[0], buf.shape[1]
    n_slab = width // slab

    def slab_copies(n):
        rows = pl.ds(pl.multiple_of(n * slab, slab), slab)
        slot = n % n_buf
        return (pltpu.make_async_copy(ot_ref.at[rows], buf.at[slot], load_sem.at[slot]),
                pltpu.make_async_copy(buf.at[slot], otg_ref.at[me // 2, rows], store_sem.at[slot]))

    @pl.when(step == 0)
    def _():
        greet(neighbours())
        links.begin()
        z[0].start()

    @pl.when(step == relay)
    def _():
        links.near(0)

    @pl.when((step >= 2) & (step < n_slab + 2))
    def _():
        slab_copies(step - 2)[1].wait()

    @pl.when((step >= 1) & (step < n_slab + 1))
    def _():
        slab_copies(step - 1)[0].wait()
        slab_copies(step - 1)[1].start()

    @pl.when(step < n_slab)
    def _():
        slab_copies(step)[0].start()

    bwd_step(step, bq, bk, q_ref, do_ref, lse_ref, k_ref, kt_ref, vt_ref, cos_ref, sin_ref, gq_ref, dkt_scr, dvt_scr, p_scr, dp_scr)

    @pl.when(step == last)
    def _():
        links.near(1)
        start_all(z[1:3])

        def kv_rows(i, _):
            rows = pl.ds(pl.multiple_of(i * bk, bk), bk)
            dk = dkt_scr[:, rows].T.astype(BF16).astype(F32)
            gk_ref[rows, :] = rotate(dk, cos_ref[rows, :], -sin_ref[rows, :]).astype(BF16)
            gv_ref[rows, :] = dvt_scr[:, rows].T.astype(BF16)
            return 0

        lax.fori_loop(0, seq // bk, kv_rows, 0)
        links.far(0)
        z[3].start()
        receive(z)
        links.finish()
        for c in z:
            c.wait_send()


def gather_backward(q, do, lse, k, kt, vt, cos_t, sin_t, ot, sp_size, bq=PAIR, bk=512):
    seq, width = q.shape
    heads = width // HEAD_DIM
    chips, tokens = sp_size // 2, seq // sp_size
    n = seq // bq
    tile = pl.BlockSpec((bq, width), row)
    tall = pl.BlockSpec((seq, HEAD_DIM), whole, **ONCE)
    wide = pl.BlockSpec((HEAD_DIM, seq), whole, **ONCE)
    return pl.pallas_call(
        functools.partial(gather_bwd_kernel, (9 * n) // 16, bq, bk), grid=(n,),
        in_specs=[tile, tile, pl.BlockSpec((heads, bq, 1), lambda i: (0, i, 0)), tall, wide, wide, tall, tall, HBM],
        out_specs=[tile, tall, tall, HBM, HBM],
        out_shape=[array(seq, width), array(seq, HEAD_DIM), array(seq, HEAD_DIM), array(chips, width, seq), array(chips, width, tokens)],
        scratch_shapes=[pltpu.VMEM((seq // bk, heads * bq, bk), F32), pltpu.VMEM((seq // bk, heads * bq, bk), F32),
                        pltpu.VMEM((HEAD_DIM, seq), F32), pltpu.VMEM((HEAD_DIM, seq), F32), pltpu.VMEM((SLOTS, width // 8, seq), BF16),
                        SEM((n_copies(1, False),)), SEM((n_copies(1, False),)), SEM((4,)), SEM((4,)), SEM((SLOTS,)), SEM((SLOTS,))],
        compiler_params=remote_params(3),
        name="gather_bwd")(q, do, lse, k, kt, vt, cos_t, sin_t, ot)


def dw_o_kernel(core_ref, ot_ref, g_ref, final_ref, send_ref):
    y = dot(ot_ref[...], g_ref[...]).astype(BF16)
    final_ref[...] = y
    send_ref[...] = y


def dw_o_half(core, ot_all, g_all, bn=1024):
    half, width, seq = ot_all.shape
    feat = g_all.shape[1]
    return pl.pallas_call(
        dw_o_kernel,
        grid_spec=pltpu.PrefetchScalarGridSpec(
            num_scalar_prefetch=1, grid=(feat // bn, half),
            in_specs=[pl.BlockSpec((None, width, seq), lambda j, s, c: (s, 0, 0)), pl.BlockSpec((seq, bn), col)],
            out_specs=[pl.BlockSpec((width, bn), lambda j, s, c: (2 * s + c[0], j)), pl.BlockSpec((width, bn), lambda j, s, c: (s, j))]),
        out_shape=[array(2 * half * width, feat), array(half * width, feat)],
        compiler_params=PARAMS, cost_estimate=cost(2 * half * width * feat * seq), name="dw_o_half")(core, ot_all, g_all)


def out_kernel(ids_ref, mine_ref, other_ref, w_ref, out_ref, o_scr):
    @pl.when(pl.program_id(0) == 0)
    def _():
        core = lax.rem(ids_ref[0], 2)
        width = mine_ref.shape[1]
        for s in range(mine_ref.shape[0]):
            for ref, d in ((mine_ref, 2 * s + core), (other_ref, 2 * s + 1 - core)):
                o_scr[:, pl.ds(pl.multiple_of(d * width, width), width)] = ref[s].T

    out_ref[...] = dot(o_scr[...], w_ref[...]).astype(BF16)


def out_proj(ids, ot_all, ot_other, w_o, bn=512):
    chips, width, tokens = ot_other.shape
    feat = w_o.shape[1]
    return pl.pallas_call(
        out_kernel,
        grid_spec=pltpu.PrefetchScalarGridSpec(
            num_scalar_prefetch=1, grid=(feat // bn,),
            in_specs=[pl.BlockSpec((chips, width, tokens), lambda i, c: (0, 0, c[0]), **ONCE), pl.BlockSpec((chips, width, tokens), lambda i, c: (0, 0, 0), **ONCE),
                      pl.BlockSpec((w_o.shape[0], bn), col)],
            out_specs=pl.BlockSpec((tokens, bn), col),
            scratch_shapes=[pltpu.VMEM((tokens, w_o.shape[0]), BF16)]),
        out_shape=array(tokens, feat), compiler_params=PARAMS, cost_estimate=cost(2 * tokens * w_o.size), name="out_proj")(ids, ot_all, ot_other, w_o)


def dw_q_kernel(ids_ref, ht_ref, g_ref, final_ref, low_ref, high_ref):
    i = pl.program_id(0)
    y = dot(ht_ref[...], g_ref[...]).astype(BF16)
    final_ref[...] = y
    n = pl.num_programs(0) // 2

    @pl.when(i < n)
    def _():
        low_ref[...] = y

    @pl.when(i >= n)
    def _():
        high_ref[...] = y


def dw_q_own(ids, ht, gq, bm=512):
    feat, seq = ht.shape
    w = gq.shape[1]
    n = feat // bm
    return pl.pallas_call(
        dw_q_kernel,
        grid_spec=pltpu.PrefetchScalarGridSpec(
            num_scalar_prefetch=1, grid=(n,), in_specs=[pl.BlockSpec((bm, seq), row), pl.BlockSpec((seq, w), whole, **ONCE)],
            out_specs=[pl.BlockSpec((bm, w), lambda i, c: (i, c[0])), pl.BlockSpec((bm, w), lambda i, c: (jnp.minimum(i, n // 2 - 1), 0)),
                       pl.BlockSpec((bm, w), lambda i, c: (jnp.maximum(i - n // 2, 0), 0))]),
        out_shape=[array(feat, feat), array(feat // 2, w), array(feat // 2, w)],
        compiler_params=PARAMS, cost_estimate=cost(2 * seq * feat * w), name="dw_q_own")(ids, ht, gq)


class Ride:
    def __init__(self, source, buf, targets, load_sem, store_sem):
        self.source, self.buf, self.targets, self.load_sem, self.store_sem = source, buf, targets, load_sem, store_sem

    def load(self, i):
        slot = lax.rem(i, SLOTS)
        return pltpu.make_async_copy(self.source(i), self.buf.at[slot], self.load_sem.at[slot])

    def stores(self, i):
        slot = lax.rem(i, SLOTS)
        return [pltpu.make_async_copy(src, dst, self.store_sem.at[slot, n]) for n, (src, dst) in enumerate(self.targets(i, self.buf.at[slot]))]

    def begin(self, i):
        @pl.when(i >= SLOTS)
        def _():
            wait_all(self.stores(i - SLOTS))

        self.load(i).start()

    def end(self, i, last):
        self.load(i).wait()
        start_all(self.stores(i))

        @pl.when(i == last)
        def _():
            for n in reversed(range(SLOTS)):
                wait_all(self.stores(i - n))


def kv_columns(rows, src, k_ref, v_ref, owners):
    out = []
    for m, ref in enumerate((k_ref, v_ref)):
        for n, dev in enumerate(owners):
            at = (m * len(owners) + n) * HEAD_DIM
            out.append((src.at[:, at:at + HEAD_DIM], ref.at[rows, pl.ds(pl.multiple_of(dev * HEAD_DIM, HEAD_DIM), HEAD_DIM)]))
    return out


def dw_kv_kernel(n_dev, ids_ref, ht_ref, *refs):
    parts, refs = refs[:2 * n_dev], refs[2 * n_dev:]
    k_ref, v_ref, send_ref, x_scr, y_scr, y_sem, send_sem, x_sem, load_sem = refs
    i, last = grid_place()
    bm, feat = ht_ref.shape[0], k_ref.shape[0]
    n_tok = send_ref.shape[0] - feat
    tokens = pltpu.make_async_copy(x_scr.at[pl.ds(pl.multiple_of(flip(ids_ref[0], CORE) * n_tok, n_tok), n_tok)], send_ref.at[pl.ds(feat, n_tok)], x_sem.at[0])
    owners = [ids_ref[1 + n] for n in range(n_dev)]

    @pl.when(i == 0)
    def _():
        loads = [pltpu.make_async_copy(p, x_scr.at[:, m * HEAD_DIM:(m + 1) * HEAD_DIM], load_sem.at[m]) for m, p in enumerate(parts)]
        start_all(loads)
        wait_all(loads)
        tokens.start()

    def stores(step):
        slot, rows = lax.rem(step, SLOTS), pl.ds(pl.multiple_of(step * bm, bm), bm)
        out = [pltpu.make_async_copy(src, dst, y_sem.at[slot, m]) for m, (src, dst) in enumerate(kv_columns(rows, y_scr.at[slot], k_ref, v_ref, owners))]
        return out + [pltpu.make_async_copy(y_scr.at[slot], send_ref.at[rows], send_sem.at[slot])]

    @pl.when(i >= SLOTS)
    def _():
        wait_all(stores(i - SLOTS))

    y_scr[lax.rem(i, SLOTS)] = dot(ht_ref[...], x_scr[...]).astype(BF16)
    start_all(stores(i))

    @pl.when(i == last)
    def _():
        tokens.wait()
        for m in reversed(range(SLOTS)):
            wait_all(stores(i - m))


def dw_kv_half(ids, ht, parts, shape, tokens, bm=512):
    feat, seq = ht.shape
    w = len(parts) * HEAD_DIM
    steps = feat // bm
    return pl.pallas_call(
        functools.partial(dw_kv_kernel, len(parts) // 2),
        grid_spec=pltpu.PrefetchScalarGridSpec(
            num_scalar_prefetch=1, grid=(steps,), in_specs=[pl.BlockSpec((bm, seq), row)] + [HBM] * len(parts), out_specs=[HBM] * 3,
            scratch_shapes=[pltpu.VMEM((seq, w), BF16), pltpu.VMEM((SLOTS, bm, w), BF16), SEM((SLOTS, len(parts))), SEM((SLOTS,)), SEM((1,)), SEM((len(parts),))]),
        out_shape=[array(*shape), array(*shape), array(feat + tokens, w)],
        compiler_params=PARAMS, cost_estimate=cost(2 * seq * feat * w), name="dw_kv_half")(ids, ht, *parts)


def dh_kernel(n_dev, ids_ref, wq_ref, wk_ref, wv_ref, x_ref, lnw_ref, tq_ref, t_ref, *refs):
    own, refs = refs[:2 * n_dev], refs[2 * n_dev:]
    kv_recv, o_recv, _, _, _, dx_ref, dlnw_ref, k_ref, v_ref, o_ref, g_scr, hat_scr, rstd_scr, sum_scr, dy_scr, *scratch = refs
    i, last = grid_place()
    tokens, feat = x_ref.shape
    bf = wq_ref.shape[0]
    others = [ids_ref[1 + n_dev + n] for n in range(n_dev)]
    kv_buf, o_buf = scratch[0], scratch[3]
    core = lax.rem(ids_ref[0], 2)
    block_rows = lambda i, buf: pl.ds(pl.multiple_of(i * buf.shape[1], buf.shape[1]), buf.shape[1])

    def o_rows(i):
        n = o_buf.shape[1]
        per = HEAD_DIM * n_dev // n
        return pl.ds(pl.multiple_of(((2 * (i // per) + 1 - core) * per + lax.rem(i, per)) * n, n), n)

    rides = [Ride(lambda i: kv_recv.at[block_rows(i, kv_buf)], kv_buf, lambda i, src: kv_columns(block_rows(i, kv_buf), src, k_ref, v_ref, others), *scratch[1:3]),
             Ride(lambda i: o_recv.at[block_rows(i, o_buf)], o_buf, lambda i, src: [(src, o_ref.at[o_rows(i)])], *scratch[4:])]
    for r in rides:
        r.begin(i)
    nq, nk = wq_ref.shape[1], wk_ref.shape[1]
    slab = tokens // 8

    @pl.when(i == 0)
    def _():
        width = tq_ref.shape[1]
        for m in range(2 * n_dev):
            g_scr[m * width:(m + 1) * width, :] = tq_ref[m * tokens:(m + 1) * tokens, :].T
        t = t_ref[...].T
        for m in range(2 * n_dev):
            for x, dev in ((own[m][...].T, ids_ref[1 + m % n_dev]), (t[m * HEAD_DIM:(m + 1) * HEAD_DIM], others[m % n_dev])):
                g_scr[pl.ds(pl.multiple_of(nq + (m // n_dev) * nk + dev * HEAD_DIM, HEAD_DIM), HEAD_DIM), :] = x

        def stats(m, _):
            here = pl.ds(pl.multiple_of(m * slab, slab), slab)
            x = x_ref[here, :].astype(F32)
            centered = x - jnp.mean(x, axis=-1, keepdims=True)
            rstd = lax.rsqrt(jnp.mean(centered * centered, axis=-1, keepdims=True) + LN_EPS)
            hat_scr[here, :] = centered * rstd
            rstd_scr[here, :] = jnp.broadcast_to(rstd, (slab, LANE))
            return 0

        lax.fori_loop(0, tokens // slab, stats, 0)
        sum_scr[...] = jnp.zeros_like(sum_scr)

    y = (dot(wq_ref[...], g_scr[:nq, :]) + dot(wk_ref[...], g_scr[nq:nq + nk, :]) + dot(wv_ref[...], g_scr[nq + nk:, :])).T
    at = pl.ds(pl.multiple_of(i * bf, bf), bf)
    hat = hat_scr[:, at]
    dlnw_ref[...] = jnp.sum(y * hat, axis=0, keepdims=True)
    y = y * lnw_ref[...]
    dy_scr[:, at] = y
    yh = y * hat
    for m in range(bf // LANE):
        part = slice(m * LANE, (m + 1) * LANE)
        sum_scr[0] += y[:, part]
        sum_scr[1] += yh[:, part]
    for r in rides:
        r.end(i, last)

    @pl.when(i == last)
    def _():
        def finish(m, _):
            here = pl.ds(pl.multiple_of(m * slab, slab), slab)
            mean_y, mean_yh = (jnp.sum(sum_scr[e, here, :], axis=1, keepdims=True) / feat for e in range(SLOTS))
            dx_ref[here, :] = (rstd_scr[here, :1] * (dy_scr[here, :] - mean_y - hat_scr[here, :] * mean_yh)).astype(BF16)
            return 0

        lax.fori_loop(0, tokens // slab, finish, 0)


def dh_proj(ids, w_q, w_k, w_v, x, ln_weight, t_q, own, kv_recv, o_recv, finals, bf=512):
    tokens, feat = x.shape
    w = kv_recv.shape[1]
    n = len(own)
    ins = [w_q, w_k, w_v, x, ln_weight.astype(F32)[None], t_q, kv_recv, *own, kv_recv, o_recv, *finals]
    specs = [pl.BlockSpec((bf, m.shape[1]), row) for m in (w_q, w_k, w_v)] + [pl.BlockSpec(x.shape, whole, **ONCE), pl.BlockSpec((1, bf), col)]
    specs += [pl.BlockSpec(t_q.shape, whole, **ONCE), pl.BlockSpec((tokens, w), lambda i, c: (feat // tokens, 0), **ONCE)]
    specs += [pl.BlockSpec((tokens, HEAD_DIM), lambda i, c: (c[0], 0), **ONCE) for _ in own]
    first = len(ins) - len(finals)
    steps = feat // bf
    return pl.pallas_call(
        functools.partial(dh_kernel, n // 2),
        grid_spec=pltpu.PrefetchScalarGridSpec(
            num_scalar_prefetch=1, grid=(steps,), in_specs=specs + [HBM] * (len(ins) - len(specs)),
            out_specs=[pl.BlockSpec(x.shape, whole, **ONCE), pl.BlockSpec((1, bf), col)] + [HBM] * len(finals),
            scratch_shapes=[pltpu.VMEM((w_q.shape[1] + 2 * w_k.shape[1], tokens), BF16), pltpu.VMEM(x.shape, F32), pltpu.VMEM((tokens, LANE), F32),
                            pltpu.VMEM((SLOTS, tokens, LANE), F32), pltpu.VMEM(x.shape, F32),
                            pltpu.VMEM((SLOTS, feat // steps, w), BF16), SEM((SLOTS,)), SEM((SLOTS, n)),
                            pltpu.VMEM((SLOTS, o_recv.shape[0] // steps, feat), BF16), SEM((SLOTS,)), SEM((SLOTS, 1))]),
        out_shape=[array(tokens, feat), array(1, feat, dtype=F32)] + [array(*f.shape) for f in finals],
        input_output_aliases={1 + first + m: 2 + m for m in range(len(finals))},
        compiler_params=PARAMS, cost_estimate=cost(2 * tokens * (w_q.size + 2 * w_k.size)), name="dh_proj")(ids, *ins)


def copy_kernel(n, places, ids_ref, *refs):
    final, buf, load_sem, store_sem = refs[n + 1:]
    rows, w = buf.shape[1:]
    loads = [pltpu.make_async_copy(refs[m], buf.at[m], load_sem.at[m]) for m in range(n)]
    start_all(loads)
    stores = []
    for m, (owner, half) in enumerate(places):
        loads[m].wait()
        at = pl.ds(pl.multiple_of(ids_ref[owner] * w, w), w)
        stores.append(pltpu.make_async_copy(buf.at[m], final.at[pl.ds(half * rows, rows), at], store_sem.at[m]))
        stores[-1].start()
    wait_all(stores)


def copy_in(ids, blocks, places, final):
    n = len(blocks)
    return pl.pallas_call(
        functools.partial(copy_kernel, n, places),
        grid_spec=pltpu.PrefetchScalarGridSpec(num_scalar_prefetch=1, grid=(1,), in_specs=[HBM] * (n + 1), out_specs=HBM,
                                               scratch_shapes=[pltpu.VMEM((n,) + blocks[0].shape, BF16), SEM((n,)), SEM((n,))]),
        out_shape=array(*final.shape), input_output_aliases={n + 1: 0}, compiler_params=PARAMS, name="copy_in")(ids, *blocks, final)


def sum_kernel(x_ref, out_ref, all_scr, send, recv):
    me = lax.axis_index("sp")
    peers = everyone()
    greet(peers)
    copies = [pltpu.make_async_remote_copy(src_ref=x_ref, dst_ref=all_scr.at[me], send_sem=send.at[n], recv_sem=recv.at[n],
                                           device_id={"sp": p}, device_id_type=MESH) for n, p in enumerate(peers)]
    for c in copies:
        c.start()
    all_scr[me] = x_ref[...]
    for c in copies:
        c.wait_recv()
    total = all_scr[0]
    for n in range(1, all_scr.shape[0]):
        total = total + all_scr[n]
    out_ref[...] = total.astype(BF16)
    for c in copies:
        c.wait_send()


def sum_devices(x, sp_size):
    n = x.shape[0] // HEAD_DIM
    vmem = pl.BlockSpec(memory_space=pltpu.VMEM)
    return pl.pallas_call(
        sum_kernel, in_specs=[vmem], out_specs=vmem, out_shape=array(n, HEAD_DIM),
        scratch_shapes=[pltpu.VMEM((sp_size, n, HEAD_DIM), F32), SEM((sp_size - 1,)), SEM((sp_size - 1,))],
        compiler_params=remote_params(4), name="sum_devices")(x.reshape(n, HEAD_DIM)).reshape(-1)


def solution(mesh):
    sp_size = mesh.shape['sp']
    row_spec = P(('dp', 'sp'), None)
    pos_spec = P(('dp', 'sp'))
    full_spec = P(None, None)
    grad_spec = P('dp', None)

    def local_step(hidden, positions, d_attn, ln_weight, w_q, w_k, w_v, w_o):
        dev = lax.axis_index('sp')
        core = lax.rem(dev, SLOTS)
        local_rows, _ = hidden.shape
        _, ht, q, k, kt, v, vt, cos_t, sin_t = gather_qkv(hidden, ln_weight, positions, w_q, w_k, w_v, sp_size)
        ot, lse, g_all, do = gather_forward(q, kt, v, d_attn, w_o)
        gq, gk, gv, ot_all, ot_other = gather_backward(q, do, lse, k, kt, vt, cos_t, sin_t, ot, sp_size)
        other = lambda d: flip(d, CORE)
        dev_x, dev_y = flip(dev, X_BIT), flip(dev, Y_BIT)
        dev_d = flip(dev_x, Y_BIT)
        owners = [dev, dev_x, dev_y, dev_d]

        def to(x, bit):
            return lax.ppermute(x, 'sp', [(i, i ^ bit) for i in range(sp_size)])

        after = lambda x, *done: lax.optimization_barrier((x,) + done)[0]
        ids = lambda *d: jnp.stack(d)
        gk_x, gv_y, gv_x, gk_y = to(gk, X_BIT), to(gv, Y_BIT), to(gv, X_BIT), to(gk, Y_BIT)
        t_q = lax.all_to_all(gq, 'sp', 0, 0, tiled=True)
        dw_q, low, high = dw_q_own(dev.reshape(1), ht, gq)
        gk_d, gv_d = to(after(gk_x, low), Y_BIT), to(after(gv_y, low), X_BIT)
        low_x, high_y, high_x, low_y = to(low, X_BIT), to(high, Y_BIT), to(high, X_BIT), to(low, Y_BIT)
        low_z, high_z = to(low, CORE), to(high, CORE)
        dw_o, o_send = dw_o_half(after(core.reshape(1), low), ot_all, g_all)
        o_recv = to(o_send, CORE)
        parts = [gk, gk_x, gk_y, gk_d, gv, gv_x, gv_y, gv_d]
        dw_k, dw_v, kv_send = dw_kv_half(ids(*owners[:1], *owners), ht, [after(parts[0], o_send)] + parts[1:], w_k.shape, local_rows)
        kv_recv = to(kv_send, CORE)
        attn_out = out_proj(dev.reshape(1), ot_all, ot_other, after(w_o, kv_send))
        low_d, high_d = to(after(low_x, attn_out), Y_BIT), to(after(high_y, attn_out), X_BIT)
        low_zx, high_zy = to(after(low_x, attn_out), CORE), to(after(high_y, attn_out), CORE)
        dx, d_lnw, dw_k, dw_v, dw_o = dh_proj(ids(*owners[:1], *owners, *map(other, owners)), w_q, w_k, w_v, hidden, ln_weight, t_q, parts, kv_recv, o_recv, [dw_k, dw_v, dw_o])
        high_zx, low_zy = to(after(high_x, dx), CORE), to(after(low_y, dx), CORE)
        d_lnw = sum_devices(d_lnw.reshape(-1), sp_size)
        near = [other(dev), dev_x, dev_y, other(dev_x), other(dev_y)]
        blocks = [low_z, high_z, low_x, high_x, low_y, high_y, low_zx, high_zx, low_zy, high_zy]
        dw_q = copy_in(ids(*near), blocks, [(n // 2, n % 2) for n in range(len(blocks))], after(dw_q, d_lnw))
        low_zd, high_zd = to(after(low_d, dw_q), CORE), to(after(high_d, dw_q), CORE)
        blocks = [low_d, high_d, low_zd, high_zd]
        dw_q = copy_in(ids(dev_d, other(dev_d)), blocks, [(n // 2, n % 2) for n in range(len(blocks))], dw_q)
        return (attn_out, dx, d_lnw, dw_q, dw_k, dw_v, dw_o)

    return jax.shard_map(local_step, mesh=mesh,
                      in_specs=(row_spec, pos_spec, row_spec, P(None), full_spec, full_spec, full_spec, full_spec),
                      out_specs=(row_spec, row_spec, P('dp'), grad_spec, grad_spec, grad_spec, grad_spec),
                      check_vma=False)
```

```python
import functools
import jax
import jax.numpy as jnp
from jax import lax
from jax.experimental import pallas as pl
from jax.experimental.pallas import tpu as pltpu
from jax.sharding import PartitionSpec as P

HEAD_DIM = LANE = 128
PAIR = 2 * HEAD_DIM
CORE, X_BIT, Y_BIT = 1, 2, 4
LOW, HIGH, SLOTS = 0, 1, 2
CHUNKS, N_PEERS = 2, 7
LN_EPS = 1e-5
ROPE_BASE = 10000.0
SCALE = HEAD_DIM ** -0.5
LOG2E = 1.4426950408889634
VMEM_LIMIT = 67_000_000
BF16 = jnp.bfloat16
F32 = jnp.float32
MESH = pl.DeviceIdType.MESH
HBM = pl.BlockSpec(memory_space=pl.ANY)
SEM = pltpu.SemaphoreType.DMA
row = lambda i, *_: (i, 0)
col = lambda i, *_: (0, i)
whole = lambda *_: (0, 0)
ONCE = dict(pipeline_mode=pl.Buffered(1))
PARAMS = pltpu.CompilerParams(vmem_limit_bytes=VMEM_LIMIT)


def grid_place():
    return pl.program_id(0), pl.num_programs(0) - 1


def dot(x, y):
    return jnp.dot(x, y, preferred_element_type=F32)


def array(*shape, dtype=BF16):
    return jax.ShapeDtypeStruct(shape, dtype)


def remote_params(number):
    return pltpu.CompilerParams(collective_id=number, has_side_effects=True, vmem_limit_bytes=VMEM_LIMIT)


def cost(flops):
    return pl.CostEstimate(flops=flops, bytes_accessed=flops // HEAD_DIM, transcendentals=0)


def rotate(x, cos_t, sin_t):
    lane = lax.broadcasted_iota(jnp.int32, x.shape, 1)
    swapped = jnp.where(lane % 2 == 0, pltpu.roll(x, HEAD_DIM - 1, 1), pltpu.roll(x, 1, 1))
    return x * cos_t + swapped * sin_t


def flip(i, bit):
    return i + bit - 2 * bit * ((i // bit) % 2)


class Exchange:
    def __init__(self, send, recv, block, own, chunks, partner):
        me = lax.axis_index("sp")
        xn, yn, zn = flip(me, X_BIT), flip(me, Y_BIT), flip(me, CORE)
        dn = flip(xn, Y_BIT)
        self.every = []

        def copy(owner, part, to, chunk=None):
            n = len(self.every)
            src = own(part) if owner is me else block(owner, part, chunk)
            self.every.append(pltpu.make_async_remote_copy(src_ref=src, dst_ref=block(owner, part, chunk), send_sem=send.at[n], recv_sem=recv.at[n],
                                                           device_id={"sp": to}, device_id_type=MESH))
            return self.every[-1]

        self.first = [copy(me, LOW, xn), copy(me, HIGH, yn)]
        self.second = [copy(me, HIGH, xn), copy(me, LOW, yn)]
        self.relay = [[copy(xn, LOW, yn, c), copy(yn, HIGH, xn, c)] for c in range(chunks)]
        if partner:
            self.to_own = [copy(me, LOW, zn), copy(me, HIGH, zn)]
            self.to_near = [[copy(xn, LOW, zn), copy(yn, HIGH, zn)], [copy(xn, HIGH, zn), copy(yn, LOW, zn)]]
            self.to_far = [[copy(dn, LOW, zn, c), copy(dn, HIGH, zn, c)] for c in range(chunks)]

    def begin(self):
        start_all(self.first)
        if hasattr(self, "to_own"):
            start_all(self.to_own)
        start_all(self.second)

    def near(self, n):
        for m, c in enumerate(self.second if n else self.first):
            c.wait_recv()
            if n == 0:
                start_all([r[m] for r in self.relay])
            if hasattr(self, "to_near"):
                self.to_near[n][m].start()

    def far(self, n):
        for m, c in enumerate(self.relay[n]):
            c.wait_recv()
            if hasattr(self, "to_far"):
                self.to_far[n][m].start()

    def finish(self):
        for c in self.every:
            c.wait_send()


def start_all(copies):
    for c in copies:
        c.start()


def wait_all(copies):
    for c in copies:
        c.wait()


def receive(copies):
    for c in copies:
        c.wait_recv()


def n_copies(chunks, partner):
    return 4 + 2 * chunks + (6 + 2 * chunks if partner else 0)


def greet(peers):
    barrier = pltpu.get_barrier_semaphore()
    for p in peers:
        pl.semaphore_signal(barrier, inc=1, device_id={"sp": p}, device_id_type=MESH)
    pl.semaphore_wait(barrier, len(peers))


def neighbours():
    me = lax.axis_index("sp")
    return [flip(me, CORE), flip(me, X_BIT), flip(me, Y_BIT)]


def everyone():
    me = lax.axis_index("sp")
    xn, yn = flip(me, X_BIT), flip(me, Y_BIT)
    dn = flip(xn, Y_BIT)
    return [flip(me, CORE), xn, flip(xn, CORE), yn, flip(yn, CORE), dn, flip(dn, CORE)]


def arrival(i, e):
    me = lax.axis_index("sp")
    g, near = i // 2, (i // 2 + 1) // 2
    owner = me + (i % 2) * (flip(me, CORE) - me) + near * ((1 - e) * (flip(me, X_BIT) - me) + e * (flip(me, Y_BIT) - me))
    return owner, e + (g // 2) * (1 - 2 * e)


def in_order(links, start, then, load, work, half, chunk, started=False):
    rows = 2 * half

    def second():
        then()
        receive(links.to_own)

    steps = [start, second, (lambda: None) if started else (lambda: links.near(0)), lambda: receive(links.to_near[0]), lambda: links.near(1),
             lambda: receive(links.to_near[1])]

    def sweep(n_pairs, steps, place, n, fetch_from):
        def pair(i, _):
            for m, act in enumerate(steps):
                @pl.when(i == m)
                def _():
                    act()
            slot0 = 2 * (i % 2)
            at = [place(i, e) for e in range(SLOTS)]
            copies = [load(slot0 + e, at[e], n) for e in range(SLOTS)]

            @pl.when(i >= fetch_from)
            def _():
                start_all(copies)
                wait_all(copies)

            def one(e, _):
                work(slot0 + e, at[0] + e * (at[1] - at[0]), n, i == 0)
                return 0

            return lax.fori_loop(0, SLOTS, one, 0)

        lax.fori_loop(0, n_pairs, pair, 0)

    def place(i, e):
        owner, part = arrival(i, e)
        return owner * rows + part * half

    sweep(len(steps), steps, place, half, 1)
    me = lax.axis_index("sp")
    dn = flip(flip(me, X_BIT), Y_BIT)

    def far_place(i, e):
        return (dn + (i % 2) * (flip(me, CORE) - me)) * rows + e * half + (i // 2) * chunk

    steps = []
    for c in range(CHUNKS):
        steps += [functools.partial(links.far, c), functools.partial(receive, links.to_far[c])]
    return lambda: sweep(len(steps), steps, far_place, chunk, 0)


def gather_qkv_kernel(x_ref, lnw_ref, pos_ref, freq_ref, wq_ref, wk_ref, wv_ref,
                      hall_ref, ht_ref, q_out, k_out, kt_out, v_out, vt_out, cos_out, sin_out, stat_ref,
                      q_ref, k_ref, kt_ref, v_ref, vt_ref, cos_ref, sin_ref, w_scr, buf, tbuf, pos_all,
                      pos_send, pos_recv, send, recv, w_sem, load_sem, store_sem, t_sem, out_sem):
    me = lax.axis_index("sp")
    rows = x_ref.shape[0]
    half = rows // 2
    chunk = half // CHUNKS
    width = q_ref.shape[1]

    def block(owner, part, c):
        start = owner * rows + part * half
        return hall_ref.at[pl.ds(pl.multiple_of(start, half), half) if c is None else pl.ds(pl.multiple_of(start + c * chunk, chunk), chunk)]

    own = lambda part: block(me, part, None)
    loads = [pltpu.make_async_copy(x_ref.at[pl.ds(p * half, half)], buf.at[p], load_sem.at[p]) for p in range(SLOTS)]
    start_all(loads)
    column = lambda n: pl.ds(pl.multiple_of(me * n, n), n)
    w_copies = [pltpu.make_async_copy(wq_ref.at[:, column(width)], w_scr.at[:, pl.ds(0, width)], w_sem.at[0]),
                pltpu.make_async_copy(wk_ref.at[:, column(HEAD_DIM)], w_scr.at[:, pl.ds(width, HEAD_DIM)], w_sem.at[1]),
                pltpu.make_async_copy(wv_ref.at[:, column(HEAD_DIM)], w_scr.at[:, pl.ds(width + HEAD_DIM, HEAD_DIM)], w_sem.at[2])]
    start_all(w_copies)
    peers = everyone()
    greet(peers)
    pos_copies = [pltpu.make_async_remote_copy(src_ref=pos_ref, dst_ref=pos_all.at[me], send_sem=pos_send.at[i], recv_sem=pos_recv.at[i],
                                               device_id={"sp": p}, device_id_type=MESH) for i, p in enumerate(peers)]
    start_all(pos_copies)
    pos_all[me] = pos_ref[...]
    links = Exchange(send, recv, block, own, CHUNKS, True)
    stores = [pltpu.make_async_copy(buf.at[p], own(p), store_sem.at[p]) for p in range(SLOTS)]
    slab = half // 8
    for p in range(SLOTS):
        loads[p].wait()

        def norm(n, _):
            here = pl.ds(pl.multiple_of(n * slab, slab), slab)
            x = buf[p, here, :].astype(F32)
            mean = jnp.mean(x, axis=-1, keepdims=True)
            centered = x - mean
            rstd = lax.rsqrt(jnp.mean(centered * centered, axis=-1, keepdims=True) + LN_EPS)
            buf[p, here, :] = (centered * rstd * lnw_ref[...]).astype(BF16)
            for m, v in enumerate((mean, rstd)):
                stat_ref[m, pl.ds(pl.multiple_of(p * half + n * slab, slab), slab), :] = jnp.broadcast_to(v, (slab, LANE))
            return 0

        lax.fori_loop(0, half // slab, norm, 0)
        stores[p].start()
    for p in range(SLOTS):
        stores[p].wait()
        links.first[p].start()
    start_all(links.second + links.to_own)
    receive(pos_copies)

    def t_copy(tslot, r0, n):
        return pltpu.make_async_copy(tbuf.at[tslot, :, pl.ds(0, n)], ht_ref.at[:, pl.ds(r0, n)], t_sem.at[tslot])

    def compute(slot, r0, n, first):
        r0 = pl.multiple_of(r0, n)
        out = pl.ds(r0, n)
        for t in range(n // LANE):
            at = r0 + t * LANE
            p = pos_all[at // rows, pl.ds((at % rows) // LANE, 1), :]
            angle = jnp.broadcast_to(p, (LANE, LANE)).T * freq_ref[...]
            sign = jnp.where(lax.broadcasted_iota(jnp.int32, (LANE, LANE), 1) % 2 == 0, -1.0, 1.0)
            tr = pl.ds(pl.multiple_of(at, LANE), LANE)
            cos_ref[tr, :] = jnp.cos(angle)
            sin_ref[tr, :] = jnp.sin(angle) * sign
        cos_t, sin_t = cos_ref[out, :], sin_ref[out, :]
        h = buf[slot, :n]
        tslot = lax.rem(slot, SLOTS)

        @pl.when(jnp.logical_not(first))
        def _():
            t_copy(tslot, 0, n).wait()

        tbuf[tslot, :, :n] = h.T
        t_copy(tslot, r0, n).start()
        for m in range(width // PAIR):
            y = dot(h, w_scr[:, m * PAIR:(m + 1) * PAIR])
            for e in range(SLOTS):
                q_ref[out, m * PAIR + e * LANE: m * PAIR + (e + 1) * LANE] = rotate(y[:, e * LANE:(e + 1) * LANE], cos_t, sin_t).astype(BF16)
        y = dot(h, w_scr[:, width:width + PAIR])
        k, v = rotate(y[:, :LANE], cos_t, sin_t), y[:, LANE:]
        k_ref[out, :] = k.astype(BF16)
        kt_ref[:, out] = k.T.astype(BF16)
        v_ref[out, :] = v.astype(BF16)
        vt_ref[:, out] = v.T.astype(BF16)
        for m, (src, dst) in enumerate(results):
            at = (slice(None), out) if src.shape[0] == HEAD_DIM else (out,)
            pltpu.make_async_copy(src.at[at], dst.at[at], out_sem.at[m]).start()

    results = list(zip((q_ref, k_ref, kt_ref, v_ref, vt_ref, cos_ref, sin_ref), (q_out, k_out, kt_out, v_out, vt_out, cos_out, sin_out)))

    def load(slot, r0, n):
        return pltpu.make_async_copy(hall_ref.at[pl.ds(pl.multiple_of(r0, n), n)], buf.at[slot, pl.ds(0, n)], load_sem.at[slot])

    far = in_order(links, lambda: wait_all(w_copies), lambda: None, load, compute, half, chunk)
    wait_all([t_copy(i, 0, half) for i in range(SLOTS)])
    far()
    wait_all([t_copy(i, 0, chunk) for i in range(SLOTS)])
    for m, (src, dst) in enumerate(results):
        pltpu.make_async_copy(src, dst, out_sem.at[m]).wait()
    links.finish()
    for c in pos_copies:
        c.wait_send()


def gather_qkv(x, ln_weight, pos, w_q, w_k, w_v, sp_size):
    rows, feat = x.shape
    seq = rows * sp_size
    width = w_q.shape[1] // sp_size
    inv_freq = ROPE_BASE ** (-jnp.arange(0, HEAD_DIM, 2, dtype=F32) / HEAD_DIM)
    freq = jnp.repeat(inv_freq, 2)[None, :]
    vmem = pl.BlockSpec(memory_space=pltpu.VMEM)
    made = [array(seq, width), array(seq, HEAD_DIM), array(HEAD_DIM, seq), array(seq, HEAD_DIM), array(HEAD_DIM, seq)]
    made += [array(seq, HEAD_DIM, dtype=F32)] * 2
    n = n_copies(CHUNKS, True)
    return pl.pallas_call(
        gather_qkv_kernel,
        in_specs=[HBM, vmem, vmem, vmem, HBM, HBM, HBM],
        out_specs=[HBM] * (2 + len(made)) + [vmem],
        out_shape=[array(seq, feat), array(feat, seq)] + made + [array(SLOTS, rows, LANE, dtype=F32)],
        scratch_shapes=[pltpu.VMEM(m.shape, m.dtype) for m in made] + [
            pltpu.VMEM((feat, width + PAIR), BF16), pltpu.VMEM((4, rows // 2, feat), BF16), pltpu.VMEM((SLOTS, feat, rows // 2), BF16),
            pltpu.VMEM((sp_size, rows // LANE, LANE), F32), SEM((N_PEERS,)), SEM((N_PEERS,)), SEM((n,)), SEM((n,)), SEM((3,)), SEM((4,)), SEM((SLOTS,)),
            SEM((SLOTS,)), SEM((len(made),))],
        compiler_params=remote_params(1),
        name="gather_qkv")(x, ln_weight.astype(F32)[None], pos.astype(F32).reshape(rows // LANE, LANE), freq, w_q, w_k, w_v)


def stack_heads(x):
    return jnp.concatenate([x[:, n * HEAD_DIM:(n + 1) * HEAD_DIM] for n in range(x.shape[1] // HEAD_DIM)], axis=0)


def causal(shape, bq, offset):
    rows = lax.rem(lax.broadcasted_iota(jnp.int32, shape, 0), bq) + offset
    return rows >= lax.broadcasted_iota(jnp.int32, shape, 1)


def fwd_step(qi, bq, bk, q_ref, kt_ref, v_ref, ot_ref, lse_ref, s_scr):
    q = stack_heads(q_ref[...])
    rows = q.shape[0]
    nfull = (qi * bq) // bk

    def scores(j):
        return dot(q, kt_ref[:, pl.ds(pl.multiple_of(j * bk, bk), bk)]) * (SCALE * LOG2E)

    def lane_max(m, s):
        for c in range(bk // LANE):
            m = jnp.maximum(m, s[:, c * LANE:(c + 1) * LANE])
        return m

    def score_step(j, m):
        s = scores(j)
        s_scr[j] = s
        return lane_max(m, s)

    m = lax.fori_loop(0, nfull, score_step, jnp.full((rows, LANE), -jnp.inf, F32))
    s = jnp.where(causal((rows, bk), bq, qi * bq - nfull * bk), scores(nfull), -jnp.inf)
    s_scr[nfull] = s
    m = jnp.max(lane_max(m, s), axis=1, keepdims=True)

    def value_step(j, carry):
        l, o = carry
        p = jnp.exp2(s_scr[j] - m)
        for t in range(bk // LANE):
            l = l + p[:, t * LANE:(t + 1) * LANE]
        o = o + dot(p.astype(BF16), v_ref[pl.ds(pl.multiple_of(j * bk, bk), bk), :])
        return l, o

    l, o = lax.fori_loop(0, nfull + 1, value_step, (jnp.zeros((rows, LANE), F32), jnp.zeros((rows, HEAD_DIM), F32)))
    l = jnp.sum(l, axis=1, keepdims=True)
    o = (o / l).astype(BF16)
    for n in range(rows // bq):
        ot_ref[n * HEAD_DIM:(n + 1) * HEAD_DIM, :] = o[n * bq:(n + 1) * bq].T
    lse_ref[...] = (m + jnp.log2(l)).reshape(lse_ref.shape)


def gather_fwd_kernel(n_fwd, relay, bq, bk, q_ref, kt_ref, v_ref, g_ref, wo_ref, ot_ref, lse_ref, gall_ref, do_ref,
                      s_scr, wo_scr, buf, send, recv, w_sem, load_sem, store_sem):
    step = pl.program_id(0)
    me = lax.axis_index("sp")
    rows, width = g_ref.shape[0], do_ref.shape[1]
    half = rows // 2
    chunk = half // CHUNKS

    def block(owner, part, c):
        start = owner * rows + part * half
        return gall_ref.at[pl.ds(pl.multiple_of(start, half), half) if c is None else pl.ds(pl.multiple_of(start + c * chunk, chunk), chunk)]

    own = lambda part: g_ref.at[pl.ds(part * half, half)]
    links = Exchange(send, recv, block, own, CHUNKS, True)
    w_copy = pltpu.make_async_copy(wo_ref.at[pl.ds(pl.multiple_of(me * width, width), width)], wo_scr, w_sem.at[0])
    loads = [pltpu.make_async_copy(own(i), buf.at[i], load_sem.at[i]) for i in range(SLOTS)]
    stores = [pltpu.make_async_copy(buf.at[i], block(me, i, None), store_sem.at[i]) for i in range(SLOTS)]

    @pl.when(step == 0)
    def _():
        greet(neighbours())
        links.begin()
        w_copy.start()
        start_all(loads)

    @pl.when(step == relay)
    def _():
        links.near(0)

    @pl.when(step < n_fwd)
    def _():
        fwd_step(step, bq, bk, q_ref, kt_ref, v_ref, ot_ref, lse_ref, s_scr)

    def load(slot, r0, n):
        return pltpu.make_async_copy(gall_ref.at[pl.ds(pl.multiple_of(r0, n), n)], buf.at[slot, pl.ds(0, n)], load_sem.at[slot])

    def compute(slot, r0, n, _):
        do_ref[pl.ds(pl.multiple_of(r0, n), n), :] = lax.dot_general(
            buf[slot, :n], wo_scr[...], (((1,), (1,)), ((), ())), preferred_element_type=F32).astype(BF16)

    def own_ready():
        wait_all(loads)
        start_all(stores)
        w_copy.wait()

    @pl.when(step == n_fwd)
    def _():
        far = in_order(links, own_ready, lambda: wait_all(stores), load, compute, half, chunk, started=True)
        far()
        links.finish()


def gather_forward(q, kt, v, g, w_o, bq=PAIR, bk=1024):
    seq, width = q.shape
    rows, feat = g.shape
    heads = width // HEAD_DIM
    n = seq // bq
    at = lambda i: jnp.minimum(i, n - 1)
    return pl.pallas_call(
        functools.partial(gather_fwd_kernel, n, (3 * n) // 4, bq, bk), grid=(n + 1,),
        in_specs=[pl.BlockSpec((bq, width), lambda i: (at(i), 0)), pl.BlockSpec((HEAD_DIM, seq), whole, **ONCE),
                  pl.BlockSpec((seq, HEAD_DIM), whole, **ONCE), HBM, HBM],
        out_specs=[pl.BlockSpec((width, bq), lambda i: (0, at(i))), pl.BlockSpec((heads, bq, 1), lambda i: (0, at(i), 0)), HBM,
                   pl.BlockSpec((seq, width), whole)],
        out_shape=[array(width, seq), array(heads, seq, 1, dtype=F32), array(seq, feat),
                   array(seq, width)],
        scratch_shapes=[pltpu.VMEM((seq // bk, heads * bq, bk), F32), pltpu.VMEM((width, feat), BF16), pltpu.VMEM((4, rows // 2, feat), BF16),
                        SEM((n_copies(CHUNKS, True),)), SEM((n_copies(CHUNKS, True),)), SEM((1,)), SEM((4,)), SEM((SLOTS,))],
        compiler_params=remote_params(2),
        name="gather_fwd")(q, kt, v, g, w_o)


def bwd_step(qi, bq, bk, q_ref, do_ref, lse_ref, k_ref, kt_ref, vt_ref, cos_ref, sin_ref, g_out, dkt_ref, dvt_ref, p_scr, dp_scr):
    q = stack_heads(q_ref[...])
    do = stack_heads(do_ref[...])
    rows = q.shape[0]
    lse = lse_ref[...].reshape(rows, 1)
    q_t = q.T
    do_t = do.T
    nfull = (qi * bq) // bk

    @pl.when(qi == 0)
    def _():
        dkt_ref[...] = jnp.zeros_like(dkt_ref)
        dvt_ref[...] = jnp.zeros_like(dvt_ref)

    def prob_step(j, r, masked):
        sl = pl.ds(pl.multiple_of(j * bk, bk), bk)
        s = dot(q, kt_ref[:, sl]) * (SCALE * LOG2E)
        p = jnp.exp2(s - lse)
        if masked:
            p = jnp.where(causal((rows, bk), bq, qi * bq - nfull * bk), p, 0.0)
        dp = dot(do, vt_ref[:, sl])
        pd = p * dp
        for t in range(bk // LANE):
            r = r + pd[:, t * LANE:(t + 1) * LANE]
        p_scr[j] = p
        dp_scr[j] = dp
        dvt_ref[:, sl] += dot(do_t, p.astype(BF16))
        return r

    r = lax.fori_loop(0, nfull, lambda j, r: prob_step(j, r, False), jnp.zeros((rows, LANE), F32))
    r = prob_step(nfull, r, True)
    r = jnp.sum(r, axis=1, keepdims=True)

    def grad_step(j, dq):
        sl = pl.ds(pl.multiple_of(j * bk, bk), bk)
        ds = (p_scr[j] * (dp_scr[j] - r) * SCALE).astype(BF16)
        dkt_ref[:, sl] += dot(q_t, ds)
        return dq + dot(ds, k_ref[sl, :])

    dq = lax.fori_loop(0, nfull + 1, grad_step, jnp.zeros((rows, HEAD_DIM), F32))
    dq = dq.astype(BF16).astype(F32)
    here = pl.ds(pl.multiple_of(qi * bq, bq), bq)
    cos_t, sin_t = cos_ref[here, :], sin_ref[here, :]
    for n in range(rows // bq):
        g_out[:, n * HEAD_DIM:(n + 1) * HEAD_DIM] = rotate(dq[n * bq:(n + 1) * bq], cos_t, -sin_t).astype(BF16)


def gather_bwd_kernel(relay, bq, bk, q_ref, do_ref, lse_ref, k_ref, kt_ref, vt_ref, cos_ref, sin_ref, ot_ref,
                      gq_ref, gk_ref, gv_ref, otg_ref, otz_ref, p_scr, dp_scr, dkt_scr, dvt_scr, buf, send, recv, z_send, z_recv, load_sem, store_sem):
    step = pl.program_id(0)
    last = pl.num_programs(0) - 1
    me = lax.axis_index("sp")
    width, seq = ot_ref.shape
    half = width // 2
    tokens = otz_ref.shape[2]
    zn = flip(me, CORE)
    own = lambda part: ot_ref.at[pl.ds(part * half, half)]
    block = lambda owner, part, _: otg_ref.at[owner // 2, pl.ds(part * half, half)]
    links = Exchange(send, recv, block, own, 1, False)
    xn, yn = flip(me, X_BIT), flip(me, Y_BIT)
    dn = flip(xn, Y_BIT)
    mine = pl.ds(pl.multiple_of(zn * tokens, tokens), tokens)

    def to_other(n, owner):
        src = ot_ref.at[:, mine] if n == 0 else otg_ref.at[owner // 2, :, mine]
        return pltpu.make_async_remote_copy(src_ref=src, dst_ref=otz_ref.at[owner // 2], send_sem=z_send.at[n], recv_sem=z_recv.at[n],
                                            device_id={"sp": zn}, device_id_type=MESH)

    z = [to_other(n, o) for n, o in enumerate((me, xn, yn, dn))]
    n_buf, slab = buf.shape[0], buf.shape[1]
    n_slab = width // slab

    def slab_copies(n):
        rows = pl.ds(pl.multiple_of(n * slab, slab), slab)
        slot = n % n_buf
        return (pltpu.make_async_copy(ot_ref.at[rows], buf.at[slot], load_sem.at[slot]),
                pltpu.make_async_copy(buf.at[slot], otg_ref.at[me // 2, rows], store_sem.at[slot]))

    @pl.when(step == 0)
    def _():
        greet(neighbours())
        links.begin()
        z[0].start()

    @pl.when(step == relay)
    def _():
        links.near(0)

    @pl.when((step >= 2) & (step < n_slab + 2))
    def _():
        slab_copies(step - 2)[1].wait()

    @pl.when((step >= 1) & (step < n_slab + 1))
    def _():
        slab_copies(step - 1)[0].wait()
        slab_copies(step - 1)[1].start()

    @pl.when(step < n_slab)
    def _():
        slab_copies(step)[0].start()

    bwd_step(step, bq, bk, q_ref, do_ref, lse_ref, k_ref, kt_ref, vt_ref, cos_ref, sin_ref, gq_ref, dkt_scr, dvt_scr, p_scr, dp_scr)

    @pl.when(step == last)
    def _():
        links.near(1)
        start_all(z[1:3])

        def kv_rows(i, _):
            rows = pl.ds(pl.multiple_of(i * bk, bk), bk)
            dk = dkt_scr[:, rows].T.astype(BF16).astype(F32)
            gk_ref[rows, :] = rotate(dk, cos_ref[rows, :], -sin_ref[rows, :]).astype(BF16)
            gv_ref[rows, :] = dvt_scr[:, rows].T.astype(BF16)
            return 0

        lax.fori_loop(0, seq // bk, kv_rows, 0)
        links.far(0)
        z[3].start()
        receive(z)
        links.finish()
        for c in z:
            c.wait_send()


def gather_backward(q, do, lse, k, kt, vt, cos_t, sin_t, ot, sp_size, bq=PAIR, bk=512):
    seq, width = q.shape
    heads = width // HEAD_DIM
    chips, tokens = sp_size // 2, seq // sp_size
    n = seq // bq
    tile = pl.BlockSpec((bq, width), row)
    tall = pl.BlockSpec((seq, HEAD_DIM), whole, **ONCE)
    wide = pl.BlockSpec((HEAD_DIM, seq), whole, **ONCE)
    return pl.pallas_call(
        functools.partial(gather_bwd_kernel, (9 * n) // 16, bq, bk), grid=(n,),
        in_specs=[tile, tile, pl.BlockSpec((heads, bq, 1), lambda i: (0, i, 0)), tall, wide, wide, tall, tall, HBM],
        out_specs=[tile, tall, tall, HBM, HBM],
        out_shape=[array(seq, width), array(seq, HEAD_DIM), array(seq, HEAD_DIM), array(chips, width, seq), array(chips, width, tokens)],
        scratch_shapes=[pltpu.VMEM((seq // bk, heads * bq, bk), F32), pltpu.VMEM((seq // bk, heads * bq, bk), F32),
                        pltpu.VMEM((HEAD_DIM, seq), F32), pltpu.VMEM((HEAD_DIM, seq), F32), pltpu.VMEM((SLOTS, width // 8, seq), BF16),
                        SEM((n_copies(1, False),)), SEM((n_copies(1, False),)), SEM((4,)), SEM((4,)), SEM((SLOTS,)), SEM((SLOTS,))],
        compiler_params=remote_params(3),
        name="gather_bwd")(q, do, lse, k, kt, vt, cos_t, sin_t, ot)


def dw_o_kernel(core_ref, ot_ref, g_ref, final_ref, send_ref):
    y = dot(ot_ref[...], g_ref[...]).astype(BF16)
    final_ref[...] = y
    send_ref[...] = y


def dw_o_half(core, ot_all, g_all, bn=1024):
    half, width, seq = ot_all.shape
    feat = g_all.shape[1]
    return pl.pallas_call(
        dw_o_kernel,
        grid_spec=pltpu.PrefetchScalarGridSpec(
            num_scalar_prefetch=1, grid=(feat // bn, half),
            in_specs=[pl.BlockSpec((None, width, seq), lambda j, s, c: (s, 0, 0)), pl.BlockSpec((seq, bn), col)],
            out_specs=[pl.BlockSpec((width, bn), lambda j, s, c: (2 * s + c[0], j)), pl.BlockSpec((width, bn), lambda j, s, c: (s, j))]),
        out_shape=[array(2 * half * width, feat), array(half * width, feat)],
        compiler_params=PARAMS, cost_estimate=cost(2 * half * width * feat * seq), name="dw_o_half")(core, ot_all, g_all)


class Ride:
    def __init__(self, source, buf, targets, load_sem, store_sem):
        self.source, self.buf, self.targets, self.load_sem, self.store_sem = source, buf, targets, load_sem, store_sem

    def load(self, i):
        slot = lax.rem(i, SLOTS)
        return pltpu.make_async_copy(self.source(i), self.buf.at[slot], self.load_sem.at[slot])

    def stores(self, i):
        slot = lax.rem(i, SLOTS)
        return [pltpu.make_async_copy(src, dst, self.store_sem.at[slot, n]) for n, (src, dst) in enumerate(self.targets(i, self.buf.at[slot]))]

    def begin(self, i):
        @pl.when(i >= SLOTS)
        def _():
            wait_all(self.stores(i - SLOTS))

        self.load(i).start()

    def end(self, i, last):
        self.load(i).wait()
        start_all(self.stores(i))

        @pl.when(i == last)
        def _():
            for n in reversed(range(SLOTS)):
                wait_all(self.stores(i - n))


def half_ride(recv, half, dev, final, scratch):
    buf = scratch[0]
    n, w = buf.shape[1:]
    at = lambda i, base: pl.ds(pl.multiple_of(base + i * n, n), n)
    return Ride(lambda i: recv.at[at(i, 0)], buf, lambda i, src: [(src, final.at[at(i, half * recv.shape[0]), pl.ds(pl.multiple_of(dev * w, w), w)])], *scratch[1:])


def half_scratch(recv, steps):
    return [pltpu.VMEM((SLOTS, recv.shape[0] // steps, recv.shape[1]), BF16), SEM((SLOTS,)), SEM((SLOTS, 1))]


def out_kernel(ids_ref, mine_ref, other_ref, w_ref, low, high, _, out_ref, q_ref, o_scr, *scratch):
    i, last = grid_place()
    rides = [half_ride(r, m, ids_ref[1 + m], q_ref, scratch[3 * m:3 * m + 3]) for m, r in enumerate((low, high))]
    for r in rides:
        r.begin(i)

    @pl.when(i == 0)
    def _():
        core = lax.rem(ids_ref[0], 2)
        width = mine_ref.shape[1]
        for s in range(mine_ref.shape[0]):
            for ref, d in ((mine_ref, 2 * s + core), (other_ref, 2 * s + 1 - core)):
                o_scr[:, pl.ds(pl.multiple_of(d * width, width), width)] = ref[s].T

    out_ref[...] = dot(o_scr[...], w_ref[...]).astype(BF16)
    for r in rides:
        r.end(i, last)


def out_proj(ids, ot_all, ot_other, w_o, low, high, dw_q, bn=512):
    chips, width, tokens = ot_other.shape
    feat = w_o.shape[1]
    steps = feat // bn
    return pl.pallas_call(
        out_kernel,
        grid_spec=pltpu.PrefetchScalarGridSpec(
            num_scalar_prefetch=1, grid=(steps,),
            in_specs=[pl.BlockSpec((chips, width, tokens), lambda i, c: (0, 0, c[0]), **ONCE), pl.BlockSpec((chips, width, tokens), lambda i, c: (0, 0, 0), **ONCE),
                      pl.BlockSpec((w_o.shape[0], bn), col)] + [HBM] * 3,
            out_specs=[pl.BlockSpec((tokens, bn), col), HBM],
            scratch_shapes=[pltpu.VMEM((tokens, w_o.shape[0]), BF16)] + half_scratch(low, steps) + half_scratch(high, steps)),
        out_shape=[array(tokens, feat), array(*dw_q.shape)], input_output_aliases={6: 1},
        compiler_params=PARAMS, cost_estimate=cost(2 * tokens * w_o.size), name="out_proj")(ids, ot_all, ot_other, w_o, low, high, dw_q)


def dw_q_kernel(ids_ref, ht_ref, g_ref, final_ref, low_ref, high_ref):
    i = pl.program_id(0)
    y = dot(ht_ref[...], g_ref[...]).astype(BF16)
    final_ref[...] = y
    n = pl.num_programs(0) // 2

    @pl.when(i < n)
    def _():
        low_ref[...] = y

    @pl.when(i >= n)
    def _():
        high_ref[...] = y


def dw_q_own(ids, ht, gq, bm=512):
    feat, seq = ht.shape
    w = gq.shape[1]
    n = feat // bm
    return pl.pallas_call(
        dw_q_kernel,
        grid_spec=pltpu.PrefetchScalarGridSpec(
            num_scalar_prefetch=1, grid=(n,), in_specs=[pl.BlockSpec((bm, seq), row), pl.BlockSpec((seq, w), whole, **ONCE)],
            out_specs=[pl.BlockSpec((bm, w), lambda i, c: (i, c[0])), pl.BlockSpec((bm, w), lambda i, c: (jnp.minimum(i, n // 2 - 1), 0)),
                       pl.BlockSpec((bm, w), lambda i, c: (jnp.maximum(i - n // 2, 0), 0))]),
        out_shape=[array(feat, feat), array(feat // 2, w), array(feat // 2, w)],
        compiler_params=PARAMS, cost_estimate=cost(2 * seq * feat * w), name="dw_q_own")(ids, ht, gq)


def kv_columns(rows, src, k_ref, v_ref, owners):
    out = []
    for m, ref in enumerate((k_ref, v_ref)):
        for n, dev in enumerate(owners):
            at = (m * len(owners) + n) * HEAD_DIM
            out.append((src.at[:, at:at + HEAD_DIM], ref.at[rows, pl.ds(pl.multiple_of(dev * HEAD_DIM, HEAD_DIM), HEAD_DIM)]))
    return out


def dw_kv_kernel(n_dev, ids_ref, ht_ref, *refs):
    parts, refs = refs[:2 * n_dev], refs[2 * n_dev:]
    recvs, (q_ref, k_ref, v_ref, send_ref, x_scr, y_scr, y_sem, send_sem, x_sem, load_sem, *scratch) = refs[:SLOTS], refs[SLOTS + 1:]
    i, last = grid_place()
    rides = [half_ride(recvs[m], m, flip(ids_ref[0], CORE), q_ref, scratch[3 * m:3 * m + 3]) for m in range(SLOTS)]
    for r in rides:
        r.begin(i)
    bm, feat = ht_ref.shape[0], k_ref.shape[0]
    n_tok = send_ref.shape[0] - feat
    tokens = pltpu.make_async_copy(x_scr.at[pl.ds(pl.multiple_of(flip(ids_ref[0], CORE) * n_tok, n_tok), n_tok)], send_ref.at[pl.ds(feat, n_tok)], x_sem.at[0])
    owners = [ids_ref[1 + n] for n in range(n_dev)]

    @pl.when(i == 0)
    def _():
        loads = [pltpu.make_async_copy(p, x_scr.at[:, m * HEAD_DIM:(m + 1) * HEAD_DIM], load_sem.at[m]) for m, p in enumerate(parts)]
        start_all(loads)
        wait_all(loads)
        tokens.start()

    def stores(step):
        slot, rows = lax.rem(step, SLOTS), pl.ds(pl.multiple_of(step * bm, bm), bm)
        out = [pltpu.make_async_copy(src, dst, y_sem.at[slot, m]) for m, (src, dst) in enumerate(kv_columns(rows, y_scr.at[slot], k_ref, v_ref, owners))]
        return out + [pltpu.make_async_copy(y_scr.at[slot], send_ref.at[rows], send_sem.at[slot])]

    @pl.when(i >= SLOTS)
    def _():
        wait_all(stores(i - SLOTS))

    y_scr[lax.rem(i, SLOTS)] = dot(ht_ref[...], x_scr[...]).astype(BF16)
    start_all(stores(i))
    for r in rides:
        r.end(i, last)

    @pl.when(i == last)
    def _():
        tokens.wait()
        for m in reversed(range(SLOTS)):
            wait_all(stores(i - m))


def dw_kv_half(ids, ht, parts, halves, dw_q, shape, tokens, bm=512):
    feat, seq = ht.shape
    w = len(parts) * HEAD_DIM
    steps = feat // bm
    return pl.pallas_call(
        functools.partial(dw_kv_kernel, len(parts) // 2),
        grid_spec=pltpu.PrefetchScalarGridSpec(
            num_scalar_prefetch=1, grid=(steps,), in_specs=[pl.BlockSpec((bm, seq), row)] + [HBM] * (len(parts) + 3), out_specs=[HBM] * 4,
            scratch_shapes=[pltpu.VMEM((seq, w), BF16), pltpu.VMEM((SLOTS, bm, w), BF16), SEM((SLOTS, len(parts))), SEM((SLOTS,)), SEM((1,)), SEM((len(parts),))]
            + half_scratch(halves[0], steps) + half_scratch(halves[1], steps)),
        out_shape=[array(*dw_q.shape), array(*shape), array(*shape), array(feat + tokens, w)], input_output_aliases={4 + len(parts): 0},
        compiler_params=PARAMS, cost_estimate=cost(2 * seq * feat * w), name="dw_kv_half")(ids, ht, *parts, *halves, dw_q)


def dh_kernel(n_dev, ids_ref, wq_ref, wk_ref, wv_ref, x_ref, stat_ref, lnw_ref, tq_ref, t_ref, *refs):
    own, refs = refs[:2 * n_dev], refs[2 * n_dev:]
    kv_recv, o_recv, _, _, _, dx_ref, dlnw_ref, k_ref, v_ref, o_ref, g_scr, sum_scr, dy_scr, *scratch = refs
    i, last = grid_place()
    tokens, feat = x_ref.shape
    bf = wq_ref.shape[0]
    others = [ids_ref[1 + n_dev + n] for n in range(n_dev)]
    kv_buf, o_buf = scratch[0], scratch[3]
    core = lax.rem(ids_ref[0], 2)
    block_rows = lambda i, buf: pl.ds(pl.multiple_of(i * buf.shape[1], buf.shape[1]), buf.shape[1])

    def o_rows(i):
        n = o_buf.shape[1]
        per = HEAD_DIM * n_dev // n
        return pl.ds(pl.multiple_of(((2 * (i // per) + 1 - core) * per + lax.rem(i, per)) * n, n), n)

    rides = [Ride(lambda i: kv_recv.at[block_rows(i, kv_buf)], kv_buf, lambda i, src: kv_columns(block_rows(i, kv_buf), src, k_ref, v_ref, others), *scratch[1:3]),
             Ride(lambda i: o_recv.at[block_rows(i, o_buf)], o_buf, lambda i, src: [(src, o_ref.at[o_rows(i)])], *scratch[4:])]
    for r in rides:
        r.begin(i)
    nq, nk = wq_ref.shape[1], wk_ref.shape[1]
    slab = tokens // 8

    @pl.when(i == 0)
    def _():
        width = tq_ref.shape[1]
        for m in range(2 * n_dev):
            g_scr[m * width:(m + 1) * width, :] = tq_ref[m * tokens:(m + 1) * tokens, :].T
        t = t_ref[...].T
        for m in range(2 * n_dev):
            for x, dev in ((own[m][...].T, ids_ref[1 + m % n_dev]), (t[m * HEAD_DIM:(m + 1) * HEAD_DIM], others[m % n_dev])):
                g_scr[pl.ds(pl.multiple_of(nq + (m // n_dev) * nk + dev * HEAD_DIM, HEAD_DIM), HEAD_DIM), :] = x

        sum_scr[...] = jnp.zeros_like(sum_scr)

    y = (dot(wq_ref[...], g_scr[:nq, :]) + dot(wk_ref[...], g_scr[nq:nq + nk, :]) + dot(wv_ref[...], g_scr[nq + nk:, :])).T
    for m in range(bf // LANE):
        part, at = slice(m * LANE, (m + 1) * LANE), pl.ds(pl.multiple_of(i * bf + m * LANE, LANE), LANE)
        hat = (x_ref[:, at].astype(F32) - stat_ref[0]) * stat_ref[1]
        dlnw_ref[:, part] = jnp.sum(y[:, part] * hat, axis=0, keepdims=True)
        dy = y[:, part] * lnw_ref[:, part]
        dy_scr[:, at] = dy
        sum_scr[0] += dy
        sum_scr[1] += dy * hat
    for r in rides:
        r.end(i, last)

    @pl.when(i == last)
    def _():
        def finish(m, _):
            here = pl.ds(pl.multiple_of(m * slab, slab), slab)
            mean_y, mean_yh = (jnp.sum(sum_scr[e, here, :], axis=1, keepdims=True) / feat for e in range(SLOTS))
            mean, rstd = (stat_ref[e, here, :1] for e in range(SLOTS))
            hat = (x_ref[here, :].astype(F32) - mean) * rstd
            dx_ref[here, :] = (rstd * (dy_scr[here, :] - mean_y - hat * mean_yh)).astype(BF16)
            return 0

        lax.fori_loop(0, tokens // slab, finish, 0)


def dh_proj(ids, w_q, w_k, w_v, x, stats, ln_weight, t_q, own, kv_recv, o_recv, finals, bf=512):
    tokens, feat = x.shape
    w = kv_recv.shape[1]
    n = len(own)
    ins = [w_q, w_k, w_v, x, stats, ln_weight.astype(F32)[None], t_q, kv_recv, *own, kv_recv, o_recv, *finals]
    specs = [pl.BlockSpec((bf, m.shape[1]), row) for m in (w_q, w_k, w_v)] + [pl.BlockSpec(x.shape, whole, **ONCE), pl.BlockSpec(stats.shape, lambda i, c: (0, 0, 0), **ONCE), pl.BlockSpec((1, bf), col)]
    specs += [pl.BlockSpec(t_q.shape, whole, **ONCE), pl.BlockSpec((tokens, w), lambda i, c: (feat // tokens, 0), **ONCE)]
    specs += [pl.BlockSpec((tokens, HEAD_DIM), lambda i, c: (c[0], 0), **ONCE) for _ in own]
    first = len(ins) - len(finals)
    steps = feat // bf
    return pl.pallas_call(
        functools.partial(dh_kernel, n // 2),
        grid_spec=pltpu.PrefetchScalarGridSpec(
            num_scalar_prefetch=1, grid=(steps,), in_specs=specs + [HBM] * (len(ins) - len(specs)),
            out_specs=[pl.BlockSpec(x.shape, whole, **ONCE), pl.BlockSpec((1, bf), col)] + [HBM] * len(finals),
            scratch_shapes=[pltpu.VMEM((w_q.shape[1] + 2 * w_k.shape[1], tokens), BF16), pltpu.VMEM((SLOTS, tokens, LANE), F32), pltpu.VMEM(x.shape, F32),
                            pltpu.VMEM((SLOTS, feat // steps, w), BF16), SEM((SLOTS,)), SEM((SLOTS, n)),
                            pltpu.VMEM((SLOTS, o_recv.shape[0] // steps, feat), BF16), SEM((SLOTS,)), SEM((SLOTS, 1))]),
        out_shape=[array(tokens, feat), array(1, feat, dtype=F32)] + [array(*f.shape) for f in finals],
        input_output_aliases={1 + first + m: 2 + m for m in range(len(finals))},
        compiler_params=PARAMS, cost_estimate=cost(2 * tokens * (w_q.size + 2 * w_k.size)), name="dh_proj")(ids, *ins)


def copy_kernel(n, places, ids_ref, *refs):
    final, buf, load_sem, store_sem = refs[n + 1:]
    rows, w = buf.shape[1:]
    loads = [pltpu.make_async_copy(refs[m], buf.at[m], load_sem.at[m]) for m in range(n)]
    start_all(loads)
    stores = []
    for m, (owner, half) in enumerate(places):
        loads[m].wait()
        at = pl.ds(pl.multiple_of(ids_ref[owner] * w, w), w)
        stores.append(pltpu.make_async_copy(buf.at[m], final.at[pl.ds(half * rows, rows), at], store_sem.at[m]))
        stores[-1].start()
    wait_all(stores)


def copy_in(ids, blocks, places, final):
    n = len(blocks)
    return pl.pallas_call(
        functools.partial(copy_kernel, n, places),
        grid_spec=pltpu.PrefetchScalarGridSpec(num_scalar_prefetch=1, grid=(1,), in_specs=[HBM] * (n + 1), out_specs=HBM,
                                               scratch_shapes=[pltpu.VMEM((n,) + blocks[0].shape, BF16), SEM((n,)), SEM((n,))]),
        out_shape=array(*final.shape), input_output_aliases={n + 1: 0}, compiler_params=PARAMS, name="copy_in")(ids, *blocks, final)


def sum_kernel(x_ref, out_ref, all_scr, send, recv):
    me = lax.axis_index("sp")
    peers = everyone()
    greet(peers)
    copies = [pltpu.make_async_remote_copy(src_ref=x_ref, dst_ref=all_scr.at[me], send_sem=send.at[n], recv_sem=recv.at[n],
                                           device_id={"sp": p}, device_id_type=MESH) for n, p in enumerate(peers)]
    for c in copies:
        c.start()
    all_scr[me] = x_ref[...]
    for c in copies:
        c.wait_recv()
    total = all_scr[0]
    for n in range(1, all_scr.shape[0]):
        total = total + all_scr[n]
    out_ref[...] = total.astype(BF16)
    for c in copies:
        c.wait_send()


def sum_devices(x, sp_size):
    n = x.shape[0] // HEAD_DIM
    vmem = pl.BlockSpec(memory_space=pltpu.VMEM)
    return pl.pallas_call(
        sum_kernel, in_specs=[vmem], out_specs=vmem, out_shape=array(n, HEAD_DIM),
        scratch_shapes=[pltpu.VMEM((sp_size, n, HEAD_DIM), F32), SEM((sp_size - 1,)), SEM((sp_size - 1,))],
        compiler_params=remote_params(4), name="sum_devices")(x.reshape(n, HEAD_DIM)).reshape(-1)


def solution(mesh):
    sp_size = mesh.shape['sp']
    row_spec = P(('dp', 'sp'), None)
    pos_spec = P(('dp', 'sp'))
    full_spec = P(None, None)
    grad_spec = P('dp', None)

    def local_step(hidden, positions, d_attn, ln_weight, w_q, w_k, w_v, w_o):
        dev = lax.axis_index('sp')
        core = lax.rem(dev, SLOTS)
        local_rows, _ = hidden.shape
        _, ht, q, k, kt, v, vt, cos_t, sin_t, stats = gather_qkv(hidden, ln_weight, positions, w_q, w_k, w_v, sp_size)
        ot, lse, g_all, do = gather_forward(q, kt, v, d_attn, w_o)
        gq, gk, gv, ot_all, ot_other = gather_backward(q, do, lse, k, kt, vt, cos_t, sin_t, ot, sp_size)
        other = lambda d: flip(d, CORE)
        dev_x, dev_y = flip(dev, X_BIT), flip(dev, Y_BIT)
        dev_d = flip(dev_x, Y_BIT)
        owners = [dev, dev_x, dev_y, dev_d]

        def to(x, bit):
            return lax.ppermute(x, 'sp', [(i, i ^ bit) for i in range(sp_size)])

        after = lambda x, *done: lax.optimization_barrier((x,) + done)[0]
        ids = lambda *d: jnp.stack(d)
        gk_x, gv_y, gv_x, gk_y = to(gk, X_BIT), to(gv, Y_BIT), to(gv, X_BIT), to(gk, Y_BIT)
        t_q = lax.all_to_all(gq, 'sp', 0, 0, tiled=True)
        dw_q, low, high = dw_q_own(dev.reshape(1), ht, gq)
        gk_d, gv_d = to(after(gk_x, low), Y_BIT), to(after(gv_y, low), X_BIT)
        low_x, high_y, high_x, low_y = to(low, X_BIT), to(high, Y_BIT), to(high, X_BIT), to(low, Y_BIT)
        low_z, high_z = to(low, CORE), to(high, CORE)
        dw_o, o_send = dw_o_half(after(core.reshape(1), low), ot_all, g_all)
        o_recv = to(o_send, CORE)
        parts = [gk, gk_x, gk_y, gk_d, gv, gv_x, gv_y, gv_d]
        dw_q, dw_k, dw_v, kv_send = dw_kv_half(ids(*owners[:1], *owners), ht, [after(parts[0], o_send)] + parts[1:], [low_z, high_z], dw_q, w_k.shape, local_rows)
        kv_recv = to(kv_send, CORE)
        attn_out, dw_q = out_proj(ids(dev, dev_x, dev_y), ot_all, ot_other, after(w_o, kv_send), low_x, high_y, dw_q)
        low_d, high_d = to(after(low_x, attn_out), Y_BIT), to(after(high_y, attn_out), X_BIT)
        low_zx, high_zy = to(after(low_x, attn_out), CORE), to(after(high_y, attn_out), CORE)
        dx, d_lnw, dw_k, dw_v, dw_o = dh_proj(ids(*owners[:1], *owners, *map(other, owners)), w_q, w_k, w_v, hidden, stats, ln_weight, t_q, parts, kv_recv, o_recv, [dw_k, dw_v, dw_o])
        high_zx, low_zy = to(after(high_x, dx), CORE), to(after(low_y, dx), CORE)
        d_lnw = sum_devices(d_lnw.reshape(-1), sp_size)
        low_zd, high_zd = to(after(low_d, d_lnw), CORE), to(after(high_d, d_lnw), CORE)
        dw_q = copy_in(ids(dev_x, dev_y, other(dev_x), other(dev_y)), [high_x, low_y, low_zx, high_zx, low_zy, high_zy],
                       [(0, HIGH), (1, LOW), (2, LOW), (2, HIGH), (3, LOW), (3, HIGH)], after(dw_q, d_lnw))
        dw_q = copy_in(ids(dev_d, other(dev_d)), [low_d, high_d, low_zd, high_zd], [(0, LOW), (0, HIGH), (1, LOW), (1, HIGH)], dw_q)
        return (attn_out, dx, d_lnw, dw_q, dw_k, dw_v, dw_o)

    return jax.shard_map(local_step, mesh=mesh,
                      in_specs=(row_spec, pos_spec, row_spec, P(None), full_spec, full_spec, full_spec, full_spec),
                      out_specs=(row_spec, row_spec, P('dp'), grad_spec, grad_spec, grad_spec, grad_spec),
                      check_vma=False)
```

```python
import functools
import math
import jax
import jax.numpy as jnp
from jax import lax
from jax.experimental import pallas as pl
from jax.experimental.pallas import tpu as pltpu
from jax.sharding import PartitionSpec as P

HEAD_DIM = LANE = 128
PAIR = 2 * HEAD_DIM
CORE, X_BIT, Y_BIT = 1, 2, 4
LOW, HIGH, SLOTS = 0, 1, 2
CHUNKS, N_PEERS = 2, 7
EARLY = (0, 32, 96)
LN_EPS = 1e-5
ROPE_BASE = 10000.0
SCALE = HEAD_DIM ** -0.5
LOG2E = 1.4426950408889634
VMEM_LIMIT = 67_000_000
COPY_LIMIT = 20_000_000
BF16 = jnp.bfloat16
F32 = jnp.float32
MESH = pl.DeviceIdType.MESH
HBM = pl.BlockSpec(memory_space=pl.ANY)
SEM = pltpu.SemaphoreType.DMA
row = lambda i, *_: (i, 0)
col = lambda i, *_: (0, i)
whole = lambda *_: (0, 0)
ONCE = dict(pipeline_mode=pl.Buffered(1))
PARAMS = pltpu.CompilerParams(vmem_limit_bytes=VMEM_LIMIT)


def grid_place():
    return pl.program_id(0), pl.num_programs(0) - 1


def dot(x, y):
    return jnp.dot(x, y, preferred_element_type=F32)


def dot_t(x, y):
    return lax.dot_general(x, y, (((1,), (1,)), ((), ())), preferred_element_type=F32)


def array(*shape, dtype=BF16):
    return jax.ShapeDtypeStruct(shape, dtype)


def remote_params(number):
    return pltpu.CompilerParams(collective_id=number, has_side_effects=True, vmem_limit_bytes=VMEM_LIMIT)


def cost(flops):
    return pl.CostEstimate(flops=flops, bytes_accessed=flops // HEAD_DIM, transcendentals=0)


def rotate(x, cos_t, sin_t):
    lane = lax.broadcasted_iota(jnp.int32, x.shape, 1)
    swapped = jnp.where(lane % 2 == 0, pltpu.roll(x, HEAD_DIM - 1, 1), pltpu.roll(x, 1, 1))
    return x * cos_t + swapped * sin_t


def flip(i, bit):
    return i + bit - 2 * bit * ((i // bit) % 2)


class Exchange:
    def __init__(self, send, recv, block, own, chunks, partner, first=None):
        me = lax.axis_index("sp")
        xn, yn, zn = flip(me, X_BIT), flip(me, Y_BIT), flip(me, CORE)
        dn = flip(xn, Y_BIT)
        self.every = []

        def copy(owner, part, to, chunk=None, refs=None):
            n = len(self.every)
            src, dst = refs or (own(part) if owner is me else block(owner, part, chunk), block(owner, part, chunk))
            self.every.append(pltpu.make_async_remote_copy(src_ref=src, dst_ref=dst, send_sem=send.at[n], recv_sem=recv.at[n],
                                                           device_id={"sp": to}, device_id_type=MESH))
            return self.every[-1]

        self.first = [copy(me, part, to, refs=first and first(part)) for part, to in ((LOW, xn), (HIGH, yn))]
        self.second = [copy(me, HIGH, xn), copy(me, LOW, yn)]
        self.relay = [[copy(xn, LOW, yn, c), copy(yn, HIGH, xn, c)] for c in range(chunks)]
        if partner:
            self.to_own = [copy(me, LOW, zn), copy(me, HIGH, zn)]
            self.to_near = [[copy(xn, LOW, zn), copy(yn, HIGH, zn)], [copy(xn, HIGH, zn), copy(yn, LOW, zn)]]
            self.to_far = [[copy(dn, LOW, zn, c), copy(dn, HIGH, zn, c)] for c in range(chunks)]

    def begin(self):
        start_all(self.first)
        if hasattr(self, "to_own"):
            start_all(self.to_own)
        start_all(self.second)

    def near(self, n):
        for m, c in enumerate(self.second if n else self.first):
            c.wait_recv()
            if n == 0:
                start_all([r[m] for r in self.relay])
            if hasattr(self, "to_near"):
                self.to_near[n][m].start()

    def far(self, n):
        for m, c in enumerate(self.relay[n]):
            c.wait_recv()
            if hasattr(self, "to_far"):
                self.to_far[n][m].start()

    def finish(self):
        for c in self.every:
            c.wait_send()


def early_rows(g_ref, gall_ref, part, start, stop):
    rows = g_ref.shape[0]
    at = part * (rows // 2) + start
    n = stop - start
    return g_ref.at[pl.ds(at, n)], gall_ref.at[pl.ds(pl.multiple_of(lax.axis_index("sp") * rows + at, math.gcd(n, at) if at else n), n)]


def start_all(copies):
    for c in copies:
        c.start()


def wait_all(copies):
    for c in copies:
        c.wait()


def receive(copies):
    for c in copies:
        c.wait_recv()


def n_copies(chunks, partner):
    return 4 + 2 * chunks + (6 + 2 * chunks if partner else 0)


def greet(peers):
    barrier = pltpu.get_barrier_semaphore()
    for p in peers:
        pl.semaphore_signal(barrier, inc=1, device_id={"sp": p}, device_id_type=MESH)
    pl.semaphore_wait(barrier, len(peers))


def neighbours():
    me = lax.axis_index("sp")
    return [flip(me, CORE), flip(me, X_BIT), flip(me, Y_BIT)]


def everyone():
    me = lax.axis_index("sp")
    xn, yn = flip(me, X_BIT), flip(me, Y_BIT)
    dn = flip(xn, Y_BIT)
    return [flip(me, CORE), xn, flip(xn, CORE), yn, flip(yn, CORE), dn, flip(dn, CORE)]


def arrival(i, e):
    me = lax.axis_index("sp")
    g, near = i // 2, (i // 2 + 1) // 2
    owner = me + (i % 2) * (flip(me, CORE) - me) + near * ((1 - e) * (flip(me, X_BIT) - me) + e * (flip(me, Y_BIT) - me))
    return owner, e + (g // 2) * (1 - 2 * e)


def in_order(links, start, then, load, work, half, chunk, started=False):
    rows = 2 * half

    def second():
        then()
        receive(links.to_own)

    steps = [start, second, (lambda: None) if started else (lambda: links.near(0)), lambda: receive(links.to_near[0]), lambda: links.near(1),
             lambda: receive(links.to_near[1])]

    def sweep(n_pairs, steps, place, n, fetch_from):
        def pair(i, _):
            for m, act in enumerate(steps):
                @pl.when(i == m)
                def _():
                    act()
            slot0 = 2 * (i % 2)
            at = [place(i, e) for e in range(SLOTS)]
            copies = [load(slot0 + e, at[e], n) for e in range(SLOTS)]

            @pl.when(i >= fetch_from)
            def _():
                start_all(copies)
                wait_all(copies)

            def one(e, _):
                work(slot0 + e, at[0] + e * (at[1] - at[0]), n, i == 0)
                return 0

            return lax.fori_loop(0, SLOTS, one, 0)

        lax.fori_loop(0, n_pairs, pair, 0)

    def place(i, e):
        owner, part = arrival(i, e)
        return owner * rows + part * half

    sweep(len(steps), steps, place, half, 1)
    me = lax.axis_index("sp")
    dn = flip(flip(me, X_BIT), Y_BIT)

    def far_place(i, e):
        return (dn + (i % 2) * (flip(me, CORE) - me)) * rows + e * half + (i // 2) * chunk

    steps = []
    for c in range(CHUNKS):
        steps += [functools.partial(links.far, c), functools.partial(receive, links.to_far[c])]
    return lambda: sweep(len(steps), steps, far_place, chunk, 0)


def gather_qkv_kernel(x_ref, lnw_ref, pos_ref, freq_ref, wq_ref, wk_ref, wv_ref, g_ref,
                      hall_ref, ht_ref, gall_ref, q_out, k_out, kt_out, v_out, vt_out, cos_out, sin_out, stat_ref,
                      q_ref, k_ref, kt_ref, v_ref, vt_ref, cos_ref, sin_ref, w_scr, buf, tbuf, pos_all,
                      pos_send, pos_recv, send, recv, w_sem, load_sem, store_sem, t_sem, out_sem, early_send, early_recv):
    me = lax.axis_index("sp")
    rows = x_ref.shape[0]
    half = rows // 2
    chunk = half // CHUNKS
    width = q_ref.shape[1]

    def block(owner, part, c):
        start = owner * rows + part * half
        return hall_ref.at[pl.ds(pl.multiple_of(start, half), half) if c is None else pl.ds(pl.multiple_of(start + c * chunk, chunk), chunk)]

    own = lambda part: block(me, part, None)
    loads = [pltpu.make_async_copy(x_ref.at[pl.ds(p * half, half)], buf.at[p], load_sem.at[p]) for p in range(SLOTS)]
    start_all(loads)
    column = lambda n: pl.ds(pl.multiple_of(me * n, n), n)
    w_copies = [pltpu.make_async_copy(wq_ref.at[:, column(width)], w_scr.at[:, pl.ds(0, width)], w_sem.at[0]),
                pltpu.make_async_copy(wk_ref.at[:, column(HEAD_DIM)], w_scr.at[:, pl.ds(width, HEAD_DIM)], w_sem.at[1]),
                pltpu.make_async_copy(wv_ref.at[:, column(HEAD_DIM)], w_scr.at[:, pl.ds(width + HEAD_DIM, HEAD_DIM)], w_sem.at[2])]
    start_all(w_copies)
    peers = everyone()
    greet(peers)
    pos_copies = [pltpu.make_async_remote_copy(src_ref=pos_ref, dst_ref=pos_all.at[me], send_sem=pos_send.at[i], recv_sem=pos_recv.at[i],
                                               device_id={"sp": p}, device_id_type=MESH) for i, p in enumerate(peers)]
    start_all(pos_copies)
    early = []
    for start, stop in zip(EARLY, EARLY[1:]):
        for part, to in ((LOW, flip(me, X_BIT)), (HIGH, flip(me, Y_BIT))):
            src, dst = early_rows(g_ref, gall_ref, part, start, stop)
            early.append(pltpu.make_async_remote_copy(src_ref=src, dst_ref=dst, send_sem=early_send.at[len(early)], recv_sem=early_recv.at[len(early)],
                                                      device_id={"sp": to}, device_id_type=MESH))
    start_all(early[:SLOTS])
    pos_all[me] = pos_ref[...]
    links = Exchange(send, recv, block, own, CHUNKS, True)
    stores = [pltpu.make_async_copy(buf.at[p], own(p), store_sem.at[p]) for p in range(SLOTS)]
    slab = half // 8
    for p in range(SLOTS):
        loads[p].wait()

        def norm(n, _):
            here = pl.ds(pl.multiple_of(n * slab, slab), slab)
            x = buf[p, here, :].astype(F32)
            mean = jnp.mean(x, axis=-1, keepdims=True)
            centered = x - mean
            rstd = lax.rsqrt(jnp.mean(centered * centered, axis=-1, keepdims=True) + LN_EPS)
            buf[p, here, :] = (centered * rstd * lnw_ref[...]).astype(BF16)
            for m, v in enumerate((mean, rstd)):
                stat_ref[m, pl.ds(pl.multiple_of(p * half + n * slab, slab), slab), :] = jnp.broadcast_to(v, (slab, LANE))
            return 0

        lax.fori_loop(0, half // slab, norm, 0)
        stores[p].start()
    for p in range(SLOTS):
        stores[p].wait()
        links.first[p].start()
    start_all(links.second + links.to_own)
    receive(pos_copies)

    def t_copy(tslot, r0, n):
        return pltpu.make_async_copy(tbuf.at[tslot, :, pl.ds(0, n)], ht_ref.at[:, pl.ds(r0, n)], t_sem.at[tslot])

    def compute(slot, r0, n, first):
        r0 = pl.multiple_of(r0, n)
        out = pl.ds(r0, n)
        for t in range(n // LANE):
            at = r0 + t * LANE
            p = pos_all[at // rows, pl.ds((at % rows) // LANE, 1), :]
            angle = jnp.broadcast_to(p, (LANE, LANE)).T * freq_ref[...]
            sign = jnp.where(lax.broadcasted_iota(jnp.int32, (LANE, LANE), 1) % 2 == 0, -1.0, 1.0)
            tr = pl.ds(pl.multiple_of(at, LANE), LANE)
            cos_ref[tr, :] = jnp.cos(angle)
            sin_ref[tr, :] = jnp.sin(angle) * sign
        cos_t, sin_t = cos_ref[out, :], sin_ref[out, :]
        h = buf[slot, :n]
        tslot = lax.rem(slot, SLOTS)

        @pl.when(jnp.logical_not(first))
        def _():
            t_copy(tslot, 0, n).wait()

        tbuf[tslot, :, :n] = h.T
        t_copy(tslot, r0, n).start()
        for m in range(width // PAIR):
            y = dot(h, w_scr[:, m * PAIR:(m + 1) * PAIR])
            for e in range(SLOTS):
                q_ref[out, m * PAIR + e * LANE: m * PAIR + (e + 1) * LANE] = rotate(y[:, e * LANE:(e + 1) * LANE], cos_t, sin_t).astype(BF16)
        y = dot(h, w_scr[:, width:width + PAIR])
        k, v = rotate(y[:, :LANE], cos_t, sin_t), y[:, LANE:]
        k_ref[out, :] = k.astype(BF16)
        kt_ref[:, out] = k.T.astype(BF16)
        v_ref[out, :] = v.astype(BF16)
        vt_ref[:, out] = v.T.astype(BF16)
        for m, (src, dst) in enumerate(results):
            at = (slice(None), out) if src.shape[0] == HEAD_DIM else (out,)
            pltpu.make_async_copy(src.at[at], dst.at[at], out_sem.at[m]).start()

    results = list(zip((q_ref, k_ref, kt_ref, v_ref, vt_ref, cos_ref, sin_ref), (q_out, k_out, kt_out, v_out, vt_out, cos_out, sin_out)))

    def load(slot, r0, n):
        return pltpu.make_async_copy(hall_ref.at[pl.ds(pl.multiple_of(r0, n), n)], buf.at[slot, pl.ds(0, n)], load_sem.at[slot])

    far = in_order(links, lambda: wait_all(w_copies), lambda: None, load, compute, half, chunk)
    start_all(early[SLOTS:])
    wait_all([t_copy(i, 0, half) for i in range(SLOTS)])
    far()
    wait_all([t_copy(i, 0, chunk) for i in range(SLOTS)])
    wait_all(early)
    for m, (src, dst) in enumerate(results):
        pltpu.make_async_copy(src, dst, out_sem.at[m]).wait()
    links.finish()
    for c in pos_copies:
        c.wait_send()


def gather_qkv(x, ln_weight, pos, w_q, w_k, w_v, g, sp_size):
    rows, feat = x.shape
    seq = rows * sp_size
    width = w_q.shape[1] // sp_size
    inv_freq = ROPE_BASE ** (-jnp.arange(0, HEAD_DIM, 2, dtype=F32) / HEAD_DIM)
    freq = jnp.repeat(inv_freq, 2)[None, :]
    vmem = pl.BlockSpec(memory_space=pltpu.VMEM)
    made = [array(seq, width), array(seq, HEAD_DIM), array(HEAD_DIM, seq), array(seq, HEAD_DIM), array(HEAD_DIM, seq)]
    made += [array(seq, HEAD_DIM, dtype=F32)] * 2
    n = n_copies(CHUNKS, True)
    return pl.pallas_call(
        gather_qkv_kernel,
        in_specs=[HBM, vmem, vmem, vmem] + [HBM] * 4,
        out_specs=[HBM] * (3 + len(made)) + [vmem],
        out_shape=[array(seq, feat), array(feat, seq), array(seq, feat)] + made + [array(SLOTS, rows, LANE, dtype=F32)],
        scratch_shapes=[pltpu.VMEM(m.shape, m.dtype) for m in made] + [
            pltpu.VMEM((feat, width + PAIR), BF16), pltpu.VMEM((4, rows // 2, feat), BF16), pltpu.VMEM((SLOTS, feat, rows // 2), BF16),
            pltpu.VMEM((sp_size, rows // LANE, LANE), F32), SEM((N_PEERS,)), SEM((N_PEERS,)), SEM((n,)), SEM((n,)), SEM((3,)), SEM((4,)), SEM((SLOTS,)),
            SEM((SLOTS,)), SEM((len(made),)), SEM((4,)), SEM((4,))],
        compiler_params=remote_params(1),
        name="gather_qkv")(x, ln_weight.astype(F32)[None], pos.astype(F32).reshape(rows // LANE, LANE), freq, w_q, w_k, w_v, g)


def stack_heads(x):
    return jnp.concatenate([x[:, n * HEAD_DIM:(n + 1) * HEAD_DIM] for n in range(x.shape[1] // HEAD_DIM)], axis=0)


def causal(shape, bq, offset):
    rows = lax.rem(lax.broadcasted_iota(jnp.int32, shape, 0), bq) + offset
    return rows >= lax.broadcasted_iota(jnp.int32, shape, 1)


def fwd_step(qi, bq, bk, q_ref, kt_ref, v_ref, ot_ref, lse_ref, s_scr):
    q = stack_heads(q_ref[...])
    rows = q.shape[0]
    nfull = (qi * bq) // bk

    def scores(j):
        return dot(q, kt_ref[:, pl.ds(pl.multiple_of(j * bk, bk), bk)]) * (SCALE * LOG2E)

    def lane_max(m, s):
        for c in range(bk // LANE):
            m = jnp.maximum(m, s[:, c * LANE:(c + 1) * LANE])
        return m

    def score_step(j, m):
        s = scores(j)
        s_scr[j] = s
        return lane_max(m, s)

    m = lax.fori_loop(0, nfull, score_step, jnp.full((rows, LANE), -jnp.inf, F32))
    s = jnp.where(causal((rows, bk), bq, qi * bq - nfull * bk), scores(nfull), -jnp.inf)
    s_scr[nfull] = s
    m = jnp.max(lane_max(m, s), axis=1, keepdims=True)

    def value_step(j, carry):
        l, o = carry
        p = jnp.exp2(s_scr[j] - m)
        for t in range(bk // LANE):
            l = l + p[:, t * LANE:(t + 1) * LANE]
        o = o + dot(p.astype(BF16), v_ref[pl.ds(pl.multiple_of(j * bk, bk), bk), :])
        return l, o

    l, o = lax.fori_loop(0, nfull + 1, value_step, (jnp.zeros((rows, LANE), F32), jnp.zeros((rows, HEAD_DIM), F32)))
    l = jnp.sum(l, axis=1, keepdims=True)
    o = (o / l).astype(BF16)
    for n in range(rows // bq):
        ot_ref[n * HEAD_DIM:(n + 1) * HEAD_DIM, :] = o[n * bq:(n + 1) * bq].T
    lse_ref[...] = (m + jnp.log2(l)).reshape(lse_ref.shape)


def gather_fwd_kernel(n_fwd, relay, bq, bk, q_ref, kt_ref, v_ref, g_ref, wo_ref, _, ot_ref, lse_ref, gall_ref, do_ref,
                      s_scr, wo_scr, buf, send, recv, w_sem, load_sem, store_sem):
    step = pl.program_id(0)
    me = lax.axis_index("sp")
    rows, width = g_ref.shape[0], do_ref.shape[1]
    half = rows // 2
    chunk = half // CHUNKS

    def block(owner, part, c):
        start = owner * rows + part * half
        return gall_ref.at[pl.ds(pl.multiple_of(start, half), half) if c is None else pl.ds(pl.multiple_of(start + c * chunk, chunk), chunk)]

    own = lambda part: g_ref.at[pl.ds(part * half, half)]
    links = Exchange(send, recv, block, own, CHUNKS, True, lambda part: early_rows(g_ref, gall_ref, part, EARLY[-1], half))
    w_copy = pltpu.make_async_copy(wo_ref.at[pl.ds(pl.multiple_of(me * width, width), width)], wo_scr, w_sem.at[0])
    loads = [pltpu.make_async_copy(own(i), buf.at[i], load_sem.at[i]) for i in range(SLOTS)]
    stores = [pltpu.make_async_copy(buf.at[i], block(me, i, None), store_sem.at[i]) for i in range(SLOTS)]

    @pl.when(step == 0)
    def _():
        greet(neighbours())
        links.begin()
        w_copy.start()
        start_all(loads)

    @pl.when(step == relay)
    def _():
        links.near(0)

    @pl.when(step < n_fwd)
    def _():
        fwd_step(step, bq, bk, q_ref, kt_ref, v_ref, ot_ref, lse_ref, s_scr)

    def load(slot, r0, n):
        return pltpu.make_async_copy(gall_ref.at[pl.ds(pl.multiple_of(r0, n), n)], buf.at[slot, pl.ds(0, n)], load_sem.at[slot])

    def compute(slot, r0, n, _):
        do_ref[pl.ds(pl.multiple_of(r0, n), n), :] = dot_t(buf[slot, :n], wo_scr[...]).astype(BF16)

    def own_ready():
        wait_all(loads)
        start_all(stores)
        w_copy.wait()

    @pl.when(step == n_fwd)
    def _():
        far = in_order(links, own_ready, lambda: wait_all(stores), load, compute, half, chunk, started=True)
        far()
        links.finish()


def gather_forward(q, kt, v, g, w_o, g_all, bq=PAIR, bk=1024):
    seq, width = q.shape
    rows, feat = g.shape
    heads = width // HEAD_DIM
    n = seq // bq
    at = lambda i: jnp.minimum(i, n - 1)
    return pl.pallas_call(
        functools.partial(gather_fwd_kernel, n, (3 * n) // 4, bq, bk), grid=(n + 1,),
        in_specs=[pl.BlockSpec((bq, width), lambda i: (at(i), 0)), pl.BlockSpec((HEAD_DIM, seq), whole, **ONCE),
                  pl.BlockSpec((seq, HEAD_DIM), whole, **ONCE)] + [HBM] * 3,
        out_specs=[pl.BlockSpec((width, bq), lambda i: (0, at(i))), pl.BlockSpec((heads, bq, 1), lambda i: (0, at(i), 0)), HBM,
                   pl.BlockSpec((seq, width), whole)],
        out_shape=[array(width, seq), array(heads, seq, 1, dtype=F32), array(seq, feat),
                   array(seq, width)],
        scratch_shapes=[pltpu.VMEM((seq // bk, heads * bq, bk), F32), pltpu.VMEM((width, feat), BF16), pltpu.VMEM((4, rows // 2, feat), BF16),
                        SEM((n_copies(CHUNKS, True),)), SEM((n_copies(CHUNKS, True),)), SEM((1,)), SEM((4,)), SEM((SLOTS,))],
        compiler_params=remote_params(2),
        input_output_aliases={5: 2}, name="gather_fwd")(q, kt, v, g, w_o, g_all)


def bwd_step(qi, bq, bk, q_ref, do_ref, lse_ref, k_ref, kt_ref, vt_ref, cos_ref, sin_ref, g_out, dkt_ref, dvt_ref, p_scr, dp_scr):
    q = stack_heads(q_ref[...])
    do = stack_heads(do_ref[...])
    rows = q.shape[0]
    lse = lse_ref[...].reshape(rows, 1)
    q_t = q.T
    do_t = do.T
    nfull = (qi * bq) // bk

    @pl.when(qi == 0)
    def _():
        dkt_ref[...] = jnp.zeros_like(dkt_ref)
        dvt_ref[...] = jnp.zeros_like(dvt_ref)

    def prob_step(j, r, masked):
        sl = pl.ds(pl.multiple_of(j * bk, bk), bk)
        s = dot(q, kt_ref[:, sl]) * (SCALE * LOG2E)
        p = jnp.exp2(s - lse)
        if masked:
            p = jnp.where(causal((rows, bk), bq, qi * bq - nfull * bk), p, 0.0)
        dp = dot(do, vt_ref[:, sl])
        pd = p * dp
        for t in range(bk // LANE):
            r = r + pd[:, t * LANE:(t + 1) * LANE]
        p_scr[j] = p
        dp_scr[j] = dp
        dvt_ref[:, sl] += dot(do_t, p.astype(BF16))
        return r

    r = lax.fori_loop(0, nfull, lambda j, r: prob_step(j, r, False), jnp.zeros((rows, LANE), F32))
    r = prob_step(nfull, r, True)
    r = jnp.sum(r, axis=1, keepdims=True)

    def grad_step(j, dq):
        sl = pl.ds(pl.multiple_of(j * bk, bk), bk)
        ds = (p_scr[j] * (dp_scr[j] - r) * SCALE).astype(BF16)
        dkt_ref[:, sl] += dot(q_t, ds)
        return dq + dot(ds, k_ref[sl, :])

    dq = lax.fori_loop(0, nfull + 1, grad_step, jnp.zeros((rows, HEAD_DIM), F32))
    dq = dq.astype(BF16).astype(F32)
    here = pl.ds(pl.multiple_of(qi * bq, bq), bq)
    cos_t, sin_t = cos_ref[here, :], sin_ref[here, :]
    for n in range(rows // bq):
        g_out[:, n * HEAD_DIM:(n + 1) * HEAD_DIM] = rotate(dq[n * bq:(n + 1) * bq], cos_t, -sin_t).astype(BF16)


def gather_bwd_kernel(relay, bq, bk, q_ref, do_ref, lse_ref, k_ref, kt_ref, vt_ref, cos_ref, sin_ref, ot_ref,
                      gq_ref, gk_ref, gv_ref, otg_ref, otz_ref, p_scr, dp_scr, dkt_scr, dvt_scr, buf, send, recv, z_send, z_recv, load_sem, store_sem):
    step = pl.program_id(0)
    last = pl.num_programs(0) - 1
    me = lax.axis_index("sp")
    width, seq = ot_ref.shape
    half = width // 2
    tokens = otz_ref.shape[2]
    zn = flip(me, CORE)
    own = lambda part: ot_ref.at[pl.ds(part * half, half)]
    block = lambda owner, part, _: otg_ref.at[owner // 2, pl.ds(part * half, half)]
    links = Exchange(send, recv, block, own, 1, False)
    xn, yn = flip(me, X_BIT), flip(me, Y_BIT)
    dn = flip(xn, Y_BIT)
    mine = pl.ds(pl.multiple_of(zn * tokens, tokens), tokens)

    def to_other(n, owner):
        src = ot_ref.at[:, mine] if n == 0 else otg_ref.at[owner // 2, :, mine]
        return pltpu.make_async_remote_copy(src_ref=src, dst_ref=otz_ref.at[owner // 2], send_sem=z_send.at[n], recv_sem=z_recv.at[n],
                                            device_id={"sp": zn}, device_id_type=MESH)

    z = [to_other(n, o) for n, o in enumerate((me, xn, yn, dn))]
    n_buf, slab = buf.shape[0], buf.shape[1]
    n_slab = width // slab

    def slab_copies(n):
        rows = pl.ds(pl.multiple_of(n * slab, slab), slab)
        slot = n % n_buf
        return (pltpu.make_async_copy(ot_ref.at[rows], buf.at[slot], load_sem.at[slot]),
                pltpu.make_async_copy(buf.at[slot], otg_ref.at[me // 2, rows], store_sem.at[slot]))

    @pl.when(step == 0)
    def _():
        greet(neighbours())
        links.begin()
        z[0].start()

    @pl.when(step == relay)
    def _():
        links.near(0)

    @pl.when((step >= 2) & (step < n_slab + 2))
    def _():
        slab_copies(step - 2)[1].wait()

    @pl.when((step >= 1) & (step < n_slab + 1))
    def _():
        slab_copies(step - 1)[0].wait()
        slab_copies(step - 1)[1].start()

    @pl.when(step < n_slab)
    def _():
        slab_copies(step)[0].start()

    bwd_step(step, bq, bk, q_ref, do_ref, lse_ref, k_ref, kt_ref, vt_ref, cos_ref, sin_ref, gq_ref, dkt_scr, dvt_scr, p_scr, dp_scr)

    @pl.when(step == last)
    def _():
        links.near(1)
        start_all(z[1:3])

        def kv_rows(i, _):
            rows = pl.ds(pl.multiple_of(i * bk, bk), bk)
            dk = dkt_scr[:, rows].T.astype(BF16).astype(F32)
            gk_ref[rows, :] = rotate(dk, cos_ref[rows, :], -sin_ref[rows, :]).astype(BF16)
            gv_ref[rows, :] = dvt_scr[:, rows].T.astype(BF16)
            return 0

        lax.fori_loop(0, seq // bk, kv_rows, 0)
        links.far(0)
        z[3].start()
        receive(z)
        links.finish()
        for c in z:
            c.wait_send()


def gather_backward(q, do, lse, k, kt, vt, cos_t, sin_t, ot, sp_size, bq=PAIR, bk=512):
    seq, width = q.shape
    heads = width // HEAD_DIM
    chips, tokens = sp_size // 2, seq // sp_size
    n = seq // bq
    tile = pl.BlockSpec((bq, width), row)
    tall = pl.BlockSpec((seq, HEAD_DIM), whole, **ONCE)
    wide = pl.BlockSpec((HEAD_DIM, seq), whole, **ONCE)
    return pl.pallas_call(
        functools.partial(gather_bwd_kernel, (9 * n) // 16, bq, bk), grid=(n,),
        in_specs=[tile, tile, pl.BlockSpec((heads, bq, 1), lambda i: (0, i, 0)), tall, wide, wide, tall, tall, HBM],
        out_specs=[tile, tall, tall, HBM, HBM],
        out_shape=[array(seq, width), array(seq, HEAD_DIM), array(seq, HEAD_DIM), array(chips, width, seq), array(chips, width, tokens)],
        scratch_shapes=[pltpu.VMEM((seq // bk, heads * bq, bk), F32), pltpu.VMEM((seq // bk, heads * bq, bk), F32),
                        pltpu.VMEM((HEAD_DIM, seq), F32), pltpu.VMEM((HEAD_DIM, seq), F32), pltpu.VMEM((SLOTS, width // 8, seq), BF16),
                        SEM((n_copies(1, False),)), SEM((n_copies(1, False),)), SEM((4,)), SEM((4,)), SEM((SLOTS,)), SEM((SLOTS,))],
        compiler_params=remote_params(3),
        name="gather_bwd")(q, do, lse, k, kt, vt, cos_t, sin_t, ot)


def dw_o_kernel(core_ref, ot_ref, g_ref, final_ref, send_ref):
    y = dot(ot_ref[...], g_ref[...]).astype(BF16)
    final_ref[...] = y
    send_ref[...] = y


def dw_o_half(core, ot_all, g_all, bn=1024):
    half, width, seq = ot_all.shape
    feat = g_all.shape[1]
    return pl.pallas_call(
        dw_o_kernel,
        grid_spec=pltpu.PrefetchScalarGridSpec(
            num_scalar_prefetch=1, grid=(feat // bn, half),
            in_specs=[pl.BlockSpec((None, width, seq), lambda j, s, c: (s, 0, 0)), pl.BlockSpec((seq, bn), col)],
            out_specs=[pl.BlockSpec((width, bn), lambda j, s, c: (2 * s + c[0], j)), pl.BlockSpec((width, bn), lambda j, s, c: (s, j))]),
        out_shape=[array(2 * half * width, feat), array(half * width, feat)],
        compiler_params=PARAMS, cost_estimate=cost(2 * half * width * feat * seq), name="dw_o_half")(core, ot_all, g_all)


class Ride:
    def __init__(self, source, buf, targets, load_sem, store_sem):
        self.source, self.buf, self.targets, self.load_sem, self.store_sem = source, buf, targets, load_sem, store_sem

    def load(self, i):
        slot = lax.rem(i, SLOTS)
        return pltpu.make_async_copy(self.source(i), self.buf.at[slot], self.load_sem.at[slot])

    def stores(self, i):
        slot = lax.rem(i, SLOTS)
        return [pltpu.make_async_copy(src, dst, self.store_sem.at[slot, n]) for n, (src, dst) in enumerate(self.targets(i, self.buf.at[slot]))]

    def begin(self, i):
        @pl.when(i >= SLOTS)
        def _():
            wait_all(self.stores(i - SLOTS))

        self.load(i).start()

    def end(self, i, last):
        self.load(i).wait()
        start_all(self.stores(i))

        @pl.when(i == last)
        def _():
            for n in reversed(range(SLOTS)):
                wait_all(self.stores(i - n))


def half_ride(recv, half, dev, final, scratch):
    buf = scratch[0]
    n, w = buf.shape[1:]
    at = lambda i, base: pl.ds(pl.multiple_of(base + i * n, n), n)
    return Ride(lambda i: recv.at[at(i, 0)], buf, lambda i, src: [(src, final.at[at(i, half * recv.shape[0]), pl.ds(pl.multiple_of(dev * w, w), w)])], *scratch[1:])


def half_scratch(recv, steps):
    return [pltpu.VMEM((SLOTS, recv.shape[0] // steps, recv.shape[1]), BF16), SEM((SLOTS,)), SEM((SLOTS, 1))]


def out_kernel(ids_ref, mine_ref, other_ref, w_ref, low, high, _, out_ref, q_ref, o_scr, *scratch):
    i, last = grid_place()
    rides = [half_ride(r, m, ids_ref[1 + m], q_ref, scratch[3 * m:3 * m + 3]) for m, r in enumerate((low, high))]
    for r in rides:
        r.begin(i)

    @pl.when(i == 0)
    def _():
        core = lax.rem(ids_ref[0], 2)
        width = mine_ref.shape[1]
        for s in range(mine_ref.shape[0]):
            for ref, d in ((mine_ref, 2 * s + core), (other_ref, 2 * s + 1 - core)):
                o_scr[:, pl.ds(pl.multiple_of(d * width, width), width)] = ref[s].T

    out_ref[...] = dot(o_scr[...], w_ref[...]).astype(BF16)
    for r in rides:
        r.end(i, last)


def out_proj(ids, ot_all, ot_other, w_o, low, high, dw_q, bn=512):
    chips, width, tokens = ot_other.shape
    feat = w_o.shape[1]
    steps = feat // bn
    return pl.pallas_call(
        out_kernel,
        grid_spec=pltpu.PrefetchScalarGridSpec(
            num_scalar_prefetch=1, grid=(steps,),
            in_specs=[pl.BlockSpec((chips, width, tokens), lambda i, c: (0, 0, c[0]), **ONCE), pl.BlockSpec((chips, width, tokens), lambda i, c: (0, 0, 0), **ONCE),
                      pl.BlockSpec((w_o.shape[0], bn), col)] + [HBM] * 3,
            out_specs=[pl.BlockSpec((tokens, bn), col), HBM],
            scratch_shapes=[pltpu.VMEM((tokens, w_o.shape[0]), BF16)] + half_scratch(low, steps) + half_scratch(high, steps)),
        out_shape=[array(tokens, feat), array(*dw_q.shape)], input_output_aliases={6: 1},
        compiler_params=PARAMS, cost_estimate=cost(2 * tokens * w_o.size), name="out_proj")(ids, ot_all, ot_other, w_o, low, high, dw_q)


def dw_q_kernel(ids_ref, ht_ref, g_ref, final_ref, low_ref, high_ref):
    i = pl.program_id(0)
    y = dot(ht_ref[...], g_ref[...]).astype(BF16)
    final_ref[...] = y
    n = pl.num_programs(0) // 2

    @pl.when(i < n)
    def _():
        low_ref[...] = y

    @pl.when(i >= n)
    def _():
        high_ref[...] = y


def dw_q_own(ids, ht, gq, bm=512):
    feat, seq = ht.shape
    w = gq.shape[1]
    n = feat // bm
    return pl.pallas_call(
        dw_q_kernel,
        grid_spec=pltpu.PrefetchScalarGridSpec(
            num_scalar_prefetch=1, grid=(n,), in_specs=[pl.BlockSpec((bm, seq), row), pl.BlockSpec((seq, w), whole, **ONCE)],
            out_specs=[pl.BlockSpec((bm, w), lambda i, c: (i, c[0])), pl.BlockSpec((bm, w), lambda i, c: (jnp.minimum(i, n // 2 - 1), 0)),
                       pl.BlockSpec((bm, w), lambda i, c: (jnp.maximum(i - n // 2, 0), 0))]),
        out_shape=[array(feat, feat), array(feat // 2, w), array(feat // 2, w)],
        compiler_params=PARAMS, cost_estimate=cost(2 * seq * feat * w), name="dw_q_own")(ids, ht, gq)


def kv_columns(rows, src, k_ref, v_ref, owners):
    out = []
    for m, ref in enumerate((k_ref, v_ref)):
        for n, dev in enumerate(owners):
            at = (m * len(owners) + n) * HEAD_DIM
            out.append((src.at[:, at:at + HEAD_DIM], ref.at[rows, pl.ds(pl.multiple_of(dev * HEAD_DIM, HEAD_DIM), HEAD_DIM)]))
    return out


def dw_kv_kernel(n_dev, ids_ref, ht_ref, *refs):
    parts, refs = refs[:2 * n_dev], refs[2 * n_dev:]
    recvs, (q_ref, k_ref, v_ref, send_ref, x_scr, y_scr, y_sem, send_sem, x_sem, load_sem, *scratch) = refs[:SLOTS], refs[SLOTS + 1:]
    i, last = grid_place()
    rides = [half_ride(recvs[m], m, flip(ids_ref[0], CORE), q_ref, scratch[3 * m:3 * m + 3]) for m in range(SLOTS)]
    for r in rides:
        r.begin(i)
    bm, feat = ht_ref.shape[0], k_ref.shape[0]
    n_tok = send_ref.shape[0] - feat
    tokens = pltpu.make_async_copy(x_scr.at[pl.ds(pl.multiple_of(flip(ids_ref[0], CORE) * n_tok, n_tok), n_tok)], send_ref.at[pl.ds(feat, n_tok)], x_sem.at[0])
    owners = [ids_ref[1 + n] for n in range(n_dev)]

    @pl.when(i == 0)
    def _():
        loads = [pltpu.make_async_copy(p, x_scr.at[:, m * HEAD_DIM:(m + 1) * HEAD_DIM], load_sem.at[m]) for m, p in enumerate(parts)]
        start_all(loads)
        wait_all(loads)
        tokens.start()

    def stores(step):
        slot, rows = lax.rem(step, SLOTS), pl.ds(pl.multiple_of(step * bm, bm), bm)
        out = [pltpu.make_async_copy(src, dst, y_sem.at[slot, m]) for m, (src, dst) in enumerate(kv_columns(rows, y_scr.at[slot], k_ref, v_ref, owners))]
        return out + [pltpu.make_async_copy(y_scr.at[slot], send_ref.at[rows], send_sem.at[slot])]

    @pl.when(i >= SLOTS)
    def _():
        wait_all(stores(i - SLOTS))

    y_scr[lax.rem(i, SLOTS)] = dot(ht_ref[...], x_scr[...]).astype(BF16)
    start_all(stores(i))
    for r in rides:
        r.end(i, last)

    @pl.when(i == last)
    def _():
        tokens.wait()
        for m in reversed(range(SLOTS)):
            wait_all(stores(i - m))


def dw_kv_half(ids, ht, parts, halves, dw_q, shape, tokens, bm=512):
    feat, seq = ht.shape
    w = len(parts) * HEAD_DIM
    steps = feat // bm
    return pl.pallas_call(
        functools.partial(dw_kv_kernel, len(parts) // 2),
        grid_spec=pltpu.PrefetchScalarGridSpec(
            num_scalar_prefetch=1, grid=(steps,), in_specs=[pl.BlockSpec((bm, seq), row)] + [HBM] * (len(parts) + 3), out_specs=[HBM] * 4,
            scratch_shapes=[pltpu.VMEM((seq, w), BF16), pltpu.VMEM((SLOTS, bm, w), BF16), SEM((SLOTS, len(parts))), SEM((SLOTS,)), SEM((1,)), SEM((len(parts),))]
            + half_scratch(halves[0], steps) + half_scratch(halves[1], steps)),
        out_shape=[array(*dw_q.shape), array(*shape), array(*shape), array(feat + tokens, w)], input_output_aliases={4 + len(parts): 0},
        compiler_params=PARAMS, cost_estimate=cost(2 * seq * feat * w), name="dw_kv_half")(ids, ht, *parts, *halves, dw_q)


def dh_kernel(n_dev, ids_ref, wq_ref, wk_ref, wv_ref, x_ref, stat_ref, lnw_ref, tq_ref, t_ref, *refs):
    own, refs = refs[:2 * n_dev], refs[2 * n_dev:]
    kv_recv, o_recv, _, _, _, dx_ref, dlnw_ref, k_ref, v_ref, o_ref, g_scr, sum_scr, dy_scr, *scratch = refs
    i, last = grid_place()
    tokens, feat = x_ref.shape
    bf = wq_ref.shape[0]
    others = [ids_ref[1 + n_dev + n] for n in range(n_dev)]
    kv_buf, o_buf = scratch[0], scratch[3]
    core = lax.rem(ids_ref[0], 2)
    block_rows = lambda i, buf: pl.ds(pl.multiple_of(i * buf.shape[1], buf.shape[1]), buf.shape[1])

    def o_rows(i):
        n = o_buf.shape[1]
        per = HEAD_DIM * n_dev // n
        return pl.ds(pl.multiple_of(((2 * (i // per) + 1 - core) * per + lax.rem(i, per)) * n, n), n)

    rides = [Ride(lambda i: kv_recv.at[block_rows(i, kv_buf)], kv_buf, lambda i, src: kv_columns(block_rows(i, kv_buf), src, k_ref, v_ref, others), *scratch[1:3]),
             Ride(lambda i: o_recv.at[block_rows(i, o_buf)], o_buf, lambda i, src: [(src, o_ref.at[o_rows(i)])], *scratch[4:])]
    for r in rides:
        r.begin(i)
    nq, nk = wq_ref.shape[1], wk_ref.shape[1]
    slab = tokens // 8

    @pl.when(i == 0)
    def _():
        width = tq_ref.shape[1]
        for m in range(2 * n_dev):
            g_scr[:, m * width:(m + 1) * width] = tq_ref[m * tokens:(m + 1) * tokens, :]
            for x, dev in ((own[m][...], ids_ref[1 + m % n_dev]), (t_ref[:, m * HEAD_DIM:(m + 1) * HEAD_DIM], others[m % n_dev])):
                g_scr[:, pl.ds(pl.multiple_of(nq + (m // n_dev) * nk + dev * HEAD_DIM, HEAD_DIM), HEAD_DIM)] = x

        sum_scr[...] = jnp.zeros_like(sum_scr)

    y = dot_t(g_scr[:, :nq], wq_ref[...]) + dot_t(g_scr[:, nq:nq + nk], wk_ref[...]) + dot_t(g_scr[:, nq + nk:], wv_ref[...])
    for m in range(bf // LANE):
        part, at = slice(m * LANE, (m + 1) * LANE), pl.ds(pl.multiple_of(i * bf + m * LANE, LANE), LANE)
        hat = (x_ref[:, at].astype(F32) - stat_ref[0]) * stat_ref[1]
        dlnw_ref[:, part] = jnp.sum(y[:, part] * hat, axis=0, keepdims=True)
        dy = y[:, part] * lnw_ref[:, part]
        dy_scr[:, at] = dy
        sum_scr[0] += dy
        sum_scr[1] += dy * hat
    for r in rides:
        r.end(i, last)

    @pl.when(i == last)
    def _():
        def finish(m, _):
            here = pl.ds(pl.multiple_of(m * slab, slab), slab)
            mean_y, mean_yh = (jnp.sum(sum_scr[e, here, :], axis=1, keepdims=True) / feat for e in range(SLOTS))
            mean, rstd = (stat_ref[e, here, :1] for e in range(SLOTS))
            hat = (x_ref[here, :].astype(F32) - mean) * rstd
            dx_ref[here, :] = (rstd * (dy_scr[here, :] - mean_y - hat * mean_yh)).astype(BF16)
            return 0

        lax.fori_loop(0, tokens // slab, finish, 0)


def dh_proj(ids, w_q, w_k, w_v, x, stats, ln_weight, t_q, own, kv_recv, o_recv, finals, bf=512):
    tokens, feat = x.shape
    w = kv_recv.shape[1]
    n = len(own)
    ins = [w_q, w_k, w_v, x, stats, ln_weight.astype(F32)[None], t_q, kv_recv, *own, kv_recv, o_recv, *finals]
    specs = [pl.BlockSpec((bf, m.shape[1]), row) for m in (w_q, w_k, w_v)] + [pl.BlockSpec(x.shape, whole, **ONCE), pl.BlockSpec(stats.shape, lambda i, c: (0, 0, 0), **ONCE), pl.BlockSpec((1, bf), col)]
    specs += [pl.BlockSpec(t_q.shape, whole, **ONCE), pl.BlockSpec((tokens, w), lambda i, c: (feat // tokens, 0), **ONCE)]
    specs += [pl.BlockSpec((tokens, HEAD_DIM), lambda i, c: (c[0], 0), **ONCE) for _ in own]
    first = len(ins) - len(finals)
    steps = feat // bf
    return pl.pallas_call(
        functools.partial(dh_kernel, n // 2),
        grid_spec=pltpu.PrefetchScalarGridSpec(
            num_scalar_prefetch=1, grid=(steps,), in_specs=specs + [HBM] * (len(ins) - len(specs)),
            out_specs=[pl.BlockSpec(x.shape, whole, **ONCE), pl.BlockSpec((1, bf), col)] + [HBM] * len(finals),
            scratch_shapes=[pltpu.VMEM((tokens, w_q.shape[1] + 2 * w_k.shape[1]), BF16), pltpu.VMEM((SLOTS, tokens, LANE), F32), pltpu.VMEM(x.shape, F32),
                            pltpu.VMEM((SLOTS, feat // steps, w), BF16), SEM((SLOTS,)), SEM((SLOTS, n)),
                            pltpu.VMEM((SLOTS, o_recv.shape[0] // steps, feat), BF16), SEM((SLOTS,)), SEM((SLOTS, 1))]),
        out_shape=[array(tokens, feat), array(1, feat, dtype=F32)] + [array(*f.shape) for f in finals],
        input_output_aliases={1 + first + m: 2 + m for m in range(len(finals))},
        compiler_params=PARAMS, cost_estimate=cost(2 * tokens * (w_q.size + 2 * w_k.size)), name="dh_proj")(ids, *ins)


def copy_kernel(n, places, ids_ref, *refs):
    final, buf, load_sem, store_sem = refs[n + 1:]
    rows, w = buf.shape[1:]
    loads = [pltpu.make_async_copy(refs[m], buf.at[m], load_sem.at[m]) for m in range(n)]
    start_all(loads)
    stores = []
    for m, (owner, half) in enumerate(places):
        loads[m].wait()
        at = pl.ds(pl.multiple_of(ids_ref[owner] * w, w), w)
        stores.append(pltpu.make_async_copy(buf.at[m], final.at[pl.ds(half * rows, rows), at], store_sem.at[m]))
        stores[-1].start()
    wait_all(stores)


def copy_in(ids, blocks, places, final):
    n = len(blocks)
    return pl.pallas_call(
        functools.partial(copy_kernel, n, places),
        grid_spec=pltpu.PrefetchScalarGridSpec(num_scalar_prefetch=1, grid=(1,), in_specs=[HBM] * (n + 1), out_specs=HBM,
                                               scratch_shapes=[pltpu.VMEM((n,) + blocks[0].shape, BF16), SEM((n,)), SEM((n,))]),
        out_shape=array(*final.shape), input_output_aliases={n + 1: 0},
        compiler_params=pltpu.CompilerParams(vmem_limit_bytes=COPY_LIMIT), name="copy_in")(ids, *blocks, final)


def sum_kernel(x_ref, out_ref, all_scr, send, recv):
    me = lax.axis_index("sp")
    peers = everyone()
    greet(peers)
    copies = [pltpu.make_async_remote_copy(src_ref=x_ref, dst_ref=all_scr.at[me], send_sem=send.at[n], recv_sem=recv.at[n],
                                           device_id={"sp": p}, device_id_type=MESH) for n, p in enumerate(peers)]
    for c in copies:
        c.start()
    all_scr[me] = x_ref[...]
    for c in copies:
        c.wait_recv()
    total = all_scr[0]
    for n in range(1, all_scr.shape[0]):
        total = total + all_scr[n]
    out_ref[...] = total.astype(BF16)
    for c in copies:
        c.wait_send()


def sum_devices(x, sp_size):
    n = x.shape[0] // HEAD_DIM
    vmem = pl.BlockSpec(memory_space=pltpu.VMEM)
    return pl.pallas_call(
        sum_kernel, in_specs=[vmem], out_specs=vmem, out_shape=array(n, HEAD_DIM),
        scratch_shapes=[pltpu.VMEM((sp_size, n, HEAD_DIM), F32), SEM((sp_size - 1,)), SEM((sp_size - 1,))],
        compiler_params=remote_params(4), name="sum_devices")(x.reshape(n, HEAD_DIM)).reshape(-1)


def solution(mesh):
    sp_size = mesh.shape['sp']
    row_spec = P(('dp', 'sp'), None)
    pos_spec = P(('dp', 'sp'))
    full_spec = P(None, None)
    grad_spec = P('dp', None)

    def local_step(hidden, positions, d_attn, ln_weight, w_q, w_k, w_v, w_o):
        dev = lax.axis_index('sp')
        core = lax.rem(dev, SLOTS)
        local_rows, _ = hidden.shape
        _, ht, g_all, q, k, kt, v, vt, cos_t, sin_t, stats = gather_qkv(hidden, ln_weight, positions, w_q, w_k, w_v, d_attn, sp_size)
        ot, lse, g_all, do = gather_forward(q, kt, v, d_attn, w_o, g_all)
        gq, gk, gv, ot_all, ot_other = gather_backward(q, do, lse, k, kt, vt, cos_t, sin_t, ot, sp_size)
        other = lambda d: flip(d, CORE)
        dev_x, dev_y = flip(dev, X_BIT), flip(dev, Y_BIT)
        dev_d = flip(dev_x, Y_BIT)
        owners = [dev, dev_x, dev_y, dev_d]

        def to(x, bit):
            return lax.ppermute(x, 'sp', [(i, i ^ bit) for i in range(sp_size)])

        after = lambda x, *done: lax.optimization_barrier((x,) + done)[0]
        ids = lambda *d: jnp.stack(d)
        gk_x, gv_y, gv_x, gk_y = to(gk, X_BIT), to(gv, Y_BIT), to(gv, X_BIT), to(gk, Y_BIT)
        t_q = lax.all_to_all(gq, 'sp', 0, 0, tiled=True)
        dw_q, low, high = dw_q_own(dev.reshape(1), ht, gq)
        gk_d, gv_d = to(after(gk_x, low), Y_BIT), to(after(gv_y, low), X_BIT)
        low_x, high_y, high_x, low_y = to(low, X_BIT), to(high, Y_BIT), to(high, X_BIT), to(low, Y_BIT)
        low_z, high_z = to(low, CORE), to(high, CORE)
        dw_o, o_send = dw_o_half(after(core.reshape(1), low), ot_all, g_all)
        o_recv = to(o_send, CORE)
        parts = [gk, gk_x, gk_y, gk_d, gv, gv_x, gv_y, gv_d]
        dw_q, dw_k, dw_v, kv_send = dw_kv_half(ids(*owners[:1], *owners), ht, [after(parts[0], o_send)] + parts[1:], [low_z, high_z], dw_q, w_k.shape, local_rows)
        kv_recv = to(kv_send, CORE)
        attn_out, dw_q = out_proj(ids(dev, dev_x, dev_y), ot_all, ot_other, after(w_o, kv_send), low_x, high_y, dw_q)
        low_d, high_d = to(after(low_x, attn_out), Y_BIT), to(after(high_y, attn_out), X_BIT)
        low_zx, high_zy = to(after(low_x, attn_out), CORE), to(after(high_y, attn_out), CORE)
        dx, d_lnw, dw_k, dw_v, dw_o = dh_proj(ids(*owners[:1], *owners, *map(other, owners)), w_q, w_k, w_v, hidden, stats, ln_weight, t_q, parts, kv_recv, o_recv, [dw_k, dw_v, dw_o])
        high_zx, low_zy = to(after(high_x, dx), CORE), to(after(low_y, dx), CORE)
        d_lnw = sum_devices(d_lnw.reshape(-1), sp_size)
        low_zd, high_zd = to(after(low_d, d_lnw), CORE), to(after(high_d, d_lnw), CORE)
        dw_q = copy_in(ids(dev_x, dev_y, other(dev_x), other(dev_y)), [high_x, low_y, low_zx, high_zx, low_zy, high_zy],
                       [(0, HIGH), (1, LOW), (2, LOW), (2, HIGH), (3, LOW), (3, HIGH)], after(dw_q, d_lnw))
        dw_q = copy_in(ids(dev_d, other(dev_d)), [low_d, high_d, low_zd, high_zd], [(0, LOW), (0, HIGH), (1, LOW), (1, HIGH)], dw_q)
        return (attn_out, dx, d_lnw, dw_q, dw_k, dw_v, dw_o)

    return jax.shard_map(local_step, mesh=mesh,
                      in_specs=(row_spec, pos_spec, row_spec, P(None), full_spec, full_spec, full_spec, full_spec),
                      out_specs=(row_spec, row_spec, P('dp'), grad_spec, grad_spec, grad_spec, grad_spec),
                      check_vma=False)
```

```python
import functools
import math
import jax
import jax.numpy as jnp
from jax import lax
from jax.experimental import pallas as pl
from jax.experimental.pallas import tpu as pltpu
from jax.sharding import PartitionSpec as P

HEAD_DIM = LANE = 128
PAIR = 2 * HEAD_DIM
CORE, X_BIT, Y_BIT = 1, 2, 4
LOW, HIGH, SLOTS = 0, 1, 2
CHUNKS, N_PEERS = 2, 7
EARLY = (0, 32, 96)
EARLY_TOKENS = 1024
LN_EPS = 1e-5
ROPE_BASE = 10000.0
SCALE = HEAD_DIM ** -0.5
LOG2E = 1.4426950408889634
VMEM_LIMIT = 67_000_000
COPY_LIMIT = 20_000_000
BF16 = jnp.bfloat16
F32 = jnp.float32
MESH = pl.DeviceIdType.MESH
HBM = pl.BlockSpec(memory_space=pl.ANY)
SEM = pltpu.SemaphoreType.DMA
row = lambda i, *_: (i, 0)
col = lambda i, *_: (0, i)
whole = lambda *_: (0, 0)
ONCE = dict(pipeline_mode=pl.Buffered(1))
PARAMS = pltpu.CompilerParams(vmem_limit_bytes=VMEM_LIMIT)


def grid_place():
    return pl.program_id(0), pl.num_programs(0) - 1


def dot(x, y):
    return jnp.dot(x, y, preferred_element_type=F32)


def dot_t(x, y):
    return lax.dot_general(x, y, (((1,), (1,)), ((), ())), preferred_element_type=F32)


def array(*shape, dtype=BF16):
    return jax.ShapeDtypeStruct(shape, dtype)


def remote_params(number):
    return pltpu.CompilerParams(collective_id=number, has_side_effects=True, vmem_limit_bytes=VMEM_LIMIT)


def cost(flops):
    return pl.CostEstimate(flops=flops, bytes_accessed=flops // HEAD_DIM, transcendentals=0)


def rotate(x, cos_t, sin_t):
    lane = lax.broadcasted_iota(jnp.int32, x.shape, 1)
    swapped = jnp.where(lane % 2 == 0, pltpu.roll(x, HEAD_DIM - 1, 1), pltpu.roll(x, 1, 1))
    return x * cos_t + swapped * sin_t


def flip(i, bit):
    return i + bit - 2 * bit * ((i // bit) % 2)


class Exchange:
    def __init__(self, send, recv, block, own, chunks, partner, first=None):
        me = lax.axis_index("sp")
        xn, yn, zn = flip(me, X_BIT), flip(me, Y_BIT), flip(me, CORE)
        dn = flip(xn, Y_BIT)
        self.every = []

        def copy(owner, part, to, chunk=None, refs=None):
            n = len(self.every)
            src, dst = refs or (own(part) if owner is me else block(owner, part, chunk), block(owner, part, chunk))
            self.every.append(pltpu.make_async_remote_copy(src_ref=src, dst_ref=dst, send_sem=send.at[n], recv_sem=recv.at[n],
                                                           device_id={"sp": to}, device_id_type=MESH))
            return self.every[-1]

        self.first = [copy(me, part, to, refs=first and first(part)) for part, to in ((LOW, xn), (HIGH, yn))]
        self.second = [copy(me, HIGH, xn), copy(me, LOW, yn)]
        self.relay = [[copy(xn, LOW, yn, c), copy(yn, HIGH, xn, c)] for c in range(chunks)]
        if partner:
            self.to_own = [copy(me, LOW, zn), copy(me, HIGH, zn)]
            self.to_near = [[copy(xn, LOW, zn), copy(yn, HIGH, zn)], [copy(xn, HIGH, zn), copy(yn, LOW, zn)]]
            self.to_far = [[copy(dn, LOW, zn, c), copy(dn, HIGH, zn, c)] for c in range(chunks)]

    def begin(self):
        start_all(self.first)
        if hasattr(self, "to_own"):
            start_all(self.to_own)
        start_all(self.second)

    def near(self, n):
        for m, c in enumerate(self.second if n else self.first):
            c.wait_recv()
            if n == 0:
                start_all([r[m] for r in self.relay])
            if hasattr(self, "to_near"):
                self.to_near[n][m].start()

    def far(self, n):
        for m, c in enumerate(self.relay[n]):
            c.wait_recv()
            if hasattr(self, "to_far"):
                self.to_far[n][m].start()

    def finish(self):
        for c in self.every:
            c.wait_send()


def early_rows(g_ref, gall_ref, part, start, stop):
    rows = g_ref.shape[0]
    at = part * (rows // 2) + start
    n = stop - start
    return g_ref.at[pl.ds(at, n)], gall_ref.at[pl.ds(pl.multiple_of(lax.axis_index("sp") * rows + at, math.gcd(n, at) if at else n), n)]


def early_tokens(ot_ref, otg_ref, part, tokens):
    half = ot_ref.shape[0] // 2
    rows = pl.ds(part * half, half)
    return ot_ref.at[rows, tokens], otg_ref.at[lax.axis_index("sp") // 2, rows, tokens]


def start_all(copies):
    for c in copies:
        c.start()


def wait_all(copies):
    for c in copies:
        c.wait()


def receive(copies):
    for c in copies:
        c.wait_recv()


def n_copies(chunks, partner):
    return 4 + 2 * chunks + (6 + 2 * chunks if partner else 0)


def greet(peers):
    barrier = pltpu.get_barrier_semaphore()
    for p in peers:
        pl.semaphore_signal(barrier, inc=1, device_id={"sp": p}, device_id_type=MESH)
    pl.semaphore_wait(barrier, len(peers))


def neighbours():
    me = lax.axis_index("sp")
    return [flip(me, CORE), flip(me, X_BIT), flip(me, Y_BIT)]


def everyone():
    me = lax.axis_index("sp")
    xn, yn = flip(me, X_BIT), flip(me, Y_BIT)
    dn = flip(xn, Y_BIT)
    return [flip(me, CORE), xn, flip(xn, CORE), yn, flip(yn, CORE), dn, flip(dn, CORE)]


def arrival(i, e):
    me = lax.axis_index("sp")
    g, near = i // 2, (i // 2 + 1) // 2
    owner = me + (i % 2) * (flip(me, CORE) - me) + near * ((1 - e) * (flip(me, X_BIT) - me) + e * (flip(me, Y_BIT) - me))
    return owner, e + (g // 2) * (1 - 2 * e)


def in_order(links, start, then, load, work, half, chunk, started=False):
    rows = 2 * half

    def second():
        then()
        receive(links.to_own)

    steps = [start, second, (lambda: None) if started else (lambda: links.near(0)), lambda: receive(links.to_near[0]), lambda: links.near(1),
             lambda: receive(links.to_near[1])]

    def sweep(n_pairs, steps, place, n, fetch_from):
        def pair(i, _):
            for m, act in enumerate(steps):
                @pl.when(i == m)
                def _():
                    act()
            slot0 = 2 * (i % 2)
            at = [place(i, e) for e in range(SLOTS)]
            copies = [load(slot0 + e, at[e], n) for e in range(SLOTS)]

            @pl.when(i >= fetch_from)
            def _():
                start_all(copies)
                wait_all(copies)

            def one(e, _):
                work(slot0 + e, at[0] + e * (at[1] - at[0]), n, i == 0)
                return 0

            return lax.fori_loop(0, SLOTS, one, 0)

        lax.fori_loop(0, n_pairs, pair, 0)

    def place(i, e):
        owner, part = arrival(i, e)
        return owner * rows + part * half

    sweep(len(steps), steps, place, half, 1)
    me = lax.axis_index("sp")
    dn = flip(flip(me, X_BIT), Y_BIT)

    def far_place(i, e):
        return (dn + (i % 2) * (flip(me, CORE) - me)) * rows + e * half + (i // 2) * chunk

    steps = []
    for c in range(CHUNKS):
        steps += [functools.partial(links.far, c), functools.partial(receive, links.to_far[c])]
    return lambda: sweep(len(steps), steps, far_place, chunk, 0)


def gather_qkv_kernel(x_ref, lnw_ref, pos_ref, freq_ref, wq_ref, wk_ref, wv_ref, g_ref,
                      hall_ref, ht_ref, gall_ref, q_out, k_out, kt_out, v_out, vt_out, cos_out, sin_out, stat_ref,
                      q_ref, k_ref, kt_ref, v_ref, vt_ref, cos_ref, sin_ref, w_scr, buf, tbuf, pos_all,
                      pos_send, pos_recv, send, recv, w_sem, load_sem, store_sem, t_sem, out_sem, early_send, early_recv):
    me = lax.axis_index("sp")
    rows = x_ref.shape[0]
    half = rows // 2
    chunk = half // CHUNKS
    width = q_ref.shape[1]

    def block(owner, part, c):
        start = owner * rows + part * half
        return hall_ref.at[pl.ds(pl.multiple_of(start, half), half) if c is None else pl.ds(pl.multiple_of(start + c * chunk, chunk), chunk)]

    own = lambda part: block(me, part, None)
    loads = [pltpu.make_async_copy(x_ref.at[pl.ds(p * half, half)], buf.at[p], load_sem.at[p]) for p in range(SLOTS)]
    start_all(loads)
    column = lambda n: pl.ds(pl.multiple_of(me * n, n), n)
    w_copies = [pltpu.make_async_copy(wq_ref.at[:, column(width)], w_scr.at[:, pl.ds(0, width)], w_sem.at[0]),
                pltpu.make_async_copy(wk_ref.at[:, column(HEAD_DIM)], w_scr.at[:, pl.ds(width, HEAD_DIM)], w_sem.at[1]),
                pltpu.make_async_copy(wv_ref.at[:, column(HEAD_DIM)], w_scr.at[:, pl.ds(width + HEAD_DIM, HEAD_DIM)], w_sem.at[2])]
    start_all(w_copies)
    peers = everyone()
    greet(peers)
    pos_copies = [pltpu.make_async_remote_copy(src_ref=pos_ref, dst_ref=pos_all.at[me], send_sem=pos_send.at[i], recv_sem=pos_recv.at[i],
                                               device_id={"sp": p}, device_id_type=MESH) for i, p in enumerate(peers)]
    start_all(pos_copies)
    early = []
    for start, stop in zip(EARLY, EARLY[1:]):
        for part, to in ((LOW, flip(me, X_BIT)), (HIGH, flip(me, Y_BIT))):
            src, dst = early_rows(g_ref, gall_ref, part, start, stop)
            early.append(pltpu.make_async_remote_copy(src_ref=src, dst_ref=dst, send_sem=early_send.at[len(early)], recv_sem=early_recv.at[len(early)],
                                                      device_id={"sp": to}, device_id_type=MESH))
    start_all(early[:SLOTS])
    pos_all[me] = pos_ref[...]
    links = Exchange(send, recv, block, own, CHUNKS, True)
    stores = [pltpu.make_async_copy(buf.at[p], own(p), store_sem.at[p]) for p in range(SLOTS)]
    slab = half // 8
    for p in range(SLOTS):
        loads[p].wait()

        def norm(n, _):
            here = pl.ds(pl.multiple_of(n * slab, slab), slab)
            x = buf[p, here, :].astype(F32)
            mean = jnp.mean(x, axis=-1, keepdims=True)
            centered = x - mean
            rstd = lax.rsqrt(jnp.mean(centered * centered, axis=-1, keepdims=True) + LN_EPS)
            buf[p, here, :] = (centered * rstd * lnw_ref[...]).astype(BF16)
            for m, v in enumerate((mean, rstd)):
                stat_ref[m, pl.ds(pl.multiple_of(p * half + n * slab, slab), slab), :] = jnp.broadcast_to(v, (slab, LANE))
            return 0

        lax.fori_loop(0, half // slab, norm, 0)
        stores[p].start()
    for p in range(SLOTS):
        stores[p].wait()
        links.first[p].start()
    start_all(links.second + links.to_own)
    receive(pos_copies)

    def t_copy(tslot, r0, n):
        return pltpu.make_async_copy(tbuf.at[tslot, :, pl.ds(0, n)], ht_ref.at[:, pl.ds(r0, n)], t_sem.at[tslot])

    def compute(slot, r0, n, first):
        r0 = pl.multiple_of(r0, n)
        out = pl.ds(r0, n)
        for t in range(n // LANE):
            at = r0 + t * LANE
            p = pos_all[at // rows, pl.ds((at % rows) // LANE, 1), :]
            angle = jnp.broadcast_to(p, (LANE, LANE)).T * freq_ref[...]
            sign = jnp.where(lax.broadcasted_iota(jnp.int32, (LANE, LANE), 1) % 2 == 0, -1.0, 1.0)
            tr = pl.ds(pl.multiple_of(at, LANE), LANE)
            cos_ref[tr, :] = jnp.cos(angle)
            sin_ref[tr, :] = jnp.sin(angle) * sign
        cos_t, sin_t = cos_ref[out, :], sin_ref[out, :]
        h = buf[slot, :n]
        tslot = lax.rem(slot, SLOTS)

        @pl.when(jnp.logical_not(first))
        def _():
            t_copy(tslot, 0, n).wait()

        tbuf[tslot, :, :n] = h.T
        t_copy(tslot, r0, n).start()
        for m in range(width // PAIR):
            y = dot(h, w_scr[:, m * PAIR:(m + 1) * PAIR])
            for e in range(SLOTS):
                q_ref[out, m * PAIR + e * LANE: m * PAIR + (e + 1) * LANE] = rotate(y[:, e * LANE:(e + 1) * LANE], cos_t, sin_t).astype(BF16)
        y = dot(h, w_scr[:, width:width + PAIR])
        k, v = rotate(y[:, :LANE], cos_t, sin_t), y[:, LANE:]
        k_ref[out, :] = k.astype(BF16)
        kt_ref[:, out] = k.T.astype(BF16)
        v_ref[out, :] = v.astype(BF16)
        vt_ref[:, out] = v.T.astype(BF16)
        for m, (src, dst) in enumerate(results):
            at = (slice(None), out) if src.shape[0] == HEAD_DIM else (out,)
            pltpu.make_async_copy(src.at[at], dst.at[at], out_sem.at[m]).start()

    results = list(zip((q_ref, k_ref, kt_ref, v_ref, vt_ref, cos_ref, sin_ref), (q_out, k_out, kt_out, v_out, vt_out, cos_out, sin_out)))

    def load(slot, r0, n):
        return pltpu.make_async_copy(hall_ref.at[pl.ds(pl.multiple_of(r0, n), n)], buf.at[slot, pl.ds(0, n)], load_sem.at[slot])

    far = in_order(links, lambda: wait_all(w_copies), lambda: None, load, compute, half, chunk)
    start_all(early[SLOTS:])
    wait_all([t_copy(i, 0, half) for i in range(SLOTS)])
    far()
    wait_all([t_copy(i, 0, chunk) for i in range(SLOTS)])
    wait_all(early)
    for m, (src, dst) in enumerate(results):
        pltpu.make_async_copy(src, dst, out_sem.at[m]).wait()
    links.finish()
    for c in pos_copies:
        c.wait_send()


def gather_qkv(x, ln_weight, pos, w_q, w_k, w_v, g, sp_size):
    rows, feat = x.shape
    seq = rows * sp_size
    width = w_q.shape[1] // sp_size
    inv_freq = ROPE_BASE ** (-jnp.arange(0, HEAD_DIM, 2, dtype=F32) / HEAD_DIM)
    freq = jnp.repeat(inv_freq, 2)[None, :]
    vmem = pl.BlockSpec(memory_space=pltpu.VMEM)
    made = [array(seq, width), array(seq, HEAD_DIM), array(HEAD_DIM, seq), array(seq, HEAD_DIM), array(HEAD_DIM, seq)]
    made += [array(seq, HEAD_DIM, dtype=F32)] * 2
    n = n_copies(CHUNKS, True)
    return pl.pallas_call(
        gather_qkv_kernel,
        in_specs=[HBM, vmem, vmem, vmem] + [HBM] * 4,
        out_specs=[HBM] * (3 + len(made)) + [vmem],
        out_shape=[array(seq, feat), array(feat, seq), array(seq, feat)] + made + [array(SLOTS, rows, LANE, dtype=F32)],
        scratch_shapes=[pltpu.VMEM(m.shape, m.dtype) for m in made] + [
            pltpu.VMEM((feat, width + PAIR), BF16), pltpu.VMEM((4, rows // 2, feat), BF16), pltpu.VMEM((SLOTS, feat, rows // 2), BF16),
            pltpu.VMEM((sp_size, rows // LANE, LANE), F32), SEM((N_PEERS,)), SEM((N_PEERS,)), SEM((n,)), SEM((n,)), SEM((3,)), SEM((4,)), SEM((SLOTS,)),
            SEM((SLOTS,)), SEM((len(made),)), SEM((4,)), SEM((4,))],
        compiler_params=remote_params(1),
        name="gather_qkv")(x, ln_weight.astype(F32)[None], pos.astype(F32).reshape(rows // LANE, LANE), freq, w_q, w_k, w_v, g)


def stack_heads(x):
    return jnp.concatenate([x[:, n * HEAD_DIM:(n + 1) * HEAD_DIM] for n in range(x.shape[1] // HEAD_DIM)], axis=0)


def causal(shape, bq, offset):
    rows = lax.rem(lax.broadcasted_iota(jnp.int32, shape, 0), bq) + offset
    return rows >= lax.broadcasted_iota(jnp.int32, shape, 1)


def fwd_step(qi, bq, bk, q_ref, kt_ref, v_ref, ot_ref, lse_ref, s_scr):
    q = stack_heads(q_ref[...])
    rows = q.shape[0]
    nfull = (qi * bq) // bk

    def scores(j):
        return dot(q, kt_ref[:, pl.ds(pl.multiple_of(j * bk, bk), bk)]) * (SCALE * LOG2E)

    def lane_max(m, s):
        for c in range(bk // LANE):
            m = jnp.maximum(m, s[:, c * LANE:(c + 1) * LANE])
        return m

    def score_step(j, m):
        s = scores(j)
        s_scr[j] = s
        return lane_max(m, s)

    m = lax.fori_loop(0, nfull, score_step, jnp.full((rows, LANE), -jnp.inf, F32))
    s = jnp.where(causal((rows, bk), bq, qi * bq - nfull * bk), scores(nfull), -jnp.inf)
    s_scr[nfull] = s
    m = jnp.max(lane_max(m, s), axis=1, keepdims=True)

    def value_step(j, carry):
        l, o = carry
        p = jnp.exp2(s_scr[j] - m)
        for t in range(bk // LANE):
            l = l + p[:, t * LANE:(t + 1) * LANE]
        o = o + dot(p.astype(BF16), v_ref[pl.ds(pl.multiple_of(j * bk, bk), bk), :])
        return l, o

    l, o = lax.fori_loop(0, nfull + 1, value_step, (jnp.zeros((rows, LANE), F32), jnp.zeros((rows, HEAD_DIM), F32)))
    l = jnp.sum(l, axis=1, keepdims=True)
    o = (o / l).astype(BF16)
    for n in range(rows // bq):
        ot_ref[n * HEAD_DIM:(n + 1) * HEAD_DIM, :] = o[n * bq:(n + 1) * bq].T
    lse_ref[...] = (m + jnp.log2(l)).reshape(lse_ref.shape)


def gather_fwd_kernel(n_fwd, relay, bq, bk, q_ref, kt_ref, v_ref, g_ref, wo_ref, _, ot_ref, lse_ref, gall_ref, do_ref, otg_ref,
                      s_scr, wo_scr, buf, ot_buf, send, recv, w_sem, load_sem, store_sem, ot_sem, early_send, early_recv):
    step = pl.program_id(0)
    me = lax.axis_index("sp")
    rows, width = g_ref.shape[0], do_ref.shape[1]
    half = rows // 2
    chunk = half // CHUNKS

    def block(owner, part, c):
        start = owner * rows + part * half
        return gall_ref.at[pl.ds(pl.multiple_of(start, half), half) if c is None else pl.ds(pl.multiple_of(start + c * chunk, chunk), chunk)]

    own = lambda part: g_ref.at[pl.ds(part * half, half)]
    links = Exchange(send, recv, block, own, CHUNKS, True, lambda part: early_rows(g_ref, gall_ref, part, EARLY[-1], half))
    w_copy = pltpu.make_async_copy(wo_ref.at[pl.ds(pl.multiple_of(me * width, width), width)], wo_scr, w_sem.at[0])
    loads = [pltpu.make_async_copy(own(i), buf.at[i], load_sem.at[i]) for i in range(SLOTS)]
    stores = [pltpu.make_async_copy(buf.at[i], block(me, i, None), store_sem.at[i]) for i in range(SLOTS)]

    @pl.when(step == 0)
    def _():
        greet(neighbours())
        links.begin()
        w_copy.start()
        start_all(loads)

    @pl.when(step == relay)
    def _():
        links.near(0)

    def ot_copy(i):
        slot = lax.rem(i, SLOTS)
        return pltpu.make_async_copy(ot_buf.at[slot], ot_ref.at[:, pl.ds(pl.multiple_of(i * bq, bq), bq)], ot_sem.at[slot])

    @pl.when(step >= SLOTS)
    def _():
        ot_copy(step - SLOTS).wait()

    @pl.when(step < n_fwd)
    def _():
        fwd_step(step, bq, bk, q_ref, kt_ref, v_ref, ot_buf.at[lax.rem(step, SLOTS)], lse_ref, s_scr)
        ot_copy(step).start()

    def load(slot, r0, n):
        return pltpu.make_async_copy(gall_ref.at[pl.ds(pl.multiple_of(r0, n), n)], buf.at[slot, pl.ds(0, n)], load_sem.at[slot])

    def compute(slot, r0, n, _):
        do_ref[pl.ds(pl.multiple_of(r0, n), n), :] = dot_t(buf[slot, :n], wo_scr[...]).astype(BF16)

    def own_ready():
        wait_all(loads)
        start_all(stores)
        w_copy.wait()

    @pl.when(step == n_fwd)
    def _():
        ot_copy(n_fwd - 1).wait()
        early = []
        for part, to in ((LOW, flip(me, X_BIT)), (HIGH, flip(me, Y_BIT))):
            src, dst = early_tokens(ot_ref, otg_ref, part, slice(0, EARLY_TOKENS))
            early.append(pltpu.make_async_remote_copy(src_ref=src, dst_ref=dst, send_sem=early_send.at[part], recv_sem=early_recv.at[part],
                                                      device_id={"sp": to}, device_id_type=MESH))
        far = in_order(links, own_ready, lambda: wait_all(stores), load, compute, half, chunk, started=True)
        start_all(early)
        far()
        wait_all(early)
        links.finish()


def gather_forward(q, kt, v, g, w_o, g_all, bq=PAIR, bk=1024):
    seq, width = q.shape
    rows, feat = g.shape
    heads = width // HEAD_DIM
    n = seq // bq
    at = lambda i: jnp.minimum(i, n - 1)
    return pl.pallas_call(
        functools.partial(gather_fwd_kernel, n, (3 * n) // 4, bq, bk), grid=(n + 1,),
        in_specs=[pl.BlockSpec((bq, width), lambda i: (at(i), 0)), pl.BlockSpec((HEAD_DIM, seq), whole, **ONCE),
                  pl.BlockSpec((seq, HEAD_DIM), whole, **ONCE)] + [HBM] * 3,
        out_specs=[HBM, pl.BlockSpec((heads, bq, 1), lambda i: (0, at(i), 0)), HBM, pl.BlockSpec((seq, width), whole, **ONCE), HBM],
        out_shape=[array(width, seq), array(heads, seq, 1, dtype=F32), array(seq, feat), array(seq, width), array(seq // rows // 2, width, seq)],
        scratch_shapes=[pltpu.VMEM((seq // bk, heads * bq, bk), F32), pltpu.VMEM((width, feat), BF16), pltpu.VMEM((4, rows // 2, feat), BF16), pltpu.VMEM((SLOTS, width, bq), BF16),
                        SEM((n_copies(CHUNKS, True),)), SEM((n_copies(CHUNKS, True),)), SEM((1,)), SEM((4,)), SEM((SLOTS,)), SEM((SLOTS,)), SEM((SLOTS,)), SEM((SLOTS,))],
        compiler_params=remote_params(2),
        input_output_aliases={5: 2}, name="gather_fwd")(q, kt, v, g, w_o, g_all)


def bwd_step(qi, bq, bk, q_ref, do_ref, lse_ref, k_ref, kt_ref, vt_ref, cos_ref, sin_ref, g_out, dkt_ref, dvt_ref, p_scr, dp_scr):
    q = stack_heads(q_ref[...])
    do = stack_heads(do_ref[...])
    rows = q.shape[0]
    lse = lse_ref[...].reshape(rows, 1)
    q_t = q.T
    do_t = do.T
    heads = rows // bq
    wide, few = 2, heads // 2
    n_big = (qi * bq) // (wide * bk)
    tail = wide * n_big
    rest = (qi * bq - tail * bk) // bk

    @pl.when(qi == 0)
    def _():
        dkt_ref[...] = jnp.zeros_like(dkt_ref)
        dvt_ref[...] = jnp.zeros_like(dvt_ref)

    def chunks(n):
        return [slice(m * (rows // n), (m + 1) * (rows // n)) for m in range(n)]

    def prob_step(j, wide, n_chunks, r, masked=False):
        sl = pl.ds(pl.multiple_of(j * bk, bk), wide * bk)
        total, out = None, []
        for c in chunks(n_chunks):
            s = dot(q[c], kt_ref[:, sl]) * (SCALE * LOG2E)
            p = jnp.exp2(s - lse[c])
            if masked:
                p = jnp.where(causal(p.shape, bq, qi * bq - j * bk), p, 0.0)
            dp = dot(do[c], vt_ref[:, sl])
            pd = p * dp
            part = r[c]
            for t in range(wide * bk // LANE):
                part = part + pd[:, t * LANE:(t + 1) * LANE]
            out.append(part)
            for e in range(wide):
                p_scr[j + e, c, :] = p[:, e * bk:(e + 1) * bk]
                dp_scr[j + e, c, :] = dp[:, e * bk:(e + 1) * bk]
            d = dot(do_t[:, c], p.astype(BF16))
            total = d if total is None else total + d
        dvt_ref[:, sl] += total
        return jnp.concatenate(out, axis=0)

    r = jnp.zeros((rows, LANE), F32)
    r = lax.fori_loop(0, n_big, lambda j, r: prob_step(wide * j, wide, heads, r), r)
    r = lax.fori_loop(0, rest, lambda j, r: prob_step(tail, 1, few, r), r)
    r = prob_step(tail + rest, 1, few, r, True)
    r = jnp.sum(r, axis=1, keepdims=True)

    def grad_step(j, wide, n_chunks, dq):
        sl = pl.ds(pl.multiple_of(j * bk, bk), wide * bk)
        total, out = None, []
        for c in chunks(n_chunks):
            ds = jnp.concatenate([(p_scr[j + e, c, :] * (dp_scr[j + e, c, :] - r[c]) * SCALE).astype(BF16) for e in range(wide)], axis=1)
            d = dot(q_t[:, c], ds)
            total = d if total is None else total + d
            out.append(dq[c] + dot(ds, k_ref[sl, :]))
        dkt_ref[:, sl] += total
        return jnp.concatenate(out, axis=0)

    dq = jnp.zeros((rows, HEAD_DIM), F32)
    dq = lax.fori_loop(0, n_big, lambda j, dq: grad_step(wide * j, wide, heads, dq), dq)
    dq = lax.fori_loop(0, rest + 1, lambda j, dq: grad_step(tail + j, 1, few, dq), dq)
    dq = dq.astype(BF16).astype(F32)
    here = pl.ds(pl.multiple_of(qi * bq, bq), bq)
    cos_t, sin_t = cos_ref[here, :], sin_ref[here, :]
    for n in range(rows // bq):
        g_out[:, n * HEAD_DIM:(n + 1) * HEAD_DIM] = rotate(dq[n * bq:(n + 1) * bq], cos_t, -sin_t).astype(BF16)


def gather_bwd_kernel(relay, bq, bk, q_ref, do_ref, lse_ref, k_ref, kt_ref, vt_ref, cos_ref, sin_ref, ot_ref, _,
                      gq_ref, gk_ref, gv_ref, otg_ref, otz_ref, p_scr, dp_scr, dkt_scr, dvt_scr, buf, send, recv, z_send, z_recv, load_sem, store_sem):
    step = pl.program_id(0)
    last = pl.num_programs(0) - 1
    me = lax.axis_index("sp")
    width, seq = ot_ref.shape
    half = width // 2
    tokens = otz_ref.shape[2]
    zn = flip(me, CORE)
    own = lambda part: ot_ref.at[pl.ds(part * half, half)]
    block = lambda owner, part, _: otg_ref.at[owner // 2, pl.ds(part * half, half)]
    links = Exchange(send, recv, block, own, 1, False, lambda part: early_tokens(ot_ref, otg_ref, part, slice(EARLY_TOKENS, seq)))
    xn, yn = flip(me, X_BIT), flip(me, Y_BIT)
    dn = flip(xn, Y_BIT)
    mine = pl.ds(pl.multiple_of(zn * tokens, tokens), tokens)

    def to_other(n, owner):
        src = ot_ref.at[:, mine] if n == 0 else otg_ref.at[owner // 2, :, mine]
        return pltpu.make_async_remote_copy(src_ref=src, dst_ref=otz_ref.at[owner // 2], send_sem=z_send.at[n], recv_sem=z_recv.at[n],
                                            device_id={"sp": zn}, device_id_type=MESH)

    z = [to_other(n, o) for n, o in enumerate((me, xn, yn, dn))]
    n_buf, slab = buf.shape[0], buf.shape[1]
    n_slab = width // slab

    def slab_copies(n):
        rows = pl.ds(pl.multiple_of(n * slab, slab), slab)
        slot = n % n_buf
        return (pltpu.make_async_copy(ot_ref.at[rows], buf.at[slot], load_sem.at[slot]),
                pltpu.make_async_copy(buf.at[slot], otg_ref.at[me // 2, rows], store_sem.at[slot]))

    @pl.when(step == 0)
    def _():
        greet(neighbours())
        links.begin()
        z[0].start()

    @pl.when(step == relay)
    def _():
        links.near(0)

    @pl.when((step >= 2) & (step < n_slab + 2))
    def _():
        slab_copies(step - 2)[1].wait()

    @pl.when((step >= 1) & (step < n_slab + 1))
    def _():
        slab_copies(step - 1)[0].wait()
        slab_copies(step - 1)[1].start()

    @pl.when(step < n_slab)
    def _():
        slab_copies(step)[0].start()

    bwd_step(step, bq, bk, q_ref, do_ref, lse_ref, k_ref, kt_ref, vt_ref, cos_ref, sin_ref, gq_ref, dkt_scr, dvt_scr, p_scr, dp_scr)

    @pl.when(step == last)
    def _():
        links.near(1)
        start_all(z[1:3])

        def kv_rows(i, _):
            rows = pl.ds(pl.multiple_of(i * bk, bk), bk)
            dk = dkt_scr[:, rows].T.astype(BF16).astype(F32)
            gk_ref[rows, :] = rotate(dk, cos_ref[rows, :], -sin_ref[rows, :]).astype(BF16)
            gv_ref[rows, :] = dvt_scr[:, rows].T.astype(BF16)
            return 0

        lax.fori_loop(0, seq // bk, kv_rows, 0)
        links.far(0)
        z[3].start()
        receive(z)
        links.finish()
        for c in z:
            c.wait_send()


def gather_backward(q, do, lse, k, kt, vt, cos_t, sin_t, ot, ot_all, sp_size, bq=PAIR, bk=512):
    seq, width = q.shape
    heads = width // HEAD_DIM
    chips, tokens = sp_size // 2, seq // sp_size
    n = seq // bq
    tile = pl.BlockSpec((bq, width), row)
    tall = pl.BlockSpec((seq, HEAD_DIM), whole, **ONCE)
    wide = pl.BlockSpec((HEAD_DIM, seq), whole, **ONCE)
    return pl.pallas_call(
        functools.partial(gather_bwd_kernel, (9 * n) // 16, bq, bk), grid=(n,),
        in_specs=[tile, tile, pl.BlockSpec((heads, bq, 1), lambda i: (0, i, 0)), tall, wide, wide, tall, tall, HBM, HBM],
        out_specs=[tile, tall, tall, HBM, HBM],
        out_shape=[array(seq, width), array(seq, HEAD_DIM), array(seq, HEAD_DIM), array(chips, width, seq), array(chips, width, tokens)],
        scratch_shapes=[pltpu.VMEM((seq // bk, heads * bq, bk), F32), pltpu.VMEM((seq // bk, heads * bq, bk), F32),
                        pltpu.VMEM((HEAD_DIM, seq), F32), pltpu.VMEM((HEAD_DIM, seq), F32), pltpu.VMEM((SLOTS, width // 8, seq), BF16),
                        SEM((n_copies(1, False),)), SEM((n_copies(1, False),)), SEM((4,)), SEM((4,)), SEM((SLOTS,)), SEM((SLOTS,))],
        compiler_params=remote_params(3), input_output_aliases={9: 3},
        name="gather_bwd")(q, do, lse, k, kt, vt, cos_t, sin_t, ot, ot_all)


def dw_o_kernel(core_ref, ot_ref, g_ref, final_ref, send_ref):
    y = dot(ot_ref[...], g_ref[...]).astype(BF16)
    final_ref[...] = y
    send_ref[...] = y


def dw_o_half(core, ot_all, g_all, bn=1024):
    half, width, seq = ot_all.shape
    feat = g_all.shape[1]
    return pl.pallas_call(
        dw_o_kernel,
        grid_spec=pltpu.PrefetchScalarGridSpec(
            num_scalar_prefetch=1, grid=(feat // bn, half),
            in_specs=[pl.BlockSpec((None, width, seq), lambda j, s, c: (s, 0, 0)), pl.BlockSpec((seq, bn), col)],
            out_specs=[pl.BlockSpec((width, bn), lambda j, s, c: (2 * s + c[0], j)), pl.BlockSpec((width, bn), lambda j, s, c: (s, j))]),
        out_shape=[array(2 * half * width, feat), array(half * width, feat)],
        compiler_params=PARAMS, cost_estimate=cost(2 * half * width * feat * seq), name="dw_o_half")(core, ot_all, g_all)


class Ride:
    def __init__(self, source, buf, targets, load_sem, store_sem):
        self.source, self.buf, self.targets, self.load_sem, self.store_sem = source, buf, targets, load_sem, store_sem

    def load(self, i):
        slot = lax.rem(i, SLOTS)
        return pltpu.make_async_copy(self.source(i), self.buf.at[slot], self.load_sem.at[slot])

    def stores(self, i):
        slot = lax.rem(i, SLOTS)
        return [pltpu.make_async_copy(src, dst, self.store_sem.at[slot, n]) for n, (src, dst) in enumerate(self.targets(i, self.buf.at[slot]))]

    def begin(self, i):
        @pl.when(i >= SLOTS)
        def _():
            wait_all(self.stores(i - SLOTS))

        self.load(i).start()

    def end(self, i, last):
        self.load(i).wait()
        start_all(self.stores(i))

        @pl.when(i == last)
        def _():
            for n in reversed(range(SLOTS)):
                wait_all(self.stores(i - n))


def half_ride(recv, half, dev, final, scratch):
    buf = scratch[0]
    n, w = buf.shape[1:]
    at = lambda i, base: pl.ds(pl.multiple_of(base + i * n, n), n)
    return Ride(lambda i: recv.at[at(i, 0)], buf, lambda i, src: [(src, final.at[at(i, half * recv.shape[0]), pl.ds(pl.multiple_of(dev * w, w), w)])], *scratch[1:])


def half_scratch(recv, steps):
    return [pltpu.VMEM((SLOTS, recv.shape[0] // steps, recv.shape[1]), BF16), SEM((SLOTS,)), SEM((SLOTS, 1))]


def out_kernel(ids_ref, mine_ref, other_ref, w_ref, low, high, _, out_ref, q_ref, o_scr, *scratch):
    i, last = grid_place()
    rides = [half_ride(r, m, ids_ref[1 + m], q_ref, scratch[3 * m:3 * m + 3]) for m, r in enumerate((low, high))]
    for r in rides:
        r.begin(i)

    @pl.when(i == 0)
    def _():
        core = lax.rem(ids_ref[0], 2)
        width = mine_ref.shape[1]
        for s in range(mine_ref.shape[0]):
            for ref, d in ((mine_ref, 2 * s + core), (other_ref, 2 * s + 1 - core)):
                o_scr[:, pl.ds(pl.multiple_of(d * width, width), width)] = ref[s].T

    out_ref[...] = dot(o_scr[...], w_ref[...]).astype(BF16)
    for r in rides:
        r.end(i, last)


def out_proj(ids, ot_all, ot_other, w_o, low, high, dw_q, bn=512):
    chips, width, tokens = ot_other.shape
    feat = w_o.shape[1]
    steps = feat // bn
    return pl.pallas_call(
        out_kernel,
        grid_spec=pltpu.PrefetchScalarGridSpec(
            num_scalar_prefetch=1, grid=(steps,),
            in_specs=[pl.BlockSpec((chips, width, tokens), lambda i, c: (0, 0, c[0]), **ONCE), pl.BlockSpec((chips, width, tokens), lambda i, c: (0, 0, 0), **ONCE),
                      pl.BlockSpec((w_o.shape[0], bn), col)] + [HBM] * 3,
            out_specs=[pl.BlockSpec((tokens, bn), col), HBM],
            scratch_shapes=[pltpu.VMEM((tokens, w_o.shape[0]), BF16)] + half_scratch(low, steps) + half_scratch(high, steps)),
        out_shape=[array(tokens, feat), array(*dw_q.shape)], input_output_aliases={6: 1},
        compiler_params=PARAMS, cost_estimate=cost(2 * tokens * w_o.size), name="out_proj")(ids, ot_all, ot_other, w_o, low, high, dw_q)


def dw_q_kernel(ids_ref, ht_ref, g_ref, final_ref, low_ref, high_ref):
    i = pl.program_id(0)
    y = dot(ht_ref[...], g_ref[...]).astype(BF16)
    final_ref[...] = y
    n = pl.num_programs(0) // 2

    @pl.when(i < n)
    def _():
        low_ref[...] = y

    @pl.when(i >= n)
    def _():
        high_ref[...] = y


def dw_q_own(ids, ht, gq, bm=512):
    feat, seq = ht.shape
    w = gq.shape[1]
    n = feat // bm
    return pl.pallas_call(
        dw_q_kernel,
        grid_spec=pltpu.PrefetchScalarGridSpec(
            num_scalar_prefetch=1, grid=(n,), in_specs=[pl.BlockSpec((bm, seq), row), pl.BlockSpec((seq, w), whole, **ONCE)],
            out_specs=[pl.BlockSpec((bm, w), lambda i, c: (i, c[0])), pl.BlockSpec((bm, w), lambda i, c: (jnp.minimum(i, n // 2 - 1), 0)),
                       pl.BlockSpec((bm, w), lambda i, c: (jnp.maximum(i - n // 2, 0), 0))]),
        out_shape=[array(feat, feat), array(feat // 2, w), array(feat // 2, w)],
        compiler_params=PARAMS, cost_estimate=cost(2 * seq * feat * w), name="dw_q_own")(ids, ht, gq)


def kv_columns(rows, src, k_ref, v_ref, owners):
    out = []
    for m, ref in enumerate((k_ref, v_ref)):
        for n, dev in enumerate(owners):
            at = (m * len(owners) + n) * HEAD_DIM
            out.append((src.at[:, at:at + HEAD_DIM], ref.at[rows, pl.ds(pl.multiple_of(dev * HEAD_DIM, HEAD_DIM), HEAD_DIM)]))
    return out


def dw_kv_kernel(n_dev, ids_ref, ht_ref, *refs):
    parts, refs = refs[:2 * n_dev], refs[2 * n_dev:]
    recvs, (q_ref, k_ref, v_ref, send_ref, x_scr, y_scr, y_sem, send_sem, x_sem, load_sem, *scratch) = refs[:SLOTS], refs[SLOTS + 1:]
    i, last = grid_place()
    rides = [half_ride(recvs[m], m, flip(ids_ref[0], CORE), q_ref, scratch[3 * m:3 * m + 3]) for m in range(SLOTS)]
    for r in rides:
        r.begin(i)
    bm, feat = ht_ref.shape[0], k_ref.shape[0]
    n_tok = send_ref.shape[0] - feat
    tokens = pltpu.make_async_copy(x_scr.at[pl.ds(pl.multiple_of(flip(ids_ref[0], CORE) * n_tok, n_tok), n_tok)], send_ref.at[pl.ds(feat, n_tok)], x_sem.at[0])
    owners = [ids_ref[1 + n] for n in range(n_dev)]

    @pl.when(i == 0)
    def _():
        loads = [pltpu.make_async_copy(p, x_scr.at[:, m * HEAD_DIM:(m + 1) * HEAD_DIM], load_sem.at[m]) for m, p in enumerate(parts)]
        start_all(loads)
        wait_all(loads)
        tokens.start()

    def stores(step):
        slot, rows = lax.rem(step, SLOTS), pl.ds(pl.multiple_of(step * bm, bm), bm)
        out = [pltpu.make_async_copy(src, dst, y_sem.at[slot, m]) for m, (src, dst) in enumerate(kv_columns(rows, y_scr.at[slot], k_ref, v_ref, owners))]
        return out + [pltpu.make_async_copy(y_scr.at[slot], send_ref.at[rows], send_sem.at[slot])]

    @pl.when(i >= SLOTS)
    def _():
        wait_all(stores(i - SLOTS))

    y_scr[lax.rem(i, SLOTS)] = dot(ht_ref[...], x_scr[...]).astype(BF16)
    start_all(stores(i))
    for r in rides:
        r.end(i, last)

    @pl.when(i == last)
    def _():
        tokens.wait()
        for m in reversed(range(SLOTS)):
            wait_all(stores(i - m))


def dw_kv_half(ids, ht, parts, halves, dw_q, shape, tokens, bm=512):
    feat, seq = ht.shape
    w = len(parts) * HEAD_DIM
    steps = feat // bm
    return pl.pallas_call(
        functools.partial(dw_kv_kernel, len(parts) // 2),
        grid_spec=pltpu.PrefetchScalarGridSpec(
            num_scalar_prefetch=1, grid=(steps,), in_specs=[pl.BlockSpec((bm, seq), row)] + [HBM] * (len(parts) + 3), out_specs=[HBM] * 4,
            scratch_shapes=[pltpu.VMEM((seq, w), BF16), pltpu.VMEM((SLOTS, bm, w), BF16), SEM((SLOTS, len(parts))), SEM((SLOTS,)), SEM((1,)), SEM((len(parts),))]
            + half_scratch(halves[0], steps) + half_scratch(halves[1], steps)),
        out_shape=[array(*dw_q.shape), array(*shape), array(*shape), array(feat + tokens, w)], input_output_aliases={4 + len(parts): 0},
        compiler_params=PARAMS, cost_estimate=cost(2 * seq * feat * w), name="dw_kv_half")(ids, ht, *parts, *halves, dw_q)


def dh_kernel(n_dev, ids_ref, wq_ref, wk_ref, wv_ref, x_ref, stat_ref, lnw_ref, tq_ref, t_ref, *refs):
    own, refs = refs[:2 * n_dev], refs[2 * n_dev:]
    kv_recv, o_recv, _, _, _, dx_ref, dlnw_ref, k_ref, v_ref, o_ref, g_scr, sum_scr, dy_scr, *scratch = refs
    i, last = grid_place()
    tokens, feat = x_ref.shape
    bf = wq_ref.shape[0]
    others = [ids_ref[1 + n_dev + n] for n in range(n_dev)]
    kv_buf, o_buf = scratch[0], scratch[3]
    core = lax.rem(ids_ref[0], 2)
    block_rows = lambda i, buf: pl.ds(pl.multiple_of(i * buf.shape[1], buf.shape[1]), buf.shape[1])

    def o_rows(i):
        n = o_buf.shape[1]
        per = HEAD_DIM * n_dev // n
        return pl.ds(pl.multiple_of(((2 * (i // per) + 1 - core) * per + lax.rem(i, per)) * n, n), n)

    rides = [Ride(lambda i: kv_recv.at[block_rows(i, kv_buf)], kv_buf, lambda i, src: kv_columns(block_rows(i, kv_buf), src, k_ref, v_ref, others), *scratch[1:3]),
             Ride(lambda i: o_recv.at[block_rows(i, o_buf)], o_buf, lambda i, src: [(src, o_ref.at[o_rows(i)])], *scratch[4:])]
    for r in rides:
        r.begin(i)
    nq, nk = wq_ref.shape[1], wk_ref.shape[1]
    slab = tokens // 8

    @pl.when(i == 0)
    def _():
        width = tq_ref.shape[1]
        for m in range(2 * n_dev):
            g_scr[:, m * width:(m + 1) * width] = tq_ref[m * tokens:(m + 1) * tokens, :]
            for x, dev in ((own[m][...], ids_ref[1 + m % n_dev]), (t_ref[:, m * HEAD_DIM:(m + 1) * HEAD_DIM], others[m % n_dev])):
                g_scr[:, pl.ds(pl.multiple_of(nq + (m // n_dev) * nk + dev * HEAD_DIM, HEAD_DIM), HEAD_DIM)] = x

        sum_scr[...] = jnp.zeros_like(sum_scr)

    y = dot_t(g_scr[:, :nq], wq_ref[...]) + dot_t(g_scr[:, nq:nq + nk], wk_ref[...]) + dot_t(g_scr[:, nq + nk:], wv_ref[...])
    for m in range(bf // LANE):
        part, at = slice(m * LANE, (m + 1) * LANE), pl.ds(pl.multiple_of(i * bf + m * LANE, LANE), LANE)
        hat = (x_ref[:, at].astype(F32) - stat_ref[0]) * stat_ref[1]
        dlnw_ref[:, part] = jnp.sum(y[:, part] * hat, axis=0, keepdims=True)
        dy = y[:, part] * lnw_ref[:, part]
        dy_scr[:, at] = dy
        sum_scr[0] += dy
        sum_scr[1] += dy * hat
    for r in rides:
        r.end(i, last)

    @pl.when(i == last)
    def _():
        def finish(m, _):
            here = pl.ds(pl.multiple_of(m * slab, slab), slab)
            mean_y, mean_yh = (jnp.sum(sum_scr[e, here, :], axis=1, keepdims=True) / feat for e in range(SLOTS))
            mean, rstd = (stat_ref[e, here, :1] for e in range(SLOTS))
            hat = (x_ref[here, :].astype(F32) - mean) * rstd
            dx_ref[here, :] = (rstd * (dy_scr[here, :] - mean_y - hat * mean_yh)).astype(BF16)
            return 0

        lax.fori_loop(0, tokens // slab, finish, 0)


def dh_proj(ids, w_q, w_k, w_v, x, stats, ln_weight, t_q, own, kv_recv, o_recv, finals, bf=512):
    tokens, feat = x.shape
    w = kv_recv.shape[1]
    n = len(own)
    ins = [w_q, w_k, w_v, x, stats, ln_weight.astype(F32)[None], t_q, kv_recv, *own, kv_recv, o_recv, *finals]
    specs = [pl.BlockSpec((bf, m.shape[1]), row) for m in (w_q, w_k, w_v)] + [pl.BlockSpec(x.shape, whole, **ONCE), pl.BlockSpec(stats.shape, lambda i, c: (0, 0, 0), **ONCE), pl.BlockSpec((1, bf), col)]
    specs += [pl.BlockSpec(t_q.shape, whole, **ONCE), pl.BlockSpec((tokens, w), lambda i, c: (feat // tokens, 0), **ONCE)]
    specs += [pl.BlockSpec((tokens, HEAD_DIM), lambda i, c: (c[0], 0), **ONCE) for _ in own]
    first = len(ins) - len(finals)
    steps = feat // bf
    return pl.pallas_call(
        functools.partial(dh_kernel, n // 2),
        grid_spec=pltpu.PrefetchScalarGridSpec(
            num_scalar_prefetch=1, grid=(steps,), in_specs=specs + [HBM] * (len(ins) - len(specs)),
            out_specs=[pl.BlockSpec(x.shape, whole, **ONCE), pl.BlockSpec((1, bf), col)] + [HBM] * len(finals),
            scratch_shapes=[pltpu.VMEM((tokens, w_q.shape[1] + 2 * w_k.shape[1]), BF16), pltpu.VMEM((SLOTS, tokens, LANE), F32), pltpu.VMEM(x.shape, F32),
                            pltpu.VMEM((SLOTS, feat // steps, w), BF16), SEM((SLOTS,)), SEM((SLOTS, n)),
                            pltpu.VMEM((SLOTS, o_recv.shape[0] // steps, feat), BF16), SEM((SLOTS,)), SEM((SLOTS, 1))]),
        out_shape=[array(tokens, feat), array(1, feat, dtype=F32)] + [array(*f.shape) for f in finals],
        input_output_aliases={1 + first + m: 2 + m for m in range(len(finals))},
        compiler_params=PARAMS, cost_estimate=cost(2 * tokens * (w_q.size + 2 * w_k.size)), name="dh_proj")(ids, *ins)


def copy_kernel(n, places, ids_ref, *refs):
    final, buf, load_sem, store_sem = refs[n + 1:]
    rows, w = buf.shape[1:]
    loads = [pltpu.make_async_copy(refs[m], buf.at[m], load_sem.at[m]) for m in range(n)]
    start_all(loads)
    stores = []
    for m, (owner, half) in enumerate(places):
        loads[m].wait()
        at = pl.ds(pl.multiple_of(ids_ref[owner] * w, w), w)
        stores.append(pltpu.make_async_copy(buf.at[m], final.at[pl.ds(half * rows, rows), at], store_sem.at[m]))
        stores[-1].start()
    wait_all(stores)


def copy_in(ids, blocks, places, final):
    n = len(blocks)
    return pl.pallas_call(
        functools.partial(copy_kernel, n, places),
        grid_spec=pltpu.PrefetchScalarGridSpec(num_scalar_prefetch=1, grid=(1,), in_specs=[HBM] * (n + 1), out_specs=HBM,
                                               scratch_shapes=[pltpu.VMEM((n,) + blocks[0].shape, BF16), SEM((n,)), SEM((n,))]),
        out_shape=array(*final.shape), input_output_aliases={n + 1: 0},
        compiler_params=pltpu.CompilerParams(vmem_limit_bytes=COPY_LIMIT), name="copy_in")(ids, *blocks, final)


def sum_kernel(x_ref, out_ref, all_scr, send, recv):
    me = lax.axis_index("sp")
    peers = everyone()
    greet(peers)
    copies = [pltpu.make_async_remote_copy(src_ref=x_ref, dst_ref=all_scr.at[me], send_sem=send.at[n], recv_sem=recv.at[n],
                                           device_id={"sp": p}, device_id_type=MESH) for n, p in enumerate(peers)]
    for c in copies:
        c.start()
    all_scr[me] = x_ref[...]
    for c in copies:
        c.wait_recv()
    total = all_scr[0]
    for n in range(1, all_scr.shape[0]):
        total = total + all_scr[n]
    out_ref[...] = total.astype(BF16)
    for c in copies:
        c.wait_send()


def sum_devices(x, sp_size):
    n = x.shape[0] // HEAD_DIM
    vmem = pl.BlockSpec(memory_space=pltpu.VMEM)
    return pl.pallas_call(
        sum_kernel, in_specs=[vmem], out_specs=vmem, out_shape=array(n, HEAD_DIM),
        scratch_shapes=[pltpu.VMEM((sp_size, n, HEAD_DIM), F32), SEM((sp_size - 1,)), SEM((sp_size - 1,))],
        compiler_params=remote_params(4), name="sum_devices")(x.reshape(n, HEAD_DIM)).reshape(-1)


def solution(mesh):
    sp_size = mesh.shape['sp']
    row_spec = P(('dp', 'sp'), None)
    pos_spec = P(('dp', 'sp'))
    full_spec = P(None, None)
    grad_spec = P('dp', None)

    def local_step(hidden, positions, d_attn, ln_weight, w_q, w_k, w_v, w_o):
        dev = lax.axis_index('sp')
        core = lax.rem(dev, SLOTS)
        local_rows, _ = hidden.shape
        _, ht, g_all, q, k, kt, v, vt, cos_t, sin_t, stats = gather_qkv(hidden, ln_weight, positions, w_q, w_k, w_v, d_attn, sp_size)
        ot, lse, g_all, do, ot_all = gather_forward(q, kt, v, d_attn, w_o, g_all)
        gq, gk, gv, ot_all, ot_other = gather_backward(q, do, lse, k, kt, vt, cos_t, sin_t, ot, ot_all, sp_size)
        other = lambda d: flip(d, CORE)
        dev_x, dev_y = flip(dev, X_BIT), flip(dev, Y_BIT)
        dev_d = flip(dev_x, Y_BIT)
        owners = [dev, dev_x, dev_y, dev_d]

        def to(x, bit):
            return lax.ppermute(x, 'sp', [(i, i ^ bit) for i in range(sp_size)])

        after = lambda x, *done: lax.optimization_barrier((x,) + done)[0]
        ids = lambda *d: jnp.stack(d)
        gk_x, gv_y, gv_x, gk_y = to(gk, X_BIT), to(gv, Y_BIT), to(gv, X_BIT), to(gk, Y_BIT)
        t_q = lax.all_to_all(gq, 'sp', 0, 0, tiled=True)
        dw_q, low, high = dw_q_own(dev.reshape(1), ht, gq)
        gk_d, gv_d = to(after(gk_x, low), Y_BIT), to(after(gv_y, low), X_BIT)
        low_x, high_y, high_x, low_y = to(low, X_BIT), to(high, Y_BIT), to(high, X_BIT), to(low, Y_BIT)
        low_z, high_z = to(low, CORE), to(high, CORE)
        dw_o, o_send = dw_o_half(after(core.reshape(1), low), ot_all, g_all)
        o_recv = to(o_send, CORE)
        parts = [gk, gk_x, gk_y, gk_d, gv, gv_x, gv_y, gv_d]
        dw_q, dw_k, dw_v, kv_send = dw_kv_half(ids(*owners[:1], *owners), ht, [after(parts[0], o_send)] + parts[1:], [low_z, high_z], dw_q, w_k.shape, local_rows)
        kv_recv = to(kv_send, CORE)
        attn_out, dw_q = out_proj(ids(dev, dev_x, dev_y), ot_all, ot_other, after(w_o, kv_send), low_x, high_y, dw_q)
        low_d, high_d = to(after(low_x, attn_out), Y_BIT), to(after(high_y, attn_out), X_BIT)
        low_zx, high_zy = to(after(low_x, attn_out), CORE), to(after(high_y, attn_out), CORE)
        dx, d_lnw, dw_k, dw_v, dw_o = dh_proj(ids(*owners[:1], *owners, *map(other, owners)), w_q, w_k, w_v, hidden, stats, ln_weight, t_q, parts, kv_recv, o_recv, [dw_k, dw_v, dw_o])
        high_zx, low_zy = to(after(high_x, dx), CORE), to(after(low_y, dx), CORE)
        d_lnw = sum_devices(d_lnw.reshape(-1), sp_size)
        low_zd, high_zd = to(after(low_d, d_lnw), CORE), to(after(high_d, d_lnw), CORE)
        dw_q = copy_in(ids(dev_x, dev_y, other(dev_x), other(dev_y)), [high_x, low_y, low_zx, high_zx, low_zy, high_zy],
                       [(0, HIGH), (1, LOW), (2, LOW), (2, HIGH), (3, LOW), (3, HIGH)], after(dw_q, d_lnw))
        dw_q = copy_in(ids(dev_d, other(dev_d)), [low_d, high_d, low_zd, high_zd], [(0, LOW), (0, HIGH), (1, LOW), (1, HIGH)], dw_q)
        return (attn_out, dx, d_lnw, dw_q, dw_k, dw_v, dw_o)

    return jax.shard_map(local_step, mesh=mesh,
                      in_specs=(row_spec, pos_spec, row_spec, P(None), full_spec, full_spec, full_spec, full_spec),
                      out_specs=(row_spec, row_spec, P('dp'), grad_spec, grad_spec, grad_spec, grad_spec),
                      check_vma=False)
```

```python
import functools
import math
import jax
import jax.numpy as jnp
from jax import lax
from jax.experimental import pallas as pl
from jax.experimental.pallas import tpu as pltpu
from jax.sharding import PartitionSpec as P

HEAD_DIM = LANE = 128
PAIR = 2 * HEAD_DIM
CORE, X_BIT, Y_BIT = 1, 2, 4
LOW, HIGH, SLOTS = 0, 1, 2
CHUNKS, N_PEERS = 2, 7
EARLY = (0, 32, 96)
EARLY_TOKENS = 1024
LN_EPS = 1e-5
ROPE_BASE = 10000.0
SCALE = HEAD_DIM ** -0.5
LOG2E = 1.4426950408889634
VMEM_LIMIT = 67_000_000
COPY_LIMIT = 20_000_000
BF16 = jnp.bfloat16
F32 = jnp.float32
MESH = pl.DeviceIdType.MESH
HBM = pl.BlockSpec(memory_space=pl.ANY)
SEM = pltpu.SemaphoreType.DMA
row = lambda i, *_: (i, 0)
col = lambda i, *_: (0, i)
whole = lambda *_: (0, 0)
ONCE = dict(pipeline_mode=pl.Buffered(1))
PARAMS = pltpu.CompilerParams(vmem_limit_bytes=VMEM_LIMIT)


def grid_place():
    return pl.program_id(0), pl.num_programs(0) - 1


def dot(x, y):
    return jnp.dot(x, y, preferred_element_type=F32)


def dot_t(x, y):
    return lax.dot_general(x, y, (((1,), (1,)), ((), ())), preferred_element_type=F32)


def array(*shape, dtype=BF16):
    return jax.ShapeDtypeStruct(shape, dtype)


def remote_params(number):
    return pltpu.CompilerParams(collective_id=number, has_side_effects=True, vmem_limit_bytes=VMEM_LIMIT)


def cost(flops):
    return pl.CostEstimate(flops=flops, bytes_accessed=flops // HEAD_DIM, transcendentals=0)


def rotate(x, cos_t, sin_t):
    lane = lax.broadcasted_iota(jnp.int32, x.shape, 1)
    swapped = jnp.where(lane % 2 == 0, pltpu.roll(x, HEAD_DIM - 1, 1), pltpu.roll(x, 1, 1))
    return x * cos_t + swapped * sin_t


def flip(i, bit):
    return i + bit - 2 * bit * ((i // bit) % 2)


class Exchange:
    def __init__(self, send, recv, block, own, chunks, partner, first=None):
        me = lax.axis_index("sp")
        xn, yn, zn = flip(me, X_BIT), flip(me, Y_BIT), flip(me, CORE)
        dn = flip(xn, Y_BIT)
        self.every = []

        def copy(owner, part, to, chunk=None, refs=None):
            n = len(self.every)
            src, dst = refs or (own(part) if owner is me else block(owner, part, chunk), block(owner, part, chunk))
            self.every.append(pltpu.make_async_remote_copy(src_ref=src, dst_ref=dst, send_sem=send.at[n], recv_sem=recv.at[n],
                                                           device_id={"sp": to}, device_id_type=MESH))
            return self.every[-1]

        self.first = [copy(me, part, to, refs=first and first(part)) for part, to in ((LOW, xn), (HIGH, yn))]
        self.second = [copy(me, HIGH, xn), copy(me, LOW, yn)]
        self.relay = [[copy(xn, LOW, yn, c), copy(yn, HIGH, xn, c)] for c in range(chunks)]
        if partner:
            self.to_own = [copy(me, LOW, zn), copy(me, HIGH, zn)]
            self.to_near = [[copy(xn, LOW, zn), copy(yn, HIGH, zn)], [copy(xn, HIGH, zn), copy(yn, LOW, zn)]]
            self.to_far = [[copy(dn, LOW, zn, c), copy(dn, HIGH, zn, c)] for c in range(chunks)]

    def begin(self):
        start_all(self.first)
        if hasattr(self, "to_own"):
            start_all(self.to_own)
        start_all(self.second)

    def near(self, n):
        for m, c in enumerate(self.second if n else self.first):
            c.wait_recv()
            if n == 0:
                start_all([r[m] for r in self.relay])
            if hasattr(self, "to_near"):
                self.to_near[n][m].start()

    def far(self, n):
        for m, c in enumerate(self.relay[n]):
            c.wait_recv()
            if hasattr(self, "to_far"):
                self.to_far[n][m].start()

    def finish(self):
        for c in self.every:
            c.wait_send()


def early_rows(g_ref, gall_ref, part, start, stop):
    rows = g_ref.shape[0]
    at = part * (rows // 2) + start
    n = stop - start
    return g_ref.at[pl.ds(at, n)], gall_ref.at[pl.ds(pl.multiple_of(lax.axis_index("sp") * rows + at, math.gcd(n, at) if at else n), n)]


def early_tokens(ot_ref, otg_ref, part, tokens):
    half = ot_ref.shape[0] // 2
    rows = pl.ds(part * half, half)
    return ot_ref.at[rows, tokens], otg_ref.at[lax.axis_index("sp") // 2, rows, tokens]


def start_all(copies):
    for c in copies:
        c.start()


def wait_all(copies):
    for c in copies:
        c.wait()


def receive(copies):
    for c in copies:
        c.wait_recv()


def n_copies(chunks, partner):
    return 4 + 2 * chunks + (6 + 2 * chunks if partner else 0)


def greet(peers):
    barrier = pltpu.get_barrier_semaphore()
    for p in peers:
        pl.semaphore_signal(barrier, inc=1, device_id={"sp": p}, device_id_type=MESH)
    pl.semaphore_wait(barrier, len(peers))


def neighbours():
    me = lax.axis_index("sp")
    return [flip(me, CORE), flip(me, X_BIT), flip(me, Y_BIT)]


def everyone():
    me = lax.axis_index("sp")
    xn, yn = flip(me, X_BIT), flip(me, Y_BIT)
    dn = flip(xn, Y_BIT)
    return [flip(me, CORE), xn, flip(xn, CORE), yn, flip(yn, CORE), dn, flip(dn, CORE)]


def arrival(i, e):
    me = lax.axis_index("sp")
    g, near = i // 2, (i // 2 + 1) // 2
    owner = me + (i % 2) * (flip(me, CORE) - me) + near * ((1 - e) * (flip(me, X_BIT) - me) + e * (flip(me, Y_BIT) - me))
    return owner, e + (g // 2) * (1 - 2 * e)


def in_order(links, start, then, load, work, half, chunk, started=False):
    rows = 2 * half

    def second():
        then()
        receive(links.to_own)

    steps = [start, second, (lambda: None) if started else (lambda: links.near(0)), lambda: receive(links.to_near[0]), lambda: links.near(1),
             lambda: receive(links.to_near[1])]

    def sweep(n_pairs, steps, place, n, fetch_from):
        def pair(i, _):
            for m, act in enumerate(steps):
                @pl.when(i == m)
                def _():
                    act()
            slot0 = 2 * (i % 2)
            at = [place(i, e) for e in range(SLOTS)]
            copies = [load(slot0 + e, at[e], n) for e in range(SLOTS)]

            @pl.when(i >= fetch_from)
            def _():
                start_all(copies)
                wait_all(copies)

            def one(e, _):
                work(slot0 + e, at[0] + e * (at[1] - at[0]), n, i == 0)
                return 0

            return lax.fori_loop(0, SLOTS, one, 0)

        lax.fori_loop(0, n_pairs, pair, 0)

    def place(i, e):
        owner, part = arrival(i, e)
        return owner * rows + part * half

    sweep(len(steps), steps, place, half, 1)
    me = lax.axis_index("sp")
    dn = flip(flip(me, X_BIT), Y_BIT)

    def far_place(i, e):
        return (dn + (i % 2) * (flip(me, CORE) - me)) * rows + e * half + (i // 2) * chunk

    steps = []
    for c in range(CHUNKS):
        steps += [functools.partial(links.far, c), functools.partial(receive, links.to_far[c])]
    return lambda: sweep(len(steps), steps, far_place, chunk, 0)


def gather_qkv_kernel(x_ref, lnw_ref, pos_ref, freq_ref, wq_ref, wk_ref, wv_ref, g_ref,
                      hall_ref, ht_ref, gall_ref, q_out, k_out, kt_out, v_out, vt_out, cos_out, sin_out, stat_ref,
                      q_ref, k_ref, kt_ref, v_ref, vt_ref, cos_ref, sin_ref, w_scr, buf, tbuf, pos_all,
                      pos_send, pos_recv, send, recv, w_sem, load_sem, store_sem, t_sem, out_sem, early_send, early_recv):
    me = lax.axis_index("sp")
    rows = x_ref.shape[0]
    half = rows // 2
    chunk = half // CHUNKS
    width = q_ref.shape[1]

    def block(owner, part, c):
        start = owner * rows + part * half
        return hall_ref.at[pl.ds(pl.multiple_of(start, half), half) if c is None else pl.ds(pl.multiple_of(start + c * chunk, chunk), chunk)]

    own = lambda part: block(me, part, None)
    loads = [pltpu.make_async_copy(x_ref.at[pl.ds(p * half, half)], buf.at[p], load_sem.at[p]) for p in range(SLOTS)]
    start_all(loads)
    column = lambda n: pl.ds(pl.multiple_of(me * n, n), n)
    w_copies = [pltpu.make_async_copy(wq_ref.at[:, column(width)], w_scr.at[:, pl.ds(0, width)], w_sem.at[0]),
                pltpu.make_async_copy(wk_ref.at[:, column(HEAD_DIM)], w_scr.at[:, pl.ds(width, HEAD_DIM)], w_sem.at[1]),
                pltpu.make_async_copy(wv_ref.at[:, column(HEAD_DIM)], w_scr.at[:, pl.ds(width + HEAD_DIM, HEAD_DIM)], w_sem.at[2])]
    start_all(w_copies)
    peers = everyone()
    greet(peers)
    pos_copies = [pltpu.make_async_remote_copy(src_ref=pos_ref, dst_ref=pos_all.at[me], send_sem=pos_send.at[i], recv_sem=pos_recv.at[i],
                                               device_id={"sp": p}, device_id_type=MESH) for i, p in enumerate(peers)]
    start_all(pos_copies)
    early = []
    for start, stop in zip(EARLY, EARLY[1:]):
        for part, to in ((LOW, flip(me, X_BIT)), (HIGH, flip(me, Y_BIT))):
            src, dst = early_rows(g_ref, gall_ref, part, start, stop)
            early.append(pltpu.make_async_remote_copy(src_ref=src, dst_ref=dst, send_sem=early_send.at[len(early)], recv_sem=early_recv.at[len(early)],
                                                      device_id={"sp": to}, device_id_type=MESH))
    start_all(early[:SLOTS])
    pos_all[me] = pos_ref[...]
    links = Exchange(send, recv, block, own, CHUNKS, True)
    stores = [pltpu.make_async_copy(buf.at[p], own(p), store_sem.at[p]) for p in range(SLOTS)]
    slab = half // 8
    for p in range(SLOTS):
        loads[p].wait()

        def norm(n, _):
            here = pl.ds(pl.multiple_of(n * slab, slab), slab)
            x = buf[p, here, :].astype(F32)
            mean = jnp.mean(x, axis=-1, keepdims=True)
            centered = x - mean
            rstd = lax.rsqrt(jnp.mean(centered * centered, axis=-1, keepdims=True) + LN_EPS)
            buf[p, here, :] = (centered * rstd * lnw_ref[...]).astype(BF16)
            for m, v in enumerate((mean, rstd)):
                stat_ref[m, pl.ds(pl.multiple_of(p * half + n * slab, slab), slab), :] = jnp.broadcast_to(v, (slab, LANE))
            return 0

        lax.fori_loop(0, half // slab, norm, 0)
        stores[p].start()
    for p in range(SLOTS):
        stores[p].wait()
        links.first[p].start()
    start_all(links.second + links.to_own)
    receive(pos_copies)

    def t_copy(tslot, r0, n):
        return pltpu.make_async_copy(tbuf.at[tslot, :, pl.ds(0, n)], ht_ref.at[:, pl.ds(r0, n)], t_sem.at[tslot])

    def compute(slot, r0, n, first):
        r0 = pl.multiple_of(r0, n)
        out = pl.ds(r0, n)
        for t in range(n // LANE):
            at = r0 + t * LANE
            p = pos_all[at // rows, pl.ds((at % rows) // LANE, 1), :]
            angle = jnp.broadcast_to(p, (LANE, LANE)).T * freq_ref[...]
            sign = jnp.where(lax.broadcasted_iota(jnp.int32, (LANE, LANE), 1) % 2 == 0, -1.0, 1.0)
            tr = pl.ds(pl.multiple_of(at, LANE), LANE)
            cos_ref[tr, :] = jnp.cos(angle)
            sin_ref[tr, :] = jnp.sin(angle) * sign
        cos_t, sin_t = cos_ref[out, :], sin_ref[out, :]
        h = buf[slot, :n]
        tslot = lax.rem(slot, SLOTS)

        @pl.when(jnp.logical_not(first))
        def _():
            t_copy(tslot, 0, n).wait()

        tbuf[tslot, :, :n] = h.T
        t_copy(tslot, r0, n).start()
        for m in range(width // PAIR):
            y = dot(h, w_scr[:, m * PAIR:(m + 1) * PAIR])
            for e in range(SLOTS):
                q_ref[out, m * PAIR + e * LANE: m * PAIR + (e + 1) * LANE] = rotate(y[:, e * LANE:(e + 1) * LANE], cos_t, sin_t).astype(BF16)
        y = dot(h, w_scr[:, width:width + PAIR])
        k, v = rotate(y[:, :LANE], cos_t, sin_t), y[:, LANE:]
        k_ref[out, :] = k.astype(BF16)
        kt_ref[:, out] = k.T.astype(BF16)
        v_ref[out, :] = v.astype(BF16)
        vt_ref[:, out] = v.T.astype(BF16)
        for m, (src, dst) in enumerate(results):
            at = (slice(None), out) if src.shape[0] == HEAD_DIM else (out,)
            pltpu.make_async_copy(src.at[at], dst.at[at], out_sem.at[m]).start()

    results = list(zip((q_ref, k_ref, kt_ref, v_ref, vt_ref, cos_ref, sin_ref), (q_out, k_out, kt_out, v_out, vt_out, cos_out, sin_out)))

    def load(slot, r0, n):
        return pltpu.make_async_copy(hall_ref.at[pl.ds(pl.multiple_of(r0, n), n)], buf.at[slot, pl.ds(0, n)], load_sem.at[slot])

    far = in_order(links, lambda: wait_all(w_copies), lambda: None, load, compute, half, chunk)
    start_all(early[SLOTS:])
    wait_all([t_copy(i, 0, half) for i in range(SLOTS)])
    far()
    wait_all([t_copy(i, 0, chunk) for i in range(SLOTS)])
    wait_all(early)
    for m, (src, dst) in enumerate(results):
        pltpu.make_async_copy(src, dst, out_sem.at[m]).wait()
    links.finish()
    for c in pos_copies:
        c.wait_send()


def gather_qkv(x, ln_weight, pos, w_q, w_k, w_v, g, sp_size):
    rows, feat = x.shape
    seq = rows * sp_size
    width = w_q.shape[1] // sp_size
    freq = ROPE_BASE ** (-(jnp.arange(HEAD_DIM) // 2 * 2).astype(F32) / HEAD_DIM)[None, :]
    vmem = pl.BlockSpec(memory_space=pltpu.VMEM)
    made = [array(seq, width), array(seq, HEAD_DIM), array(HEAD_DIM, seq), array(seq, HEAD_DIM), array(HEAD_DIM, seq)]
    made += [array(seq, HEAD_DIM, dtype=F32)] * 2
    n = n_copies(CHUNKS, True)
    return pl.pallas_call(
        gather_qkv_kernel,
        in_specs=[HBM, vmem, vmem, vmem] + [HBM] * 4,
        out_specs=[HBM] * (3 + len(made)) + [vmem],
        out_shape=[array(seq, feat), array(feat, seq), array(seq, feat)] + made + [array(SLOTS, rows, LANE, dtype=F32)],
        scratch_shapes=[pltpu.VMEM(m.shape, m.dtype) for m in made] + [
            pltpu.VMEM((feat, width + PAIR), BF16), pltpu.VMEM((4, rows // 2, feat), BF16), pltpu.VMEM((SLOTS, feat, rows // 2), BF16),
            pltpu.VMEM((sp_size, rows // LANE, LANE), F32), SEM((N_PEERS,)), SEM((N_PEERS,)), SEM((n,)), SEM((n,)), SEM((3,)), SEM((4,)), SEM((SLOTS,)),
            SEM((SLOTS,)), SEM((len(made),)), SEM((4,)), SEM((4,))],
        compiler_params=remote_params(1),
        name="gather_qkv")(x, ln_weight.astype(F32)[None], pos.astype(F32).reshape(rows // LANE, LANE), freq, w_q, w_k, w_v, g)


def stack_heads(x):
    return jnp.concatenate([x[:, n * HEAD_DIM:(n + 1) * HEAD_DIM] for n in range(x.shape[1] // HEAD_DIM)], axis=0)


def causal(shape, bq, offset):
    rows = lax.rem(lax.broadcasted_iota(jnp.int32, shape, 0), bq) + offset
    return rows >= lax.broadcasted_iota(jnp.int32, shape, 1)


def fwd_step(qi, bq, bk, q_ref, kt_ref, v_ref, ot_ref, lse_ref, s_scr):
    q = stack_heads(q_ref[...])
    rows = q.shape[0]
    nfull = (qi * bq) // bk

    def scores(j):
        return dot(q, kt_ref[:, pl.ds(pl.multiple_of(j * bk, bk), bk)]) * (SCALE * LOG2E)

    def lane_max(m, s):
        for c in range(bk // LANE):
            m = jnp.maximum(m, s[:, c * LANE:(c + 1) * LANE])
        return m

    def score_step(j, m):
        s = scores(j)
        s_scr[j] = s
        return lane_max(m, s)

    m = lax.fori_loop(0, nfull, score_step, jnp.full((rows, LANE), -jnp.inf, F32))
    s = jnp.where(causal((rows, bk), bq, qi * bq - nfull * bk), scores(nfull), -jnp.inf)
    s_scr[nfull] = s
    m = jnp.max(lane_max(m, s), axis=1, keepdims=True)

    def value_step(j, carry):
        l, o = carry
        p = jnp.exp2(s_scr[j] - m)
        for t in range(bk // LANE):
            l = l + p[:, t * LANE:(t + 1) * LANE]
        o = o + dot(p.astype(BF16), v_ref[pl.ds(pl.multiple_of(j * bk, bk), bk), :])
        return l, o

    l, o = lax.fori_loop(0, nfull + 1, value_step, (jnp.zeros((rows, LANE), F32), jnp.zeros((rows, HEAD_DIM), F32)))
    l = jnp.sum(l, axis=1, keepdims=True)
    o = (o / l).astype(BF16)
    for n in range(rows // bq):
        ot_ref[n * HEAD_DIM:(n + 1) * HEAD_DIM, :] = o[n * bq:(n + 1) * bq].T
    lse_ref[...] = (m + jnp.log2(l)).reshape(lse_ref.shape)


def gather_fwd_kernel(n_fwd, relay, bq, bk, q_ref, kt_ref, v_ref, g_ref, wo_ref, _, ot_ref, lse_ref, gall_ref, do_ref, otg_ref,
                      s_scr, wo_scr, buf, ot_buf, send, recv, w_sem, load_sem, store_sem, ot_sem, early_send, early_recv):
    step = pl.program_id(0)
    me = lax.axis_index("sp")
    rows, width = g_ref.shape[0], do_ref.shape[1]
    half = rows // 2
    chunk = half // CHUNKS

    def block(owner, part, c):
        start = owner * rows + part * half
        return gall_ref.at[pl.ds(pl.multiple_of(start, half), half) if c is None else pl.ds(pl.multiple_of(start + c * chunk, chunk), chunk)]

    own = lambda part: g_ref.at[pl.ds(part * half, half)]
    links = Exchange(send, recv, block, own, CHUNKS, True, lambda part: early_rows(g_ref, gall_ref, part, EARLY[-1], half))
    w_copy = pltpu.make_async_copy(wo_ref.at[pl.ds(pl.multiple_of(me * width, width), width)], wo_scr, w_sem.at[0])
    loads = [pltpu.make_async_copy(own(i), buf.at[i], load_sem.at[i]) for i in range(SLOTS)]
    stores = [pltpu.make_async_copy(buf.at[i], block(me, i, None), store_sem.at[i]) for i in range(SLOTS)]

    @pl.when(step == 0)
    def _():
        greet(neighbours())
        links.begin()
        w_copy.start()
        start_all(loads)

    @pl.when(step == relay)
    def _():
        links.near(0)

    def ot_copy(i):
        slot = lax.rem(i, SLOTS)
        return pltpu.make_async_copy(ot_buf.at[slot], ot_ref.at[:, pl.ds(pl.multiple_of(i * bq, bq), bq)], ot_sem.at[slot])

    @pl.when(step >= SLOTS)
    def _():
        ot_copy(step - SLOTS).wait()

    @pl.when(step < n_fwd)
    def _():
        fwd_step(step, bq, bk, q_ref, kt_ref, v_ref, ot_buf.at[lax.rem(step, SLOTS)], lse_ref, s_scr)
        ot_copy(step).start()

    def load(slot, r0, n):
        return pltpu.make_async_copy(gall_ref.at[pl.ds(pl.multiple_of(r0, n), n)], buf.at[slot, pl.ds(0, n)], load_sem.at[slot])

    def compute(slot, r0, n, _):
        do_ref[pl.ds(pl.multiple_of(r0, n), n), :] = dot_t(buf[slot, :n], wo_scr[...]).astype(BF16)

    def own_ready():
        wait_all(loads)
        start_all(stores)
        w_copy.wait()

    @pl.when(step == n_fwd)
    def _():
        ot_copy(n_fwd - 1).wait()
        early = []
        for part, to in ((LOW, flip(me, X_BIT)), (HIGH, flip(me, Y_BIT))):
            src, dst = early_tokens(ot_ref, otg_ref, part, slice(0, EARLY_TOKENS))
            early.append(pltpu.make_async_remote_copy(src_ref=src, dst_ref=dst, send_sem=early_send.at[part], recv_sem=early_recv.at[part],
                                                      device_id={"sp": to}, device_id_type=MESH))
        far = in_order(links, own_ready, lambda: wait_all(stores), load, compute, half, chunk, started=True)
        start_all(early)
        far()
        wait_all(early)
        links.finish()


def gather_forward(q, kt, v, g, w_o, g_all, bq=PAIR, bk=1024):
    seq, width = q.shape
    rows, feat = g.shape
    heads = width // HEAD_DIM
    n = seq // bq
    at = lambda i: jnp.minimum(i, n - 1)
    return pl.pallas_call(
        functools.partial(gather_fwd_kernel, n, (3 * n) // 4, bq, bk), grid=(n + 1,),
        in_specs=[pl.BlockSpec((bq, width), lambda i: (at(i), 0)), pl.BlockSpec((HEAD_DIM, seq), whole, **ONCE),
                  pl.BlockSpec((seq, HEAD_DIM), whole, **ONCE)] + [HBM] * 3,
        out_specs=[HBM, pl.BlockSpec((heads, bq, 1), lambda i: (0, at(i), 0)), HBM, pl.BlockSpec((seq, width), whole, **ONCE), HBM],
        out_shape=[array(width, seq), array(heads, seq, 1, dtype=F32), array(seq, feat), array(seq, width), array(seq // rows // 2, width, seq)],
        scratch_shapes=[pltpu.VMEM((seq // bk, heads * bq, bk), F32), pltpu.VMEM((width, feat), BF16), pltpu.VMEM((4, rows // 2, feat), BF16), pltpu.VMEM((SLOTS, width, bq), BF16),
                        SEM((n_copies(CHUNKS, True),)), SEM((n_copies(CHUNKS, True),)), SEM((1,)), SEM((4,)), SEM((SLOTS,)), SEM((SLOTS,)), SEM((SLOTS,)), SEM((SLOTS,))],
        compiler_params=remote_params(2),
        input_output_aliases={5: 2}, name="gather_fwd")(q, kt, v, g, w_o, g_all)


def bwd_step(qi, bq, bk, q_ref, do_ref, lse_ref, k_ref, kt_ref, vt_ref, cos_ref, sin_ref, g_out, dkt_ref, dvt_ref, p_scr, dp_scr):
    q = stack_heads(q_ref[...])
    do = stack_heads(do_ref[...])
    rows = q.shape[0]
    lse = lse_ref[...].reshape(rows, 1)
    q_t = q.T
    do_t = do.T
    heads = rows // bq
    wide, few = 2, heads // 2
    n_big = (qi * bq) // (wide * bk)
    tail = wide * n_big
    rest = (qi * bq - tail * bk) // bk

    @pl.when(qi == 0)
    def _():
        dkt_ref[...] = jnp.zeros_like(dkt_ref)
        dvt_ref[...] = jnp.zeros_like(dvt_ref)

    def chunks(n):
        return [slice(m * (rows // n), (m + 1) * (rows // n)) for m in range(n)]

    def prob_step(j, wide, n_chunks, r, masked=False):
        sl = pl.ds(pl.multiple_of(j * bk, bk), wide * bk)
        total, out = None, []
        for c in chunks(n_chunks):
            s = dot(q[c], kt_ref[:, sl]) * (SCALE * LOG2E)
            p = jnp.exp2(s - lse[c])
            if masked:
                p = jnp.where(causal(p.shape, bq, qi * bq - j * bk), p, 0.0)
            dp = dot(do[c], vt_ref[:, sl])
            pd = p * dp
            part = r[c]
            for t in range(wide * bk // LANE):
                part = part + pd[:, t * LANE:(t + 1) * LANE]
            out.append(part)
            for e in range(wide):
                p_scr[j + e, c, :] = p[:, e * bk:(e + 1) * bk]
                dp_scr[j + e, c, :] = dp[:, e * bk:(e + 1) * bk]
            d = dot(do_t[:, c], p.astype(BF16))
            total = d if total is None else total + d
        dvt_ref[:, sl] += total
        return jnp.concatenate(out, axis=0)

    r = jnp.zeros((rows, LANE), F32)
    r = lax.fori_loop(0, n_big, lambda j, r: prob_step(wide * j, wide, heads, r), r)
    r = lax.fori_loop(0, rest, lambda j, r: prob_step(tail, 1, few, r), r)
    r = prob_step(tail + rest, 1, few, r, True)
    r = jnp.sum(r, axis=1, keepdims=True)

    def grad_step(j, wide, n_chunks, dq):
        sl = pl.ds(pl.multiple_of(j * bk, bk), wide * bk)
        total, out = None, []
        for c in chunks(n_chunks):
            ds = jnp.concatenate([(p_scr[j + e, c, :] * (dp_scr[j + e, c, :] - r[c]) * SCALE).astype(BF16) for e in range(wide)], axis=1)
            d = dot(q_t[:, c], ds)
            total = d if total is None else total + d
            out.append(dq[c] + dot(ds, k_ref[sl, :]))
        dkt_ref[:, sl] += total
        return jnp.concatenate(out, axis=0)

    dq = jnp.zeros((rows, HEAD_DIM), F32)
    dq = lax.fori_loop(0, n_big, lambda j, dq: grad_step(wide * j, wide, heads, dq), dq)
    dq = lax.fori_loop(0, rest + 1, lambda j, dq: grad_step(tail + j, 1, few, dq), dq)
    dq = dq.astype(BF16).astype(F32)
    here = pl.ds(pl.multiple_of(qi * bq, bq), bq)
    cos_t, sin_t = cos_ref[here, :], sin_ref[here, :]
    for n in range(rows // bq):
        g_out[:, n * HEAD_DIM:(n + 1) * HEAD_DIM] = rotate(dq[n * bq:(n + 1) * bq], cos_t, -sin_t).astype(BF16)


def gather_bwd_kernel(relay, bq, bk, q_ref, do_ref, lse_ref, k_ref, kt_ref, vt_ref, cos_ref, sin_ref, ot_ref, _,
                      gq_ref, gk_ref, gv_ref, otg_ref, otz_ref, p_scr, dp_scr, dkt_scr, dvt_scr, buf, send, recv, z_send, z_recv, load_sem, store_sem):
    step = pl.program_id(0)
    last = pl.num_programs(0) - 1
    me = lax.axis_index("sp")
    width, seq = ot_ref.shape
    half = width // 2
    tokens = otz_ref.shape[2]
    zn = flip(me, CORE)
    own = lambda part: ot_ref.at[pl.ds(part * half, half)]
    block = lambda owner, part, _: otg_ref.at[owner // 2, pl.ds(part * half, half)]
    links = Exchange(send, recv, block, own, 1, False, lambda part: early_tokens(ot_ref, otg_ref, part, slice(EARLY_TOKENS, seq)))
    xn, yn = flip(me, X_BIT), flip(me, Y_BIT)
    dn = flip(xn, Y_BIT)
    mine = pl.ds(pl.multiple_of(zn * tokens, tokens), tokens)

    def to_other(n, owner):
        src = ot_ref.at[:, mine] if n == 0 else otg_ref.at[owner // 2, :, mine]
        return pltpu.make_async_remote_copy(src_ref=src, dst_ref=otz_ref.at[owner // 2], send_sem=z_send.at[n], recv_sem=z_recv.at[n],
                                            device_id={"sp": zn}, device_id_type=MESH)

    z = [to_other(n, o) for n, o in enumerate((me, xn, yn, dn))]
    n_buf, slab = buf.shape[0], buf.shape[1]
    n_slab = width // slab

    def slab_copies(n):
        rows = pl.ds(pl.multiple_of(n * slab, slab), slab)
        slot = n % n_buf
        return (pltpu.make_async_copy(ot_ref.at[rows], buf.at[slot], load_sem.at[slot]),
                pltpu.make_async_copy(buf.at[slot], otg_ref.at[me // 2, rows], store_sem.at[slot]))

    @pl.when(step == 0)
    def _():
        greet(neighbours())
        links.begin()
        z[0].start()

    @pl.when(step == relay)
    def _():
        links.near(0)

    @pl.when((step >= 2) & (step < n_slab + 2))
    def _():
        slab_copies(step - 2)[1].wait()

    @pl.when((step >= 1) & (step < n_slab + 1))
    def _():
        slab_copies(step - 1)[0].wait()
        slab_copies(step - 1)[1].start()

    @pl.when(step < n_slab)
    def _():
        slab_copies(step)[0].start()

    bwd_step(step, bq, bk, q_ref, do_ref, lse_ref, k_ref, kt_ref, vt_ref, cos_ref, sin_ref, gq_ref, dkt_scr, dvt_scr, p_scr, dp_scr)

    @pl.when(step == last)
    def _():
        links.near(1)
        start_all(z[1:3])

        def kv_rows(i, _):
            rows = pl.ds(pl.multiple_of(i * bk, bk), bk)
            dk = dkt_scr[:, rows].T.astype(BF16).astype(F32)
            gk_ref[rows, :] = rotate(dk, cos_ref[rows, :], -sin_ref[rows, :]).astype(BF16)
            gv_ref[rows, :] = dvt_scr[:, rows].T.astype(BF16)
            return 0

        lax.fori_loop(0, seq // bk, kv_rows, 0)
        links.far(0)
        z[3].start()
        receive(z)
        links.finish()
        for c in z:
            c.wait_send()


def gather_backward(q, do, lse, k, kt, vt, cos_t, sin_t, ot, ot_all, sp_size, bq=PAIR, bk=512):
    seq, width = q.shape
    heads = width // HEAD_DIM
    chips, tokens = sp_size // 2, seq // sp_size
    n = seq // bq
    tile = pl.BlockSpec((bq, width), row)
    tall = pl.BlockSpec((seq, HEAD_DIM), whole, **ONCE)
    wide = pl.BlockSpec((HEAD_DIM, seq), whole, **ONCE)
    return pl.pallas_call(
        functools.partial(gather_bwd_kernel, (9 * n) // 16, bq, bk), grid=(n,),
        in_specs=[tile, tile, pl.BlockSpec((heads, bq, 1), lambda i: (0, i, 0)), tall, wide, wide, tall, tall, HBM, HBM],
        out_specs=[tile, tall, tall, HBM, HBM],
        out_shape=[array(seq, width), array(seq, HEAD_DIM), array(seq, HEAD_DIM), array(chips, width, seq), array(chips, width, tokens)],
        scratch_shapes=[pltpu.VMEM((seq // bk, heads * bq, bk), F32), pltpu.VMEM((seq // bk, heads * bq, bk), F32),
                        pltpu.VMEM((HEAD_DIM, seq), F32), pltpu.VMEM((HEAD_DIM, seq), F32), pltpu.VMEM((SLOTS, width // 8, seq), BF16),
                        SEM((n_copies(1, False),)), SEM((n_copies(1, False),)), SEM((4,)), SEM((4,)), SEM((SLOTS,)), SEM((SLOTS,))],
        compiler_params=remote_params(3), input_output_aliases={9: 3},
        name="gather_bwd")(q, do, lse, k, kt, vt, cos_t, sin_t, ot, ot_all)


def dw_o_kernel(core_ref, ot_ref, g_ref, final_ref, send_ref):
    y = dot(ot_ref[...], g_ref[...]).astype(BF16)
    final_ref[...] = y
    send_ref[...] = y


def dw_o_half(core, ot_all, g_all, bn=1024):
    half, width, seq = ot_all.shape
    feat = g_all.shape[1]
    return pl.pallas_call(
        dw_o_kernel,
        grid_spec=pltpu.PrefetchScalarGridSpec(
            num_scalar_prefetch=1, grid=(feat // bn, half),
            in_specs=[pl.BlockSpec((None, width, seq), lambda j, s, c: (s, 0, 0)), pl.BlockSpec((seq, bn), col)],
            out_specs=[pl.BlockSpec((width, bn), lambda j, s, c: (2 * s + c[0], j)), pl.BlockSpec((width, bn), lambda j, s, c: (s, j))]),
        out_shape=[array(2 * half * width, feat), array(half * width, feat)],
        compiler_params=PARAMS, cost_estimate=cost(2 * half * width * feat * seq), name="dw_o_half")(core, ot_all, g_all)


class Ride:
    def __init__(self, source, buf, targets, load_sem, store_sem):
        self.source, self.buf, self.targets, self.load_sem, self.store_sem = source, buf, targets, load_sem, store_sem

    def load(self, i):
        slot = lax.rem(i, SLOTS)
        return pltpu.make_async_copy(self.source(i), self.buf.at[slot], self.load_sem.at[slot])

    def stores(self, i):
        slot = lax.rem(i, SLOTS)
        return [pltpu.make_async_copy(src, dst, self.store_sem.at[slot, n]) for n, (src, dst) in enumerate(self.targets(i, self.buf.at[slot]))]

    def begin(self, i):
        @pl.when(i >= SLOTS)
        def _():
            wait_all(self.stores(i - SLOTS))

        self.load(i).start()

    def end(self, i, last):
        self.load(i).wait()
        start_all(self.stores(i))

        @pl.when(i == last)
        def _():
            for n in reversed(range(SLOTS)):
                wait_all(self.stores(i - n))


def half_ride(recv, half, dev, final, scratch):
    buf = scratch[0]
    n, w = buf.shape[1:]
    at = lambda i, base: pl.ds(pl.multiple_of(base + i * n, n), n)
    return Ride(lambda i: recv.at[at(i, 0)], buf, lambda i, src: [(src, final.at[at(i, half * recv.shape[0]), pl.ds(pl.multiple_of(dev * w, w), w)])], *scratch[1:])


def half_scratch(recv, steps):
    return [pltpu.VMEM((SLOTS, recv.shape[0] // steps, recv.shape[1]), BF16), SEM((SLOTS,)), SEM((SLOTS, 1))]


def out_kernel(ids_ref, mine_ref, other_ref, w_ref, low, high, _, out_ref, q_ref, o_scr, *scratch):
    i, last = grid_place()
    rides = [half_ride(r, m, ids_ref[1 + m], q_ref, scratch[3 * m:3 * m + 3]) for m, r in enumerate((low, high))]
    for r in rides:
        r.begin(i)

    @pl.when(i == 0)
    def _():
        core = lax.rem(ids_ref[0], 2)
        width = mine_ref.shape[1]
        for s in range(mine_ref.shape[0]):
            for ref, d in ((mine_ref, 2 * s + core), (other_ref, 2 * s + 1 - core)):
                o_scr[:, pl.ds(pl.multiple_of(d * width, width), width)] = ref[s].T

    out_ref[...] = dot(o_scr[...], w_ref[...]).astype(BF16)
    for r in rides:
        r.end(i, last)


def out_proj(ids, ot_all, ot_other, w_o, low, high, dw_q, bn=512):
    chips, width, tokens = ot_other.shape
    feat = w_o.shape[1]
    steps = feat // bn
    return pl.pallas_call(
        out_kernel,
        grid_spec=pltpu.PrefetchScalarGridSpec(
            num_scalar_prefetch=1, grid=(steps,),
            in_specs=[pl.BlockSpec((chips, width, tokens), lambda i, c: (0, 0, c[0]), **ONCE), pl.BlockSpec((chips, width, tokens), lambda i, c: (0, 0, 0), **ONCE),
                      pl.BlockSpec((w_o.shape[0], bn), col)] + [HBM] * 3,
            out_specs=[pl.BlockSpec((tokens, bn), col), HBM],
            scratch_shapes=[pltpu.VMEM((tokens, w_o.shape[0]), BF16)] + half_scratch(low, steps) + half_scratch(high, steps)),
        out_shape=[array(tokens, feat), array(*dw_q.shape)], input_output_aliases={6: 1},
        compiler_params=PARAMS, cost_estimate=cost(2 * tokens * w_o.size), name="out_proj")(ids, ot_all, ot_other, w_o, low, high, dw_q)


def dw_q_kernel(ids_ref, ht_ref, g_ref, final_ref, all_ref, low_ref, high_ref):
    i = pl.program_id(0)
    y = dot(ht_ref[...], g_ref[...]).astype(BF16)
    final_ref[...] = y
    all_ref[...] = y
    n = pl.num_programs(0) // 2

    @pl.when(i < n)
    def _():
        low_ref[...] = y

    @pl.when(i >= n)
    def _():
        high_ref[...] = y


def dw_q_own(ids, ht, gq, bm=512):
    feat, seq = ht.shape
    w = gq.shape[1]
    n = feat // bm
    return pl.pallas_call(
        dw_q_kernel,
        grid_spec=pltpu.PrefetchScalarGridSpec(
            num_scalar_prefetch=1, grid=(n,), in_specs=[pl.BlockSpec((bm, seq), row), pl.BlockSpec((seq, w), whole, **ONCE)],
            out_specs=[pl.BlockSpec((bm, w), lambda i, c: (i, c[0])), pl.BlockSpec((bm, w), row), pl.BlockSpec((bm, w), lambda i, c: (jnp.minimum(i, n // 2 - 1), 0)),
                       pl.BlockSpec((bm, w), lambda i, c: (jnp.maximum(i - n // 2, 0), 0))]),
        out_shape=[array(feat, feat), array(feat, w), array(feat // 2, w), array(feat // 2, w)],
        compiler_params=PARAMS, cost_estimate=cost(2 * seq * feat * w), name="dw_q_own")(ids, ht, gq)


def kv_columns(rows, src, k_ref, v_ref, owners):
    out = []
    for m, ref in enumerate((k_ref, v_ref)):
        for n, dev in enumerate(owners):
            at = (m * len(owners) + n) * HEAD_DIM
            out.append((src.at[:, at:at + HEAD_DIM], ref.at[rows, pl.ds(pl.multiple_of(dev * HEAD_DIM, HEAD_DIM), HEAD_DIM)]))
    return out


def dw_kv_kernel(n_dev, ids_ref, ht_ref, *refs):
    parts, refs = refs[:2 * n_dev], refs[2 * n_dev:]
    recv, _, q_ref, k_ref, v_ref, send_ref, x_scr, y_scr, y_sem, send_sem, x_sem, load_sem, *scratch = refs
    i, last = grid_place()
    ride = half_ride(recv, LOW, flip(ids_ref[0], CORE), q_ref, scratch)
    ride.begin(i)
    bm, feat = ht_ref.shape[0], k_ref.shape[0]
    n_tok = send_ref.shape[0] - feat
    tokens = pltpu.make_async_copy(x_scr.at[pl.ds(pl.multiple_of(flip(ids_ref[0], CORE) * n_tok, n_tok), n_tok)], send_ref.at[pl.ds(feat, n_tok)], x_sem.at[0])
    owners = [ids_ref[1 + n] for n in range(n_dev)]

    @pl.when(i == 0)
    def _():
        loads = [pltpu.make_async_copy(p, x_scr.at[:, m * HEAD_DIM:(m + 1) * HEAD_DIM], load_sem.at[m]) for m, p in enumerate(parts)]
        start_all(loads)
        wait_all(loads)
        tokens.start()

    def stores(step):
        slot, rows = lax.rem(step, SLOTS), pl.ds(pl.multiple_of(step * bm, bm), bm)
        out = [pltpu.make_async_copy(src, dst, y_sem.at[slot, m]) for m, (src, dst) in enumerate(kv_columns(rows, y_scr.at[slot], k_ref, v_ref, owners))]
        return out + [pltpu.make_async_copy(y_scr.at[slot], send_ref.at[rows], send_sem.at[slot])]

    @pl.when(i >= SLOTS)
    def _():
        wait_all(stores(i - SLOTS))

    y_scr[lax.rem(i, SLOTS)] = dot(ht_ref[...], x_scr[...]).astype(BF16)
    start_all(stores(i))
    ride.end(i, last)

    @pl.when(i == last)
    def _():
        tokens.wait()
        for m in reversed(range(SLOTS)):
            wait_all(stores(i - m))


def dw_kv_half(ids, ht, parts, recv, dw_q, shape, tokens, bm=512):
    feat, seq = ht.shape
    w = len(parts) * HEAD_DIM
    steps = feat // bm
    return pl.pallas_call(
        functools.partial(dw_kv_kernel, len(parts) // 2),
        grid_spec=pltpu.PrefetchScalarGridSpec(
            num_scalar_prefetch=1, grid=(steps,), in_specs=[pl.BlockSpec((bm, seq), row)] + [HBM] * (len(parts) + 2), out_specs=[HBM] * 4,
            scratch_shapes=[pltpu.VMEM((seq, w), BF16), pltpu.VMEM((SLOTS, bm, w), BF16), SEM((SLOTS, len(parts))), SEM((SLOTS,)), SEM((1,)), SEM((len(parts),))]
            + half_scratch(recv, steps)),
        out_shape=[array(*dw_q.shape), array(*shape), array(*shape), array(feat + tokens, w)], input_output_aliases={3 + len(parts): 0},
        compiler_params=PARAMS, cost_estimate=cost(2 * seq * feat * w), name="dw_kv_half")(ids, ht, *parts, recv, dw_q)


def dh_kernel(n_dev, ids_ref, wq_ref, wk_ref, wv_ref, x_ref, stat_ref, lnw_ref, tq_ref, t_ref, *refs):
    own, refs = refs[:2 * n_dev], refs[2 * n_dev:]
    kv_recv, o_recv, _, _, _, dx_ref, dlnw_ref, k_ref, v_ref, o_ref, g_scr, sum_scr, dy_scr, *scratch = refs
    i, last = grid_place()
    tokens, feat = x_ref.shape
    bf = wq_ref.shape[0]
    others = [ids_ref[1 + n_dev + n] for n in range(n_dev)]
    kv_buf, o_buf = scratch[0], scratch[3]
    core = lax.rem(ids_ref[0], 2)
    block_rows = lambda i, buf: pl.ds(pl.multiple_of(i * buf.shape[1], buf.shape[1]), buf.shape[1])

    def o_rows(i):
        n = o_buf.shape[1]
        per = HEAD_DIM * n_dev // n
        return pl.ds(pl.multiple_of(((2 * (i // per) + 1 - core) * per + lax.rem(i, per)) * n, n), n)

    rides = [Ride(lambda i: kv_recv.at[block_rows(i, kv_buf)], kv_buf, lambda i, src: kv_columns(block_rows(i, kv_buf), src, k_ref, v_ref, others), *scratch[1:3]),
             Ride(lambda i: o_recv.at[block_rows(i, o_buf)], o_buf, lambda i, src: [(src, o_ref.at[o_rows(i)])], *scratch[4:])]
    for r in rides:
        r.begin(i)
    nq, nk = wq_ref.shape[1], wk_ref.shape[1]
    slab = tokens // 8

    @pl.when(i == 0)
    def _():
        width = tq_ref.shape[1]
        for m in range(2 * n_dev):
            g_scr[:, m * width:(m + 1) * width] = tq_ref[m * tokens:(m + 1) * tokens, :]
            for x, dev in ((own[m][...], ids_ref[1 + m % n_dev]), (t_ref[:, m * HEAD_DIM:(m + 1) * HEAD_DIM], others[m % n_dev])):
                g_scr[:, pl.ds(pl.multiple_of(nq + (m // n_dev) * nk + dev * HEAD_DIM, HEAD_DIM), HEAD_DIM)] = x

        sum_scr[...] = jnp.zeros_like(sum_scr)

    y = dot_t(g_scr[:, :nq], wq_ref[...]) + dot_t(g_scr[:, nq:nq + nk], wk_ref[...]) + dot_t(g_scr[:, nq + nk:], wv_ref[...])
    for m in range(bf // LANE):
        part, at = slice(m * LANE, (m + 1) * LANE), pl.ds(pl.multiple_of(i * bf + m * LANE, LANE), LANE)
        hat = (x_ref[:, at].astype(F32) - stat_ref[0]) * stat_ref[1]
        dlnw_ref[:, part] = jnp.sum(y[:, part] * hat, axis=0, keepdims=True)
        dy = y[:, part] * lnw_ref[:, part]
        dy_scr[:, at] = dy
        sum_scr[0] += dy
        sum_scr[1] += dy * hat
    for r in rides:
        r.end(i, last)

    @pl.when(i == last)
    def _():
        def finish(m, _):
            here = pl.ds(pl.multiple_of(m * slab, slab), slab)
            mean_y, mean_yh = (jnp.sum(sum_scr[e, here, :], axis=1, keepdims=True) / feat for e in range(SLOTS))
            mean, rstd = (stat_ref[e, here, :1] for e in range(SLOTS))
            hat = (x_ref[here, :].astype(F32) - mean) * rstd
            dx_ref[here, :] = (rstd * (dy_scr[here, :] - mean_y - hat * mean_yh)).astype(BF16)
            return 0

        lax.fori_loop(0, tokens // slab, finish, 0)


def dh_proj(ids, w_q, w_k, w_v, x, stats, ln_weight, t_q, own, kv_recv, o_recv, finals, bf=512):
    tokens, feat = x.shape
    w = kv_recv.shape[1]
    n = len(own)
    ins = [w_q, w_k, w_v, x, stats, ln_weight.astype(F32)[None], t_q, kv_recv, *own, kv_recv, o_recv, *finals]
    specs = [pl.BlockSpec((bf, m.shape[1]), row) for m in (w_q, w_k, w_v)] + [pl.BlockSpec(x.shape, whole, **ONCE), pl.BlockSpec(stats.shape, lambda i, c: (0, 0, 0), **ONCE), pl.BlockSpec((1, bf), col)]
    specs += [pl.BlockSpec(t_q.shape, whole, **ONCE), pl.BlockSpec((tokens, w), lambda i, c: (feat // tokens, 0), **ONCE)]
    specs += [pl.BlockSpec((tokens, HEAD_DIM), lambda i, c: (c[0], 0), **ONCE) for _ in own]
    first = len(ins) - len(finals)
    steps = feat // bf
    return pl.pallas_call(
        functools.partial(dh_kernel, n // 2),
        grid_spec=pltpu.PrefetchScalarGridSpec(
            num_scalar_prefetch=1, grid=(steps,), in_specs=specs + [HBM] * (len(ins) - len(specs)),
            out_specs=[pl.BlockSpec(x.shape, whole, **ONCE), pl.BlockSpec((1, bf), col)] + [HBM] * len(finals),
            scratch_shapes=[pltpu.VMEM((tokens, w_q.shape[1] + 2 * w_k.shape[1]), BF16), pltpu.VMEM((SLOTS, tokens, LANE), F32), pltpu.VMEM(x.shape, F32),
                            pltpu.VMEM((SLOTS, feat // steps, w), BF16), SEM((SLOTS,)), SEM((SLOTS, n)),
                            pltpu.VMEM((SLOTS, o_recv.shape[0] // steps, feat), BF16), SEM((SLOTS,)), SEM((SLOTS, 1))]),
        out_shape=[array(tokens, feat), array(1, feat, dtype=F32)] + [array(*f.shape) for f in finals],
        input_output_aliases={1 + first + m: 2 + m for m in range(len(finals))},
        compiler_params=PARAMS, cost_estimate=cost(2 * tokens * (w_q.size + 2 * w_k.size)), name="dh_proj")(ids, *ins)


def copy_kernel(n, places, ids_ref, *refs):
    final, buf, load_sem, store_sem = refs[n + 1:]
    rows, w = buf.shape[1:]
    loads = [pltpu.make_async_copy(refs[m], buf.at[m], load_sem.at[m]) for m in range(n)]
    start_all(loads)
    stores = []
    for m, (owner, half) in enumerate(places):
        loads[m].wait()
        at = pl.ds(pl.multiple_of(ids_ref[owner] * w, w), w)
        stores.append(pltpu.make_async_copy(buf.at[m], final.at[pl.ds(half * rows, rows), at], store_sem.at[m]))
        stores[-1].start()
    wait_all(stores)


def copy_in(ids, blocks, places, final):
    n = len(blocks)
    return pl.pallas_call(
        functools.partial(copy_kernel, n, places),
        grid_spec=pltpu.PrefetchScalarGridSpec(num_scalar_prefetch=1, grid=(1,), in_specs=[HBM] * (n + 1), out_specs=HBM,
                                               scratch_shapes=[pltpu.VMEM((n,) + blocks[0].shape, BF16), SEM((n,)), SEM((n,))]),
        out_shape=array(*final.shape), input_output_aliases={n + 1: 0},
        compiler_params=pltpu.CompilerParams(vmem_limit_bytes=COPY_LIMIT), name="copy_in")(ids, *blocks, final)


def sum_kernel(x_ref, out_ref, all_scr, send, recv):
    me = lax.axis_index("sp")
    peers = everyone()
    greet(peers)
    copies = [pltpu.make_async_remote_copy(src_ref=x_ref, dst_ref=all_scr.at[me], send_sem=send.at[n], recv_sem=recv.at[n],
                                           device_id={"sp": p}, device_id_type=MESH) for n, p in enumerate(peers)]
    for c in copies:
        c.start()
    all_scr[me] = x_ref[...]
    for c in copies:
        c.wait_recv()
    total = all_scr[0]
    for n in range(1, all_scr.shape[0]):
        total = total + all_scr[n]
    out_ref[...] = total.astype(BF16)
    for c in copies:
        c.wait_send()


def sum_devices(x, sp_size):
    n = x.shape[0] // HEAD_DIM
    vmem = pl.BlockSpec(memory_space=pltpu.VMEM)
    return pl.pallas_call(
        sum_kernel, in_specs=[vmem], out_specs=vmem, out_shape=array(n, HEAD_DIM),
        scratch_shapes=[pltpu.VMEM((sp_size, n, HEAD_DIM), F32), SEM((sp_size - 1,)), SEM((sp_size - 1,))],
        compiler_params=remote_params(4), name="sum_devices")(x.reshape(n, HEAD_DIM)).reshape(-1)


def solution(mesh):
    sp_size = mesh.shape['sp']
    row_spec = P(('dp', 'sp'), None)
    pos_spec = P(('dp', 'sp'))
    full_spec = P(None, None)
    grad_spec = P('dp', None)

    def local_step(hidden, positions, d_attn, ln_weight, w_q, w_k, w_v, w_o):
        dev = lax.axis_index('sp')
        core = lax.rem(dev, SLOTS)
        local_rows, _ = hidden.shape
        _, ht, g_all, q, k, kt, v, vt, cos_t, sin_t, stats = gather_qkv(hidden, ln_weight, positions, w_q, w_k, w_v, d_attn, sp_size)
        ot, lse, g_all, do, ot_all = gather_forward(q, kt, v, d_attn, w_o, g_all)
        gq, gk, gv, ot_all, ot_other = gather_backward(q, do, lse, k, kt, vt, cos_t, sin_t, ot, ot_all, sp_size)
        other = lambda d: flip(d, CORE)
        dev_x, dev_y = flip(dev, X_BIT), flip(dev, Y_BIT)
        dev_d = flip(dev_x, Y_BIT)
        owners = [dev, dev_x, dev_y, dev_d]

        def to(x, bit):
            return lax.ppermute(x, 'sp', [(i, i ^ bit) for i in range(sp_size)])

        after = lambda x, *done: lax.optimization_barrier((x,) + done)[0]
        ids = lambda *d: jnp.stack(d)
        gk_x, gv_y, gv_x, gk_y = to(gk, X_BIT), to(gv, Y_BIT), to(gv, X_BIT), to(gk, Y_BIT)
        t_q = lax.all_to_all(gq, 'sp', 0, 0, tiled=True)
        dw_q, columns, low, high = dw_q_own(dev.reshape(1), ht, gq)
        gk_d, gv_d = to(after(gk_x, low), Y_BIT), to(after(gv_y, low), X_BIT)
        low_x, high_y, high_x, low_y = to(low, X_BIT), to(high, Y_BIT), to(high, X_BIT), to(low, Y_BIT)
        columns_z = to(columns, CORE)
        dw_o, o_send = dw_o_half(after(core.reshape(1), low), ot_all, g_all)
        o_recv = to(o_send, CORE)
        parts = [gk, gk_x, gk_y, gk_d, gv, gv_x, gv_y, gv_d]
        dw_q, dw_k, dw_v, kv_send = dw_kv_half(ids(*owners[:1], *owners), ht, [after(parts[0], o_send)] + parts[1:], columns_z, dw_q, w_k.shape, local_rows)
        kv_recv = to(kv_send, CORE)
        attn_out, dw_q = out_proj(ids(dev, dev_x, dev_y), ot_all, ot_other, after(w_o, kv_send), low_x, high_y, dw_q)
        low_d, high_d = to(after(low_x, attn_out), Y_BIT), to(after(high_y, attn_out), X_BIT)
        low_zx, high_zy = to(after(low_x, attn_out), CORE), to(after(high_y, attn_out), CORE)
        dx, d_lnw, dw_k, dw_v, dw_o = dh_proj(ids(*owners[:1], *owners, *map(other, owners)), w_q, w_k, w_v, hidden, stats, ln_weight, t_q, parts, kv_recv, o_recv, [dw_k, dw_v, dw_o])
        high_zx, low_zy = to(after(high_x, dx), CORE), to(after(low_y, dx), CORE)
        d_lnw = sum_devices(d_lnw.reshape(-1), sp_size)
        low_zd, high_zd = to(after(low_d, d_lnw), CORE), to(after(high_d, d_lnw), CORE)
        dw_q = copy_in(ids(dev_x, dev_y, other(dev_x), other(dev_y)), [high_x, low_y, low_zx, high_zx, low_zy, high_zy],
                       [(0, HIGH), (1, LOW), (2, LOW), (2, HIGH), (3, LOW), (3, HIGH)], after(dw_q, d_lnw))
        dw_q = copy_in(ids(dev_d, other(dev_d)), [low_d, high_d, low_zd, high_zd], [(0, LOW), (0, HIGH), (1, LOW), (1, HIGH)], dw_q)
        return (attn_out, dx, d_lnw, dw_q, dw_k, dw_v, dw_o)

    return jax.shard_map(local_step, mesh=mesh,
                      in_specs=(row_spec, pos_spec, row_spec, P(None), full_spec, full_spec, full_spec, full_spec),
                      out_specs=(row_spec, row_spec, P('dp'), grad_spec, grad_spec, grad_spec, grad_spec),
                      check_vma=False)
```
